32 devices in a mesh: dp: 1 (over z), sp: 32 (over y, x, core).
Axes of the slice: x: 4, y: 4, z: 1, core: 2. Of those that a mesh axis runs over, the one named last changes fastest.
The devices are a block of a 4x4x8 slice.
Arguments:
- x_tok: bfloat16 [16384, 2048], P(('dp', 'sp'))
- doc_start: int32 [16384], P(('dp', 'sp'))
- w_q: bfloat16 [2048, 32, 64], replicated
- w_k: bfloat16 [2048, 32, 64], replicated
- w_v: bfloat16 [2048, 32, 64], replicated
- w_o: bfloat16 [32, 64, 2048], replicated
- dy_tok: bfloat16 [16384, 2048], P(('dp', 'sp'))
Outputs:
- output 1: bfloat16 [16384, 2048], P(('dp', 'sp'))
- output 2: bfloat16 [16384, 2048], P(('dp', 'sp'))
- output 3: float32 [2048, 32, 64], P('dp')
- output 4: float32 [2048, 32, 64], P('dp')
- output 5: float32 [2048, 32, 64], P('dp')
- output 6: float32 [32, 64, 2048], P('dp')
All inputs are finite; a program needn't handle non-finite values.
Results may differ from the reference program's by a relative error of at most 0.00242.
Values are sent between devices in bfloat16 or wider.
A program may use at most 768 MiB of HBM per device.

```python
import math
import jax
import jax.numpy as jnp
from jax import lax

D_MODEL = 2048
HEAD_DIM = 64
TOK_DEV = 512
SEQ_DEVS = 32

NUM_HEADS = D_MODEL // HEAD_DIM
SEQ_LEN = SEQ_DEVS * TOK_DEV
NUM_BOUNDS = SEQ_DEVS // 2 + 1
SCORE_SCALE = 1.0 / (math.sqrt(HEAD_DIM) * TOK_DEV)


def setup_inputs(seed: int = 0, part: int = 0) -> dict:
    key_list = jax.random.split(jax.random.key(seed), 9)
    k_tok = jax.random.fold_in(key_list[0], part)
    k_tok_mean = jax.random.fold_in(key_list[1], part)
    k_grad = jax.random.fold_in(key_list[2], part)
    k_grad_mean = jax.random.fold_in(key_list[3], part)
    k_doc = jax.random.fold_in(key_list[4], part)
    w_scale = D_MODEL ** -0.5
    x_tok = (jax.random.normal(k_tok, (SEQ_LEN, D_MODEL), jnp.float32)
             + jax.random.normal(k_tok_mean, (1, D_MODEL), jnp.float32)).astype(jnp.bfloat16)
    dy_tok = (jax.random.normal(k_grad, (SEQ_LEN, D_MODEL), jnp.float32)
              + jax.random.normal(k_grad_mean, (1, D_MODEL), jnp.float32)).astype(jnp.bfloat16)
    bound_pos = jax.random.randint(k_doc, (NUM_BOUNDS,), 0, SEQ_LEN)
    doc_start = jnp.zeros((SEQ_LEN,), jnp.int32).at[bound_pos].set(1)
    w_q = (jax.random.normal(key_list[5], (D_MODEL, NUM_HEADS, HEAD_DIM), jnp.float32) * w_scale).astype(jnp.bfloat16)
    w_k = (jax.random.normal(key_list[6], (D_MODEL, NUM_HEADS, HEAD_DIM), jnp.float32) * w_scale).astype(jnp.bfloat16)
    w_v = (jax.random.normal(key_list[7], (D_MODEL, NUM_HEADS, HEAD_DIM), jnp.float32) * w_scale).astype(jnp.bfloat16)
    w_o = (jax.random.normal(key_list[8], (NUM_HEADS, HEAD_DIM, D_MODEL), jnp.float32) * w_scale).astype(jnp.bfloat16)
    return {'x_tok': x_tok, 'doc_start': doc_start, 'w_q': w_q, 'w_k': w_k, 'w_v': w_v, 'w_o': w_o, 'dy_tok': dy_tok}


def block_masks(flag_loc):
    positions = jnp.arange(TOK_DEV)
    seg_ids = jnp.cumsum(flag_loc)
    first_pos = jnp.min(jnp.where(flag_loc > 0, positions, TOK_DEV))
    last_pos = jnp.max(jnp.where(flag_loc > 0, positions, -1))
    head_mask = (positions < first_pos).astype(jnp.float32)
    tail_mask = (positions >= last_pos).astype(jnp.float32)
    same_doc = (seg_ids[:, None] == seg_ids[None, :]) & (positions[None, :] <= positions[:, None])
    doc_gate = (last_pos < 0).astype(jnp.float32)
    return head_mask, tail_mask, same_doc, doc_gate


def reference(x_tok, doc_start, w_q, w_k, w_v, w_o, dy_tok):
    wq_mat = w_q.reshape(D_MODEL, D_MODEL)
    wk_mat = w_k.reshape(D_MODEL, D_MODEL)
    wv_mat = w_v.reshape(D_MODEL, D_MODEL)
    wo_mat = w_o.reshape(D_MODEL, D_MODEL)

    def project(x_loc):
        q_rows = jnp.dot(x_loc, wq_mat, preferred_element_type=jnp.float32).astype(jnp.bfloat16).astype(jnp.float32)
        k_rows = jnp.dot(x_loc, wk_mat, preferred_element_type=jnp.float32).astype(jnp.bfloat16).astype(jnp.float32)
        v_rows = jnp.dot(x_loc, wv_mat, preferred_element_type=jnp.float32).astype(jnp.bfloat16).astype(jnp.float32)
        shape3 = (TOK_DEV, NUM_HEADS, HEAD_DIM)
        return q_rows.reshape(shape3), k_rows.reshape(shape3), v_rows.reshape(shape3)

    def forward_step(fwd_state, step_in):
        x_loc, flag_loc = step_in
        head_mask, tail_mask, same_doc, doc_gate = block_masks(flag_loc)
        q_rows, k_rows, v_rows = project(x_loc)
        scores = jnp.einsum('thk,shk->hts', q_rows, k_rows)
        attn_prob = jnp.where(same_doc[None], scores * SCORE_SCALE, 0.0).astype(jnp.bfloat16).astype(jnp.float32)
        intra_sum = jnp.einsum('hts,shv->thv', attn_prob, v_rows)
        state_low = fwd_state.astype(jnp.bfloat16).astype(jnp.float32)
        inter_sum = jnp.einsum('thk,hkv->thv', q_rows, state_low) * (SCORE_SCALE * head_mask)[:, None, None]
        out_rows = (intra_sum + inter_sum).astype(jnp.bfloat16).reshape(TOK_DEV, D_MODEL)
        y_loc = jnp.dot(out_rows, wo_mat, preferred_element_type=jnp.float32).astype(jnp.bfloat16)
        m_tail = jnp.einsum('shk,shv->hkv', k_rows, v_rows * tail_mask[:, None, None])
        next_state = doc_gate * fwd_state + m_tail
        return next_state, (out_rows, y_loc, fwd_state)

    def backward_step(scan_carry, step_in):
        rev_state, acc_q, acc_k, acc_v, acc_o = scan_carry
        x_loc, flag_loc, dy_loc, out_rows, fwd_state = step_in
        head_mask, tail_mask, same_doc, doc_gate = block_masks(flag_loc)
        q_rows, k_rows, v_rows = project(x_loc)
        scores = jnp.einsum('thk,shk->hts', q_rows, k_rows)
        attn_prob = jnp.where(same_doc[None], scores * SCORE_SCALE, 0.0).astype(jnp.bfloat16).astype(jnp.float32)
        d_out = jnp.dot(dy_loc, wo_mat.T, preferred_element_type=jnp.float32).astype(jnp.bfloat16).astype(jnp.float32)
        d_out = d_out.reshape(TOK_DEV, NUM_HEADS, HEAD_DIM)
        dp_raw = jnp.einsum('thv,shv->hts', d_out, v_rows)
        d_prob = jnp.where(same_doc[None], dp_raw * SCORE_SCALE, 0.0).astype(jnp.bfloat16).astype(jnp.float32)
        state_low = fwd_state.astype(jnp.bfloat16).astype(jnp.float32)
        rev_low = rev_state.astype(jnp.bfloat16).astype(jnp.float32)
        head_col = (SCORE_SCALE * head_mask)[:, None, None]
        tail_col = (SCORE_SCALE * tail_mask)[:, None, None]
        dq_rows = (jnp.einsum('hts,shk->thk', d_prob, k_rows)
                   + jnp.einsum('thv,hkv->thk', d_out, state_low) * head_col).astype(jnp.bfloat16).reshape(TOK_DEV, D_MODEL)
        dk_rows = (jnp.einsum('hts,thk->shk', d_prob, q_rows)
                   + jnp.einsum('shv,hkv->shk', v_rows, rev_low) * tail_col).astype(jnp.bfloat16).reshape(TOK_DEV, D_MODEL)
        dv_rows = (jnp.einsum('hts,thv->shv', attn_prob, d_out)
                   + jnp.einsum('shk,hkv->shv', k_rows, rev_low) * tail_col).astype(jnp.bfloat16).reshape(TOK_DEV, D_MODEL)
        dx_loc = (jnp.dot(dq_rows, wq_mat.T, preferred_element_type=jnp.float32)
                  + jnp.dot(dk_rows, wk_mat.T, preferred_element_type=jnp.float32)
                  + jnp.dot(dv_rows, wv_mat.T, preferred_element_type=jnp.float32)).astype(jnp.bfloat16)
        acc_q = acc_q + jnp.dot(x_loc.T, dq_rows, preferred_element_type=jnp.float32)
        acc_k = acc_k + jnp.dot(x_loc.T, dk_rows, preferred_element_type=jnp.float32)
        acc_v = acc_v + jnp.dot(x_loc.T, dv_rows, preferred_element_type=jnp.float32)
        acc_o = acc_o + jnp.dot(out_rows.T, dy_loc, preferred_element_type=jnp.float32)
        n_head = jnp.einsum('thk,thv->hkv', q_rows, d_out * head_mask[:, None, None])
        next_rev = doc_gate * rev_state + n_head
        return (next_rev, acc_q, acc_k, acc_v, acc_o), dx_loc

    x_blocks = x_tok.reshape(SEQ_DEVS, TOK_DEV, D_MODEL)
    flag_blocks = doc_start.reshape(SEQ_DEVS, TOK_DEV)
    dy_blocks = dy_tok.reshape(SEQ_DEVS, TOK_DEV, D_MODEL)
    zero_state = jnp.zeros((NUM_HEADS, HEAD_DIM, HEAD_DIM), jnp.float32)
    last_state, fwd_outs = lax.scan(forward_step, zero_state, (x_blocks, flag_blocks))
    out_blocks, y_blocks, state_blocks = fwd_outs
    zero_grad = jnp.zeros((D_MODEL, D_MODEL), jnp.float32)
    grad_carry, dx_blocks = lax.scan(backward_step, (zero_state, zero_grad, zero_grad, zero_grad, zero_grad),
                                     (x_blocks, flag_blocks, dy_blocks, out_blocks, state_blocks), reverse=True)
    acc_q = grad_carry[1]
    acc_k = grad_carry[2]
    acc_v = grad_carry[3]
    acc_o = grad_carry[4]
    return (y_blocks.reshape(SEQ_LEN, D_MODEL), dx_blocks.reshape(SEQ_LEN, D_MODEL),
            acc_q.reshape(D_MODEL, NUM_HEADS, HEAD_DIM), acc_k.reshape(D_MODEL, NUM_HEADS, HEAD_DIM),
            acc_v.reshape(D_MODEL, NUM_HEADS, HEAD_DIM), acc_o.reshape(NUM_HEADS, HEAD_DIM, D_MODEL))
```

```python
import math
import jax
import jax.numpy as jnp
from jax import lax
from jax.sharding import PartitionSpec as P


def block_masks(flag_loc):
    tok_count = flag_loc.shape[0]
    positions = jnp.arange(tok_count)
    seg_ids = jnp.cumsum(flag_loc)
    first_pos = jnp.min(jnp.where(flag_loc > 0, positions, tok_count))
    last_pos = jnp.max(jnp.where(flag_loc > 0, positions, -1))
    head_col = (positions < first_pos)[:, None, None]
    tail_col = (positions >= last_pos)[:, None, None]
    same_doc = (seg_ids[:, None] == seg_ids[None, :]) & (positions[None, :] <= positions[:, None])
    doc_gate = (last_pos < 0).astype(jnp.float32)
    return head_col, tail_col, same_doc, doc_gate


def solution(mesh):
    seq_devs = mesh.shape['sp']

    def scan_weights(gates):
        me = lax.axis_index('sp')
        idx = jnp.arange(seq_devs)
        closed = (gates < 0.5).astype(jnp.int32)
        csum = jnp.cumsum(closed)
        total_before_me = jnp.sum(jnp.where(idx < me, closed, 0))
        total_to_me = jnp.sum(jnp.where(idx <= me, closed, 0))
        use_fwd = (idx < me) & (total_before_me == csum)
        use_bwd = (idx > me) & (csum - closed == total_to_me)
        return use_fwd, use_bwd

    def gathered_state(local_state, use):
        every = lax.all_gather(local_state, 'sp', axis=0, tiled=False)
        return jnp.sum(jnp.where(use[:, None, None, None], every, 0.0), axis=0)

    def device_body(x_loc, flag_loc, w_q, w_k, w_v, w_o, dy_loc):
        tok_count, d_model = x_loc.shape
        n_heads, head_dim = w_q.shape[1], w_q.shape[2]
        score_scale = 1.0 / (math.sqrt(head_dim) * tok_count)
        head_col, tail_col, same_doc, doc_gate = block_masks(flag_loc)
        gates = lax.all_gather(doc_gate, 'sp')
        use_fwd, use_bwd = scan_weights(gates)
        k_rows = jnp.einsum('td,dhk->thk', x_loc, w_k, preferred_element_type=jnp.float32).astype(jnp.bfloat16)
        v_rows = jnp.einsum('td,dhk->thk', x_loc, w_v, preferred_element_type=jnp.float32).astype(jnp.bfloat16)
        m_tail = jnp.einsum('til,tiw->ilw', k_rows, jnp.where(tail_col, v_rows, 0.0), preferred_element_type=jnp.float32)
        fwd_state = gathered_state(m_tail, use_fwd)
        q_rows = jnp.einsum('td,dhk->thk', x_loc, w_q, preferred_element_type=jnp.float32).astype(jnp.bfloat16)
        d_out = jnp.einsum('tc,hkc->thk', dy_loc, w_o, preferred_element_type=jnp.float32).astype(jnp.bfloat16)
        n_head = jnp.einsum('uil,uiw->ilw', q_rows, jnp.where(head_col, d_out, 0.0), preferred_element_type=jnp.float32)
        rev_state = gathered_state(n_head, use_bwd)
        scores = jnp.einsum('thk,shk->hts', q_rows, k_rows, preferred_element_type=jnp.float32)
        attn_prob = jnp.where(same_doc, scores * score_scale, 0.0).astype(jnp.bfloat16)
        state_low = fwd_state.astype(jnp.bfloat16)
        rev_low = rev_state.astype(jnp.bfloat16)
        intra_sum = jnp.einsum('hts,shv->thv', attn_prob, v_rows, preferred_element_type=jnp.float32)
        inter_sum = jnp.einsum('uil,ilw->uiw', q_rows, state_low, preferred_element_type=jnp.float32)
        out_rows = (intra_sum + jnp.where(head_col, inter_sum * score_scale, 0.0)).astype(jnp.bfloat16)

        def grad_t(rows, other):
            part = jnp.einsum('tn,td->nd', rows.reshape(tok_count, -1), other, preferred_element_type=jnp.float32)
            piece = lax.psum_scatter(part, 'sp', scatter_dimension=0, tiled=True)
            return lax.all_gather(piece, 'sp', axis=0, tiled=True)

        dw_o = grad_t(out_rows, dy_loc)
        dv_rows = (jnp.einsum('hts,thv->shv', attn_prob, d_out, preferred_element_type=jnp.float32)
                   + jnp.where(tail_col, jnp.einsum('til,ilw->tiw', k_rows, rev_low, preferred_element_type=jnp.float32) * score_scale, 0.0)).astype(jnp.bfloat16)
        dw_v = grad_t(dv_rows, x_loc)
        dp_raw = jnp.einsum('thv,shv->hts', d_out, v_rows, preferred_element_type=jnp.float32)
        d_prob = jnp.where(same_doc, dp_raw * score_scale, 0.0).astype(jnp.bfloat16)
        dq_rows = (jnp.einsum('hts,shk->thk', d_prob, k_rows, preferred_element_type=jnp.float32)
                   + jnp.where(head_col, jnp.einsum('uiw,ilw->uil', d_out, state_low, preferred_element_type=jnp.float32) * score_scale, 0.0)).astype(jnp.bfloat16)
        dw_q = grad_t(dq_rows, x_loc)
        dk_rows = (jnp.einsum('hts,thk->shk', d_prob, q_rows, preferred_element_type=jnp.float32)
                   + jnp.where(tail_col, jnp.einsum('tiw,ilw->til', v_rows, rev_low, preferred_element_type=jnp.float32) * score_scale, 0.0)).astype(jnp.bfloat16)
        dw_k = grad_t(dk_rows, x_loc)
        y_loc = jnp.einsum('thk,hkc->tc', out_rows, w_o, preferred_element_type=jnp.float32).astype(jnp.bfloat16)
        dx_loc = (jnp.einsum('thk,dhk->td', dq_rows, w_q, preferred_element_type=jnp.float32)
                  + jnp.einsum('thk,dhk->td', dk_rows, w_k, preferred_element_type=jnp.float32)
                  + jnp.einsum('thk,dhk->td', dv_rows, w_v, preferred_element_type=jnp.float32)).astype(jnp.bfloat16)

        def as_w(grad):
            return grad.reshape(n_heads, head_dim, d_model).transpose(2, 0, 1)
        return y_loc, dx_loc, as_w(dw_q), as_w(dw_k), as_w(dw_v), dw_o.reshape(n_heads, head_dim, d_model)

    row_spec = P(('dp', 'sp'), None)
    flag_spec = P(('dp', 'sp'))
    w_spec = P(None, None, None)
    dw_spec = P('dp', None, None)
    mapped = jax.shard_map(device_body, mesh=mesh,
                           in_specs=(row_spec, flag_spec, w_spec, w_spec, w_spec, w_spec, row_spec),
                           out_specs=(row_spec, row_spec, dw_spec, dw_spec, dw_spec, dw_spec),
                           check_vma=False)
    return mapped
```

```python
import functools
import math
import jax
import jax.numpy as jnp
from jax import lax
from jax.experimental import pallas as pl
from jax.experimental.pallas import tpu as pltpu
from jax.sharding import PartitionSpec as P

MESH = pl.DeviceIdType.MESH
CORES = 2
RING = 4
TYPES = 4
O_TYPE = 3
LIVE_LIMIT = 62 * 1024 * 1024
BF16 = jnp.bfloat16
F32 = jnp.float32


def place(me):
    core = lax.rem(me, CORES)
    chip = me // CORES
    return lax.rem(chip, RING), chip // RING, core


def index_of(x, y, core):
    return (lax.rem(y, RING) * RING + lax.rem(x, RING)) * CORES + core


def remote(src, dst, send_sem, recv_sem, peer):
    return pltpu.make_async_remote_copy(src_ref=src, dst_ref=dst, send_sem=send_sem, recv_sem=recv_sem,
                                        device_id={'sp': peer}, device_id_type=MESH)


def meet(peers):
    barrier = pltpu.get_barrier_semaphore()
    for peer in peers:
        pl.semaphore_signal(barrier, inc=1, device_id={'sp': peer}, device_id_type=MESH)
    pl.semaphore_wait(barrier, len(peers))


def dot(a, b, dims):
    return lax.dot_general(a, b, (dims, ((), ())), preferred_element_type=F32)


def block_masks(flag_loc):
    tok_count = flag_loc.shape[0]
    positions = jnp.arange(tok_count)
    seg_ids = jnp.sum(jnp.where(positions[None, :] <= positions[:, None], flag_loc[None, :], 0), axis=1)
    first_pos = jnp.min(jnp.where(flag_loc > 0, positions, tok_count))
    last_pos = jnp.max(jnp.where(flag_loc > 0, positions, -1))
    head = (positions < first_pos).astype(F32)
    tail = (positions >= last_pos).astype(F32)
    doc_gate = (last_pos < 0).astype(F32)
    return seg_ids, head, tail, doc_gate


def state_kernel(q_ref, k_ref, v_ref, do_ref, head_ref, tail_ref, gate_ref, out_ref,
                 packed, held, formed, send_sem, recv_sem, back_send, back_recv):
    me = lax.axis_index('sp')
    n_dev, per_dev = packed.shape[0], packed.shape[1]
    dim = q_ref.shape[0] // (n_dev * per_dev)

    barrier = pltpu.get_barrier_semaphore()

    @pl.loop(1, n_dev)
    def _(step):
        pl.semaphore_signal(barrier, inc=1, device_id={'sp': lax.rem(me + step, n_dev)}, device_id_type=MESH)

    head = head_ref[...] > 0.5
    tail = tail_ref[...] > 0.5
    zero = jnp.zeros((dim, q_ref.shape[1]), BF16)

    @pl.loop(0, n_dev)
    def _(dev):
        for sub in range(per_dev):
            rows = pl.ds(pl.multiple_of((dev * per_dev + sub) * dim, dim), dim)
            v_tail = jnp.concatenate([jnp.where(tail, v_ref[rows, :], zero), zero], axis=0)
            do_head = jnp.concatenate([zero, jnp.where(head, do_ref[rows, :], zero)], axis=0)
            both = dot(k_ref[rows, :], v_tail, ((1,), (1,))) + dot(q_ref[rows, :], do_head, ((1,), (1,)))
            packed[dev, sub, 0:dim, :] = both
            packed[dev, sub, dim:dim + 8, :] = gate_ref[...]

    pl.semaphore_wait(barrier, n_dev - 1)

    def out_copy(step):
        peer = lax.rem(me + step, n_dev)
        return remote(packed.at[peer], held.at[me], send_sem.at[step], recv_sem.at[step], peer)

    def back_copy(step):
        peer = lax.rem(me + step, n_dev)
        return remote(formed.at[peer], out_ref.at[me], back_send.at[step], back_recv.at[step], peer)

    @pl.loop(1, n_dev)
    def _(step):
        out_copy(step).start()

    held[me] = packed[me]

    @pl.loop(1, n_dev)
    def _(step):
        out_copy(step).wait_recv()

    lane = lax.broadcasted_iota(jnp.int32, (per_dev, dim, 2 * dim), 2)
    start = jnp.zeros((per_dev, dim, 2 * dim), F32)

    def forward(block, state):
        formed[block] = state.astype(BF16)
        return held[block, :, dim:dim + 1, :] * state + held[block, :, 0:dim, :]

    lax.fori_loop(0, n_dev, forward, start)

    def backward(step, state):
        block = n_dev - 1 - step
        formed[block] = jnp.where(lane < dim, formed[block].astype(F32), state).astype(BF16)
        return held[block, :, dim:dim + 1, :] * state + held[block, :, 0:dim, :]

    lax.fori_loop(0, n_dev, backward, start)

    @pl.loop(1, n_dev)
    def _(step):
        back_copy(step).start()

    out_ref[me] = formed[me]

    @pl.loop(1, n_dev)
    def _(step):
        back_copy(step).wait_recv()

    @pl.loop(1, n_dev)
    def _(step):
        out_copy(step).wait_send()
        back_copy(step).wait_send()


def states(qt, kt, vt, dot_t, head, tail, gate, n_dev, n_heads):
    width, tok = qt.shape
    dim = width // n_heads
    per_dev = n_heads // n_dev
    vmem = pl.BlockSpec(memory_space=pltpu.VMEM)
    out = pl.pallas_call(
        state_kernel,
        name='states',
        out_shape=jax.ShapeDtypeStruct((n_dev, per_dev, dim, 2 * dim), BF16),
        in_specs=[vmem] * 7,
        out_specs=vmem,
        scratch_shapes=[
            pltpu.VMEM((n_dev, per_dev, dim + 8, 2 * dim), F32),
            pltpu.VMEM((n_dev, per_dev, dim + 8, 2 * dim), F32),
            pltpu.VMEM((n_dev, per_dev, dim, 2 * dim), BF16),
            pltpu.SemaphoreType.DMA((n_dev,)),
            pltpu.SemaphoreType.DMA((n_dev,)),
            pltpu.SemaphoreType.DMA((n_dev,)),
            pltpu.SemaphoreType.DMA((n_dev,)),
        ],
        compiler_params=pltpu.CompilerParams(collective_id=0, has_side_effects=True, vmem_limit_bytes=32 * 1024 * 1024),
        cost_estimate=pl.CostEstimate(flops=40 * 10**9, bytes_accessed=8 * width * tok, transcendentals=0),
    )(qt, kt, vt, dot_t, head[None, :], tail[None, :], jnp.broadcast_to(gate, (8, 2 * dim)))
    return out.reshape(n_heads, dim, 2 * dim)


def attention_kernel(scale, dim, seg_col_ref, seg_row_ref, head_ref, tail_ref, q_ref, k_ref, v_ref, do_ref, st_ref, g_ref):
    tok = q_ref.shape[1]
    half = tok // 2
    seg_row = seg_row_ref[...]
    t_pos = lax.broadcasted_iota(jnp.int32, (half, tok), 0)
    s_pos = lax.broadcasted_iota(jnp.int32, (half, tok), 1)
    see_top = ((seg_col_ref[0:half, :] == seg_row) & (s_pos <= t_pos))[:, 0:half]
    see_low = (seg_col_ref[half:tok, :] == seg_row) & (s_pos <= t_pos + half)
    head = head_ref[...] > 0.5
    tail = tail_ref[...] > 0.5
    zero = jnp.zeros((dim, tok), BF16)

    for sub in range(q_ref.shape[0] // dim):
        rows = slice(sub * dim, (sub + 1) * dim)
        q, k, v, do = q_ref[rows, :], k_ref[rows, :], v_ref[rows, :], do_ref[rows, :]
        st = st_ref[sub]

        def pair(a, b):
            top = dot(a[:, 0:half], b[:, 0:half], ((0,), (0,)))
            low = dot(a[:, half:tok], b, ((0,), (0,)))
            return (jnp.where(see_top, top * scale, 0.0).astype(BF16), jnp.where(see_low, low * scale, 0.0).astype(BF16))

        def over_keys(rows_t, probs):
            top, low = probs
            return jnp.concatenate([dot(rows_t[:, 0:half], top, ((1,), (1,))), dot(rows_t, low, ((1,), (1,)))], axis=1)

        def over_queries(rows_t, probs):
            top, low = probs
            from_low = dot(rows_t[:, half:tok], low, ((1,), (0,)))
            first = dot(rows_t[:, 0:half], top, ((1,), (0,))) + from_low[:, 0:half]
            return jnp.concatenate([first, from_low[:, half:tok]], axis=1)

        probs = pair(q, k)
        d_probs = pair(do, v)
        from_q = dot(st, q, ((0,), (0,)))
        from_k = dot(st, k, ((0,), (0,)))
        o_inter = from_q[0:dim]
        dv_inter = from_k[dim:2 * dim]
        dq_inter = dot(st, jnp.concatenate([do, zero], axis=0), ((1,), (0,)))
        dk_inter = dot(st, jnp.concatenate([zero, v], axis=0), ((1,), (0,)))
        g_ref[0, rows, :] = (over_keys(k, d_probs) + jnp.where(head, dq_inter * scale, 0.0)).astype(BF16)
        g_ref[1, rows, :] = (over_queries(q, d_probs) + jnp.where(tail, dk_inter * scale, 0.0)).astype(BF16)
        g_ref[2, rows, :] = (over_queries(do, probs) + jnp.where(tail, dv_inter * scale, 0.0)).astype(BF16)
        g_ref[3, rows, :] = (over_keys(v, probs) + jnp.where(head, o_inter * scale, 0.0)).astype(BF16)


def attention(qt, kt, vt, dot_t, st, seg_ids, head, tail, scale, n_heads):
    width, tok = qt.shape
    dim = width // n_heads
    group = width // (CORES * RING)
    rows = pl.BlockSpec((group, tok), lambda g: (g, 0))
    whole = lambda shape: pl.BlockSpec(shape, lambda g: (0,) * len(shape))
    return pl.pallas_call(
        functools.partial(attention_kernel, scale, dim),
        name='attention',
        grid=(width // group,),
        out_shape=jax.ShapeDtypeStruct((TYPES, width, tok), BF16),
        in_specs=[whole((tok, 1)), whole((1, tok)), whole((1, tok)), whole((1, tok)), rows, rows, rows, rows,
                  pl.BlockSpec((group // dim, dim, 2 * dim), lambda g: (g, 0, 0))],
        out_specs=pl.BlockSpec((TYPES, group, tok), lambda g: (0, g, 0)),
        compiler_params=pltpu.CompilerParams(vmem_limit_bytes=40 * 1024 * 1024),
        cost_estimate=pl.CostEstimate(flops=12 * width * tok * tok * 4, bytes_accessed=16 * width * tok, transcendentals=0),
    )(seg_ids[:, None], seg_ids[None, :], head[None, :], tail[None, :], qt, kt, vt, dot_t, st)


ORDER = (2, 1, 3, 0)


def reduce_kernel(g_ref, *refs):
    z_refs = refs[:2 * RING]
    (out_ref, zbuf, rows_in, stage, a_out, a_in, b_out, b_in, z_sem,
     far_send, stage_sem, half_send, row_send, row_recv, half_recv, a_send, a_recv, b_send, b_recv) = refs[2 * RING:]
    me = lax.axis_index('sp')
    x, y, core = place(me)
    block = rows_in.shape[2]
    part = block // 2
    n_col, cols = a_out.shape[0], a_out.shape[3]

    meet([index_of(x, y, 1 - core)]
         + [index_of(x + dx, y + dy, other) for dx, dy in ((1, 0), (3, 0), (0, 1), (0, 3)) for other in range(CORES)])

    for i in range(2 * RING):
        pltpu.make_async_copy(z_refs[i], zbuf.at[i], z_sem.at[i]).start()

    def ring_of(ring):
        along, across = (x, y) if ring == 0 else (y, x)
        peer = (lambda step, owner_core: index_of(x + step, y, owner_core)) if ring == 0 else (
            lambda step, owner_core: index_of(x, y + step, owner_core))
        return along, across, peer, lax.rem(core + ring, CORES)

    def source(ring, bi, step):
        along, across, _, _ = ring_of(ring)
        kind = lax.rem(along + step, RING)
        first = (ring * RING + lax.rem(across + ORDER[bi], RING)) * block
        return kind, pl.multiple_of(first, block)

    def near_copy(ring, bi, step):
        _, _, peer, flip = ring_of(ring)
        kind, first = source(ring, bi, step)
        slot = 2 * step + flip
        return remote(g_ref.at[kind, pl.ds(first, block)], rows_in.at[slot, bi], row_send.at[ring, bi, step],
                      row_recv.at[slot, bi], peer(step, ring))

    def far_copy(ring, bi, way):
        _, _, peer, _ = ring_of(ring)
        kind, first = source(ring, bi, 2)
        return remote(g_ref.at[kind, pl.ds(pl.multiple_of(first + way * part, part), part)], stage.at[ring, bi, way],
                      far_send.at[ring, bi, way], stage_sem.at[ring, bi, way], peer((1, 3)[way], core))

    def pass_copy(ring, bi, way):
        _, _, peer, flip = ring_of(ring)
        return remote(stage.at[ring, bi, way], rows_in.at[4 + flip, bi, pl.ds(way * part, part)],
                      half_send.at[ring, bi, way], half_recv.at[flip, bi, way], peer((1, 3)[way], ring))

    for bi in range(RING):
        for ring in range(2):
            for way in range(2):
                far_copy(ring, bi, way).start()
            near_copy(ring, bi, 1).start()
            near_copy(ring, bi, 3).start()

            @pl.when(core != ring)
            def _(ring=ring, bi=bi):
                near_copy(ring, bi, 0).start()

            @pl.when(core == ring)
            def _(ring=ring, bi=bi):
                kind, first = source(ring, bi, 0)
                pltpu.make_async_copy(g_ref.at[kind, pl.ds(first, block)], rows_in.at[0, bi], row_recv.at[0, bi]).start()

    def pass_on(bi):
        for ring in range(2):
            for way in range(2):
                far_copy(ring, bi, way).wait_recv()
                pass_copy(ring, bi, way).start()

    def arrived(bi):
        for slot in (0, 1, 2, 3, 6, 7):
            pltpu.make_async_copy(g_ref.at[0, pl.ds(0, block)], rows_in.at[slot, bi], row_recv.at[slot, bi]).wait()
        for flip in range(CORES):
            for way in range(2):
                half = rows_in.at[4 + flip, bi, pl.ds(way * part, part)]
                pltpu.make_async_copy(g_ref.at[0, pl.ds(0, part)], half, half_recv.at[flip, bi, way]).wait()

    def product(bi, ch):
        at = pl.ds(pl.multiple_of(ch * cols, cols), cols)
        total = dot(rows_in[0, bi], zbuf[0, :, at], ((1,), (0,)))
        for slot in range(1, 2 * RING):
            total = total + dot(rows_in[slot, bi], zbuf[slot, :, at], ((1,), (0,)))
        return total

    across_peer = [jnp.where(core == 0, index_of(x, y + step, core), index_of(x + step, y, core)) for step in (1, 3)]

    def a_copy(ch, way):
        return remote(a_out.at[ch, way], a_in.at[ch, way], a_send.at[ch, way], a_recv.at[ch, way], across_peer[way])

    def b_copy(ch, way):
        return remote(b_out.at[ch, way], b_in.at[ch, way], b_send.at[ch, way], b_recv.at[ch, way], across_peer[way])

    pass_on(0)
    pass_on(1)
    for i in range(2 * RING):
        pltpu.make_async_copy(z_refs[i], zbuf.at[i], z_sem.at[i]).wait()
    arrived(0)

    @pl.loop(0, n_col)
    def _(ch):
        total = product(0, ch)
        a_out[ch, 0] = total[0:part]
        a_out[ch, 1] = total[part:block]
        a_copy(ch, 0).start()
        a_copy(ch, 1).start()

    pass_on(2)
    arrived(1)

    @pl.loop(0, n_col)
    def _(ch):
        total = product(1, ch)
        a_copy(ch, 0).wait_recv()
        b_out[ch, 0, 0:part] = total[0:part] + a_in[ch, 0]
        b_out[ch, 0, part:block] = total[part:block]
        b_copy(ch, 0).start()

    pass_on(3)
    arrived(2)

    @pl.loop(0, n_col)
    def _(ch):
        total = product(2, ch)
        a_copy(ch, 1).wait_recv()
        b_out[ch, 1, 0:part] = total[0:part]
        b_out[ch, 1, part:block] = total[part:block] + a_in[ch, 1]
        b_copy(ch, 1).start()

    arrived(3)

    @pl.loop(0, n_col)
    def _(ch):
        total = product(3, ch)
        b_copy(ch, 0).wait_recv()
        b_copy(ch, 1).wait_recv()
        out_ref[:, pl.ds(pl.multiple_of(ch * cols, cols), cols)] = total + b_in[ch, 0] + b_in[ch, 1]

    for bi in range(RING):
        for ring in range(2):
            for way in range(2):
                far_copy(ring, bi, way).wait_send()
                pass_copy(ring, bi, way).wait_send()
            near_copy(ring, bi, 1).wait_send()
            near_copy(ring, bi, 3).wait_send()

            @pl.when(core != ring)
            def _(ring=ring, bi=bi):
                near_copy(ring, bi, 0).wait_send()

    for ch in range(n_col):
        for way in range(2):
            a_copy(ch, way).wait_send()
            b_copy(ch, way).wait_send()


def reduce_rows(g, zs):
    width, tok = g.shape[1], g.shape[2]
    d_model = zs[0].shape[1]
    block = width // (CORES * RING)
    n_col = 4
    cols = d_model // n_col
    anywhere = pl.BlockSpec(memory_space=pl.ANY)
    dma = pltpu.SemaphoreType.DMA
    return pl.pallas_call(
        reduce_kernel,
        name='reduce_rows',
        out_shape=jax.ShapeDtypeStruct((block, d_model), F32),
        in_specs=[anywhere] * (1 + len(zs)),
        out_specs=pl.BlockSpec(memory_space=pltpu.VMEM),
        scratch_shapes=[
            pltpu.VMEM((2 * RING, tok, d_model), BF16),
            pltpu.VMEM((2 * RING, RING, block, tok), BF16),
            pltpu.VMEM((2, RING, 2, block // 2, tok), BF16),
            pltpu.VMEM((n_col, 2, block // 2, cols), F32),
            pltpu.VMEM((n_col, 2, block // 2, cols), F32),
            pltpu.VMEM((n_col, 2, block, cols), F32),
            pltpu.VMEM((n_col, 2, block, cols), F32),
            dma((2 * RING,)),
            dma((2, RING, 2)), dma((2, RING, 2)), dma((2, RING, 2)),
            dma((2, RING, RING)), dma((2 * RING, RING)), dma((CORES, RING, 2)),
            dma((n_col, 2)), dma((n_col, 2)), dma((n_col, 2)), dma((n_col, 2)),
        ],
        compiler_params=pltpu.CompilerParams(collective_id=1, has_side_effects=True, vmem_limit_bytes=LIVE_LIMIT),
        cost_estimate=pl.CostEstimate(flops=200 * 10**9, bytes_accessed=100 * 10**6, transcendentals=0),
    )(g, *zs)


def gather_kernel(piece_ref, out_ref, own_sem, send_sem, recv_sem, side_send, side_recv):
    me = lax.axis_index('sp')
    x, y, core = place(me)
    rows = piece_ref.shape[0]
    part = rows // 2
    quarter = part // 2

    def base(sx, sy):
        px, py = lax.rem(x + sx, RING), lax.rem(y + sy, RING)
        kind = jnp.where(core == 0, px, py)
        slot = jnp.where(core == 0, py, px)
        return ((kind * CORES + core) * RING + slot) * rows

    def spot(leg, i, j, lo=0, size=None):
        sx, sy = (i, j) if leg == 0 else (j, i)
        return out_ref.at[pl.ds(pl.multiple_of(base(sx, sy) + leg * part + lo, quarter), part if size is None else size)]

    def step_peer(leg, second, step):
        along_x = (leg == 0) != second
        return index_of(x + step, y, core) if along_x else index_of(x, y + step, core)

    started = []

    def push(leg, second, i, j, step, half):
        there = ((i, (j - step) % RING) if second else ((i - step) % RING, j))
        lo, size = (0, part) if half is None else (half * quarter, quarter)
        src = spot(leg, i, j, lo, size)
        if i == 0 and j == 0:
            src = piece_ref.at[pl.ds(leg * part + lo, size)]
        n = len(started)
        copy = remote(src, spot(leg, i, j, lo, size), send_sem.at[n],
                      recv_sem.at[leg, there[0], there[1], 0 if half is None else half], step_peer(leg, second, step))
        copy.start()
        started.append(copy)

    def landed(leg, i, j):
        halves = [None] if 2 not in (i, j) or (j == 0 and i != 2) or (j != 0 and j != 2) else [0, 1]
        for half in halves:
            lo, size = (0, part) if half is None else (half * quarter, quarter)
            here = spot(leg, i, j, lo, size)
            pltpu.make_async_copy(here, here, recv_sem.at[leg, i, j, 0 if half is None else half]).wait()

    side = []

    def to_sibling(leg, i, j):
        src = spot(leg, i, j)
        if i == 0 and j == 0:
            src = piece_ref.at[pl.ds(leg * part, part)]
        copy = remote(src, spot(leg, i, j), side_send.at[leg, i, j], side_recv.at[leg, i, j], index_of(x, y, 1 - core))
        copy.start()
        side.append(copy)

    meet([index_of(x, y, 1 - core)] + [index_of(x + dx, y + dy, core) for dx, dy in ((1, 0), (3, 0), (0, 1), (0, 3))])

    def spread(leg, i):
        push(leg, True, i, 0, 1, None)
        push(leg, True, i, 0, 3, None)
        to_sibling(leg, i, 0)

    for leg in range(2):
        push(leg, False, 0, 0, 1, None)
        push(leg, False, 0, 0, 3, None)
    for leg in range(2):
        spread(leg, 0)
    own = pltpu.make_async_copy(piece_ref, out_ref.at[pl.ds(pl.multiple_of(base(0, 0), rows), rows)], own_sem)
    own.start()

    for leg in range(2):
        landed(leg, 3, 0)
        push(leg, False, 3, 0, 1, 0)
        spread(leg, 3)
        landed(leg, 1, 0)
        push(leg, False, 1, 0, 3, 1)
        spread(leg, 1)

    def second_near(leg, i):
        landed(leg, i, 3)
        push(leg, True, i, 3, 1, 0)
        to_sibling(leg, i, 3)
        landed(leg, i, 1)
        push(leg, True, i, 1, 3, 1)
        to_sibling(leg, i, 1)

    for leg in range(2):
        second_near(leg, 0)
    for leg in range(2):
        landed(leg, 2, 0)
        spread(leg, 2)
    for i in (3, 1, 2):
        for leg in range(2):
            second_near(leg, i)
    for i in (0, 3, 1, 2):
        for leg in range(2):
            landed(leg, i, 2)
            to_sibling(leg, i, 2)

    own.wait()
    for copy in started:
        copy.wait_send()
    for copy in side:
        copy.wait_send()

    def side_base(i, j, leg):
        sx, sy = (i, j) if leg == 0 else (j, i)
        px, py = lax.rem(x + sx, RING), lax.rem(y + sy, RING)
        kind = jnp.where(core == 0, py, px)
        slot = jnp.where(core == 0, px, py)
        return pl.multiple_of(((kind * CORES + 1 - core) * RING + slot) * rows + leg * part, part)

    for leg in range(2):
        for i in range(RING):
            for j in range(RING):
                here = out_ref.at[pl.ds(side_base(i, j, leg), part)]
                pltpu.make_async_copy(here, here, side_recv.at[leg, i, j]).wait()


def gather_rows(piece, n_dev):
    rows, d_model = piece.shape
    dma = pltpu.SemaphoreType.DMA
    return pl.pallas_call(
        gather_kernel,
        name='gather_rows',
        out_shape=jax.ShapeDtypeStruct((n_dev * rows, d_model), F32),
        in_specs=[pl.BlockSpec(memory_space=pltpu.VMEM)],
        out_specs=pl.BlockSpec(memory_space=pl.ANY),
        scratch_shapes=[dma, dma((40,)), dma((2, RING, RING, 2)), dma((2, RING, RING)), dma((2, RING, RING))],
        compiler_params=pltpu.CompilerParams(collective_id=2, has_side_effects=True, vmem_limit_bytes=16 * 1024 * 1024),
        cost_estimate=pl.CostEstimate(flops=700 * 10**9, bytes_accessed=128 * 10**6, transcendentals=0),
    )(piece)


def solution(mesh):
    n_dev = mesh.shape['sp']
    assert n_dev == CORES * RING * RING

    def token_operands(x_loc, dy_loc):
        me = lax.axis_index('sp')
        x, y, core = place(me)
        found = []
        for step in range(RING):
            for flip in range(CORES):
                owner = lax.rem(core + flip, CORES)
                kind = lax.rem(jnp.where(owner == 0, x, y) + step, RING)
                load = jnp.where(kind == O_TYPE, dy_loc, x_loc)
                if step or flip:
                    pairs = []
                    for src in range(n_dev):
                        sx, sy, sc = (src // CORES) % RING, src // (CORES * RING), src % CORES
                        oc = (sc + flip) % CORES
                        ox, oy = ((sx + step) % RING, sy) if oc == 0 else (sx, (sy + step) % RING)
                        pairs.append((src, (oy * RING + ox) * CORES + oc))
                    load = lax.ppermute(load, 'sp', pairs)
                found.append(load)
        return found

    def device_body(x_loc, flag_loc, w_q, w_k, w_v, w_o, dy_loc):
        tok_count, d_model = x_loc.shape
        n_heads, head_dim = w_q.shape[1], w_q.shape[2]
        width = n_heads * head_dim
        score_scale = 1.0 / (math.sqrt(head_dim) * tok_count)
        seg_ids, head, tail, doc_gate = block_masks(flag_loc)
        zs = token_operands(x_loc, dy_loc)

        def flat(w):
            return w.transpose(1, 2, 0).reshape(width, d_model)
        wq, wk, wv, wo = flat(w_q), flat(w_k), flat(w_v), w_o.reshape(width, d_model)
        qt, kt, vt, dot_t = (jnp.einsum('nd,td->nt', w, rows, preferred_element_type=F32).astype(BF16)
                             for w, rows in ((wq, x_loc), (wk, x_loc), (wv, x_loc), (wo, dy_loc)))
        st = states(qt, kt, vt, dot_t, head, tail, doc_gate, n_dev, n_heads)
        g = attention(qt, kt, vt, dot_t, st, seg_ids, head, tail, score_scale, n_heads)
        y_loc = jnp.einsum('nt,nd->td', g[3], wo, preferred_element_type=F32).astype(BF16)
        dx_loc = (jnp.einsum('nt,nd->td', g[0], wq, preferred_element_type=F32)
                  + jnp.einsum('nt,nd->td', g[1], wk, preferred_element_type=F32)
                  + jnp.einsum('nt,nd->td', g[2], wv, preferred_element_type=F32)).astype(BF16)
        piece = reduce_rows(g, zs)
        grads = gather_rows(piece, n_dev).reshape(TYPES, n_heads, head_dim, d_model)
        dw_q, dw_k, dw_v = (grads[i].transpose(2, 0, 1) for i in range(3))
        return y_loc, dx_loc, dw_q, dw_k, dw_v, grads[O_TYPE]

    row_spec = P(('dp', 'sp'), None)
    flag_spec = P(('dp', 'sp'))
    w_spec = P(None, None, None)
    dw_spec = P('dp', None, None)
    return jax.shard_map(device_body, mesh=mesh,
                         in_specs=(row_spec, flag_spec, w_spec, w_spec, w_spec, w_spec, row_spec),
                         out_specs=(row_spec, row_spec, dw_spec, dw_spec, dw_spec, dw_spec),
                         check_vma=False)
```

```python
import functools
import math
import jax
import jax.numpy as jnp
from jax import lax
from jax.experimental import pallas as pl
from jax.experimental.pallas import tpu as pltpu
from jax.sharding import PartitionSpec as P


MESH = pl.DeviceIdType.MESH
CORES = 2
RING = 4
TYPES = 4
O_TYPE = 3
REDUCE_LIMIT = 48 * 1024 * 1024
BF16 = jnp.bfloat16
F32 = jnp.float32


def place(me):
    core = lax.rem(me, CORES)
    chip = me // CORES
    return lax.rem(chip, RING), chip // RING, core


def index_of(x, y, core):
    return (lax.rem(y, RING) * RING + lax.rem(x, RING)) * CORES + core


def remote(src, dst, send_sem, recv_sem, peer):
    return pltpu.make_async_remote_copy(src_ref=src, dst_ref=dst, send_sem=send_sem, recv_sem=recv_sem,
                                        device_id={'sp': peer}, device_id_type=MESH)


def meet(peers):
    barrier = pltpu.get_barrier_semaphore()
    for peer in peers:
        pl.semaphore_signal(barrier, inc=1, device_id={'sp': peer}, device_id_type=MESH)
    pl.semaphore_wait(barrier, len(peers))


def dot(a, b, dims):
    return lax.dot_general(a, b, (dims, ((), ())), preferred_element_type=F32)


def block_masks(flag_loc):
    tok_count = flag_loc.shape[0]
    positions = jnp.arange(tok_count)
    seg_ids = jnp.sum(jnp.where(positions[None, :] <= positions[:, None], flag_loc[None, :], 0), axis=1)
    first_pos = jnp.min(jnp.where(flag_loc > 0, positions, tok_count))
    last_pos = jnp.max(jnp.where(flag_loc > 0, positions, -1))
    head = (positions < first_pos).astype(F32)
    tail = (positions >= last_pos).astype(F32)
    doc_gate = (last_pos < 0).astype(F32)
    return seg_ids, head, tail, doc_gate


def state_kernel(q_ref, k_ref, v_ref, do_ref, head_ref, tail_ref, gate_ref, out_ref,
                 packed, held, formed, send_sem, recv_sem, back_send, back_recv):
    me = lax.axis_index('sp')
    n_dev, per_dev = packed.shape[0], packed.shape[1]
    dim = q_ref.shape[0] // (n_dev * per_dev)

    barrier = pltpu.get_barrier_semaphore()

    @pl.loop(1, n_dev)
    def _(step):
        pl.semaphore_signal(barrier, inc=1, device_id={'sp': lax.rem(me + step, n_dev)}, device_id_type=MESH)

    head = head_ref[...] > 0.5
    tail = tail_ref[...] > 0.5
    zero = jnp.zeros((dim, q_ref.shape[1]), BF16)

    @pl.loop(0, n_dev)
    def _(dev):
        for sub in range(per_dev):
            rows = pl.ds(pl.multiple_of((dev * per_dev + sub) * dim, dim), dim)
            v_tail = jnp.concatenate([jnp.where(tail, v_ref[rows, :], zero), zero], axis=0)
            do_head = jnp.concatenate([zero, jnp.where(head, do_ref[rows, :], zero)], axis=0)
            both = dot(k_ref[rows, :], v_tail, ((1,), (1,))) + dot(q_ref[rows, :], do_head, ((1,), (1,)))
            packed[dev, sub, 0:dim, :] = both
            packed[dev, sub, dim:dim + 8, :] = gate_ref[...]

    pl.semaphore_wait(barrier, n_dev - 1)

    def out_copy(step):
        peer = lax.rem(me + step, n_dev)
        return remote(packed.at[peer], held.at[me], send_sem.at[step], recv_sem.at[step], peer)

    def back_copy(step):
        peer = lax.rem(me + step, n_dev)
        return remote(formed.at[peer], out_ref.at[me], back_send.at[step], back_recv.at[step], peer)

    @pl.loop(1, n_dev)
    def _(step):
        out_copy(step).start()

    held[me] = packed[me]

    @pl.loop(1, n_dev)
    def _(step):
        out_copy(step).wait_recv()

    lane = lax.broadcasted_iota(jnp.int32, (per_dev, dim, 2 * dim), 2)
    start = jnp.zeros((per_dev, dim, 2 * dim), F32)

    def forward(block, state):
        formed[block] = state.astype(BF16)
        return held[block, :, dim:dim + 1, :] * state + held[block, :, 0:dim, :]

    lax.fori_loop(0, n_dev, forward, start)

    def backward(step, state):
        block = n_dev - 1 - step
        formed[block] = jnp.where(lane < dim, formed[block].astype(F32), state).astype(BF16)
        return held[block, :, dim:dim + 1, :] * state + held[block, :, 0:dim, :]

    lax.fori_loop(0, n_dev, backward, start)

    @pl.loop(1, n_dev)
    def _(step):
        back_copy(step).start()

    out_ref[me] = formed[me]

    @pl.loop(1, n_dev)
    def _(step):
        back_copy(step).wait_recv()

    @pl.loop(1, n_dev)
    def _(step):
        out_copy(step).wait_send()
        back_copy(step).wait_send()


def states(qt, kt, vt, dot_t, head, tail, gate, n_dev, n_heads):
    width, tok = qt.shape
    dim = width // n_heads
    per_dev = n_heads // n_dev
    vmem = pl.BlockSpec(memory_space=pltpu.VMEM)
    out = pl.pallas_call(
        state_kernel,
        name='states',
        out_shape=jax.ShapeDtypeStruct((n_dev, per_dev, dim, 2 * dim), BF16),
        in_specs=[vmem] * 7,
        out_specs=vmem,
        scratch_shapes=[
            pltpu.VMEM((n_dev, per_dev, dim + 8, 2 * dim), F32),
            pltpu.VMEM((n_dev, per_dev, dim + 8, 2 * dim), F32),
            pltpu.VMEM((n_dev, per_dev, dim, 2 * dim), BF16),
            pltpu.SemaphoreType.DMA((n_dev,)),
            pltpu.SemaphoreType.DMA((n_dev,)),
            pltpu.SemaphoreType.DMA((n_dev,)),
            pltpu.SemaphoreType.DMA((n_dev,)),
        ],
        compiler_params=pltpu.CompilerParams(collective_id=0, has_side_effects=True, vmem_limit_bytes=32 * 1024 * 1024),
        cost_estimate=pl.CostEstimate(flops=40 * 10**9, bytes_accessed=8 * width * tok, transcendentals=0),
    )(qt, kt, vt, dot_t, head[None, :], tail[None, :], jnp.broadcast_to(gate, (8, 2 * dim)))
    return out.reshape(n_heads, dim, 2 * dim)


def attention_kernel(scale, dim, seg_col_ref, seg_row_ref, head_ref, tail_ref, q_ref, k_ref, v_ref, do_ref, st_ref, g_ref):
    tok = q_ref.shape[1]
    half = tok // 2
    seg_row = seg_row_ref[...]
    t_pos = lax.broadcasted_iota(jnp.int32, (half, tok), 0)
    s_pos = lax.broadcasted_iota(jnp.int32, (half, tok), 1)
    see_top = ((seg_col_ref[0:half, :] == seg_row) & (s_pos <= t_pos))[:, 0:half]
    see_low = (seg_col_ref[half:tok, :] == seg_row) & (s_pos <= t_pos + half)
    head = head_ref[...] > 0.5
    tail = tail_ref[...] > 0.5
    zero = jnp.zeros((dim, tok), BF16)

    for sub in range(q_ref.shape[0] // dim):
        rows = slice(sub * dim, (sub + 1) * dim)
        q, k, v, do = q_ref[rows, :], k_ref[rows, :], v_ref[rows, :], do_ref[rows, :]
        st = st_ref[sub]

        def pair(a, b):
            top = dot(a[:, 0:half], b[:, 0:half], ((0,), (0,)))
            low = dot(a[:, half:tok], b, ((0,), (0,)))
            return (jnp.where(see_top, top * scale, 0.0).astype(BF16), jnp.where(see_low, low * scale, 0.0).astype(BF16))

        def over_keys(rows_t, probs):
            top, low = probs
            return jnp.concatenate([dot(rows_t[:, 0:half], top, ((1,), (1,))), dot(rows_t, low, ((1,), (1,)))], axis=1)

        def over_queries(rows_t, probs):
            top, low = probs
            from_low = dot(rows_t[:, half:tok], low, ((1,), (0,)))
            first = dot(rows_t[:, 0:half], top, ((1,), (0,))) + from_low[:, 0:half]
            return jnp.concatenate([first, from_low[:, half:tok]], axis=1)

        probs = pair(q, k)
        d_probs = pair(do, v)
        from_q = dot(st, q, ((0,), (0,)))
        from_k = dot(st, k, ((0,), (0,)))
        o_inter = from_q[0:dim]
        dv_inter = from_k[dim:2 * dim]
        dq_inter = dot(st, jnp.concatenate([do, zero], axis=0), ((1,), (0,)))
        dk_inter = dot(st, jnp.concatenate([zero, v], axis=0), ((1,), (0,)))
        g_ref[0, rows, :] = (over_keys(k, d_probs) + jnp.where(head, dq_inter * scale, 0.0)).astype(BF16)
        g_ref[1, rows, :] = (over_queries(q, d_probs) + jnp.where(tail, dk_inter * scale, 0.0)).astype(BF16)
        g_ref[2, rows, :] = (over_queries(do, probs) + jnp.where(tail, dv_inter * scale, 0.0)).astype(BF16)
        g_ref[3, rows, :] = (over_keys(v, probs) + jnp.where(head, o_inter * scale, 0.0)).astype(BF16)


def attention(qt, kt, vt, dot_t, st, seg_ids, head, tail, scale, n_heads):
    width, tok = qt.shape
    dim = width // n_heads
    group = width // (CORES * RING)
    rows = pl.BlockSpec((group, tok), lambda g: (g, 0))
    whole = lambda shape: pl.BlockSpec(shape, lambda g: (0,) * len(shape))
    return pl.pallas_call(
        functools.partial(attention_kernel, scale, dim),
        name='attention',
        grid=(width // group,),
        out_shape=jax.ShapeDtypeStruct((TYPES, width, tok), BF16),
        in_specs=[whole((tok, 1)), whole((1, tok)), whole((1, tok)), whole((1, tok)), rows, rows, rows, rows,
                  pl.BlockSpec((group // dim, dim, 2 * dim), lambda g: (g, 0, 0))],
        out_specs=pl.BlockSpec((TYPES, group, tok), lambda g: (0, g, 0)),
        compiler_params=pltpu.CompilerParams(vmem_limit_bytes=40 * 1024 * 1024),
        cost_estimate=pl.CostEstimate(flops=12 * width * tok * tok * 4, bytes_accessed=16 * width * tok, transcendentals=0),
    )(seg_ids[:, None], seg_ids[None, :], head[None, :], tail[None, :], qt, kt, vt, dot_t, st)


ORDER = (2, 1, 3, 0)


def reduce_kernel(g_ref, *refs):
    z_refs = refs[:2 * RING]
    (out_ref, zbuf, rows_in, stage, a_out, a_in, b_out, b_in, z_sem,
     far_send, stage_sem, half_send, row_send, row_recv, half_recv, a_send, a_recv, b_send, b_recv) = refs[2 * RING:]
    me = lax.axis_index('sp')
    x, y, core = place(me)
    block = rows_in.shape[2]
    part = block // 2
    n_col, cols = a_out.shape[0], a_out.shape[3]

    meet([index_of(x, y, 1 - core)]
         + [index_of(x + dx, y + dy, other) for dx, dy in ((1, 0), (3, 0), (0, 1), (0, 3)) for other in range(CORES)])

    for i in range(2 * RING):
        pltpu.make_async_copy(z_refs[i], zbuf.at[i], z_sem.at[i]).start()

    def ring_of(ring):
        along, across = (x, y) if ring == 0 else (y, x)
        peer = (lambda step, owner_core: index_of(x + step, y, owner_core)) if ring == 0 else (
            lambda step, owner_core: index_of(x, y + step, owner_core))
        return along, across, peer, lax.rem(core + ring, CORES)

    def source(ring, bi, step):
        along, across, _, _ = ring_of(ring)
        kind = lax.rem(along + step, RING)
        first = (ring * RING + lax.rem(across + ORDER[bi], RING)) * block
        return kind, pl.multiple_of(first, block)

    def near_copy(ring, bi, step):
        _, _, peer, flip = ring_of(ring)
        kind, first = source(ring, bi, step)
        slot = 2 * step + flip
        return remote(g_ref.at[kind, pl.ds(first, block)], rows_in.at[slot, bi], row_send.at[ring, bi, step],
                      row_recv.at[slot, bi], peer(step, ring))

    def far_copy(ring, bi, way):
        _, _, peer, _ = ring_of(ring)
        kind, first = source(ring, bi, 2)
        return remote(g_ref.at[kind, pl.ds(pl.multiple_of(first + way * part, part), part)], stage.at[ring, bi, way],
                      far_send.at[ring, bi, way], stage_sem.at[ring, bi, way], peer((1, 3)[way], core))

    def pass_copy(ring, bi, way):
        _, _, peer, flip = ring_of(ring)
        return remote(stage.at[ring, bi, way], rows_in.at[4 + flip, bi, pl.ds(way * part, part)],
                      half_send.at[ring, bi, way], half_recv.at[flip, bi, way], peer((1, 3)[way], ring))

    for bi in range(RING):
        for ring in range(2):
            for way in range(2):
                far_copy(ring, bi, way).start()
            near_copy(ring, bi, 1).start()
            near_copy(ring, bi, 3).start()

            @pl.when(core != ring)
            def _(ring=ring, bi=bi):
                near_copy(ring, bi, 0).start()

            @pl.when(core == ring)
            def _(ring=ring, bi=bi):
                kind, first = source(ring, bi, 0)
                pltpu.make_async_copy(g_ref.at[kind, pl.ds(first, block)], rows_in.at[0, bi], row_recv.at[0, bi]).start()

    def pass_on(bi):
        for ring in range(2):
            for way in range(2):
                far_copy(ring, bi, way).wait_recv()
                pass_copy(ring, bi, way).start()

    def arrived(bi):
        for slot in (0, 1, 2, 3, 6, 7):
            pltpu.make_async_copy(g_ref.at[0, pl.ds(0, block)], rows_in.at[slot, bi], row_recv.at[slot, bi]).wait()
        for flip in range(CORES):
            for way in range(2):
                half = rows_in.at[4 + flip, bi, pl.ds(way * part, part)]
                pltpu.make_async_copy(g_ref.at[0, pl.ds(0, part)], half, half_recv.at[flip, bi, way]).wait()

    def product(bi, ch):
        at = pl.ds(pl.multiple_of(ch * cols, cols), cols)
        total = dot(rows_in[0, bi], zbuf[0, :, at], ((1,), (0,)))
        for slot in range(1, 2 * RING):
            total = total + dot(rows_in[slot, bi], zbuf[slot, :, at], ((1,), (0,)))
        return total

    across_peer = [jnp.where(core == 0, index_of(x, y + step, core), index_of(x + step, y, core)) for step in (1, 3)]

    def a_copy(ch, way):
        return remote(a_out.at[ch, way], a_in.at[ch, way], a_send.at[ch, way], a_recv.at[ch, way], across_peer[way])

    def b_copy(ch, way):
        return remote(b_out.at[ch, way], b_in.at[ch, way], b_send.at[ch, way], b_recv.at[ch, way], across_peer[way])

    pass_on(0)
    pass_on(1)
    for i in range(2 * RING):
        pltpu.make_async_copy(z_refs[i], zbuf.at[i], z_sem.at[i]).wait()
    arrived(0)

    @pl.loop(0, n_col)
    def _(ch):
        total = product(0, ch)
        a_out[ch, 0] = total[0:part]
        a_out[ch, 1] = total[part:block]
        a_copy(ch, 0).start()
        a_copy(ch, 1).start()

    pass_on(2)
    arrived(1)

    @pl.loop(0, n_col)
    def _(ch):
        total = product(1, ch)
        a_copy(ch, 0).wait_recv()
        b_out[ch, 0, 0:part] = total[0:part] + a_in[ch, 0]
        b_out[ch, 0, part:block] = total[part:block]
        b_copy(ch, 0).start()

    pass_on(3)
    arrived(2)

    @pl.loop(0, n_col)
    def _(ch):
        total = product(2, ch)
        a_copy(ch, 1).wait_recv()
        b_out[ch, 1, 0:part] = total[0:part]
        b_out[ch, 1, part:block] = total[part:block] + a_in[ch, 1]
        b_copy(ch, 1).start()

    arrived(3)

    @pl.loop(0, n_col)
    def _(ch):
        total = product(3, ch)
        b_copy(ch, 0).wait_recv()
        b_copy(ch, 1).wait_recv()
        out_ref[:, pl.ds(pl.multiple_of(ch * cols, cols), cols)] = total + b_in[ch, 0] + b_in[ch, 1]

    for bi in range(RING):
        for ring in range(2):
            for way in range(2):
                far_copy(ring, bi, way).wait_send()
                pass_copy(ring, bi, way).wait_send()
            near_copy(ring, bi, 1).wait_send()
            near_copy(ring, bi, 3).wait_send()

            @pl.when(core != ring)
            def _(ring=ring, bi=bi):
                near_copy(ring, bi, 0).wait_send()

    for ch in range(n_col):
        for way in range(2):
            a_copy(ch, way).wait_send()
            b_copy(ch, way).wait_send()


def reduce_rows(g, zs):
    width, tok = g.shape[1], g.shape[2]
    d_model = zs[0].shape[1]
    block = width // (CORES * RING)
    n_col = 4
    cols = d_model // n_col
    anywhere = pl.BlockSpec(memory_space=pl.ANY)
    dma = pltpu.SemaphoreType.DMA
    return pl.pallas_call(
        reduce_kernel,
        name='reduce_rows',
        out_shape=pltpu.VMEM((block, d_model), F32),
        in_specs=[anywhere] * (1 + len(zs)),
        out_specs=pl.BlockSpec(memory_space=pltpu.VMEM),
        scratch_shapes=[
            pltpu.VMEM((2 * RING, tok, d_model), BF16),
            pltpu.VMEM((2 * RING, RING, block, tok), BF16),
            pltpu.VMEM((2, RING, 2, block // 2, tok), BF16),
            pltpu.VMEM((n_col, 2, block // 2, cols), F32),
            pltpu.VMEM((n_col, 2, block // 2, cols), F32),
            pltpu.VMEM((n_col, 2, block, cols), F32),
            pltpu.VMEM((n_col, 2, block, cols), F32),
            dma((2 * RING,)),
            dma((2, RING, 2)), dma((2, RING, 2)), dma((2, RING, 2)),
            dma((2, RING, RING)), dma((2 * RING, RING)), dma((CORES, RING, 2)),
            dma((n_col, 2)), dma((n_col, 2)), dma((n_col, 2)), dma((n_col, 2)),
        ],
        compiler_params=pltpu.CompilerParams(collective_id=1, has_side_effects=True, vmem_limit_bytes=REDUCE_LIMIT),
        cost_estimate=pl.CostEstimate(flops=200 * 10**9, bytes_accessed=100 * 10**6, transcendentals=0),
    )(g, *zs)


def row_products(g_ref, w_refs, y_ref, dx_ref, rows_in, rows_t, w_tile, total, g_sem, w_sem):
    width = rows_in.shape[1]
    cols = w_tile.shape[2]
    n_tile = total.shape[1] // cols
    step = width // 8
    order = (O_TYPE, 0, 1, 2)

    def g_copy(i):
        return pltpu.make_async_copy(g_ref.at[order[i]], rows_in.at[i % 2], g_sem.at[i % 2])

    def w_copy(i, n, slot):
        at = pl.ds(pl.multiple_of(n * cols, cols), cols)
        return pltpu.make_async_copy(w_refs[order[i]].at[:, at], w_tile.at[slot], w_sem.at[slot])

    g_copy(0).start()
    w_copy(0, 0, 0).start()
    for i in range(TYPES):
        if i + 1 < TYPES:
            g_copy(i + 1).start()
        g_copy(i).wait()

        @pl.loop(0, width // step)
        def _(b):
            at = pl.ds(pl.multiple_of(b * step, step), step)
            rows_t[:, at] = jnp.transpose(rows_in[i % 2, at, :])

        @pl.loop(0, n_tile)
        def _(n):
            slot = lax.rem(n, 2)

            @pl.when(n + 1 < n_tile)
            def _():
                w_copy(i, n + 1, 1 - slot).start()

            if i + 1 < TYPES:
                @pl.when(n + 1 == n_tile)
                def _():
                    w_copy(i + 1, 0, 0).start()

            w_copy(i, n, slot).wait()
            at = pl.ds(pl.multiple_of(n * cols, cols), cols)
            prod = dot(rows_t[...], w_tile[slot], ((1,), (0,)))
            if i == 0:
                y_ref[:, at] = prod.astype(BF16)
            elif i == 1:
                total[:, at] = prod
            elif i == 2:
                total[:, at] = total[:, at] + prod
            else:
                dx_ref[:, at] = (total[:, at] + prod).astype(BF16)


def gather_kernel(piece_ref, g_ref, wq_ref, wk_ref, wv_ref, wo_ref, near_ref, far_ref, y_ref, dx_ref,
                  rows_in, rows_t, w_tile, total, g_sem, w_sem, send_sem, recv_sem, side_send, side_recv):
    me = lax.axis_index('sp')
    x, y, core = place(me)
    rows = piece_ref.shape[0]
    part = rows // 2
    quarter = part // 2

    def base(sx, sy):
        px, py = lax.rem(x + sx, RING), lax.rem(y + sy, RING)
        kind = jnp.where(core == 0, px, py)
        slot = jnp.where(core == 0, py, px)
        return (kind * RING + slot) * rows

    def spot(leg, i, j, half=None, ref=near_ref):
        sx, sy = (i, j) if leg == 0 else (j, i)
        lo, size = (0, part) if half is None else (half * quarter, quarter)
        return ref.at[pl.ds(pl.multiple_of(base(sx, sy) + leg * part + lo, quarter), size)]

    def own(leg, half=None):
        lo, size = (0, part) if half is None else (half * quarter, quarter)
        return piece_ref.at[pl.ds(leg * part + lo, size)]

    def step_peer(leg, second, step):
        along_x = (leg == 0) != second
        return index_of(x + step, y, core) if along_x else index_of(x, y + step, core)

    started = []

    def push(leg, second, i, j, step, half):
        there = (i, (j - step) % RING) if second else ((i - step) % RING, j)
        src = own(leg, half) if i == 0 and j == 0 else spot(leg, i, j, half)
        copy = remote(src, spot(leg, i, j, half), send_sem.at[len(started)],
                      recv_sem.at[leg, there[0], there[1], half or 0], step_peer(leg, second, step))
        copy.start()
        started.append(copy)

    def landed(leg, i, j):
        in_halves = j == 2 or (j == 0 and i == 2)
        for half in ((0, 1) if in_halves else (None,)):
            here = spot(leg, i, j, half)
            remote(here, here, send_sem.at[0], recv_sem.at[leg, i, j, half or 0], me).wait_recv()

    side = []

    def to_sibling(leg, i, j):
        src = own(leg) if i == 0 and j == 0 else spot(leg, i, j)
        copy = remote(src, spot(leg, i, j, None, far_ref), side_send.at[leg, i, j], side_recv.at[leg, i, j],
                      index_of(x, y, 1 - core))
        copy.start()
        side.append(copy)

    meet([index_of(x, y, 1 - core)] + [index_of(x + dx, y + dy, core) for dx, dy in ((1, 0), (3, 0), (0, 1), (0, 3))])

    def spread(leg, i):
        push(leg, True, i, 0, 1, None)
        push(leg, True, i, 0, 3, None)
        to_sibling(leg, i, 0)

    for leg in range(2):
        push(leg, False, 0, 0, 1, None)
        push(leg, False, 0, 0, 3, None)
    for leg in range(2):
        spread(leg, 0)
    near_ref[pl.ds(pl.multiple_of(base(0, 0), rows), rows), :] = piece_ref[...]
    row_products(g_ref, (wq_ref, wk_ref, wv_ref, wo_ref), y_ref, dx_ref, rows_in, rows_t, w_tile, total, g_sem, w_sem)

    for leg in range(2):
        landed(leg, 3, 0)
        push(leg, False, 3, 0, 1, 0)
        spread(leg, 3)
        landed(leg, 1, 0)
        push(leg, False, 1, 0, 3, 1)
        spread(leg, 1)

    def second_near(leg, i):
        landed(leg, i, 3)
        push(leg, True, i, 3, 1, 0)
        to_sibling(leg, i, 3)
        landed(leg, i, 1)
        push(leg, True, i, 1, 3, 1)
        to_sibling(leg, i, 1)

    for leg in range(2):
        second_near(leg, 0)
    for leg in range(2):
        landed(leg, 2, 0)
        spread(leg, 2)
    for i in (3, 1, 2):
        for leg in range(2):
            second_near(leg, i)
    for i in (0, 3, 1, 2):
        for leg in range(2):
            landed(leg, i, 2)
            to_sibling(leg, i, 2)

    for copy in started + side:
        copy.wait_send()

    def side_spot(leg, i, j):
        sx, sy = (i, j) if leg == 0 else (j, i)
        px, py = lax.rem(x + sx, RING), lax.rem(y + sy, RING)
        kind = jnp.where(core == 0, py, px)
        slot = jnp.where(core == 0, px, py)
        return far_ref.at[pl.ds(pl.multiple_of((kind * RING + slot) * rows + leg * part, part), part)]

    for leg in range(2):
        for i in range(RING):
            for j in range(RING):
                here = side_spot(leg, i, j)
                remote(here, here, side_send.at[leg, i, j], side_recv.at[leg, i, j], me).wait_recv()


def gather_rows(piece, g, weights, n_dev):
    rows, d_model = piece.shape
    width, tok = g.shape[1], g.shape[2]
    half = n_dev * rows // CORES
    cols = min(256, d_model // 2)
    dma = pltpu.SemaphoreType.DMA
    vmem = pl.BlockSpec(memory_space=pltpu.VMEM)
    anywhere = pl.BlockSpec(memory_space=pl.ANY)
    return pl.pallas_call(
        gather_kernel,
        name='gather_rows',
        out_shape=(pltpu.VMEM((half, d_model), F32), jax.ShapeDtypeStruct((half, d_model), F32),
                   pltpu.VMEM((tok, d_model), BF16), pltpu.VMEM((tok, d_model), BF16)),
        in_specs=[vmem] + [anywhere] * 5,
        out_specs=(vmem, anywhere, vmem, vmem),
        scratch_shapes=[pltpu.VMEM((2, width, tok), BF16), pltpu.VMEM((tok, width), BF16), pltpu.VMEM((2, width, cols), BF16),
                        pltpu.VMEM((tok, d_model), F32), dma((2,)), dma((2,)),
                        dma((40,)), dma((2, RING, RING, 2)), dma((2, RING, RING)), dma((2, RING, RING))],
        compiler_params=pltpu.CompilerParams(collective_id=2, has_side_effects=True, vmem_limit_bytes=20 * 1024 * 1024),
        cost_estimate=pl.CostEstimate(flops=700 * 10**9, bytes_accessed=128 * 10**6, transcendentals=0),
    )(piece, g, *weights)


def store_kernel(near_ref, far_ref, y_ref, dx_ref, y_out, dx_out, dq_out, dk_out, dv_out, do_out, tile, put_sem, in_sem, out_sem):
    core = lax.rem(lax.axis_index('sp'), CORES)
    outs = (dq_out, dk_out, dv_out, do_out)
    rows = near_ref.shape[0] // TYPES
    n_slot, chunk = tile.shape[0], tile.shape[1]
    per_type = rows // chunk
    n = TYPES * per_type
    puts = [pltpu.make_async_copy(y_ref, y_out, put_sem.at[TYPES]), pltpu.make_async_copy(dx_ref, dx_out, put_sem.at[TYPES + 1])]
    for kind in range(TYPES):
        puts.append(pltpu.make_async_copy(near_ref.at[pl.ds(kind * rows, rows)],
                                          outs[kind].at[pl.ds(pl.multiple_of(core * rows, rows), rows)], put_sem.at[kind]))

    def load(i):
        return pltpu.make_async_copy(far_ref.at[pl.ds(i * chunk, chunk)], tile.at[i % n_slot], in_sem.at[i % n_slot])

    def save(i):
        at = pl.multiple_of((1 - core) * rows + (i % per_type) * chunk, chunk)
        return pltpu.make_async_copy(tile.at[i % n_slot], outs[i // per_type].at[pl.ds(at, chunk)], out_sem.at[i % n_slot])

    ahead = n_slot // 2
    for i in range(ahead):
        load(i).start()
    for put in puts:
        put.start()
    for i in range(n):
        load(i).wait()
        save(i).start()
        if i + ahead < n:
            if i + ahead >= n_slot:
                save(i + ahead - n_slot).wait()
            load(i + ahead).start()
    for i in range(max(0, n - n_slot), n):
        save(i).wait()
    for put in puts:
        put.wait()


def store(near, far, y_rows, dx_rows):
    half, d_model = near.shape
    chunk = half // 32
    vmem = pl.BlockSpec(memory_space=pltpu.VMEM)
    anywhere = pl.BlockSpec(memory_space=pl.ANY)
    dma = pltpu.SemaphoreType.DMA
    grad = jax.ShapeDtypeStruct((half * CORES // TYPES, d_model), F32)
    return pl.pallas_call(
        store_kernel,
        name='store',
        out_shape=(jax.ShapeDtypeStruct(y_rows.shape, BF16), jax.ShapeDtypeStruct(dx_rows.shape, BF16), grad, grad, grad, grad),
        in_specs=[vmem, anywhere, vmem, vmem],
        out_specs=(anywhere,) * 6,
        scratch_shapes=[pltpu.VMEM((8, chunk, d_model), F32), dma((TYPES + 2,)), dma((8,)), dma((8,))],
        compiler_params=pltpu.CompilerParams(vmem_limit_bytes=16 * 1024 * 1024),
        cost_estimate=pl.CostEstimate(flops=10**9, bytes_accessed=100 * 10**6, transcendentals=0),
    )(near, far, y_rows, dx_rows)


def solution(mesh):
    n_dev = mesh.shape['sp']
    assert n_dev == CORES * RING * RING

    def token_operand(x_loc, dy_loc, step, flip):
        x, y, core = place(lax.axis_index('sp'))
        owner = lax.rem(core + flip, CORES)
        kind = lax.rem(jnp.where(owner == 0, x, y) + step, RING)
        load = jnp.where(kind == O_TYPE, dy_loc, x_loc)
        if not step and not flip:
            return load
        pairs = []
        for src in range(n_dev):
            sx, sy, sc = (src // CORES) % RING, src // (CORES * RING), src % CORES
            oc = (sc + flip) % CORES
            ox, oy = ((sx + step) % RING, sy) if oc == 0 else (sx, (sy + step) % RING)
            pairs.append((src, (oy * RING + ox) * CORES + oc))
        return lax.ppermute(load, 'sp', pairs)

    def device_program(x_loc, flag_loc, w_q, w_k, w_v, w_o, dy_loc):
        tok_count, d_model = x_loc.shape
        n_heads, head_dim = w_q.shape[1], w_q.shape[2]
        width = n_heads * head_dim
        score_scale = 1.0 / (math.sqrt(head_dim) * tok_count)
        seg_ids, head, tail, doc_gate = block_masks(flag_loc)
        slots = [(step, flip) for step in range(RING) for flip in range(CORES)]
        early = [slot for slot in slots if slot[1] == 0 or slot[0] == 0]
        zs = {slot: token_operand(x_loc, dy_loc, *slot) for slot in early}

        def flat(w):
            return w.transpose(1, 2, 0).reshape(width, d_model)

        wq, wk, wv, wo = flat(w_q), flat(w_k), flat(w_v), w_o.reshape(width, d_model)

        def project(w, rows):
            return jnp.einsum('nd,td->nt', w, rows, preferred_element_type=F32).astype(BF16)

        qt, kt, vt = project(wq, x_loc), project(wk, x_loc), project(wv, x_loc)
        dot_t = project(wo, dy_loc)
        st = states(qt, kt, vt, dot_t, head, tail, doc_gate, n_dev, n_heads)
        late_x, late_dy, st = lax.optimization_barrier((x_loc, dy_loc, st))
        zs.update({slot: token_operand(late_x, late_dy, *slot) for slot in slots if slot not in early})
        g = attention(qt, kt, vt, dot_t, st, seg_ids, head, tail, score_scale, n_heads)
        piece = reduce_rows(g, [zs[slot] for slot in slots])
        near, far, y_rows, dx_rows = gather_rows(piece, g, (wq, wk, wv, wo), n_dev)
        y_loc, dx_loc, *grads = store(near, far, y_rows, dx_rows)
        grads = [grad.reshape(n_heads, head_dim, d_model) for grad in grads]
        dw_q, dw_k, dw_v = (grads[i].transpose(2, 0, 1) for i in range(3))
        return y_loc, dx_loc, dw_q, dw_k, dw_v, grads[O_TYPE]

    row_spec = P(('dp', 'sp'), None)
    flag_spec = P(('dp', 'sp'))
    w_spec = P(None, None, None)
    dw_spec = P('dp', None, None)
    return jax.shard_map(device_program, mesh=mesh,
                         in_specs=(row_spec, flag_spec, w_spec, w_spec, w_spec, w_spec, row_spec),
                         out_specs=(row_spec, row_spec, dw_spec, dw_spec, dw_spec, dw_spec),
                         check_vma=False)
```

```python
import functools
import math
import jax
import jax.numpy as jnp
from jax import lax
from jax.experimental import pallas as pl
from jax.experimental.pallas import tpu as pltpu
from jax.sharding import PartitionSpec as P

MESH = pl.DeviceIdType.MESH
CORES = 2
RING = 4
SLOTS = CORES * RING
TYPES = 4
O_TYPE = TYPES - 1
MIB = 1024 * 1024
BF16 = jnp.bfloat16
F32 = jnp.float32
ROWS = ((1,), (1,))
INNER = ((1,), (0,))
OUTER = ((0,), (0,))
VMEM = pl.BlockSpec(memory_space=pltpu.VMEM)
ANY = pl.BlockSpec(memory_space=pl.ANY)
DMA = pltpu.SemaphoreType.DMA


def place(me):
    core = lax.rem(me, CORES)
    chip = me // CORES
    return lax.rem(chip, RING), chip // RING, core


def index_of(x, y, core):
    return (lax.rem(y, RING) * RING + lax.rem(x, RING)) * CORES + core


def remote(src, dst, send_sem, recv_sem, peer):
    return pltpu.make_async_remote_copy(src_ref=src, dst_ref=dst, send_sem=send_sem, recv_sem=recv_sem,
                                        device_id={'sp': peer}, device_id_type=MESH)


def signal(peer):
    pl.semaphore_signal(pltpu.get_barrier_semaphore(), inc=1, device_id={'sp': peer}, device_id_type=MESH)


def meet(peers):
    for peer in peers:
        signal(peer)
    pl.semaphore_wait(pltpu.get_barrier_semaphore(), len(peers))


def chips_around(x, y):
    return ((x + 1, y), (x + RING - 1, y), (x, y + 1), (x, y + RING - 1))


def dot(a, b, dims):
    return lax.dot_general(a, b, (dims, ((), ())), preferred_element_type=F32)


def in_vmem(value):
    return pltpu.with_memory_space_constraint(value, pltpu.VMEM)


def span(start, size):
    return pl.ds(pl.multiple_of(start, size), size)


def stream(n_outer, n_inner, copy, use, before=None):
    copy(0, 0, 0).start()
    for i in range(n_outer):
        if before is not None:
            before(i)

        @pl.loop(0, n_inner)
        def _(n):
            slot = lax.rem(n, 2)

            @pl.when(n + 1 < n_inner)
            def _():
                copy(i, n + 1, 1 - slot).start()

            if i + 1 < n_outer:
                @pl.when(n + 1 == n_inner)
                def _():
                    copy(i + 1, 0, 0).start()

            copy(i, n, slot).wait()
            use(i, n, slot)


def block_masks(flag_loc):
    tok_count = flag_loc.shape[0]
    positions = jnp.arange(tok_count)
    seg_ids = jnp.sum(jnp.where(positions[None, :] <= positions[:, None], flag_loc[None, :], 0), axis=1)
    first_pos = jnp.min(jnp.where(flag_loc > 0, positions, tok_count))
    last_pos = jnp.max(jnp.where(flag_loc > 0, positions, -1))
    head = (positions < first_pos).astype(F32)
    tail = (positions >= last_pos).astype(F32)
    doc_gate = (last_pos < 0).astype(F32)
    return seg_ids, head, tail, doc_gate


class Ring:
    def __init__(self, ring, me):
        x, y, core = place(me)
        self.ring = ring
        self.along, self.across = (x, y) if ring == 0 else (y, x)
        self.flip = lax.rem(core + ring, CORES)
        self.peer = lambda step: index_of(x + step, y, ring) if ring == 0 else index_of(x, y + step, ring)

    def kind(self, step):
        return lax.rem(self.along + step, RING)


def start_tokens(ring, step, x_ref, dy_ref, copy):
    kind = ring.kind(step)

    @pl.when(kind == O_TYPE)
    def _():
        copy(dy_ref).start()

    @pl.when(kind != O_TYPE)
    def _():
        copy(x_ref).start()


def front_kernel(scale, dim, seg_col_ref, seg_row_ref, head_ref, tail_ref, gate_ref, x_ref, dy_ref, wq_ref, wk_ref, wv_ref, wo_ref,
                 g_ref, z_ref, tok_in, w_tile, rows_ref, total, packed, held, formed, states,
                 tok_sem, w_sem, g_sem, z_send, z_recv, side_sem, send_sem, recv_sem, back_send, back_recv):
    me = lax.axis_index('sp')
    _, _, core = place(me)
    n_dev, per_dev = packed.shape[0], packed.shape[1]
    width, tok = rows_ref.shape[1], rows_ref.shape[2]
    half = tok // 2
    n_piece = z_recv.shape[1]
    piece = tok // n_piece
    n_group = SLOTS
    group = width // n_group
    tile_rows = w_tile.shape[1]

    @pl.loop(1, n_dev)
    def _(step):
        signal(lax.rem(me + step, n_dev))

    loads = [pltpu.make_async_copy(ref, tok_in.at[i], tok_sem.at[i]) for i, ref in enumerate((x_ref, dy_ref))]
    for load in loads:
        load.start()

    rings = [Ring(ring, me) for ring in range(CORES)]
    near_steps = (1, RING - 1)

    def token_copy(ring, step, n):
        slot = CORES * step + ring.flip
        at = pl.ds(n * piece, piece)
        return lambda ref: remote(ref.at[at], z_ref.at[slot, at], z_send.at[ring.ring, step // 2, n], z_recv.at[slot, n], ring.peer(step))

    def push_tokens(lo, hi):
        for n in range(lo, hi):
            for ring in rings:
                for step in near_steps:
                    start_tokens(ring, step, x_ref, dy_ref, token_copy(ring, step, n))

    def sibling_copy(ring):
        return lambda ref: remote(ref, z_ref.at[1], side_sem.at[0], side_sem.at[1], ring.peer(0))

    pl.semaphore_wait(pltpu.get_barrier_semaphore(), n_dev - 1)
    push_tokens(0, n_piece // 2)
    for ring in rings:
        @pl.when(ring.flip == 1)
        def _(ring=ring):
            start_tokens(ring, 0, x_ref, dy_ref, sibling_copy(ring))

    weights = (wk_ref, wv_ref, wq_ref, wo_ref)
    kinds = (1, 2, 0, O_TYPE)

    def w_copy(i, n, slot):
        return pltpu.make_async_copy(weights[i].at[span(n * tile_rows, tile_rows)], w_tile.at[slot], w_sem.at[slot])

    def project(i, n, slot):
        rows_ref[kinds[i], span(n * tile_rows, tile_rows), :] = dot(w_tile[slot], tok_in[i // O_TYPE], ROWS).astype(BF16)

    def loaded(i):
        if i in (0, O_TYPE):
            loads[i // O_TYPE].wait()

    stream(TYPES, width // tile_rows, w_copy, project, loaded)

    head = head_ref[...] > 0.5
    tail = tail_ref[...] > 0.5
    zero = jnp.zeros((dim, tok), BF16)

    @pl.loop(0, n_dev)
    def _(dev):
        for sub in range(per_dev):
            rows = span((dev * per_dev + sub) * dim, dim)
            v_tail = jnp.concatenate([jnp.where(tail, rows_ref[2, rows, :], zero), zero], axis=0)
            do_head = jnp.concatenate([zero, jnp.where(head, rows_ref[O_TYPE, rows, :], zero)], axis=0)
            packed[dev, sub, 0:dim, :] = dot(rows_ref[1, rows, :], v_tail, ROWS) + dot(rows_ref[0, rows, :], do_head, ROWS)
            packed[dev, sub, dim:, :] = gate_ref[...]

    def out_copy(step):
        peer = lax.rem(me + step, n_dev)
        return remote(packed.at[peer], held.at[me], send_sem.at[step], recv_sem.at[step], peer)

    def back_copy(step):
        peer = lax.rem(me + step, n_dev)
        return remote(formed.at[peer], states.at[me], back_send.at[step], back_recv.at[step], peer)

    def each(do):
        pl.loop(1, n_dev)(do)

    each(lambda step: out_copy(step).start())
    held[me] = packed[me]
    push_tokens(n_piece // 2, n_piece - n_piece // 4)

    def form_states():
        each(lambda step: out_copy(step).wait_recv())
        shape = (per_dev, dim, 2 * dim)
        lane = lax.broadcasted_iota(jnp.int32, shape, 2)
        start = jnp.zeros(shape, F32)

        def advance(block, state):
            return held[block, :, dim:dim + 1, :] * state + held[block, :, 0:dim, :]

        def forward(block, state):
            formed[block] = state.astype(BF16)
            return advance(block, state)

        def backward(step, state):
            block = n_dev - 1 - step
            formed[block] = jnp.where(lane < dim, formed[block].astype(F32), state).astype(BF16)
            return advance(block, state)

        lax.fori_loop(0, n_dev, forward, start)
        lax.fori_loop(0, n_dev, backward, start)
        each(lambda step: back_copy(step).start())
        states[me] = formed[me]
        push_tokens(n_piece - n_piece // 4, n_piece)

    seg_row = seg_row_ref[...]
    t_pos = lax.broadcasted_iota(jnp.int32, (half, tok), 0)
    s_pos = lax.broadcasted_iota(jnp.int32, (half, tok), 1)

    def pair(a, b):
        see_top = ((seg_col_ref[0:half, :] == seg_row) & (s_pos <= t_pos))[:, 0:half]
        see_low = (seg_col_ref[half:, :] == seg_row) & (s_pos <= t_pos + half)
        top = dot(a[:, 0:half], b[:, 0:half], OUTER)
        low = dot(a[:, half:], b, OUTER)
        return (jnp.where(see_top, top * scale, 0).astype(BF16), jnp.where(see_low, low * scale, 0).astype(BF16))

    def over_keys(at, rows_t, probs):
        total[at[0], at[1], 0:half] = dot(rows_t[:, 0:half], probs[0], ROWS)
        total[at[0], at[1], half:] = dot(rows_t, probs[1], ROWS)

    def over_queries(at, rows_t, probs):
        from_low = dot(rows_t[:, half:], probs[1], INNER)
        total[at[0], at[1], 0:half] = dot(rows_t[:, 0:half], probs[0], INNER) + from_low[:, 0:half]
        total[at[0], at[1], half:] = from_low[:, half:]

    def heads_of(grp):
        return [grp * (group // dim) + sub for sub in range(group // dim)]

    @pl.loop(0, n_group)
    def _(grp):
        @pl.when(grp == n_group - 3)
        def _():
            form_states()

        for index in heads_of(grp):
            rows = span(index * dim, dim)
            q, k, v, do = (rows_ref[kind, rows, :] for kind in range(TYPES))
            d_probs = pair(do, v)
            over_keys((0, rows), k, d_probs)
            over_queries((1, rows), q, d_probs)
            probs = pair(q, k)
            over_queries((2, rows), do, probs)
            over_keys((O_TYPE, rows), v, probs)

    each(lambda step: back_copy(step).wait_recv())

    def g_copy(grp):
        at = span(grp * group, group)
        return pltpu.make_async_copy(rows_ref.at[:, at], g_ref.at[:, at], g_sem.at[grp])

    @pl.loop(0, n_group)
    def _(grp):
        for index in heads_of(grp):
            rows = span(index * dim, dim)
            q, k, v, do = (rows_ref[kind, rows, :] for kind in range(TYPES))
            st = states[index // per_dev, lax.rem(index, per_dev)]
            d_q = dot(st, jnp.concatenate([do, zero], axis=0), INNER)
            d_k = dot(st, jnp.concatenate([zero, v], axis=0), INNER)
            d_v = dot(st, k, OUTER)[dim:]
            out = dot(st, q, OUTER)[0:dim]
            for kind, mask, inter in ((0, head, d_q), (1, tail, d_k), (2, tail, d_v), (O_TYPE, head, out)):
                rows_ref[kind, rows, :] = (total[kind, rows, :] + jnp.where(mask, inter * scale, 0)).astype(BF16)
        g_copy(grp).start()

    pl.loop(0, n_group)(lambda grp: g_copy(grp).wait())
    each(lambda step: out_copy(step).wait_send())
    each(lambda step: back_copy(step).wait_send())
    for ring in rings:
        for step in near_steps:
            for n in range(n_piece):
                token_copy(ring, step, n)(x_ref).wait_send()
    for step in near_steps:
        for flip in range(CORES):
            for n in range(n_piece):
                slot, at = CORES * step + flip, pl.ds(n * piece, piece)
                remote(x_ref.at[at], z_ref.at[slot, at], side_sem.at[0], z_recv.at[slot, n], me).wait_recv()
    sibling_copy(rings[0])(x_ref).wait()


def front(seg_ids, head, tail, gate, x_loc, dy_loc, weights, scale, n_dev, n_heads):
    tok, d_model = x_loc.shape
    width = weights[0].shape[0]
    dim = width // n_heads
    per_dev = n_heads // n_dev
    n_piece = 8
    pack = (n_dev, per_dev, dim + 8, 2 * dim)
    back = (n_dev, per_dev, dim, 2 * dim)
    return pl.pallas_call(
        functools.partial(front_kernel, scale, dim),
        name='front',
        out_shape=(jax.ShapeDtypeStruct((TYPES, width, tok), BF16), jax.ShapeDtypeStruct((SLOTS, tok, d_model), BF16)),
        in_specs=[VMEM] * 5 + [ANY] * 6,
        out_specs=(ANY, ANY),
        scratch_shapes=[
            pltpu.VMEM((2, tok, d_model), BF16), pltpu.VMEM((2, width // RING, d_model), BF16),
            pltpu.VMEM((TYPES, width, tok), BF16), pltpu.VMEM((TYPES, width, tok), F32),
            pltpu.VMEM(pack, F32), pltpu.VMEM(pack, F32), pltpu.VMEM(back, BF16), pltpu.VMEM(back, BF16),
            DMA((2,)), DMA((2,)), DMA((SLOTS,)), DMA((CORES, 2, n_piece)), DMA((SLOTS, n_piece)), DMA((2,)),
            DMA((n_dev,)), DMA((n_dev,)), DMA((n_dev,)), DMA((n_dev,))],
        compiler_params=pltpu.CompilerParams(collective_id=0, has_side_effects=True, vmem_limit_bytes=56 * MIB),
    )(seg_ids[:, None], seg_ids[None, :], head[None, :], tail[None, :], jnp.broadcast_to(gate, (8, 2 * dim)), x_loc, dy_loc, *weights)


def reduce_kernel(g_ref, z_ref, x_ref, dy_ref, out_ref, zbuf, rows_in, a_out, a_in, b_out, b_in,
                  z_sem, far_send, row_send, row_recv, a_send, a_recv, b_send, b_recv):
    me = lax.axis_index('sp')
    x, y, core = place(me)
    block = rows_in.shape[2]
    part = block // 2
    n_col, cols = a_out.shape[0], a_out.shape[3]
    rings = [Ring(ring, me) for ring in range(CORES)]
    order = (2, 1, RING - 1, 0)

    meet([index_of(x, y, 1 - core)] + [index_of(*chip, other) for other in range(CORES) for chip in chips_around(x, y)]
         + [ring.peer(2) + other - ring.ring for other in range(CORES) for ring in rings])

    def far_copy(ring):
        slot = 2 * CORES + ring.flip
        return lambda ref: remote(ref, zbuf.at[slot], far_send.at[ring.ring], z_sem.at[slot], ring.peer(2))

    def own_copy(ref):
        return pltpu.make_async_copy(ref, zbuf.at[0], z_sem.at[0])

    def near_copy(slot):
        return pltpu.make_async_copy(z_ref.at[slot], zbuf.at[slot], z_sem.at[slot])

    near_slots = [slot for slot in range(1, SLOTS) if slot // CORES != 2]
    for ring in rings:
        start_tokens(ring, 2, x_ref, dy_ref, far_copy(ring))
    for ring in rings:
        @pl.when(ring.flip == 0)
        def _(ring=ring):
            start_tokens(ring, 0, x_ref, dy_ref, own_copy)
    for slot in near_slots:
        near_copy(slot).start()

    def row_source(ring, bi, step):
        first = (ring.ring * RING + lax.rem(ring.across + order[bi], RING)) * block
        return g_ref.at[ring.kind(step), span(first, block)]

    def row_copy(ring, bi, step):
        slot = CORES * step + ring.flip
        return remote(row_source(ring, bi, step), rows_in.at[slot, bi], row_send.at[ring.ring, bi, step],
                      row_recv.at[slot, bi], ring.peer(step))

    def own_rows(ring, bi):
        return pltpu.make_async_copy(row_source(ring, bi, 0), rows_in.at[0, bi], row_recv.at[0, bi])

    for bi in range(RING):
        for ring in rings:
            for step in (2, 1, RING - 1):
                row_copy(ring, bi, step).start()

            @pl.when(ring.flip == 1)
            def _(ring=ring, bi=bi):
                row_copy(ring, bi, 0).start()

            @pl.when(ring.flip == 0)
            def _(ring=ring, bi=bi):
                own_rows(ring, bi).start()

    def arrived(bi):
        for slot in range(SLOTS):
            pltpu.make_async_copy(g_ref.at[0, pl.ds(0, block)], rows_in.at[slot, bi], row_recv.at[slot, bi]).wait()

    def product(bi, ch):
        at = span(ch * cols, cols)
        total = dot(rows_in[0, bi], zbuf[0, :, at], INNER)
        for slot in range(1, SLOTS):
            total = total + dot(rows_in[slot, bi], zbuf[slot, :, at], INNER)
        return total

    across = [jnp.where(core == 0, index_of(x, y + step, core), index_of(x + step, y, core)) for step in (1, RING - 1)]

    def a_copy(ch, way):
        return remote(a_out.at[ch, way], a_in.at[ch, way], a_send.at[ch, way], a_recv.at[ch, way], across[way])

    def b_copy(ch, way):
        return remote(b_out.at[ch, way], b_in.at[ch, way], b_send.at[ch, way], b_recv.at[ch, way], across[way])

    own_copy(x_ref).wait()
    for slot in near_slots:
        near_copy(slot).wait()
    for ring in rings:
        far_copy(ring)(x_ref).wait_recv()

    def two_away(ch):
        total = product(0, ch)
        for way in range(2):
            a_out[ch, way] = total[way * part:(way + 1) * part]
            a_copy(ch, way).start()

    def next_to(way, ch):
        total = product(1 + way, ch)
        a_copy(ch, way).wait_recv()
        b_out[ch, way] = total
        b_out[ch, way, pl.ds(way * part, part)] += a_in[ch, way]
        b_copy(ch, way).start()

    def own(ch):
        total = product(RING - 1, ch)
        for way in range(2):
            b_copy(ch, way).wait_recv()
            total = total + b_in[ch, way]
        out_ref[:, span(ch * cols, cols)] = total

    for bi, step in enumerate((two_away, functools.partial(next_to, 0), functools.partial(next_to, 1), own)):
        arrived(bi)
        pl.loop(0, n_col)(step)

    for ring in rings:
        far_copy(ring)(x_ref).wait_send()
        for bi in range(RING):
            for step in range(1, RING):
                row_copy(ring, bi, step).wait_send()

            @pl.when(ring.flip == 1)
            def _(ring=ring, bi=bi):
                row_copy(ring, bi, 0).wait_send()

    for ch in range(n_col):
        for way in range(2):
            a_copy(ch, way).wait_send()
            b_copy(ch, way).wait_send()


def reduce_rows(g, z, x_loc, dy_loc):
    width, tok = g.shape[1], g.shape[2]
    d_model = x_loc.shape[1]
    block = width // SLOTS
    n_col = RING
    part = (n_col, 2, block // 2, d_model // n_col)
    full = (n_col, 2, block, d_model // n_col)
    return pl.pallas_call(
        reduce_kernel,
        name='reduce_rows',
        out_shape=pltpu.VMEM((block, d_model), F32),
        in_specs=[ANY] * 4,
        out_specs=VMEM,
        scratch_shapes=[
            pltpu.VMEM((SLOTS, tok, d_model), BF16), pltpu.VMEM((SLOTS, RING, block, tok), BF16),
            pltpu.VMEM(part, F32), pltpu.VMEM(part, F32), pltpu.VMEM(full, F32), pltpu.VMEM(full, F32),
            DMA((SLOTS,)), DMA((CORES,)), DMA((CORES, RING, RING)), DMA((SLOTS, RING)),
            DMA((n_col, 2)), DMA((n_col, 2)), DMA((n_col, 2)), DMA((n_col, 2))],
        compiler_params=pltpu.CompilerParams(collective_id=1, has_side_effects=True, vmem_limit_bytes=48 * MIB),
    )(g, z, x_loc, dy_loc)


def row_products(g_ref, w_refs, y_ref, dx_ref, rows_in, rows_t, w_tile, total, g_sem, w_sem):
    width = rows_in.shape[1]
    cols = w_tile.shape[2]
    n_tile = total.shape[1] // cols
    step = width // 8
    order = (O_TYPE, 0, 1, 2)

    def g_copy(i):
        return pltpu.make_async_copy(g_ref.at[order[i]], rows_in.at[i % 2], g_sem.at[i % 2])

    def w_copy(i, n, slot):
        at = span(n * cols, cols)
        return pltpu.make_async_copy(w_refs[order[i]].at[:, at], w_tile.at[slot], w_sem.at[slot])

    def turned(i):
        if i + 1 < TYPES:
            g_copy(i + 1).start()
        g_copy(i).wait()

        @pl.loop(0, width // step)
        def _(b):
            at = span(b * step, step)
            rows_t[:, at] = jnp.transpose(rows_in[i % 2, at, :])

    def use(i, n, slot):
        at = span(n * cols, cols)
        prod = dot(rows_t[...], w_tile[slot], INNER)
        if i == 0:
            y_ref[:, at] = prod.astype(BF16)
        elif i == 1:
            total[:, at] = prod
        elif i + 1 < TYPES:
            total[:, at] = total[:, at] + prod
        else:
            dx_ref[:, at] = (total[:, at] + prod).astype(BF16)

    g_copy(0).start()
    stream(TYPES, n_tile, w_copy, use, turned)


def gather_kernel(piece_ref, g_ref, wq_ref, wk_ref, wv_ref, wo_ref, near_ref, far_ref, y_ref, dx_ref,
                  rows_in, rows_t, w_tile, total, g_sem, w_sem, send_sem, recv_sem, side_send, side_recv):
    me = lax.axis_index('sp')
    x, y, core = place(me)
    rows = piece_ref.shape[0]
    part = rows // 2
    quarter = part // 2

    def base(sx, sy):
        px, py = lax.rem(x + sx, RING), lax.rem(y + sy, RING)
        kind = jnp.where(core == 0, px, py)
        slot = jnp.where(core == 0, py, px)
        return (kind * RING + slot) * rows

    def spot(leg, i, j, half=None, ref=near_ref):
        sx, sy = (i, j) if leg == 0 else (j, i)
        lo, size = (0, part) if half is None else (half * quarter, quarter)
        return ref.at[pl.ds(pl.multiple_of(base(sx, sy) + leg * part + lo, quarter), size)]

    def own(leg, half=None):
        lo, size = (0, part) if half is None else (half * quarter, quarter)
        return piece_ref.at[pl.ds(leg * part + lo, size)]

    def step_peer(leg, second, step):
        along_x = (leg == 0) != second
        return index_of(x + step, y, core) if along_x else index_of(x, y + step, core)

    started = []

    def push(leg, second, i, j, step, half):
        there = (i, (j - step) % RING) if second else ((i - step) % RING, j)
        src = own(leg, half) if i == 0 and j == 0 else spot(leg, i, j, half)
        copy = remote(src, spot(leg, i, j, half), send_sem.at[len(started)],
                      recv_sem.at[leg, there[0], there[1], half or 0], step_peer(leg, second, step))
        copy.start()
        started.append(copy)

    def landed(leg, i, j):
        in_halves = j == 2 or (j == 0 and i == 2)
        for half in ((0, 1) if in_halves else (None,)):
            here = spot(leg, i, j, half)
            remote(here, here, send_sem.at[0], recv_sem.at[leg, i, j, half or 0], me).wait_recv()

    side = []

    def to_sibling(leg, i, j):
        src = own(leg) if i == 0 and j == 0 else spot(leg, i, j)
        copy = remote(src, spot(leg, i, j, None, far_ref), side_send.at[leg, i, j], side_recv.at[leg, i, j],
                      index_of(x, y, 1 - core))
        copy.start()
        side.append(copy)

    meet([index_of(x, y, 1 - core)] + [index_of(*chip, core) for chip in chips_around(x, y)])

    def spread(leg, i):
        push(leg, True, i, 0, 1, None)
        push(leg, True, i, 0, 3, None)
        to_sibling(leg, i, 0)

    for leg in range(2):
        push(leg, False, 0, 0, 1, None)
        push(leg, False, 0, 0, 3, None)
    for leg in range(2):
        spread(leg, 0)
    near_ref[pl.ds(pl.multiple_of(base(0, 0), rows), rows), :] = piece_ref[...]
    row_products(g_ref, (wq_ref, wk_ref, wv_ref, wo_ref), y_ref, dx_ref, rows_in, rows_t, w_tile, total, g_sem, w_sem)

    for leg in range(2):
        landed(leg, 3, 0)
        push(leg, False, 3, 0, 1, 0)
        spread(leg, 3)
        landed(leg, 1, 0)
        push(leg, False, 1, 0, 3, 1)
        spread(leg, 1)

    def second_near(leg, i):
        landed(leg, i, 3)
        push(leg, True, i, 3, 1, 0)
        to_sibling(leg, i, 3)
        landed(leg, i, 1)
        push(leg, True, i, 1, 3, 1)
        to_sibling(leg, i, 1)

    for leg in range(2):
        second_near(leg, 0)
    for leg in range(2):
        landed(leg, 2, 0)
        spread(leg, 2)
    for i in (3, 1, 2):
        for leg in range(2):
            second_near(leg, i)
    for i in (0, 3, 1, 2):
        for leg in range(2):
            landed(leg, i, 2)
            to_sibling(leg, i, 2)

    for copy in started + side:
        copy.wait_send()

    def side_spot(leg, i, j):
        sx, sy = (i, j) if leg == 0 else (j, i)
        px, py = lax.rem(x + sx, RING), lax.rem(y + sy, RING)
        kind = jnp.where(core == 0, py, px)
        slot = jnp.where(core == 0, px, py)
        return far_ref.at[pl.ds(pl.multiple_of((kind * RING + slot) * rows + leg * part, part), part)]

    for leg in range(2):
        for i in range(RING):
            for j in range(RING):
                here = side_spot(leg, i, j)
                remote(here, here, side_send.at[leg, i, j], side_recv.at[leg, i, j], me).wait_recv()


def gather_rows(piece, g, weights, n_dev):
    rows, d_model = piece.shape
    width, tok = g.shape[1], g.shape[2]
    half = n_dev * rows // CORES
    cols = min(256, d_model // 2)
    return pl.pallas_call(
        gather_kernel,
        name='gather_rows',
        out_shape=(pltpu.VMEM((half, d_model), F32), jax.ShapeDtypeStruct((half, d_model), F32),
                   pltpu.VMEM((tok, d_model), BF16), pltpu.VMEM((tok, d_model), BF16)),
        in_specs=[VMEM] + [ANY] * 5,
        out_specs=(VMEM, ANY, VMEM, VMEM),
        scratch_shapes=[pltpu.VMEM((2, width, tok), BF16), pltpu.VMEM((tok, width), BF16), pltpu.VMEM((2, width, cols), BF16),
                        pltpu.VMEM((tok, d_model), F32), DMA((2,)), DMA((2,)),
                        DMA((40,)), DMA((2, RING, RING, 2)), DMA((2, RING, RING)), DMA((2, RING, RING))],
        compiler_params=pltpu.CompilerParams(collective_id=2, has_side_effects=True, vmem_limit_bytes=17 * MIB),
    )(piece, g, *weights)


def store_kernel(near_ref, far_ref, y_ref, dx_ref, y_out, dx_out, dq_out, dk_out, dv_out, do_out, tile, put_sem, in_sem, out_sem):
    core = lax.rem(lax.axis_index('sp'), CORES)
    outs = (dq_out, dk_out, dv_out, do_out)
    rows = near_ref.shape[0] // TYPES
    n_slot, chunk = tile.shape[0], tile.shape[1]
    per_type = rows // chunk
    n = TYPES * per_type
    puts = [pltpu.make_async_copy(y_ref, y_out, put_sem.at[TYPES]), pltpu.make_async_copy(dx_ref, dx_out, put_sem.at[TYPES + 1])]
    for kind in range(TYPES):
        puts.append(pltpu.make_async_copy(near_ref.at[pl.ds(kind * rows, rows)],
                                          outs[kind].at[pl.ds(pl.multiple_of(core * rows, rows), rows)], put_sem.at[kind]))

    def load(i):
        return pltpu.make_async_copy(far_ref.at[pl.ds(i * chunk, chunk)], tile.at[i % n_slot], in_sem.at[i % n_slot])

    def save(i):
        at = pl.multiple_of((1 - core) * rows + (i % per_type) * chunk, chunk)
        return pltpu.make_async_copy(tile.at[i % n_slot], outs[i // per_type].at[pl.ds(at, chunk)], out_sem.at[i % n_slot])

    ahead = n_slot // 2
    for i in range(ahead):
        load(i).start()
    for put in puts:
        put.start()
    for i in range(n):
        load(i).wait()
        save(i).start()
        if i + ahead < n:
            if i + ahead >= n_slot:
                save(i + ahead - n_slot).wait()
            load(i + ahead).start()
    for i in range(max(0, n - n_slot), n):
        save(i).wait()
    for put in puts:
        put.wait()


def store(near, far, y_rows, dx_rows):
    half, d_model = near.shape
    chunk = half // 32
    grad = jax.ShapeDtypeStruct((half * CORES // TYPES, d_model), F32)
    return pl.pallas_call(
        store_kernel,
        name='store',
        out_shape=(jax.ShapeDtypeStruct(y_rows.shape, BF16), jax.ShapeDtypeStruct(dx_rows.shape, BF16), grad, grad, grad, grad),
        in_specs=[VMEM, ANY, VMEM, VMEM],
        out_specs=(ANY,) * 6,
        scratch_shapes=[pltpu.VMEM((8, chunk, d_model), F32), DMA((TYPES + 2,)), DMA((8,)), DMA((8,))],
        compiler_params=pltpu.CompilerParams(vmem_limit_bytes=17 * MIB),
    )(near, far, y_rows, dx_rows)


def solution(mesh):
    n_dev = mesh.shape['sp']
    assert n_dev == CORES * RING * RING

    def device_body(x_loc, flag_loc, w_q, w_k, w_v, w_o, dy_loc):
        tok_count, d_model = x_loc.shape
        n_heads, head_dim = w_q.shape[1], w_q.shape[2]
        width = n_heads * head_dim
        score_scale = 1.0 / (math.sqrt(head_dim) * tok_count)
        masks = block_masks(flag_loc)
        weights = [w.transpose(1, 2, 0).reshape(width, d_model) for w in (w_q, w_k, w_v)] + [w_o.reshape(width, d_model)]
        g, z = front(*masks, x_loc, dy_loc, weights, score_scale, n_dev, n_heads)
        piece = reduce_rows(g, z, x_loc, dy_loc)
        near, far, y_rows, dx_rows = gather_rows(piece, g, weights, n_dev)
        y_loc, dx_loc, *grads = store(near, far, y_rows, dx_rows)
        dw_q, dw_k, dw_v, dw_o = (grad.reshape(n_heads, head_dim, d_model) for grad in grads)
        return y_loc, dx_loc, dw_q.transpose(2, 0, 1), dw_k.transpose(2, 0, 1), dw_v.transpose(2, 0, 1), dw_o

    row_spec = P(('dp', 'sp'), None)
    flag_spec = P(('dp', 'sp'))
    w_spec = P(None, None, None)
    dw_spec = P('dp', None, None)
    return jax.shard_map(device_body, mesh=mesh,
                         in_specs=(row_spec, flag_spec, w_spec, w_spec, w_spec, w_spec, row_spec),
                         out_specs=(row_spec, row_spec, dw_spec, dw_spec, dw_spec, dw_spec),
                         check_vma=False)
```

```python
import functools
import math
import jax
import jax.numpy as jnp
from jax import lax
from jax.experimental import pallas as pl
from jax.experimental.pallas import tpu as pltpu
from jax.sharding import PartitionSpec as P

MESH = pl.DeviceIdType.MESH
CORES = 2
RING = 4
SLOTS = CORES * RING
TYPES = 4
O_TYPE = TYPES - 1
MIB = 1024 * 1024
PIECES = 16
PUSH = 4
STORE_LIMIT = 9 * MIB
BF16 = jnp.bfloat16
F32 = jnp.float32
ROWS = ((1,), (1,))
INNER = ((1,), (0,))
OUTER = ((0,), (0,))
VMEM = pl.BlockSpec(memory_space=pltpu.VMEM)
ANY = pl.BlockSpec(memory_space=pltpu.HBM)
DMA = pltpu.SemaphoreType.DMA


def place(me):
    core = lax.rem(me, CORES)
    chip = me // CORES
    return lax.rem(chip, RING), chip // RING, core


def index_of(x, y, core):
    return (lax.rem(y, RING) * RING + lax.rem(x, RING)) * CORES + core


def remote(src, dst, send_sem, recv_sem, peer):
    return pltpu.make_async_remote_copy(src_ref=src, dst_ref=dst, send_sem=send_sem, recv_sem=recv_sem,
                                        device_id={'sp': peer}, device_id_type=MESH)


def signal(peer):
    pl.semaphore_signal(pltpu.get_barrier_semaphore(), inc=1, device_id={'sp': peer}, device_id_type=MESH)


def meet(peers):
    for peer in peers:
        signal(peer)
    pl.semaphore_wait(pltpu.get_barrier_semaphore(), len(peers))


def chips_around(x, y):
    return ((x + 1, y), (x + RING - 1, y), (x, y + 1), (x, y + RING - 1))


def dot(a, b, dims):
    return lax.dot_general(a, b, (dims, ((), ())), preferred_element_type=F32)


def in_vmem(value):
    return pltpu.with_memory_space_constraint(value, pltpu.VMEM)


def span(start, size):
    return pl.ds(pl.multiple_of(start, size), size)


def stream(n_outer, n_inner, copy, use, before=None):
    copy(0, 0, 0).start()
    for i in range(n_outer):
        if before is not None:
            before(i)

        @pl.loop(0, n_inner)
        def _(n):
            slot = lax.rem(n, 2)

            @pl.when(n + 1 < n_inner)
            def _():
                copy(i, n + 1, 1 - slot).start()

            if i + 1 < n_outer:
                @pl.when(n + 1 == n_inner)
                def _():
                    copy(i + 1, 0, 0).start()

            copy(i, n, slot).wait()
            use(i, n, slot)


def form_masks(flag_ref, seg_col_ref, seg_row_ref, head_ref, tail_ref, gate_ref):
    tok = flag_ref.shape[1]
    flags = flag_ref[...] > 0
    t_pos = lax.broadcasted_iota(jnp.int32, (tok, tok), 0)
    s_pos = lax.broadcasted_iota(jnp.int32, (tok, tok), 1)
    seg_col = jnp.sum(jnp.where(flags & (s_pos <= t_pos), 1.0, 0), axis=1, keepdims=True)
    seg_col_ref[...] = seg_col
    seg_row_ref[...] = jnp.sum(jnp.where(s_pos == t_pos, seg_col, 0), axis=0, keepdims=True)
    positions = lax.broadcasted_iota(jnp.int32, (1, tok), 1).astype(F32)
    first_pos = jnp.min(jnp.where(flags, positions, tok), axis=1, keepdims=True)
    last_pos = jnp.max(jnp.where(flags, positions, -1), axis=1, keepdims=True)
    head_ref[...] = jnp.where(positions < first_pos, 1.0, 0)
    tail_ref[...] = jnp.where(positions >= last_pos, 1.0, 0)
    gate_ref[...] = jnp.broadcast_to(jnp.where(last_pos < 0, 1.0, 0), gate_ref.shape)


class Ring:
    def __init__(self, ring, me):
        x, y, core = place(me)
        self.ring = ring
        self.along, self.across = (x, y) if ring == 0 else (y, x)
        self.flip = lax.rem(core + ring, CORES)
        self.peer = lambda step: index_of(x + step, y, ring) if ring == 0 else index_of(x, y + step, ring)

    def kind(self, step):
        return lax.rem(self.along + step, RING)


def start_tokens(ring, step, x_ref, dy_ref, copy):
    kind = ring.kind(step)

    @pl.when(kind == O_TYPE)
    def _():
        copy(dy_ref).start()

    @pl.when(kind != O_TYPE)
    def _():
        copy(x_ref).start()


def front_kernel(scale, dim, n_push, flag_ref, x_ref, dy_ref, wq_ref, wk_ref, wv_ref, wo_ref,
                 g_ref, z_ref, seg_col_ref, seg_row_ref, head_ref, tail_ref, gate_ref, tok_in, w_tile, rows_ref, total,
                 packed, held, formed, states,
                 tok_sem, w_sem, g_sem, z_send, z_recv, side_sem, send_sem, recv_sem, back_send, back_recv):
    me = lax.axis_index('sp')
    _, _, core = place(me)
    n_dev, per_dev = packed.shape[0], packed.shape[1]
    width, tok = rows_ref.shape[1], rows_ref.shape[2]
    half = tok // 2
    n_piece = z_recv.shape[1]
    piece = tok // (n_piece + n_push)
    n_group = SLOTS
    group = width // n_group
    tile_rows = w_tile.shape[1]

    @pl.loop(1, n_dev)
    def _(step):
        signal(lax.rem(me + step, n_dev))

    loads = [pltpu.make_async_copy(ref, tok_in.at[i], tok_sem.at[i]) for i, ref in enumerate((x_ref, dy_ref))]
    for load in loads:
        load.start()

    rings = [Ring(ring, me) for ring in range(CORES)]
    near_steps = (1, RING - 1)

    def token_copy(ring, step, n):
        slot = CORES * step + ring.flip
        at = span(n * piece, piece)
        return lambda ref: remote(ref.at[at], z_ref.at[slot, at], z_send.at[ring.ring, step // 2, n], z_recv.at[slot, n], ring.peer(step))

    def push_tokens(n):
        for ring in rings:
            for step in near_steps:
                start_tokens(ring, step, x_ref, dy_ref, token_copy(ring, step, n))

    def sibling_copy(ring):
        return lambda ref: remote(ref, z_ref.at[1], side_sem.at[0], side_sem.at[1], ring.peer(0))

    form_masks(flag_ref, seg_col_ref, seg_row_ref, head_ref, tail_ref, gate_ref)
    pl.semaphore_wait(pltpu.get_barrier_semaphore(), n_dev - 1)
    pl.loop(0, 2)(push_tokens)
    for ring in rings:
        @pl.when(ring.flip == 1)
        def _(ring=ring):
            start_tokens(ring, 0, x_ref, dy_ref, sibling_copy(ring))

    weights = (wk_ref, wv_ref, wq_ref, wo_ref)
    kinds = (1, 2, 0, O_TYPE)

    def w_copy(i, n, slot):
        return pltpu.make_async_copy(weights[i].at[span(n * tile_rows, tile_rows)], w_tile.at[slot], w_sem.at[slot])

    def project(i, n, slot):
        rows_ref[kinds[i], span(n * tile_rows, tile_rows), :] = dot(w_tile[slot], tok_in[i // O_TYPE], ROWS).astype(BF16)

    def loaded(i):
        if i in (0, O_TYPE):
            loads[i // O_TYPE].wait()
        if i:
            pl.loop(2 * i, 2 * i + 2)(push_tokens)

    stream(TYPES, width // tile_rows, w_copy, project, loaded)

    head = head_ref[...] > 0.5
    tail = tail_ref[...] > 0.5
    zero = jnp.zeros((dim, tok), BF16)

    @pl.loop(0, n_dev, unroll=4)
    def _(dev):
        for sub in range(per_dev):
            rows = span((dev * per_dev + sub) * dim, dim)
            v_tail = jnp.concatenate([jnp.where(tail, rows_ref[2, rows, :], zero), zero], axis=0)
            do_head = jnp.concatenate([zero, jnp.where(head, rows_ref[O_TYPE, rows, :], zero)], axis=0)
            packed[dev, sub, 0:dim, :] = dot(rows_ref[1, rows, :], v_tail, ROWS) + dot(rows_ref[0, rows, :], do_head, ROWS)
            packed[dev, sub, dim:, :] = gate_ref[...]

    def out_copy(step):
        peer = lax.rem(me + step, n_dev)
        return remote(packed.at[peer], held.at[me], send_sem.at[step], recv_sem.at[step], peer)

    def back_copy(step):
        peer = lax.rem(me + step, n_dev)
        return remote(formed.at[peer], states.at[me], back_send.at[step], back_recv.at[step], peer)

    def each(do):
        pl.loop(1, n_dev)(do)

    each(lambda step: out_copy(step).start())
    held[me] = packed[me]

    def form_states():
        each(lambda step: out_copy(step).wait_recv())
        shape = (per_dev, dim, 2 * dim)
        lane = lax.broadcasted_iota(jnp.int32, shape, 2)
        start = jnp.zeros(shape, F32)

        def advance(block, state):
            return held[block, :, dim:dim + 1, :] * state + held[block, :, 0:dim, :]

        def forward(block, state):
            formed[block] = state.astype(BF16)
            return advance(block, state)

        def backward(step, state):
            block = n_dev - 1 - step
            formed[block] = jnp.where(lane < dim, formed[block].astype(F32), state).astype(BF16)
            return advance(block, state)

        lax.fori_loop(0, n_dev, forward, start)
        lax.fori_loop(0, n_dev, backward, start)
        each(lambda step: back_copy(step).start())
        states[me] = formed[me]

    seg_row = seg_row_ref[...]
    t_pos = lax.broadcasted_iota(jnp.int32, (half, tok), 0)
    s_pos = lax.broadcasted_iota(jnp.int32, (half, tok), 1)

    def pair(a, b):
        see_top = ((seg_col_ref[0:half, :] == seg_row) & (s_pos <= t_pos))[:, 0:half]
        see_low = (seg_col_ref[half:, :] == seg_row) & (s_pos <= t_pos + half)
        top = dot(a[:, 0:half], b[:, 0:half], OUTER)
        low = dot(a[:, half:], b, OUTER)
        return (jnp.where(see_top, top * scale, 0).astype(BF16), jnp.where(see_low, low * scale, 0).astype(BF16))

    def over_keys(at, rows_t, probs):
        total[at[0], at[1], 0:half] = dot(rows_t[:, 0:half], probs[0], ROWS)
        total[at[0], at[1], half:] = dot(rows_t, probs[1], ROWS)

    def over_queries(at, rows_t, probs):
        from_low = dot(rows_t[:, half:], probs[1], INNER)
        total[at[0], at[1], 0:half] = dot(rows_t[:, 0:half], probs[0], INNER) + from_low[:, 0:half]
        total[at[0], at[1], half:] = from_low[:, half:]

    def heads_of(grp):
        return [grp * (group // dim) + sub for sub in range(group // dim)]

    @pl.loop(0, n_group)
    def _(grp):
        @pl.when(grp == n_group - 3)
        def _():
            form_states()

        @pl.when(lax.rem(grp, 2) == 0)
        def _():
            push_tokens(SLOTS + grp // 2)

        for index in heads_of(grp):
            rows = span(index * dim, dim)
            q, k, v, do = (rows_ref[kind, rows, :] for kind in range(TYPES))
            d_probs = pair(do, v)
            over_keys((0, rows), k, d_probs)
            over_queries((1, rows), q, d_probs)
            probs = pair(q, k)
            over_queries((2, rows), do, probs)
            over_keys((O_TYPE, rows), v, probs)

    each(lambda step: back_copy(step).wait_recv())

    def g_copy(grp):
        at = span(grp * group, group)
        return pltpu.make_async_copy(rows_ref.at[:, at], g_ref.at[:, at], g_sem.at[grp])

    @pl.loop(0, n_group)
    def _(grp):
        for index in heads_of(grp):
            rows = span(index * dim, dim)
            q, k, v, do = (rows_ref[kind, rows, :] for kind in range(TYPES))
            st = states[index // per_dev, lax.rem(index, per_dev)]
            d_q = dot(st, jnp.concatenate([do, zero], axis=0), INNER)
            d_k = dot(st, jnp.concatenate([zero, v], axis=0), INNER)
            d_v = dot(st, k, OUTER)[dim:]
            out = dot(st, q, OUTER)[0:dim]
            for kind, mask, inter in ((0, head, d_q), (1, tail, d_k), (2, tail, d_v), (O_TYPE, head, out)):
                rows_ref[kind, rows, :] = (total[kind, rows, :] + jnp.where(mask, inter * scale, 0)).astype(BF16)
        g_copy(grp).start()

    pl.loop(0, n_group)(lambda grp: g_copy(grp).wait())
    each(lambda step: out_copy(step).wait_send())
    each(lambda step: back_copy(step).wait_send())
    for ring in rings:
        for step in near_steps:
            @pl.loop(0, n_piece)
            def _(n, ring=ring, step=step):
                token_copy(ring, step, n)(x_ref).wait_send()

            @pl.loop(0, n_piece)
            def _(n, slot=CORES * step + ring.ring):
                at = span(n * piece, piece)
                remote(x_ref.at[at], z_ref.at[slot, at], side_sem.at[0], z_recv.at[slot, n], me).wait_recv()

    sibling_copy(rings[0])(x_ref).wait()


def front(flags, x_loc, dy_loc, weights, scale, n_dev, n_heads):
    tok, d_model = x_loc.shape
    width = weights[0].shape[0]
    dim = width // n_heads
    per_dev = n_heads // n_dev
    n_piece = PIECES - PUSH
    pack = (n_dev, per_dev, dim + 8, 2 * dim)
    back = (n_dev, per_dev, dim, 2 * dim)
    return pl.pallas_call(
        functools.partial(front_kernel, scale, dim, PUSH),
        name='front',
        out_shape=(jax.ShapeDtypeStruct((TYPES, width, tok), BF16), jax.ShapeDtypeStruct((SLOTS, tok, d_model), BF16)),
        in_specs=[VMEM] + [ANY] * 6,
        out_specs=(ANY, ANY),
        scratch_shapes=[
            pltpu.VMEM((tok, 1), F32), pltpu.VMEM((1, tok), F32), pltpu.VMEM((1, tok), F32), pltpu.VMEM((1, tok), F32), pltpu.VMEM((8, 2 * dim), F32),
            pltpu.VMEM((2, tok, d_model), BF16), pltpu.VMEM((2, width // RING, d_model), BF16),
            pltpu.VMEM((TYPES, width, tok), BF16), pltpu.VMEM((TYPES, width, tok), F32),
            pltpu.VMEM(pack, F32), pltpu.VMEM(pack, F32), pltpu.VMEM(back, BF16), pltpu.VMEM(back, BF16),
            DMA((2,)), DMA((2,)), DMA((SLOTS,)), DMA((CORES, 2, n_piece)), DMA((SLOTS, n_piece)), DMA((2,)),
            DMA((n_dev,)), DMA((n_dev,)), DMA((n_dev,)), DMA((n_dev,))],
        compiler_params=pltpu.CompilerParams(collective_id=0, has_side_effects=True, vmem_limit_bytes=56 * MIB),
    )(flags[None, :], x_loc, dy_loc, *weights)


def row_products(g_ref, w_refs, y_ref, dx_ref, rows_in, rows_t, w_tile, total, g_sem, w_sem):
    width = rows_in.shape[1]
    cols = w_tile.shape[2]
    n_tile = total.shape[1] // cols
    step = width // 8
    order = (O_TYPE, 0, 1, 2)

    def g_copy(i):
        return pltpu.make_async_copy(g_ref.at[order[i]], rows_in.at[i % 2], g_sem.at[i % 2])

    def w_copy(i, n, slot):
        at = span(n * cols, cols)
        return pltpu.make_async_copy(w_refs[order[i]].at[:, at], w_tile.at[slot], w_sem.at[slot])

    def turned(i):
        if i + 1 < TYPES:
            g_copy(i + 1).start()
        g_copy(i).wait()

        @pl.loop(0, width // step)
        def _(b):
            at = span(b * step, step)
            rows_t[:, at] = jnp.transpose(rows_in[i % 2, at, :])

    def use(i, n, slot):
        at = span(n * cols, cols)
        prod = dot(rows_t[...], w_tile[slot], INNER)
        if i == 0:
            y_ref[:, at] = prod.astype(BF16)
        elif i == 1:
            total[:, at] = prod
        elif i + 1 < TYPES:
            total[:, at] = total[:, at] + prod
        else:
            dx_ref[:, at] = (total[:, at] + prod).astype(BF16)

    g_copy(0).start()
    stream(TYPES, n_tile, w_copy, use, turned)


def reduce_kernel(g_ref, z_ref, x_ref, dy_ref, wq_ref, wk_ref, wv_ref, wo_ref, out_ref, y_ref, dx_ref,
                  zbuf, rows_in, a_out, a_in, b_out, b_in, kind_rows, rows_t, w_tile, total, y_out, dx_out,
                  z_sem, far_send, rest_send, rest_sem, row_send, row_recv, a_send, a_recv, b_send, b_recv, g_sem, w_sem):
    me = lax.axis_index('sp')
    x, y, core = place(me)
    block = rows_in.shape[2]
    part = block // 2
    n_col, cols = a_out.shape[0], a_out.shape[3]
    rings = [Ring(ring, me) for ring in range(CORES)]
    order = (2, 1, RING - 1, 0)

    meet([index_of(x, y, 1 - core)] + [index_of(*chip, other) for other in range(CORES) for chip in chips_around(x, y)]
         + [ring.peer(2) + other - ring.ring for other in range(CORES) for ring in rings])

    def far_copy(ring):
        slot = 2 * CORES + ring.flip
        return lambda ref: remote(ref, zbuf.at[slot], far_send.at[ring.ring], z_sem.at[slot], ring.peer(2))

    def own_copy(ref):
        return pltpu.make_async_copy(ref, zbuf.at[0], z_sem.at[0])

    def near_copy(slot):
        at = pl.ds(0, kept if slot // CORES else tok)
        return pltpu.make_async_copy(z_ref.at[slot, at], zbuf.at[slot, at], z_sem.at[slot])

    near_slots = [slot for slot in range(1, SLOTS) if slot // CORES != 2]
    tok = zbuf.shape[1]
    kept = tok - tok * PUSH // PIECES
    rest = pl.ds(kept, tok - kept)

    def rest_copy(ring, step):
        slot = CORES * step + ring.flip
        return lambda ref: remote(ref.at[rest], zbuf.at[slot, rest], rest_send.at[ring.ring, step // 2], rest_sem.at[slot], ring.peer(step))
    for ring in rings:
        for step in (1, RING - 1):
            start_tokens(ring, step, x_ref, dy_ref, rest_copy(ring, step))
        start_tokens(ring, 2, x_ref, dy_ref, far_copy(ring))
    for ring in rings:
        @pl.when(ring.flip == 0)
        def _(ring=ring):
            start_tokens(ring, 0, x_ref, dy_ref, own_copy)
    for slot in near_slots:
        near_copy(slot).start()

    def row_source(ring, bi, step):
        first = (ring.ring * RING + lax.rem(ring.across + order[bi], RING)) * block
        return g_ref.at[ring.kind(step), span(first, block)]

    def row_copy(ring, bi, step):
        slot = CORES * step + ring.flip
        return remote(row_source(ring, bi, step), rows_in.at[slot, bi], row_send.at[ring.ring, bi, step],
                      row_recv.at[slot, bi], ring.peer(step))

    def own_rows(ring, bi):
        return pltpu.make_async_copy(row_source(ring, bi, 0), rows_in.at[0, bi], row_recv.at[0, bi])

    for bi in range(RING):
        for ring in rings:
            for step in (2, 1, RING - 1):
                row_copy(ring, bi, step).start()

            @pl.when(ring.flip == 1)
            def _(ring=ring, bi=bi):
                row_copy(ring, bi, 0).start()

            @pl.when(ring.flip == 0)
            def _(ring=ring, bi=bi):
                own_rows(ring, bi).start()

    def arrived(bi):
        for slot in range(SLOTS):
            pltpu.make_async_copy(g_ref.at[0, pl.ds(0, block)], rows_in.at[slot, bi], row_recv.at[slot, bi]).wait()

    def product(bi, ch):
        at = span(ch * cols, cols)
        total = dot(rows_in[0, bi], zbuf[0, :, at], INNER)
        for slot in range(1, SLOTS):
            total = total + dot(rows_in[slot, bi], zbuf[slot, :, at], INNER)
        return total

    across = [jnp.where(core == 0, index_of(x, y + step, core), index_of(x + step, y, core)) for step in (1, RING - 1)]

    def a_copy(ch, way):
        return remote(a_out.at[ch, way], a_in.at[ch, way], a_send.at[ch, way], a_recv.at[ch, way], across[way])

    def b_copy(ch, way):
        return remote(b_out.at[ch, way], b_in.at[ch, way], b_send.at[ch, way], b_recv.at[ch, way], across[way])

    row_products(g_ref, (wq_ref, wk_ref, wv_ref, wo_ref), y_out, dx_out, kind_rows, rows_t, w_tile, total, g_sem, w_sem)
    puts = [pltpu.make_async_copy(y_out, y_ref, g_sem.at[0]), pltpu.make_async_copy(dx_out, dx_ref, g_sem.at[1])]
    for put in puts:
        put.start()

    own_copy(x_ref).wait()
    for slot in near_slots:
        near_copy(slot).wait()
    for ring in rings:
        far_copy(ring)(x_ref).wait_recv()
        for step in (1, RING - 1):
            slot = CORES * step + ring.ring
            remote(x_ref.at[rest], zbuf.at[slot, rest], rest_send.at[0, 0], rest_sem.at[slot], me).wait_recv()

    def two_away(ch):
        total = product(0, ch)
        for way in range(2):
            a_out[ch, way] = total[way * part:(way + 1) * part]
            a_copy(ch, way).start()

    def next_to(way, ch):
        total = product(1 + way, ch)
        a_copy(ch, way).wait_recv()
        b_out[ch, way] = total
        b_out[ch, way, pl.ds(way * part, part)] += a_in[ch, way]
        b_copy(ch, way).start()

    def own(ch):
        total = product(RING - 1, ch)
        for way in range(2):
            b_copy(ch, way).wait_recv()
            total = total + b_in[ch, way]
        out_ref[:, span(ch * cols, cols)] = total

    for bi, step in enumerate((two_away, functools.partial(next_to, 0), functools.partial(next_to, 1), own)):
        arrived(bi)
        pl.loop(0, n_col)(step)

    for put in puts:
        put.wait()
    for ring in rings:
        far_copy(ring)(x_ref).wait_send()
        for step in (1, RING - 1):
            rest_copy(ring, step)(x_ref).wait_send()
        for bi in range(RING):
            for step in range(1, RING):
                row_copy(ring, bi, step).wait_send()

            @pl.when(ring.flip == 1)
            def _(ring=ring, bi=bi):
                row_copy(ring, bi, 0).wait_send()

    for ch in range(n_col):
        for way in range(2):
            a_copy(ch, way).wait_send()
            b_copy(ch, way).wait_send()


def reduce_rows(g, z, x_loc, dy_loc, weights):
    width, tok = g.shape[1], g.shape[2]
    d_model = x_loc.shape[1]
    block = width // SLOTS
    n_col = RING
    part = (n_col, 2, block // 2, d_model // n_col)
    full = (n_col, 2, block, d_model // n_col)
    return pl.pallas_call(
        reduce_kernel,
        name='reduce_rows',
        out_shape=(pltpu.VMEM((block, d_model), F32), jax.ShapeDtypeStruct((tok, d_model), BF16), jax.ShapeDtypeStruct((tok, d_model), BF16)),
        in_specs=[ANY] * 8,
        out_specs=(VMEM, ANY, ANY),
        scratch_shapes=[
            pltpu.VMEM((SLOTS, tok, d_model), BF16), pltpu.VMEM((SLOTS, RING, block, tok), BF16),
            pltpu.VMEM(part, F32), pltpu.VMEM(part, F32), pltpu.VMEM(full, F32), pltpu.VMEM(full, F32),
            pltpu.VMEM((2, width, tok), BF16), pltpu.VMEM((tok, width), BF16), pltpu.VMEM((2, width, min(256, d_model // 2)), BF16),
            pltpu.VMEM((tok, d_model), F32), pltpu.VMEM((tok, d_model), BF16), pltpu.VMEM((tok, d_model), BF16),
            DMA((SLOTS,)), DMA((CORES,)), DMA((CORES, 2)), DMA((SLOTS,)), DMA((CORES, RING, RING)), DMA((SLOTS, RING)),
            DMA((n_col, 2)), DMA((n_col, 2)), DMA((n_col, 2)), DMA((n_col, 2)), DMA((2,)), DMA((2,))],
        compiler_params=pltpu.CompilerParams(collective_id=1, has_side_effects=True, vmem_limit_bytes=58 * MIB),
    )(g, z, x_loc, dy_loc, *weights)


def gather_kernel(piece_ref, near_ref, far_a_ref, far_b_ref, send_sem, recv_sem, side_send, side_recv):
    me = lax.axis_index('sp')
    x, y, core = place(me)
    rows = piece_ref.shape[0]
    part = rows // 2
    quarter = part // 2

    def number(leg, i, j, plane):
        sx, sy = (i, j) if leg == 0 else (j, i)
        px, py = lax.rem(x + sx, RING), lax.rem(y + sy, RING)
        return jnp.where(plane == 0, px * RING + py, py * RING + px)

    def spot(leg, i, j, half=None):
        lo, size = (0, part) if half is None else (half * quarter, quarter)
        return near_ref.at[pl.ds(pl.multiple_of(number(leg, i, j, core) * rows + leg * part + lo, quarter), size)]

    def far_spot(leg, i, j, plane):
        return (far_a_ref, far_b_ref)[leg].at[span(number(leg, i, j, plane) * part, part)]

    def own(leg, half=None):
        lo, size = (0, part) if half is None else (half * quarter, quarter)
        return piece_ref.at[pl.ds(leg * part + lo, size)]

    def step_peer(leg, second, step):
        along_x = (leg == 0) != second
        return index_of(x + step, y, core) if along_x else index_of(x, y + step, core)

    started = []

    def push(leg, second, i, j, step, half):
        there = (i, (j - step) % RING) if second else ((i - step) % RING, j)
        src = own(leg, half) if i == 0 and j == 0 else spot(leg, i, j, half)
        copy = remote(src, spot(leg, i, j, half), send_sem.at[len(started)],
                      recv_sem.at[leg, there[0], there[1], half or 0], step_peer(leg, second, step))
        copy.start()
        started.append(copy)

    def landed(leg, i, j):
        in_halves = j == 2 or (j == 0 and i == 2)
        for half in ((0, 1) if in_halves else (None,)):
            here = spot(leg, i, j, half)
            remote(here, here, send_sem.at[0], recv_sem.at[leg, i, j, half or 0], me).wait_recv()

    side = []

    def to_sibling(leg, i, j):
        src = own(leg) if i == 0 and j == 0 else spot(leg, i, j)
        copy = remote(src, far_spot(leg, i, j, core), side_send.at[leg, i, j], side_recv.at[leg, i, j],
                      index_of(x, y, 1 - core))
        copy.start()
        side.append(copy)

    meet([index_of(x, y, 1 - core)] + [index_of(*chip, core) for chip in chips_around(x, y)])

    def spread(leg, i):
        push(leg, True, i, 0, 1, None)
        push(leg, True, i, 0, 3, None)
        to_sibling(leg, i, 0)

    for leg in range(2):
        push(leg, False, 0, 0, 1, None)
        push(leg, False, 0, 0, 3, None)
    for leg in range(2):
        spread(leg, 0)
    near_ref[span(number(0, 0, 0, core) * rows, rows), :] = piece_ref[...]

    for leg in range(2):
        landed(leg, 3, 0)
        push(leg, False, 3, 0, 1, 0)
        spread(leg, 3)
        landed(leg, 1, 0)
        push(leg, False, 1, 0, 3, 1)
        spread(leg, 1)

    def second_near(leg, i):
        landed(leg, i, 3)
        push(leg, True, i, 3, 1, 0)
        to_sibling(leg, i, 3)
        landed(leg, i, 1)
        push(leg, True, i, 1, 3, 1)
        to_sibling(leg, i, 1)

    for leg in range(2):
        second_near(leg, 0)
    for leg in range(2):
        landed(leg, 2, 0)
        spread(leg, 2)
    for i in (3, 1, 2):
        for leg in range(2):
            second_near(leg, i)
    for i in (0, 3, 1, 2):
        for leg in range(2):
            landed(leg, i, 2)
            to_sibling(leg, i, 2)

    for copy in started + side:
        copy.wait_send()

    for leg in range(2):
        for i in range(RING):
            for j in range(RING):
                here = far_spot(leg, i, j, 1 - core)
                remote(here, here, side_send.at[leg, i, j], side_recv.at[leg, i, j], me).wait_recv()


def gather_rows(piece, n_dev):
    rows, d_model = piece.shape
    half = n_dev * rows // CORES
    return pl.pallas_call(
        gather_kernel,
        name='gather_rows',
        out_shape=(pltpu.VMEM((half, d_model), F32), pltpu.VMEM((half // 2, d_model), F32), jax.ShapeDtypeStruct((half // 2, d_model), F32)),
        in_specs=[VMEM],
        out_specs=(VMEM, VMEM, ANY),
        scratch_shapes=[DMA((40,)), DMA((2, RING, RING, 2)), DMA((2, RING, RING)), DMA((2, RING, RING))],
        compiler_params=pltpu.CompilerParams(collective_id=2, has_side_effects=True, vmem_limit_bytes=STORE_LIMIT),
    )(piece)


def store_kernel(near_ref, far_a_ref, far_b_ref, dq_out, dk_out, dv_out, do_out, tile, put_sem, side_sem, in_sem, out_sem):
    core = lax.rem(lax.axis_index('sp'), CORES)
    outs = (dq_out, dk_out, dv_out, do_out)
    rows = near_ref.shape[0] // TYPES
    n_slot, chunk = tile.shape[0], tile.shape[1]
    n = far_b_ref.shape[0] // chunk

    def far_out(i, leg):
        first = (1 - core) * rows + (i % RING * 2 + leg) * chunk
        return outs[i // RING].at[pl.ds(pl.multiple_of(first, chunk), chunk)]

    puts = [pltpu.make_async_copy(near_ref.at[pl.ds(kind * rows, rows)], outs[kind].at[span(core * rows, rows)], put_sem.at[kind])
            for kind in range(TYPES)]
    puts += [pltpu.make_async_copy(far_a_ref.at[pl.ds(i * chunk, chunk)], far_out(i, 0), side_sem.at[i]) for i in range(n)]

    def load(i):
        return pltpu.make_async_copy(far_b_ref.at[pl.ds(i * chunk, chunk)], tile.at[i % n_slot], in_sem.at[i % n_slot])

    def save(i):
        return pltpu.make_async_copy(tile.at[i % n_slot], far_out(i, 1), out_sem.at[i % n_slot])

    ahead = n_slot // 2
    for i in range(ahead):
        load(i).start()
    for put in puts:
        put.start()
    for i in range(n):
        load(i).wait()
        save(i).start()
        if i + ahead < n:
            if i + ahead >= n_slot:
                save(i + ahead - n_slot).wait()
            load(i + ahead).start()
    for i in range(n - n_slot, n):
        save(i).wait()
    for put in puts:
        put.wait()


def store(near, far_a, far_b):
    half, d_model = near.shape
    n = RING * RING
    chunk = far_b.shape[0] // n
    grad = jax.ShapeDtypeStruct((half * CORES // TYPES, d_model), F32)
    return pl.pallas_call(
        store_kernel,
        name='store',
        out_shape=(grad,) * TYPES,
        in_specs=[VMEM, VMEM, ANY],
        out_specs=(ANY,) * TYPES,
        scratch_shapes=[pltpu.VMEM((8, chunk, d_model), F32), DMA((TYPES,)), DMA((n,)), DMA((8,)), DMA((8,))],
        compiler_params=pltpu.CompilerParams(vmem_limit_bytes=STORE_LIMIT),
    )(in_vmem(near), in_vmem(far_a), pltpu.with_memory_space_constraint(far_b, pltpu.HBM))


def solution(mesh):
    n_dev = mesh.shape['sp']
    assert n_dev == CORES * RING * RING

    def device_body(x_loc, flag_loc, w_q, w_k, w_v, w_o, dy_loc):
        tok_count, d_model = x_loc.shape
        n_heads, head_dim = w_q.shape[1], w_q.shape[2]
        width = n_heads * head_dim
        score_scale = 1.0 / (math.sqrt(head_dim) * tok_count)
        weights = [w.transpose(1, 2, 0).reshape(width, d_model) for w in (w_q, w_k, w_v)] + [w_o.reshape(width, d_model)]
        g, z = front(flag_loc, x_loc, dy_loc, weights, score_scale, n_dev, n_heads)
        piece, y_loc, dx_loc = reduce_rows(g, z, x_loc, dy_loc, weights)
        grads = store(*gather_rows(piece, n_dev))
        dw_q, dw_k, dw_v, dw_o = (grad.reshape(n_heads, head_dim, d_model) for grad in grads)
        return y_loc, dx_loc, dw_q.transpose(2, 0, 1), dw_k.transpose(2, 0, 1), dw_v.transpose(2, 0, 1), dw_o

    row_spec = P(('dp', 'sp'), None)
    flag_spec = P(('dp', 'sp'))
    w_spec = P(None, None, None)
    dw_spec = P('dp', None, None)
    return jax.shard_map(device_body, mesh=mesh,
                         in_specs=(row_spec, flag_spec, w_spec, w_spec, w_spec, w_spec, row_spec),
                         out_specs=(row_spec, row_spec, dw_spec, dw_spec, dw_spec, dw_spec),
                         check_vma=False)
```

```python
import functools
import math
import jax
import jax.numpy as jnp
from jax import lax
from jax.experimental import pallas as pl
from jax.experimental.pallas import tpu as pltpu
from jax.sharding import PartitionSpec as P

MESH = pl.DeviceIdType.MESH
CORES = 2
RING = 4
SLOTS = CORES * RING
TYPES = 4
O_TYPE = TYPES - 1
MIB = 1024 * 1024
PIECES = 16
PUSH = 3
STORE_LIMIT = 9 * MIB
BF16 = jnp.bfloat16
F32 = jnp.float32
ROWS = ((1,), (1,))
INNER = ((1,), (0,))
OUTER = ((0,), (0,))
VMEM = pl.BlockSpec(memory_space=pltpu.VMEM)
ANY = pl.BlockSpec(memory_space=pltpu.HBM)
DMA = pltpu.SemaphoreType.DMA


def place(me):
    core = lax.rem(me, CORES)
    chip = me // CORES
    return lax.rem(chip, RING), chip // RING, core


def index_of(x, y, core):
    return (lax.rem(y, RING) * RING + lax.rem(x, RING)) * CORES + core


def remote(src, dst, send_sem, recv_sem, peer):
    return pltpu.make_async_remote_copy(src_ref=src, dst_ref=dst, send_sem=send_sem, recv_sem=recv_sem,
                                        device_id={'sp': peer}, device_id_type=MESH)


def signal(peer):
    pl.semaphore_signal(pltpu.get_barrier_semaphore(), inc=1, device_id={'sp': peer}, device_id_type=MESH)


def meet(peers):
    for peer in peers:
        signal(peer)
    pl.semaphore_wait(pltpu.get_barrier_semaphore(), len(peers))


def chips_around(x, y):
    return ((x + 1, y), (x + RING - 1, y), (x, y + 1), (x, y + RING - 1))


def dot(a, b, dims):
    return lax.dot_general(a, b, (dims, ((), ())), preferred_element_type=F32)


def in_vmem(value):
    return pltpu.with_memory_space_constraint(value, pltpu.VMEM)


def span(start, size):
    return pl.ds(pl.multiple_of(start, size), size)


def stream(n_outer, n_inner, copy, use, before=None):
    copy(0, 0, 0).start()
    for i in range(n_outer):
        if before is not None:
            before(i)

        @pl.loop(0, n_inner)
        def _(n):
            slot = lax.rem(n, 2)

            @pl.when(n + 1 < n_inner)
            def _():
                copy(i, n + 1, 1 - slot).start()

            if i + 1 < n_outer:
                @pl.when(n + 1 == n_inner)
                def _():
                    copy(i + 1, 0, 0).start()

            copy(i, n, slot).wait()
            use(i, n, slot)


def form_masks(flag_ref, seg_col_ref, seg_row_ref, head_ref, tail_ref, gate_ref):
    tok = flag_ref.shape[1]
    flags = flag_ref[...] > 0
    t_pos = lax.broadcasted_iota(jnp.int32, (tok, tok), 0)
    s_pos = lax.broadcasted_iota(jnp.int32, (tok, tok), 1)
    seg_col = jnp.sum(jnp.where(flags & (s_pos <= t_pos), 1.0, 0), axis=1, keepdims=True)
    seg_col_ref[...] = seg_col
    seg_row_ref[...] = jnp.sum(jnp.where(s_pos == t_pos, seg_col, 0), axis=0, keepdims=True)
    positions = lax.broadcasted_iota(jnp.int32, (1, tok), 1).astype(F32)
    first_pos = jnp.min(jnp.where(flags, positions, tok), axis=1, keepdims=True)
    last_pos = jnp.max(jnp.where(flags, positions, -1), axis=1, keepdims=True)
    head_ref[...] = jnp.where(positions < first_pos, 1.0, 0)
    tail_ref[...] = jnp.where(positions >= last_pos, 1.0, 0)
    gate_ref[...] = jnp.broadcast_to(jnp.where(last_pos < 0, 1.0, 0), gate_ref.shape)


class Ring:
    def __init__(self, ring, me):
        x, y, core = place(me)
        self.ring = ring
        self.along, self.across = (x, y) if ring == 0 else (y, x)
        self.flip = lax.rem(core + ring, CORES)
        self.peer = lambda step: index_of(x + step, y, ring) if ring == 0 else index_of(x, y + step, ring)

    def kind(self, step):
        return lax.rem(self.along + step, RING)


def start_tokens(ring, step, x_ref, dy_ref, copy):
    kind = ring.kind(step)

    @pl.when(kind == O_TYPE)
    def _():
        copy(dy_ref).start()

    @pl.when(kind != O_TYPE)
    def _():
        copy(x_ref).start()


def front_kernel(scale, dim, n_push, flag_ref, x_ref, dy_ref, wq_ref, wk_ref, wv_ref, wo_ref,
                 g_ref, z_ref, seg_col_ref, seg_row_ref, head_ref, tail_ref, gate_ref, tok_in, w_tile, rows_ref, total,
                 packed, held, formed, states,
                 tok_sem, w_sem, g_sem, z_send, z_recv, side_sem, send_sem, recv_sem, back_send, back_recv):
    me = lax.axis_index('sp')
    _, _, core = place(me)
    n_dev, per_dev, low = formed.shape[1:4]
    width, tok = rows_ref.shape[1], rows_ref.shape[2]
    half = tok // 2
    n_piece = z_recv.shape[1]
    piece = tok // (n_piece + n_push)
    n_group = SLOTS
    group = width // n_group
    tile_rows = w_tile.shape[1]

    @pl.loop(1, n_dev)
    def _(step):
        signal(lax.rem(me + step, n_dev))

    loads = [pltpu.make_async_copy(ref, tok_in.at[i], tok_sem.at[i]) for i, ref in enumerate((x_ref, dy_ref))]
    for load in loads:
        load.start()

    rings = [Ring(ring, me) for ring in range(CORES)]
    near_steps = (1, RING - 1)

    def token_copy(ring, step, n):
        slot = CORES * step + ring.flip
        at = span(n * piece, piece)
        return lambda ref: remote(ref.at[at], z_ref.at[slot, at], z_send.at[ring.ring, step // 2, n], z_recv.at[slot, n], ring.peer(step))

    def push_tokens(n):
        for ring in rings:
            for step in near_steps:
                start_tokens(ring, step, x_ref, dy_ref, token_copy(ring, step, n))

    def sibling_copy(ring):
        return lambda ref: remote(ref, z_ref.at[1], side_sem.at[0], side_sem.at[1], ring.peer(0))

    form_masks(flag_ref, seg_col_ref, seg_row_ref, head_ref, tail_ref, gate_ref)
    pl.semaphore_wait(pltpu.get_barrier_semaphore(), n_dev - 1)
    pl.loop(0, 2)(push_tokens)
    for ring in rings:
        @pl.when(ring.flip == 1)
        def _(ring=ring):
            start_tokens(ring, 0, x_ref, dy_ref, sibling_copy(ring))

    weights = (wk_ref, wv_ref, wq_ref, wo_ref)
    kinds = (1, 2, 0, O_TYPE)

    def w_copy(i, n, slot):
        return pltpu.make_async_copy(weights[i].at[span(n * tile_rows, tile_rows)], w_tile.at[slot], w_sem.at[slot])

    def project(i, n, slot):
        rows_ref[kinds[i], span(n * tile_rows, tile_rows), :] = dot(w_tile[slot], tok_in[i // O_TYPE], ROWS).astype(BF16)

    def loaded(i):
        if i in (0, O_TYPE):
            loads[i // O_TYPE].wait()
        if i == 2:
            send_products(0)
        if i:
            pl.loop(2 * i, 2 * i + 2)(push_tokens)

    head = head_ref[...] > 0.5
    tail = tail_ref[...] > 0.5
    zero = jnp.zeros((dim, tok), BF16)

    def each(do):
        pl.loop(1, n_dev)(do)

    def out_copy(which, step):
        peer = lax.rem(me + step, n_dev)
        at = pl.ds(0, packed.shape[3] if which == 0 else low)
        return remote(packed.at[which, peer, :, at], held.at[which, me, :, at], send_sem.at[which, step], recv_sem.at[which, step], peer)

    def back_copy(which, step):
        peer = lax.rem(me + step, n_dev)
        return remote(formed.at[which, peer], states.at[which, me], back_send.at[which, step], back_recv.at[which, step], peer)

    def send_products(which):
        left, right, mask = ((1, 2, tail), (0, O_TYPE, head))[which]

        @pl.loop(0, n_dev, unroll=4)
        def _(dev):
            for sub in range(per_dev):
                rows = span((dev * per_dev + sub) * dim, dim)
                a = rows_ref[left, rows, :]
                b = jnp.where(mask, rows_ref[right, rows, :], zero)
                packed[which, dev, sub, 0:low, :] = (dot(a[0:low], jnp.concatenate([b, zero], axis=0), ROWS)
                                                     + dot(a[low:], jnp.concatenate([zero, b], axis=0), ROWS))
                packed[which, dev, sub, low:, :] = gate_ref[...]

        each(lambda step: out_copy(which, step).start())
        held[which, me] = packed[which, me]

    def form_states(which):
        each(lambda step: out_copy(which, step).wait_recv())

        def advance(step, state):
            block = step if which == 0 else n_dev - 1 - step
            formed[which, block] = state.astype(BF16)
            return held[0, block, :, low:low + 1, :] * state + held[which, block, :, 0:low, :]

        lax.fori_loop(0, n_dev, advance, jnp.zeros((per_dev, low, 2 * dim), F32))
        each(lambda step: back_copy(which, step).start())
        states[which, me] = formed[which, me]

    stream(TYPES, width // tile_rows, w_copy, project, loaded)
    send_products(1)
    push_tokens(SLOTS)

    seg_row = seg_row_ref[...]
    t_pos = lax.broadcasted_iota(jnp.int32, (half, tok), 0)
    s_pos = lax.broadcasted_iota(jnp.int32, (half, tok), 1)

    def pair(a, b):
        see_top = ((seg_col_ref[0:half, :] == seg_row) & (s_pos <= t_pos))[:, 0:half]
        see_low = (seg_col_ref[half:, :] == seg_row) & (s_pos <= t_pos + half)
        top = dot(a[:, 0:half], b[:, 0:half], OUTER)
        low = dot(a[:, half:], b, OUTER)
        return (jnp.where(see_top, top * scale, 0).astype(BF16), jnp.where(see_low, low * scale, 0).astype(BF16))

    def over_keys(at, rows_t, probs):
        total[at[0], at[1], 0:half] = dot(rows_t[:, 0:half], probs[0], ROWS)
        total[at[0], at[1], half:] = dot(rows_t, probs[1], ROWS)

    def over_queries(at, rows_t, probs):
        from_low = dot(rows_t[:, half:], probs[1], INNER)
        total[at[0], at[1], 0:half] = dot(rows_t[:, 0:half], probs[0], INNER) + from_low[:, 0:half]
        total[at[0], at[1], half:] = from_low[:, half:]

    def heads_of(grp):
        return [grp * (group // dim) + sub for sub in range(group // dim)]

    @pl.loop(0, n_group)
    def _(grp):
        @pl.when(grp == 2)
        def _():
            form_states(0)

        @pl.when(grp == n_group - 2)
        def _():
            form_states(1)

        @pl.when(lax.rem(grp, 2) == 1)
        def _():
            push_tokens(SLOTS + 1 + grp // 2)

        for index in heads_of(grp):
            rows = span(index * dim, dim)
            q, k, v, do = (rows_ref[kind, rows, :] for kind in range(TYPES))
            d_probs = pair(do, v)
            over_keys((0, rows), k, d_probs)
            over_queries((1, rows), q, d_probs)
            probs = pair(q, k)
            over_queries((2, rows), do, probs)
            over_keys((O_TYPE, rows), v, probs)

    for which in range(2):
        each(lambda step, which=which: back_copy(which, step).wait_recv())
    lane = lax.broadcasted_iota(jnp.int32, (low, 2 * dim), 1)

    def both_states(index):
        s_pair, r_pair = (states[which, index // per_dev, lax.rem(index, per_dev)].astype(F32) for which in range(2))
        first = jnp.where(lane < dim, s_pair, pltpu.roll(r_pair, dim, 1))
        second = jnp.where(lane < dim, pltpu.roll(s_pair, dim, 1), r_pair)
        return jnp.concatenate([first, second], axis=0).astype(BF16)

    def g_copy(grp):
        at = span(grp * group, group)
        return pltpu.make_async_copy(rows_ref.at[:, at], g_ref.at[:, at], g_sem.at[grp])

    @pl.loop(0, n_group)
    def _(grp):
        for index in heads_of(grp):
            rows = span(index * dim, dim)
            q, k, v, do = (rows_ref[kind, rows, :] for kind in range(TYPES))
            st = both_states(index)
            d_q = dot(st, jnp.concatenate([do, zero], axis=0), INNER)
            d_k = dot(st, jnp.concatenate([zero, v], axis=0), INNER)
            d_v = dot(st, k, OUTER)[dim:]
            out = dot(st, q, OUTER)[0:dim]
            for kind, mask, inter in ((0, head, d_q), (1, tail, d_k), (2, tail, d_v), (O_TYPE, head, out)):
                rows_ref[kind, rows, :] = (total[kind, rows, :] + jnp.where(mask, inter * scale, 0)).astype(BF16)
        g_copy(grp).start()

    pl.loop(0, n_group)(lambda grp: g_copy(grp).wait())
    for which in range(2):
        each(lambda step, which=which: out_copy(which, step).wait_send())
        each(lambda step, which=which: back_copy(which, step).wait_send())
    for ring in rings:
        for step in near_steps:
            @pl.loop(0, n_piece)
            def _(n, ring=ring, step=step):
                token_copy(ring, step, n)(x_ref).wait_send()

            @pl.loop(0, n_piece)
            def _(n, slot=CORES * step + ring.ring):
                at = span(n * piece, piece)
                remote(x_ref.at[at], z_ref.at[slot, at], side_sem.at[0], z_recv.at[slot, n], me).wait_recv()

    sibling_copy(rings[0])(x_ref).wait()


def front(flags, x_loc, dy_loc, weights, scale, n_dev, n_heads):
    tok, d_model = x_loc.shape
    width = weights[0].shape[0]
    dim = width // n_heads
    per_dev = n_heads // n_dev
    n_piece = PIECES - PUSH
    pack = (2, n_dev, per_dev, dim // 2 + 8, 2 * dim)
    back = (2, n_dev, per_dev, dim // 2, 2 * dim)
    return pl.pallas_call(
        functools.partial(front_kernel, scale, dim, PUSH),
        name='front',
        out_shape=(jax.ShapeDtypeStruct((TYPES, width, tok), BF16), jax.ShapeDtypeStruct((SLOTS, tok, d_model), BF16)),
        in_specs=[VMEM] + [ANY] * 6,
        out_specs=(ANY, ANY),
        scratch_shapes=[
            pltpu.VMEM((tok, 1), F32), pltpu.VMEM((1, tok), F32), pltpu.VMEM((1, tok), F32), pltpu.VMEM((1, tok), F32), pltpu.VMEM((8, 2 * dim), F32),
            pltpu.VMEM((2, tok, d_model), BF16), pltpu.VMEM((2, width // RING, d_model), BF16),
            pltpu.VMEM((TYPES, width, tok), BF16), pltpu.VMEM((TYPES, width, tok), F32),
            pltpu.VMEM(pack, F32), pltpu.VMEM(pack, F32), pltpu.VMEM(back, BF16), pltpu.VMEM(back, BF16),
            DMA((2,)), DMA((2,)), DMA((SLOTS,)), DMA((CORES, 2, n_piece)), DMA((SLOTS, n_piece)), DMA((2,)),
            DMA((2, n_dev)), DMA((2, n_dev)), DMA((2, n_dev)), DMA((2, n_dev))],
        compiler_params=pltpu.CompilerParams(collective_id=0, has_side_effects=True, vmem_limit_bytes=56 * MIB),
    )(flags[None, :], x_loc, dy_loc, *weights)


def row_products(g_ref, w_refs, y_ref, dx_ref, rows_in, rows_t, w_tile, total, g_sem, w_sem):
    width = rows_in.shape[1]
    cols = w_tile.shape[2]
    n_tile = total.shape[1] // cols
    step = width // 8
    order = (O_TYPE, 0, 1, 2)

    def g_copy(i):
        return pltpu.make_async_copy(g_ref.at[order[i]], rows_in.at[i % 2], g_sem.at[i % 2])

    def w_copy(i, n, slot):
        at = span(n * cols, cols)
        return pltpu.make_async_copy(w_refs[order[i]].at[:, at], w_tile.at[slot], w_sem.at[slot])

    def turned(i):
        if i + 1 < TYPES:
            g_copy(i + 1).start()
        g_copy(i).wait()

        @pl.loop(0, width // step)
        def _(b):
            at = span(b * step, step)
            rows_t[:, at] = jnp.transpose(rows_in[i % 2, at, :])

    def use(i, n, slot):
        at = span(n * cols, cols)
        prod = dot(rows_t[...], w_tile[slot], INNER)
        if i == 0:
            y_ref[:, at] = prod.astype(BF16)
        elif i == 1:
            total[:, at] = prod
        elif i + 1 < TYPES:
            total[:, at] = total[:, at] + prod
        else:
            dx_ref[:, at] = (total[:, at] + prod).astype(BF16)

    g_copy(0).start()
    stream(TYPES, n_tile, w_copy, use, turned)


def reduce_kernel(g_ref, z_ref, x_ref, dy_ref, wq_ref, wk_ref, wv_ref, wo_ref, out_ref, y_ref, dx_ref,
                  zbuf, rows_in, a_out, a_in, b_out, b_in, kind_rows, rows_t, w_tile, total, y_out, dx_out,
                  z_sem, far_send, rest_send, rest_sem, row_send, row_recv, a_send, a_recv, b_send, b_recv, g_sem, w_sem):
    me = lax.axis_index('sp')
    x, y, core = place(me)
    block = rows_in.shape[2]
    part = block // 2
    n_col, cols = a_out.shape[0], a_out.shape[3]
    rings = [Ring(ring, me) for ring in range(CORES)]
    order = (2, 1, RING - 1, 0)

    meet([index_of(x, y, 1 - core)] + [index_of(*chip, other) for other in range(CORES) for chip in chips_around(x, y)]
         + [ring.peer(2) + other - ring.ring for other in range(CORES) for ring in rings])

    def far_copy(ring):
        slot = 2 * CORES + ring.flip
        return lambda ref: remote(ref, zbuf.at[slot], far_send.at[ring.ring], z_sem.at[slot], ring.peer(2))

    def own_copy(ref):
        return pltpu.make_async_copy(ref, zbuf.at[0], z_sem.at[0])

    def near_copy(slot):
        at = pl.ds(0, kept if slot // CORES else tok)
        return pltpu.make_async_copy(z_ref.at[slot, at], zbuf.at[slot, at], z_sem.at[slot])

    near_slots = [slot for slot in range(1, SLOTS) if slot // CORES != 2]
    tok = zbuf.shape[1]
    kept = tok - tok * PUSH // PIECES
    rest = pl.ds(kept, tok - kept)

    def rest_copy(ring, step):
        slot = CORES * step + ring.flip
        return lambda ref: remote(ref.at[rest], zbuf.at[slot, rest], rest_send.at[ring.ring, step // 2], rest_sem.at[slot], ring.peer(step))
    for ring in rings:
        for step in (1, RING - 1):
            start_tokens(ring, step, x_ref, dy_ref, rest_copy(ring, step))
        start_tokens(ring, 2, x_ref, dy_ref, far_copy(ring))
    for ring in rings:
        @pl.when(ring.flip == 0)
        def _(ring=ring):
            start_tokens(ring, 0, x_ref, dy_ref, own_copy)
    for slot in near_slots:
        near_copy(slot).start()

    def row_source(ring, bi, step):
        first = (ring.ring * RING + lax.rem(ring.across + order[bi], RING)) * block
        return g_ref.at[ring.kind(step), span(first, block)]

    def row_copy(ring, bi, step):
        slot = CORES * step + ring.flip
        return remote(row_source(ring, bi, step), rows_in.at[slot, bi], row_send.at[ring.ring, bi, step],
                      row_recv.at[slot, bi], ring.peer(step))

    def own_rows(ring, bi):
        return pltpu.make_async_copy(row_source(ring, bi, 0), rows_in.at[0, bi], row_recv.at[0, bi])

    for bi in range(RING):
        for ring in rings:
            for step in (2, 1, RING - 1):
                row_copy(ring, bi, step).start()

            @pl.when(ring.flip == 1)
            def _(ring=ring, bi=bi):
                row_copy(ring, bi, 0).start()

            @pl.when(ring.flip == 0)
            def _(ring=ring, bi=bi):
                own_rows(ring, bi).start()

    def arrived(bi):
        for slot in range(SLOTS):
            pltpu.make_async_copy(g_ref.at[0, pl.ds(0, block)], rows_in.at[slot, bi], row_recv.at[slot, bi]).wait()

    def product(bi, ch):
        at = span(ch * cols, cols)
        total = dot(rows_in[0, bi], zbuf[0, :, at], INNER)
        for slot in range(1, SLOTS):
            total = total + dot(rows_in[slot, bi], zbuf[slot, :, at], INNER)
        return total

    across = [jnp.where(core == 0, index_of(x, y + step, core), index_of(x + step, y, core)) for step in (1, RING - 1)]

    def a_copy(ch, way):
        return remote(a_out.at[ch, way], a_in.at[ch, way], a_send.at[ch, way], a_recv.at[ch, way], across[way])

    def b_copy(ch, way):
        return remote(b_out.at[ch, way], b_in.at[ch, way], b_send.at[ch, way], b_recv.at[ch, way], across[way])

    row_products(g_ref, (wq_ref, wk_ref, wv_ref, wo_ref), y_out, dx_out, kind_rows, rows_t, w_tile, total, g_sem, w_sem)
    puts = [pltpu.make_async_copy(y_out, y_ref, g_sem.at[0]), pltpu.make_async_copy(dx_out, dx_ref, g_sem.at[1])]
    for put in puts:
        put.start()

    own_copy(x_ref).wait()
    for slot in near_slots:
        near_copy(slot).wait()
    for ring in rings:
        far_copy(ring)(x_ref).wait_recv()
        for step in (1, RING - 1):
            slot = CORES * step + ring.ring
            remote(x_ref.at[rest], zbuf.at[slot, rest], rest_send.at[0, 0], rest_sem.at[slot], me).wait_recv()

    def two_away(ch):
        total = product(0, ch)
        for way in range(2):
            a_out[ch, way] = total[way * part:(way + 1) * part]
            a_copy(ch, way).start()

    def next_to(way, ch):
        total = product(1 + way, ch)
        a_copy(ch, way).wait_recv()
        b_out[ch, way] = total
        b_out[ch, way, pl.ds(way * part, part)] += a_in[ch, way]
        b_copy(ch, way).start()

    def own(ch):
        total = product(RING - 1, ch)
        for way in range(2):
            b_copy(ch, way).wait_recv()
            total = total + b_in[ch, way]
        out_ref[:, span(ch * cols, cols)] = total

    for bi, step in enumerate((two_away, functools.partial(next_to, 0), functools.partial(next_to, 1), own)):
        arrived(bi)
        pl.loop(0, n_col)(step)

    for put in puts:
        put.wait()
    for ring in rings:
        far_copy(ring)(x_ref).wait_send()
        for step in (1, RING - 1):
            rest_copy(ring, step)(x_ref).wait_send()
        for bi in range(RING):
            for step in range(1, RING):
                row_copy(ring, bi, step).wait_send()

            @pl.when(ring.flip == 1)
            def _(ring=ring, bi=bi):
                row_copy(ring, bi, 0).wait_send()

    for ch in range(n_col):
        for way in range(2):
            a_copy(ch, way).wait_send()
            b_copy(ch, way).wait_send()


def reduce_rows(g, z, x_loc, dy_loc, weights):
    width, tok = g.shape[1], g.shape[2]
    d_model = x_loc.shape[1]
    block = width // SLOTS
    n_col = RING
    part = (n_col, 2, block // 2, d_model // n_col)
    full = (n_col, 2, block, d_model // n_col)
    return pl.pallas_call(
        reduce_kernel,
        name='reduce_rows',
        out_shape=(pltpu.VMEM((block, d_model), F32), jax.ShapeDtypeStruct((tok, d_model), BF16), jax.ShapeDtypeStruct((tok, d_model), BF16)),
        in_specs=[ANY] * 8,
        out_specs=(VMEM, ANY, ANY),
        scratch_shapes=[
            pltpu.VMEM((SLOTS, tok, d_model), BF16), pltpu.VMEM((SLOTS, RING, block, tok), BF16),
            pltpu.VMEM(part, F32), pltpu.VMEM(part, F32), pltpu.VMEM(full, F32), pltpu.VMEM(full, F32),
            pltpu.VMEM((2, width, tok), BF16), pltpu.VMEM((tok, width), BF16), pltpu.VMEM((2, width, min(256, d_model // 2)), BF16),
            pltpu.VMEM((tok, d_model), F32), pltpu.VMEM((tok, d_model), BF16), pltpu.VMEM((tok, d_model), BF16),
            DMA((SLOTS,)), DMA((CORES,)), DMA((CORES, 2)), DMA((SLOTS,)), DMA((CORES, RING, RING)), DMA((SLOTS, RING)),
            DMA((n_col, 2)), DMA((n_col, 2)), DMA((n_col, 2)), DMA((n_col, 2)), DMA((2,)), DMA((2,))],
        compiler_params=pltpu.CompilerParams(collective_id=1, has_side_effects=True, vmem_limit_bytes=58 * MIB),
    )(g, z, x_loc, dy_loc, *weights)


def gather_kernel(piece_ref, near_ref, far_a_ref, far_b_ref, send_sem, recv_sem, side_send, side_recv):
    me = lax.axis_index('sp')
    x, y, core = place(me)
    rows = piece_ref.shape[0]
    part = rows // 2
    quarter = part // 2

    def number(leg, i, j, plane):
        sx, sy = (i, j) if leg == 0 else (j, i)
        px, py = lax.rem(x + sx, RING), lax.rem(y + sy, RING)
        return jnp.where(plane == 0, px * RING + py, py * RING + px)

    def spot(leg, i, j, half=None):
        lo, size = (0, part) if half is None else (half * quarter, quarter)
        return near_ref.at[pl.ds(pl.multiple_of(number(leg, i, j, core) * rows + leg * part + lo, quarter), size)]

    def far_spot(leg, i, j, plane):
        return (far_a_ref, far_b_ref)[leg].at[span(number(leg, i, j, plane) * part, part)]

    def own(leg, half=None):
        lo, size = (0, part) if half is None else (half * quarter, quarter)
        return piece_ref.at[pl.ds(leg * part + lo, size)]

    def step_peer(leg, second, step):
        along_x = (leg == 0) != second
        return index_of(x + step, y, core) if along_x else index_of(x, y + step, core)

    started = []

    def push(leg, second, i, j, step, half):
        there = (i, (j - step) % RING) if second else ((i - step) % RING, j)
        src = own(leg, half) if i == 0 and j == 0 else spot(leg, i, j, half)
        copy = remote(src, spot(leg, i, j, half), send_sem.at[len(started)],
                      recv_sem.at[leg, there[0], there[1], half or 0], step_peer(leg, second, step))
        copy.start()
        started.append(copy)

    def landed(leg, i, j):
        in_halves = j == 2 or (j == 0 and i == 2)
        for half in ((0, 1) if in_halves else (None,)):
            here = spot(leg, i, j, half)
            remote(here, here, send_sem.at[0], recv_sem.at[leg, i, j, half or 0], me).wait_recv()

    side = []

    def to_sibling(leg, i, j):
        src = own(leg) if i == 0 and j == 0 else spot(leg, i, j)
        copy = remote(src, far_spot(leg, i, j, core), side_send.at[leg, i, j], side_recv.at[leg, i, j],
                      index_of(x, y, 1 - core))
        copy.start()
        side.append(copy)

    meet([index_of(x, y, 1 - core)] + [index_of(*chip, core) for chip in chips_around(x, y)])

    def spread(leg, i):
        push(leg, True, i, 0, 1, None)
        push(leg, True, i, 0, 3, None)
        to_sibling(leg, i, 0)

    for leg in range(2):
        push(leg, False, 0, 0, 1, None)
        push(leg, False, 0, 0, 3, None)
    for leg in range(2):
        spread(leg, 0)
    near_ref[span(number(0, 0, 0, core) * rows, rows), :] = piece_ref[...]

    for leg in range(2):
        landed(leg, 3, 0)
        push(leg, False, 3, 0, 1, 0)
        spread(leg, 3)
        landed(leg, 1, 0)
        push(leg, False, 1, 0, 3, 1)
        spread(leg, 1)

    def second_near(leg, i):
        landed(leg, i, 3)
        push(leg, True, i, 3, 1, 0)
        to_sibling(leg, i, 3)
        landed(leg, i, 1)
        push(leg, True, i, 1, 3, 1)
        to_sibling(leg, i, 1)

    for leg in range(2):
        second_near(leg, 0)
    for leg in range(2):
        landed(leg, 2, 0)
        spread(leg, 2)
    for i in (3, 1, 2):
        for leg in range(2):
            second_near(leg, i)
    for i in (0, 3, 1, 2):
        for leg in range(2):
            landed(leg, i, 2)
            to_sibling(leg, i, 2)

    for copy in started + side:
        copy.wait_send()

    for leg in range(2):
        for i in range(RING):
            for j in range(RING):
                here = far_spot(leg, i, j, 1 - core)
                remote(here, here, side_send.at[leg, i, j], side_recv.at[leg, i, j], me).wait_recv()


def gather_rows(piece, n_dev):
    rows, d_model = piece.shape
    half = n_dev * rows // CORES
    return pl.pallas_call(
        gather_kernel,
        name='gather_rows',
        out_shape=(pltpu.VMEM((half, d_model), F32), pltpu.VMEM((half // 2, d_model), F32), jax.ShapeDtypeStruct((half // 2, d_model), F32)),
        in_specs=[VMEM],
        out_specs=(VMEM, VMEM, ANY),
        scratch_shapes=[DMA((40,)), DMA((2, RING, RING, 2)), DMA((2, RING, RING)), DMA((2, RING, RING))],
        compiler_params=pltpu.CompilerParams(collective_id=2, has_side_effects=True, vmem_limit_bytes=STORE_LIMIT),
    )(piece)


def store_kernel(near_ref, far_a_ref, far_b_ref, dq_out, dk_out, dv_out, do_out, tile, put_sem, side_sem, in_sem, out_sem):
    core = lax.rem(lax.axis_index('sp'), CORES)
    outs = (dq_out, dk_out, dv_out, do_out)
    rows = near_ref.shape[0] // TYPES
    n_slot, chunk = tile.shape[0], tile.shape[1]
    n = far_b_ref.shape[0] // chunk

    def far_out(i, leg):
        first = (1 - core) * rows + (i % RING * 2 + leg) * chunk
        return outs[i // RING].at[pl.ds(pl.multiple_of(first, chunk), chunk)]

    puts = [pltpu.make_async_copy(near_ref.at[pl.ds(kind * rows, rows)], outs[kind].at[span(core * rows, rows)], put_sem.at[kind])
            for kind in range(TYPES)]
    puts += [pltpu.make_async_copy(far_a_ref.at[pl.ds(i * chunk, chunk)], far_out(i, 0), side_sem.at[i]) for i in range(n)]

    def load(i):
        return pltpu.make_async_copy(far_b_ref.at[pl.ds(i * chunk, chunk)], tile.at[i % n_slot], in_sem.at[i % n_slot])

    def save(i):
        return pltpu.make_async_copy(tile.at[i % n_slot], far_out(i, 1), out_sem.at[i % n_slot])

    ahead = n_slot // 2
    for i in range(ahead):
        load(i).start()
    for put in puts:
        put.start()
    for i in range(n):
        load(i).wait()
        save(i).start()
        if i + ahead < n:
            if i + ahead >= n_slot:
                save(i + ahead - n_slot).wait()
            load(i + ahead).start()
    for i in range(n - n_slot, n):
        save(i).wait()
    for put in puts:
        put.wait()


def store(near, far_a, far_b):
    half, d_model = near.shape
    n = RING * RING
    chunk = far_b.shape[0] // n
    grad = jax.ShapeDtypeStruct((half * CORES // TYPES, d_model), F32)
    return pl.pallas_call(
        store_kernel,
        name='store',
        out_shape=(grad,) * TYPES,
        in_specs=[VMEM, VMEM, ANY],
        out_specs=(ANY,) * TYPES,
        scratch_shapes=[pltpu.VMEM((8, chunk, d_model), F32), DMA((TYPES,)), DMA((n,)), DMA((8,)), DMA((8,))],
        compiler_params=pltpu.CompilerParams(vmem_limit_bytes=STORE_LIMIT),
    )(in_vmem(near), in_vmem(far_a), pltpu.with_memory_space_constraint(far_b, pltpu.HBM))


def solution(mesh):
    n_dev = mesh.shape['sp']
    assert n_dev == CORES * RING * RING

    def device_body(x_loc, flag_loc, w_q, w_k, w_v, w_o, dy_loc):
        tok_count, d_model = x_loc.shape
        n_heads, head_dim = w_q.shape[1], w_q.shape[2]
        width = n_heads * head_dim
        score_scale = 1.0 / (math.sqrt(head_dim) * tok_count)
        weights = [w.transpose(1, 2, 0).reshape(width, d_model) for w in (w_q, w_k, w_v)] + [w_o.reshape(width, d_model)]
        g, z = front(flag_loc, x_loc, dy_loc, weights, score_scale, n_dev, n_heads)
        piece, y_loc, dx_loc = reduce_rows(g, z, x_loc, dy_loc, weights)
        grads = store(*gather_rows(piece, n_dev))
        dw_q, dw_k, dw_v, dw_o = (grad.reshape(n_heads, head_dim, d_model) for grad in grads)
        return y_loc, dx_loc, dw_q.transpose(2, 0, 1), dw_k.transpose(2, 0, 1), dw_v.transpose(2, 0, 1), dw_o

    row_spec = P(('dp', 'sp'), None)
    flag_spec = P(('dp', 'sp'))
    w_spec = P(None, None, None)
    dw_spec = P('dp', None, None)
    return jax.shard_map(device_body, mesh=mesh,
                         in_specs=(row_spec, flag_spec, w_spec, w_spec, w_spec, w_spec, row_spec),
                         out_specs=(row_spec, row_spec, dw_spec, dw_spec, dw_spec, dw_spec),
                         check_vma=False)
```

```python
import functools
import math
import jax
import jax.numpy as jnp
from jax import lax
from jax.experimental import pallas as pl
from jax.experimental.pallas import tpu as pltpu
from jax.sharding import PartitionSpec as P

MESH = pl.DeviceIdType.MESH
CORES = 2
RING = 4
SLOTS = CORES * RING
TYPES = 4
O_TYPE = TYPES - 1
MIB = 1024 * 1024
STORE_LIMIT = 9 * MIB
BF16 = jnp.bfloat16
F32 = jnp.float32
ROWS = ((1,), (1,))
INNER = ((1,), (0,))
OUTER = ((0,), (0,))
VMEM = pl.BlockSpec(memory_space=pltpu.VMEM)
ANY = pl.BlockSpec(memory_space=pltpu.HBM)
DMA = pltpu.SemaphoreType.DMA


def place(me):
    core = lax.rem(me, CORES)
    chip = me // CORES
    return lax.rem(chip, RING), chip // RING, core


def index_of(x, y, core):
    return (lax.rem(y, RING) * RING + lax.rem(x, RING)) * CORES + core


def remote(src, dst, send_sem, recv_sem, peer):
    return pltpu.make_async_remote_copy(src_ref=src, dst_ref=dst, send_sem=send_sem, recv_sem=recv_sem,
                                        device_id={'sp': peer}, device_id_type=MESH)


def signal(peer):
    pl.semaphore_signal(pltpu.get_barrier_semaphore(), inc=1, device_id={'sp': peer}, device_id_type=MESH)


def meet(peers):
    for peer in peers:
        signal(peer)
    pl.semaphore_wait(pltpu.get_barrier_semaphore(), len(peers))


def chips_around(x, y):
    return ((x + 1, y), (x + RING - 1, y), (x, y + 1), (x, y + RING - 1))


def dot(a, b, dims):
    return lax.dot_general(a, b, (dims, ((), ())), preferred_element_type=F32)


def in_vmem(value):
    return pltpu.with_memory_space_constraint(value, pltpu.VMEM)


def span(start, size):
    return pl.ds(pl.multiple_of(start, size), size)


def stream(n_outer, n_inner, depth, copy, use, before):
    ahead = depth - 1
    for n in range(ahead):
        copy(0, n, n).start()
    for i in range(n_outer):
        before(i)

        @pl.loop(0, n_inner)
        def _(n):
            at = i * n_inner + n
            slot, free = lax.rem(at, depth), lax.rem(at + ahead, depth)

            @pl.when(n + ahead < n_inner)
            def _():
                copy(i, n + ahead, free).start()

            if i + 1 < n_outer:
                @pl.when(n + ahead >= n_inner)
                def _():
                    copy(i + 1, n + ahead - n_inner, free).start()

            copy(i, n, slot).wait()
            use(i, n, slot)


def form_masks(flag_ref, seg_col_ref, seg_row_ref, head_ref, tail_ref, gate_ref):
    tok = flag_ref.shape[1]
    flags = flag_ref[...] > 0
    t_pos = lax.broadcasted_iota(jnp.int32, (tok, tok), 0)
    s_pos = lax.broadcasted_iota(jnp.int32, (tok, tok), 1)
    seg_col = jnp.sum(jnp.where(flags & (s_pos <= t_pos), 1.0, 0), axis=1, keepdims=True)
    seg_col_ref[...] = seg_col
    seg_row_ref[...] = jnp.sum(jnp.where(s_pos == t_pos, seg_col, 0), axis=0, keepdims=True)
    positions = lax.broadcasted_iota(jnp.int32, (1, tok), 1).astype(F32)
    first_pos = jnp.min(jnp.where(flags, positions, tok), axis=1, keepdims=True)
    last_pos = jnp.max(jnp.where(flags, positions, -1), axis=1, keepdims=True)
    head_ref[...] = jnp.where(positions < first_pos, 1.0, 0)
    tail_ref[...] = jnp.where(positions >= last_pos, 1.0, 0)
    gate_ref[...] = jnp.broadcast_to(jnp.where(last_pos < 0, 1.0, 0), gate_ref.shape)


class Square:
    def __init__(self, me):
        x, y, core = place(me)
        across_x, across_y = (lax.rem(a + 1 + RING - 2 * lax.rem(a + core, 2), RING) for a in (x, y))
        self.core = core
        self.chips = [(x, y), (across_x, y), (x, across_y), (across_x, across_y)]

    def peer(self, k):
        return index_of(*self.chips[k], self.core)

    def kind(self, k):
        return owned_type(*self.chips[k])


def owned_type(x, y):
    return lax.rem(x, 2) + 2 * lax.rem(y, 2)


def lattice(x, y):
    return lax.rem(x // 2, 2), lax.rem(y // 2, 2)


def start_tokens(kind, x_ref, dy_ref, copy):
    @pl.when(kind == O_TYPE)
    def _():
        copy(dy_ref).start()

    @pl.when(kind != O_TYPE)
    def _():
        copy(x_ref).start()


def front_kernel(scale, dim, flag_ref, x_ref, dy_ref, wq_ref, wk_ref, wv_ref, wo_ref,
                 g_ref, z_ref, seg_col_ref, seg_row_ref, head_ref, tail_ref, gate_ref, tok_in, w_tile, rows_ref, total,
                 packed, held, formed, states,
                 tok_sem, w_sem, g_sem, z_send, z_recv, send_sem, recv_sem, back_send, back_recv):
    me = lax.axis_index('sp')
    n_dev, per_dev, low = formed.shape[1:4]
    width, tok = rows_ref.shape[1], rows_ref.shape[2]
    half = tok // 2
    n_piece = z_recv.shape[1]
    piece = tok // n_piece
    n_group = SLOTS
    group = width // n_group
    tile_rows = w_tile.shape[1]

    @pl.loop(1, n_dev)
    def _(step):
        signal(lax.rem(me + step, n_dev))

    loads = [pltpu.make_async_copy(ref, tok_in.at[i], tok_sem.at[i]) for i, ref in enumerate((x_ref, dy_ref))]
    for load in loads:
        load.start()

    square = Square(me)

    def token_copy(k, n):
        at = span(n * piece, piece)
        return lambda ref: remote(ref.at[at], z_ref.at[k - 1, at], z_send.at[k - 1, n], z_recv.at[k - 1, n], square.peer(k))

    def push_tokens(n):
        for k in range(1, TYPES):
            start_tokens(square.kind(k), x_ref, dy_ref, token_copy(k, n))

    form_masks(flag_ref, seg_col_ref, seg_row_ref, head_ref, tail_ref, gate_ref)
    pl.semaphore_wait(pltpu.get_barrier_semaphore(), n_dev - 1)
    push_tokens(0)

    weights = (wk_ref, wv_ref, wq_ref, wo_ref)
    kinds = (1, 2, 0, O_TYPE)

    def w_copy(i, n, slot):
        return pltpu.make_async_copy(weights[i].at[span(n * tile_rows, tile_rows)], w_tile.at[slot], w_sem.at[slot])

    def project(i, n, slot):
        rows_ref[kinds[i], span(n * tile_rows, tile_rows), :] = dot(w_tile[slot], tok_in[i // O_TYPE], ROWS).astype(BF16)

    def loaded(i):
        if i in (0, O_TYPE):
            loads[i // O_TYPE].wait()
        if i == 2:
            send_products(0)
        if i:
            push_tokens(i)

    head = head_ref[...] > 0.5
    tail = tail_ref[...] > 0.5
    zero = jnp.zeros((dim, tok), BF16)

    def each(do):
        pl.loop(1, n_dev)(do)

    def out_copy(which, step):
        peer = lax.rem(me + step, n_dev)
        at = pl.ds(0, packed.shape[3] if which == 0 else low)
        return remote(packed.at[which, peer, :, at], held.at[which, me, :, at], send_sem.at[which, step], recv_sem.at[which, step], peer)

    def back_copy(which, step):
        peer = lax.rem(me + step, n_dev)
        return remote(formed.at[which, peer], states.at[which, me], back_send.at[which, step], back_recv.at[which, step], peer)

    def send_products(which):
        left, right, mask = ((1, 2, tail), (0, O_TYPE, head))[which]

        @pl.loop(0, n_dev, unroll=4)
        def _(dev):
            for sub in range(per_dev):
                rows = span((dev * per_dev + sub) * dim, dim)
                a = rows_ref[left, rows, :]
                b = jnp.where(mask, rows_ref[right, rows, :], zero)
                packed[which, dev, sub, 0:low, :] = (dot(a[0:low], jnp.concatenate([b, zero], axis=0), ROWS)
                                                     + dot(a[low:], jnp.concatenate([zero, b], axis=0), ROWS))
                packed[which, dev, sub, low:, :] = gate_ref[...]

        each(lambda step: out_copy(which, step).start())
        held[which, me] = packed[which, me]

    def form_states(which):
        each(lambda step: out_copy(which, step).wait_recv())

        def advance(step, state):
            block = step if which == 0 else n_dev - 1 - step
            formed[which, block] = state.astype(BF16)
            return held[0, block, :, low:low + 1, :] * state + held[which, block, :, 0:low, :]

        lax.fori_loop(0, n_dev, advance, jnp.zeros((per_dev, low, 2 * dim), F32))
        each(lambda step: back_copy(which, step).start())
        states[which, me] = formed[which, me]

    stream(TYPES, width // tile_rows, w_tile.shape[0], w_copy, project, loaded)
    send_products(1)
    push_tokens(TYPES)

    seg_row = seg_row_ref[...]
    t_pos = lax.broadcasted_iota(jnp.int32, (half, tok), 0)
    s_pos = lax.broadcasted_iota(jnp.int32, (half, tok), 1)

    def pair(a, b):
        see_top = ((seg_col_ref[0:half, :] == seg_row) & (s_pos <= t_pos))[:, 0:half]
        see_low = (seg_col_ref[half:, :] == seg_row) & (s_pos <= t_pos + half)
        top = dot(a[:, 0:half], b[:, 0:half], OUTER)
        low = dot(a[:, half:], b, OUTER)
        return (jnp.where(see_top, top * scale, 0).astype(BF16), jnp.where(see_low, low * scale, 0).astype(BF16))

    def over_keys(at, rows_t, probs):
        total[at[0], at[1], 0:half] = dot(rows_t[:, 0:half], probs[0], ROWS)
        total[at[0], at[1], half:] = dot(rows_t, probs[1], ROWS)

    def over_queries(at, rows_t, probs):
        from_low = dot(rows_t[:, half:], probs[1], INNER)
        total[at[0], at[1], 0:half] = dot(rows_t[:, 0:half], probs[0], INNER) + from_low[:, 0:half]
        total[at[0], at[1], half:] = from_low[:, half:]

    def heads_of(grp):
        return [grp * (group // dim) + sub for sub in range(group // dim)]

    @pl.loop(0, n_group)
    def _(grp):
        @pl.when(grp == 2)
        def _():
            form_states(0)

        @pl.when(grp == n_group - 2)
        def _():
            form_states(1)

        @pl.when((lax.rem(grp, 2) == 1) & (grp < n_group - 1))
        def _():
            push_tokens(TYPES + 1 + grp // 2)

        for index in heads_of(grp):
            rows = span(index * dim, dim)
            q, k, v, do = (rows_ref[kind, rows, :] for kind in range(TYPES))
            d_probs = pair(do, v)
            over_keys((0, rows), k, d_probs)
            over_queries((1, rows), q, d_probs)
            probs = pair(q, k)
            over_queries((2, rows), do, probs)
            over_keys((O_TYPE, rows), v, probs)

    for which in range(2):
        each(lambda step, which=which: back_copy(which, step).wait_recv())
    lane = lax.broadcasted_iota(jnp.int32, (low, 2 * dim), 1)

    def both_states(index):
        s_pair, r_pair = (states[which, index // per_dev, lax.rem(index, per_dev)].astype(F32) for which in range(2))
        first = jnp.where(lane < dim, s_pair, pltpu.roll(r_pair, dim, 1))
        second = jnp.where(lane < dim, pltpu.roll(s_pair, dim, 1), r_pair)
        return jnp.concatenate([first, second], axis=0).astype(BF16)

    def g_copy(grp):
        at = span(grp * group, group)
        return pltpu.make_async_copy(rows_ref.at[:, at], g_ref.at[:, at], g_sem.at[grp])

    @pl.loop(0, n_group)
    def _(grp):
        for index in heads_of(grp):
            rows = span(index * dim, dim)
            q, k, v, do = (rows_ref[kind, rows, :] for kind in range(TYPES))
            st = both_states(index)
            d_q = dot(st, jnp.concatenate([do, zero], axis=0), INNER)
            d_k = dot(st, jnp.concatenate([zero, v], axis=0), INNER)
            d_v = dot(st, k, OUTER)[dim:]
            out = dot(st, q, OUTER)[0:dim]
            for kind, mask, inter in ((0, head, d_q), (1, tail, d_k), (2, tail, d_v), (O_TYPE, head, out)):
                rows_ref[kind, rows, :] = (total[kind, rows, :] + jnp.where(mask, inter * scale, 0)).astype(BF16)
        g_copy(grp).start()

    pl.loop(0, n_group)(lambda grp: g_copy(grp).wait())
    for which in range(2):
        each(lambda step, which=which: out_copy(which, step).wait_send())
        each(lambda step, which=which: back_copy(which, step).wait_send())
    for k in range(1, TYPES):
        pl.loop(0, n_piece)(lambda n, k=k: token_copy(k, n)(x_ref).wait())


def front(flags, x_loc, dy_loc, weights, scale, n_dev, n_heads):
    tok, d_model = x_loc.shape
    width = weights[0].shape[0]
    dim = width // n_heads
    per_dev = n_heads // n_dev
    n_piece = SLOTS
    pack = (2, n_dev, per_dev, dim // 2 + 8, 2 * dim)
    back = (2, n_dev, per_dev, dim // 2, 2 * dim)
    return pl.pallas_call(
        functools.partial(front_kernel, scale, dim),
        name='front',
        out_shape=(jax.ShapeDtypeStruct((TYPES, width, tok), BF16), jax.ShapeDtypeStruct((TYPES - 1, tok, d_model), BF16)),
        in_specs=[VMEM] + [ANY] * 6,
        out_specs=(ANY, ANY),
        scratch_shapes=[
            pltpu.VMEM((tok, 1), F32), pltpu.VMEM((1, tok), F32), pltpu.VMEM((1, tok), F32), pltpu.VMEM((1, tok), F32), pltpu.VMEM((8, 2 * dim), F32),
            pltpu.VMEM((2, tok, d_model), BF16), pltpu.VMEM((4, width // RING, d_model), BF16),
            pltpu.VMEM((TYPES, width, tok), BF16), pltpu.VMEM((TYPES, width, tok), F32),
            pltpu.VMEM(pack, F32), pltpu.VMEM(pack, F32), pltpu.VMEM(back, BF16), pltpu.VMEM(back, BF16),
            DMA((2,)), DMA((4,)), DMA((SLOTS,)), DMA((TYPES - 1, n_piece)), DMA((TYPES - 1, n_piece)),
            DMA((2, n_dev)), DMA((2, n_dev)), DMA((2, n_dev)), DMA((2, n_dev))],
        compiler_params=pltpu.CompilerParams(collective_id=0, has_side_effects=True, vmem_limit_bytes=56 * MIB),
    )(flags[None, :], x_loc, dy_loc, *weights)


def row_products(g_ref, w_refs, y_ref, dx_ref, rows_in, rows_t, w_tile, total, done, g_sem, w_sem, put_sem):
    width = rows_in.shape[0]
    cols = w_tile.shape[2]
    n_tile = total.shape[1] // cols
    step = width // SLOTS
    order = (O_TYPE, 0, 1, 2)

    def g_copy(i):
        return pltpu.make_async_copy(g_ref.at[order[i]], rows_in, g_sem)

    def w_copy(i, n, slot):
        return pltpu.make_async_copy(w_refs[order[i]].at[:, span(n * cols, cols)], w_tile.at[slot], w_sem.at[slot])

    puts = [pltpu.make_async_copy(done, ref, put_sem) for ref in (y_ref, dx_ref)]

    def turned(i):
        if i == 1:
            puts[0].start()
        if i == O_TYPE:
            puts[0].wait()
        g_copy(i).wait()

        @pl.loop(0, width // step)
        def _(b):
            at = span(b * step, step)
            rows_t[:, at] = jnp.transpose(rows_in[at, :])

        if i < O_TYPE:
            g_copy(i + 1).start()

    def use(i, n, slot):
        at = span(n * cols, cols)
        prod = dot(rows_t[...], w_tile[slot], INNER)
        if i == 0:
            done[:, at] = prod.astype(BF16)
        elif i == 1:
            total[:, at] = prod
        elif i < O_TYPE:
            total[:, at] = total[:, at] + prod
        else:
            done[:, at] = (total[:, at] + prod).astype(BF16)

    g_copy(0).start()
    stream(TYPES, n_tile, w_tile.shape[0], w_copy, use, turned)
    puts[1].start()
    return puts[1]


FLIPS = ((1, 1), (1, 0), (0, 1), (0, 0))


def reduce_kernel(g_ref, z_ref, x_ref, dy_ref, wq_ref, wk_ref, wv_ref, wo_ref, out_ref, y_ref, dx_ref,
                  zbuf, rows_in, side_out, side_in, first_out, first_in, second_out, second_in, kind_rows, rows_t, w_tile, sums, done,
                  z_sem, row_send, row_recv, side_send, side_recv, first_send, first_recv, second_send, second_recv, g_sem, w_sem, put_sem):
    me = lax.axis_index('sp')
    x, y, core = place(me)
    square = Square(me)
    block = rows_in.shape[3]
    part = block // 2
    n_col, cols = second_out.shape[1], second_out.shape[3]
    sibling = index_of(x, y, 1 - core)
    across = (index_of(x + 2, y, core), index_of(x, y + 2, core))

    meet([sibling, *across] + [square.peer(k) for k in range(1, TYPES)])

    def own_copy(ref):
        return pltpu.make_async_copy(ref, zbuf.at[0], z_sem.at[0])

    z_copies = [pltpu.make_async_copy(z_ref.at[k - 1], zbuf.at[k], z_sem.at[k]) for k in range(1, TYPES)]

    def row_source(k, mine, t):
        px, py = lattice(*square.chips[k])
        half = core if mine else 1 - core
        index = half * RING + lax.rem(px + FLIPS[t][0], 2) + 2 * lax.rem(py + FLIPS[t][1], 2)
        return g_ref.at[square.kind(k), span(index * block, block)]

    def row_copy(k, mine, t):
        dst, recv = rows_in.at[k, mine, t], row_recv.at[k, mine, t]
        if k == 0:
            return pltpu.make_async_copy(row_source(k, mine, t), dst, recv)
        return remote(row_source(k, mine, t), dst, row_send.at[k - 1, mine, t], recv, square.peer(k))

    every_row = [(k, mine, t) for t in range(TYPES) for mine in range(2) for k in range(TYPES)]
    for where in every_row:
        row_copy(*where).start()
    start_tokens(square.kind(0), x_ref, dy_ref, own_copy)
    for copy in z_copies:
        copy.start()

    last_put = row_products(g_ref, (wq_ref, wk_ref, wv_ref, wo_ref), y_ref, dx_ref, kind_rows, rows_t, w_tile, sums, done, g_sem, w_sem, put_sem)

    own_copy(x_ref).wait()
    for copy in z_copies:
        copy.wait()

    def product(mine, t, ch):
        at = span(ch * cols, cols)
        total = dot(rows_in[0, mine, t], zbuf[0, :, at], INNER)
        for k in range(1, TYPES):
            total = total + dot(rows_in[k, mine, t], zbuf[k, :, at], INNER)
        return total

    def side_copy(t, ch):
        return remote(side_out.at[t % 2, ch], side_in.at[t, ch], side_send.at[t, ch], side_recv.at[t, ch], sibling)

    def first_copy(leg, q, ch):
        return remote(first_out.at[leg, q, ch], first_in.at[leg, q, ch], first_send.at[leg, q, ch], first_recv.at[leg, q, ch], across[leg])

    def second_copy(leg, ch):
        return remote(second_out.at[leg, ch], second_in.at[leg, ch], second_send.at[leg, ch], second_recv.at[leg, ch], across[1 - leg])

    for t in range(TYPES):
        for mine in range(2):
            for k in range(TYPES):
                copy = row_copy(k, mine, t)
                if k:
                    copy.wait_recv()
                else:
                    copy.wait()

        @pl.loop(0, n_col)
        def _(ch, t=t):
            if t >= 2:
                side_copy(t - 2, ch).wait_send()
            side_out[t % 2, ch] = product(0, t, ch)
            side_copy(t, ch).start()

        @pl.loop(0, n_col)
        def _(ch, t=t):
            total = product(1, t, ch)
            side_copy(t, ch).wait_recv()
            total = total + side_in[t, ch]
            for leg in range(2):
                half = total[leg * part:(leg + 1) * part]
                step, other = FLIPS[t][leg], FLIPS[t][1 - leg]
                if step:
                    first_out[leg, other, ch] = half
                    first_copy(leg, other, ch).start()
                    continue
                first_copy(leg, other, ch).wait_recv()
                half = half + first_in[leg, other, ch]
                if other:
                    second_out[leg, ch] = half
                    second_copy(leg, ch).start()
                else:
                    second_copy(leg, ch).wait_recv()
                    out_ref[leg * part:(leg + 1) * part, span(ch * cols, cols)] = half + second_in[leg, ch]

    last_put.wait()
    for where in every_row:
        if where[0]:
            row_copy(*where).wait_send()

    @pl.loop(0, n_col)
    def _(ch):
        for t in range(2, TYPES):
            side_copy(t, ch).wait_send()
        for leg in range(2):
            for q in range(2):
                first_copy(leg, q, ch).wait_send()
            second_copy(leg, ch).wait_send()


def reduce_rows(g, z, x_loc, dy_loc, weights):
    width, tok = g.shape[1], g.shape[2]
    d_model = x_loc.shape[1]
    block = width // SLOTS
    n_col = RING
    cols = d_model // n_col
    tokens = jax.ShapeDtypeStruct((tok, d_model), BF16)
    halves = lambda *lead: pltpu.VMEM((*lead, n_col, block // 2, cols), F32)
    blocks = lambda lead: pltpu.VMEM((lead, n_col, block, cols), F32)
    return pl.pallas_call(
        reduce_kernel,
        name='reduce_rows',
        out_shape=(pltpu.VMEM((block, d_model), F32), tokens, tokens),
        in_specs=[ANY] * 8,
        out_specs=(VMEM, ANY, ANY),
        scratch_shapes=[
            pltpu.VMEM((TYPES, tok, d_model), BF16), pltpu.VMEM((TYPES, 2, TYPES, block, tok), BF16),
            blocks(2), blocks(TYPES), halves(2, 2), halves(2, 2), halves(2), halves(2),
            pltpu.VMEM((width, tok), BF16), pltpu.VMEM((tok, width), BF16), pltpu.VMEM((3, width, min(256, d_model // 4)), BF16),
            pltpu.VMEM((tok, d_model), F32), pltpu.VMEM((tok, d_model), BF16),
            DMA((TYPES,)), DMA((TYPES - 1, 2, TYPES)), DMA((TYPES, 2, TYPES)), DMA((TYPES, n_col)), DMA((TYPES, n_col)),
            DMA((2, 2, n_col)), DMA((2, 2, n_col)), DMA((2, n_col)), DMA((2, n_col)), DMA, DMA((3,)), DMA],
        compiler_params=pltpu.CompilerParams(collective_id=1, has_side_effects=True, vmem_limit_bytes=58 * MIB),
    )(g, z, x_loc, dy_loc, *weights)


def gather_kernel(piece_ref, near_ref, far_a_ref, far_b_ref, send_sem, recv_sem, side_send, side_recv):
    me = lax.axis_index('sp')
    x, y, core = place(me)
    rows = piece_ref.shape[0]
    part = rows // 2
    quarter = part // 2

    def number(leg, i, j):
        sx, sy = (i, j) if leg == 0 else (j, i)
        px, py = lax.rem(x + sx, RING), lax.rem(y + sy, RING)
        lx, ly = lattice(px, py)
        return owned_type(px, py) * RING + lx + 2 * ly

    def spot(leg, i, j, half=None):
        lo, size = (0, part) if half is None else (half * quarter, quarter)
        return near_ref.at[pl.ds(pl.multiple_of(number(leg, i, j) * rows + leg * part + lo, quarter), size)]

    def far_spot(leg, i, j):
        return (far_a_ref, far_b_ref)[leg].at[span(number(leg, i, j) * part, part)]

    def own(leg, half=None):
        lo, size = (0, part) if half is None else (half * quarter, quarter)
        return piece_ref.at[pl.ds(leg * part + lo, size)]

    def step_peer(leg, second, step):
        along_x = (leg == 0) != second
        return index_of(x + step, y, core) if along_x else index_of(x, y + step, core)

    started = []

    def push(leg, second, i, j, step, half):
        there = (i, (j - step) % RING) if second else ((i - step) % RING, j)
        src = own(leg, half) if i == 0 and j == 0 else spot(leg, i, j, half)
        copy = remote(src, spot(leg, i, j, half), send_sem.at[len(started)],
                      recv_sem.at[leg, there[0], there[1], half or 0], step_peer(leg, second, step))
        copy.start()
        started.append(copy)

    def landed(leg, i, j):
        in_halves = j == 2 or (j == 0 and i == 2)
        for half in ((0, 1) if in_halves else (None,)):
            here = spot(leg, i, j, half)
            remote(here, here, send_sem.at[0], recv_sem.at[leg, i, j, half or 0], me).wait_recv()

    side = []

    def to_sibling(leg, i, j):
        src = own(leg) if i == 0 and j == 0 else spot(leg, i, j)
        copy = remote(src, far_spot(leg, i, j), side_send.at[leg, i, j], side_recv.at[leg, i, j],
                      index_of(x, y, 1 - core))
        copy.start()
        side.append(copy)

    meet([index_of(x, y, 1 - core)] + [index_of(*chip, core) for chip in chips_around(x, y)])

    def spread(leg, i):
        push(leg, True, i, 0, 1, None)
        push(leg, True, i, 0, 3, None)
        to_sibling(leg, i, 0)

    for leg in range(2):
        push(leg, False, 0, 0, 1, None)
        push(leg, False, 0, 0, 3, None)
    for leg in range(2):
        spread(leg, 0)
    near_ref[span(number(0, 0, 0) * rows, rows), :] = piece_ref[...]

    for leg in range(2):
        landed(leg, 3, 0)
        push(leg, False, 3, 0, 1, 0)
        spread(leg, 3)
        landed(leg, 1, 0)
        push(leg, False, 1, 0, 3, 1)
        spread(leg, 1)

    def second_near(leg, i):
        landed(leg, i, 3)
        push(leg, True, i, 3, 1, 0)
        to_sibling(leg, i, 3)
        landed(leg, i, 1)
        push(leg, True, i, 1, 3, 1)
        to_sibling(leg, i, 1)

    for leg in range(2):
        second_near(leg, 0)
    for leg in range(2):
        landed(leg, 2, 0)
        spread(leg, 2)
    for i in (3, 1, 2):
        for leg in range(2):
            second_near(leg, i)
    for i in (0, 3, 1, 2):
        for leg in range(2):
            landed(leg, i, 2)
            to_sibling(leg, i, 2)

    for copy in started + side:
        copy.wait_send()

    for leg in range(2):
        for i in range(RING):
            for j in range(RING):
                here = far_spot(leg, i, j)
                remote(here, here, side_send.at[leg, i, j], side_recv.at[leg, i, j], me).wait_recv()


def gather_rows(piece, n_dev):
    rows, d_model = piece.shape
    half = n_dev * rows // CORES
    return pl.pallas_call(
        gather_kernel,
        name='gather_rows',
        out_shape=(pltpu.VMEM((half, d_model), F32), pltpu.VMEM((half // 2, d_model), F32), jax.ShapeDtypeStruct((half // 2, d_model), F32)),
        in_specs=[VMEM],
        out_specs=(VMEM, VMEM, ANY),
        scratch_shapes=[DMA((40,)), DMA((2, RING, RING, 2)), DMA((2, RING, RING)), DMA((2, RING, RING))],
        compiler_params=pltpu.CompilerParams(collective_id=2, has_side_effects=True, vmem_limit_bytes=STORE_LIMIT),
    )(piece)


def store_kernel(near_ref, far_a_ref, far_b_ref, dq_out, dk_out, dv_out, do_out, tile, put_sem, side_sem, in_sem, out_sem):
    core = lax.rem(lax.axis_index('sp'), CORES)
    outs = (dq_out, dk_out, dv_out, do_out)
    rows = near_ref.shape[0] // TYPES
    n_slot, chunk = tile.shape[0], tile.shape[1]
    n = far_b_ref.shape[0] // chunk

    def far_out(i, leg):
        first = (1 - core) * rows + (i % RING * 2 + leg) * chunk
        return outs[i // RING].at[pl.ds(pl.multiple_of(first, chunk), chunk)]

    puts = [pltpu.make_async_copy(near_ref.at[pl.ds(kind * rows, rows)], outs[kind].at[span(core * rows, rows)], put_sem.at[kind])
            for kind in range(TYPES)]
    puts += [pltpu.make_async_copy(far_a_ref.at[pl.ds(i * chunk, chunk)], far_out(i, 0), side_sem.at[i]) for i in range(n)]

    def load(i):
        return pltpu.make_async_copy(far_b_ref.at[pl.ds(i * chunk, chunk)], tile.at[i % n_slot], in_sem.at[i % n_slot])

    def save(i):
        return pltpu.make_async_copy(tile.at[i % n_slot], far_out(i, 1), out_sem.at[i % n_slot])

    ahead = n_slot // 2
    for i in range(ahead):
        load(i).start()
    for put in puts:
        put.start()
    for i in range(n):
        load(i).wait()
        save(i).start()
        if i + ahead < n:
            if i + ahead >= n_slot:
                save(i + ahead - n_slot).wait()
            load(i + ahead).start()
    for i in range(n - n_slot, n):
        save(i).wait()
    for put in puts:
        put.wait()


def store(near, far_a, far_b):
    half, d_model = near.shape
    n = RING * RING
    chunk = far_b.shape[0] // n
    grad = jax.ShapeDtypeStruct((half * CORES // TYPES, d_model), F32)
    return pl.pallas_call(
        store_kernel,
        name='store',
        out_shape=(grad,) * TYPES,
        in_specs=[VMEM, VMEM, ANY],
        out_specs=(ANY,) * TYPES,
        scratch_shapes=[pltpu.VMEM((8, chunk, d_model), F32), DMA((TYPES,)), DMA((n,)), DMA((8,)), DMA((8,))],
        compiler_params=pltpu.CompilerParams(vmem_limit_bytes=STORE_LIMIT),
    )(in_vmem(near), in_vmem(far_a), pltpu.with_memory_space_constraint(far_b, pltpu.HBM))


def solution(mesh):
    n_dev = mesh.shape['sp']
    assert n_dev == CORES * RING * RING

    def device_body(x_loc, flag_loc, w_q, w_k, w_v, w_o, dy_loc):
        tok_count, d_model = x_loc.shape
        n_heads, head_dim = w_q.shape[1], w_q.shape[2]
        width = n_heads * head_dim
        score_scale = 1.0 / (math.sqrt(head_dim) * tok_count)
        weights = [w.transpose(1, 2, 0).reshape(width, d_model) for w in (w_q, w_k, w_v)] + [w_o.reshape(width, d_model)]
        g, z = front(flag_loc, x_loc, dy_loc, weights, score_scale, n_dev, n_heads)
        piece, y_loc, dx_loc = reduce_rows(g, z, x_loc, dy_loc, weights)
        grads = store(*gather_rows(piece, n_dev))
        dw_q, dw_k, dw_v, dw_o = (grad.reshape(n_heads, head_dim, d_model) for grad in grads)
        return y_loc, dx_loc, dw_q.transpose(2, 0, 1), dw_k.transpose(2, 0, 1), dw_v.transpose(2, 0, 1), dw_o

    row_spec = P(('dp', 'sp'), None)
    flag_spec = P(('dp', 'sp'))
    w_spec = P(None, None, None)
    dw_spec = P('dp', None, None)
    return jax.shard_map(device_body, mesh=mesh,
                         in_specs=(row_spec, flag_spec, w_spec, w_spec, w_spec, w_spec, row_spec),
                         out_specs=(row_spec, row_spec, dw_spec, dw_spec, dw_spec, dw_spec),
                         check_vma=False)
```

```python
import functools
import math
import jax
import jax.numpy as jnp
from jax import lax
from jax.experimental import pallas as pl
from jax.experimental.pallas import tpu as pltpu
from jax.sharding import PartitionSpec as P

MESH = pl.DeviceIdType.MESH
CORES = 2
RING = 4
SLOTS = CORES * RING
TYPES = 4
O_TYPE = TYPES - 1
MIB = 1024 * 1024
STORE_LIMIT = 9 * MIB
BF16 = jnp.bfloat16
F32 = jnp.float32
ROWS = ((1,), (1,))
INNER = ((1,), (0,))
OUTER = ((0,), (0,))
VMEM = pl.BlockSpec(memory_space=pltpu.VMEM)
ANY = pl.BlockSpec(memory_space=pltpu.HBM)
DMA = pltpu.SemaphoreType.DMA


def place(me):
    core = lax.rem(me, CORES)
    chip = me // CORES
    return lax.rem(chip, RING), chip // RING, core


def index_of(x, y, core):
    return (lax.rem(y, RING) * RING + lax.rem(x, RING)) * CORES + core


def remote(src, dst, send_sem, recv_sem, peer):
    return pltpu.make_async_remote_copy(src_ref=src, dst_ref=dst, send_sem=send_sem, recv_sem=recv_sem,
                                        device_id={'sp': peer}, device_id_type=MESH)


def signal(peer):
    pl.semaphore_signal(pltpu.get_barrier_semaphore(), inc=1, device_id={'sp': peer}, device_id_type=MESH)


def meet(peers):
    for peer in peers:
        signal(peer)
    pl.semaphore_wait(pltpu.get_barrier_semaphore(), len(peers))


def chips_around(x, y):
    return ((x + 1, y), (x + RING - 1, y), (x, y + 1), (x, y + RING - 1))


def dot(a, b, dims):
    return lax.dot_general(a, b, (dims, ((), ())), preferred_element_type=F32)


def in_vmem(value):
    return pltpu.with_memory_space_constraint(value, pltpu.VMEM)


def span(start, size):
    return pl.ds(pl.multiple_of(start, size), size)


def stream(n_outer, n_inner, depth, copy, use, before):
    ahead = depth - 1
    for n in range(ahead):
        copy(0, n, n).start()
    for i in range(n_outer):
        before(i)

        @pl.loop(0, n_inner)
        def _(n):
            at = i * n_inner + n
            slot, free = lax.rem(at, depth), lax.rem(at + ahead, depth)

            @pl.when(n + ahead < n_inner)
            def _():
                copy(i, n + ahead, free).start()

            if i + 1 < n_outer:
                @pl.when(n + ahead >= n_inner)
                def _():
                    copy(i + 1, n + ahead - n_inner, free).start()

            copy(i, n, slot).wait()
            use(i, n, slot)


def form_masks(flag_ref, seg_col_ref, seg_row_ref, head_ref, tail_ref, gate_ref):
    tok = flag_ref.shape[1]
    flags = flag_ref[...] > 0
    t_pos = lax.broadcasted_iota(jnp.int32, (tok, tok), 0)
    s_pos = lax.broadcasted_iota(jnp.int32, (tok, tok), 1)
    seg_col = jnp.sum(jnp.where(flags & (s_pos <= t_pos), 1.0, 0), axis=1, keepdims=True)
    seg_col_ref[...] = seg_col
    seg_row_ref[...] = jnp.sum(jnp.where(s_pos == t_pos, seg_col, 0), axis=0, keepdims=True)
    positions = lax.broadcasted_iota(jnp.int32, (1, tok), 1).astype(F32)
    first_pos = jnp.min(jnp.where(flags, positions, tok), axis=1, keepdims=True)
    last_pos = jnp.max(jnp.where(flags, positions, -1), axis=1, keepdims=True)
    head_ref[...] = jnp.where(positions < first_pos, 1.0, 0)
    tail_ref[...] = jnp.where(positions >= last_pos, 1.0, 0)
    gate_ref[...] = jnp.broadcast_to(jnp.where(last_pos < 0, 1.0, 0), gate_ref.shape)


class Square:
    def __init__(self, me):
        x, y, core = place(me)
        across_x, across_y = (lax.rem(a + 1 + RING - 2 * lax.rem(a + core, 2), RING) for a in (x, y))
        self.core = core
        self.chips = [(x, y), (across_x, y), (x, across_y), (across_x, across_y)]

    def peer(self, k):
        return index_of(*self.chips[k], self.core)

    def kind(self, k):
        return owned_type(*self.chips[k])


def owned_type(x, y):
    return lax.rem(x, 2) + 2 * lax.rem(y, 2)


def lattice(x, y):
    return lax.rem(x // 2, 2), lax.rem(y // 2, 2)


def start_tokens(kind, x_ref, dy_ref, copy):
    @pl.when(kind == O_TYPE)
    def _():
        copy(dy_ref).start()

    @pl.when(kind != O_TYPE)
    def _():
        copy(x_ref).start()


def front_kernel(scale, dim, flag_ref, x_ref, dy_ref, wq_ref, wk_ref, wv_ref, wo_ref,
                 g_ref, z_ref, seg_col_ref, seg_row_ref, head_ref, tail_ref, gate_ref, tok_in, w_tile, rows_ref, total,
                 packed, held, formed, states,
                 tok_sem, w_sem, g_sem, z_send, z_recv, send_sem, recv_sem, back_send, back_recv):
    me = lax.axis_index('sp')
    n_dev, per_dev, low = formed.shape[1:4]
    width, tok = rows_ref.shape[1], rows_ref.shape[2]
    half = tok // 2
    n_piece = z_recv.shape[1]
    piece = tok // n_piece
    n_group = SLOTS
    group = width // n_group
    tile_rows = w_tile.shape[1]

    @pl.loop(1, n_dev)
    def _(step):
        signal(lax.rem(me + step, n_dev))

    loads = [pltpu.make_async_copy(ref, tok_in.at[i], tok_sem.at[i]) for i, ref in enumerate((x_ref, dy_ref))]
    for load in loads:
        load.start()

    square = Square(me)

    def token_copy(k, n):
        at = span(n * piece, piece)
        return lambda ref: remote(ref.at[at], z_ref.at[k - 1, at], z_send.at[k - 1, n], z_recv.at[k - 1, n], square.peer(k))

    def push_tokens(n):
        for k in range(1, TYPES):
            start_tokens(square.kind(k), x_ref, dy_ref, token_copy(k, n))

    form_masks(flag_ref, seg_col_ref, seg_row_ref, head_ref, tail_ref, gate_ref)
    pl.semaphore_wait(pltpu.get_barrier_semaphore(), n_dev - 1)
    pl.loop(0, 2)(push_tokens)

    weights = (wk_ref, wv_ref, wq_ref, wo_ref)
    kinds = (1, 2, 0, O_TYPE)

    def w_copy(i, n, slot):
        return pltpu.make_async_copy(weights[i].at[span(n * tile_rows, tile_rows)], w_tile.at[slot], w_sem.at[slot])

    def project(i, n, slot):
        rows_ref[kinds[i], span(n * tile_rows, tile_rows), :] = dot(w_tile[slot], tok_in[i // O_TYPE], ROWS).astype(BF16)

    def loaded(i):
        if i in (0, O_TYPE):
            loads[i // O_TYPE].wait()
        if i == 2:
            send_products(0)
        if i == 1:
            push_tokens(2)

    head = head_ref[...] > 0.5
    tail = tail_ref[...] > 0.5

    def each(do):
        pl.loop(1, n_dev)(do)

    def out_copy(which, step):
        peer = lax.rem(me + step, n_dev)
        at = pl.ds(0, packed.shape[3] if which == 0 else low)
        return remote(packed.at[which, peer, :, at], held.at[which, me, :, at], send_sem.at[which, step], recv_sem.at[which, step], peer)

    def back_copy(which, step):
        peer = lax.rem(me + step, n_dev)
        return remote(formed.at[which, peer], states.at[which, me], back_send.at[which, step], back_recv.at[which, step], peer)

    pair_lane = lax.broadcasted_iota(jnp.int32, (low, 2 * dim), 1) // dim

    def turn(pair):
        return pltpu.roll(pair, dim, 1)

    def send_products(which):
        left, right, mask = ((1, 2, tail), (0, O_TYPE, head))[which]

        @pl.loop(0, n_group)
        def _(grp):
            at = span(grp * group, group)
            full = dot(rows_ref[left, at, :], jnp.where(mask, rows_ref[right, at, :], jnp.zeros((group, tok), BF16)), ROWS)
            for sub in range(group // dim):
                spot = sub % 2
                block = full[sub * dim:(sub + 1) * dim, (sub // 2) * 2 * dim:(sub // 2 + 1) * 2 * dim]
                first, second = block[0:low], block[low:]
                if spot == 0:
                    second = turn(second)
                else:
                    first = turn(first)
                index = grp * (group // dim) + sub
                dev, own = index // per_dev, lax.rem(index, per_dev)
                packed[which, dev, own, 0:low, :] = jnp.where(pair_lane == 0, first, second)
                packed[which, dev, own, low:, :] = gate_ref[...]

        each(lambda step: out_copy(which, step).start())
        held[which, me] = packed[which, me]

    def form_states(which):
        each(lambda step: out_copy(which, step).wait_recv())

        def advance(step, state):
            block = step if which == 0 else n_dev - 1 - step
            formed[which, block] = state.astype(BF16)
            return held[0, block, :, low:low + 1, :] * state + held[which, block, :, 0:low, :]

        lax.fori_loop(0, n_dev, advance, jnp.zeros((per_dev, low, 2 * dim), F32))
        each(lambda step: back_copy(which, step).start())
        states[which, me] = formed[which, me]

    stream(TYPES, width // tile_rows, w_tile.shape[0], w_copy, project, loaded)
    send_products(1)

    seg_row = seg_row_ref[...]
    t_pos = lax.broadcasted_iota(jnp.int32, (half, tok), 0)
    s_pos = lax.broadcasted_iota(jnp.int32, (half, tok), 1)

    def pair(a, b):
        see_top = ((seg_col_ref[0:half, :] == seg_row) & (s_pos <= t_pos))[:, 0:half]
        see_low = (seg_col_ref[half:, :] == seg_row) & (s_pos <= t_pos + half)
        top = dot(a[:, 0:half], b[:, 0:half], OUTER)
        low = dot(a[:, half:], b, OUTER)
        return (jnp.where(see_top, top * scale, 0).astype(BF16), jnp.where(see_low, low * scale, 0).astype(BF16))

    def over_keys(at, rows_t, probs):
        total[at[0], at[1], 0:half] = dot(rows_t[:, 0:half], probs[0], ROWS)
        total[at[0], at[1], half:] = dot(rows_t, probs[1], ROWS)

    def over_queries(at, rows_t, probs):
        from_low = dot(rows_t[:, half:], probs[1], INNER)
        total[at[0], at[1], 0:half] = dot(rows_t[:, 0:half], probs[0], INNER) + from_low[:, 0:half]
        total[at[0], at[1], half:] = from_low[:, half:]

    def heads_of(grp):
        return [grp * (group // dim) + sub for sub in range(group // dim)]

    @pl.loop(0, n_group)
    def _(grp):
        @pl.when(grp == 1)
        def _():
            form_states(0)

        @pl.when(grp == n_group // 2)
        def _():
            form_states(1)
            push_tokens(O_TYPE)

        @pl.when(grp >= n_group // 2)
        def _():
            push_tokens(grp)

        for index in heads_of(grp):
            rows = span(index * dim, dim)
            q, k, v, do = (rows_ref[kind, rows, :] for kind in range(TYPES))
            d_probs = pair(do, v)
            over_keys((0, rows), k, d_probs)
            over_queries((1, rows), q, d_probs)
            probs = pair(q, k)
            over_queries((2, rows), do, probs)
            over_keys((O_TYPE, rows), v, probs)

    def diagonal(which, grp):
        rows = []
        for sub in range(group // dim):
            index = grp * (group // dim) + sub
            pair = states[which, index // per_dev, lax.rem(index, per_dev)].astype(F32)
            spot = sub % 2
            block = jnp.concatenate([turn(pair), pair] if spot else [pair, turn(pair)], axis=0)
            block = jnp.where(jnp.concatenate([pair_lane, pair_lane], axis=0) == spot, block, 0)
            empty = jnp.zeros_like(block)
            rows.append(jnp.concatenate([empty, block] if sub // 2 else [block, empty], axis=1))
        return jnp.concatenate(rows, axis=0).astype(BF16)

    def finish(kind, at, mask, inter):
        rows_ref[kind, at, :] = (total[kind, at, :] + jnp.where(mask, inter * scale, 0)).astype(BF16)

    def row_put(kind, grp):
        at = span(grp * group, group)
        return pltpu.make_async_copy(rows_ref.at[kind, at], g_ref.at[kind, at], g_sem.at[kind, grp])

    each(lambda step: back_copy(0, step).wait_recv())

    @pl.loop(0, n_group)
    def _(grp):
        at = span(grp * group, group)
        st = diagonal(0, grp)
        d_q = dot(st, rows_ref[O_TYPE, at, :], INNER)
        out = dot(st, rows_ref[0, at, :], OUTER)
        finish(0, at, head, d_q)
        finish(O_TYPE, at, head, out)
        for kind in (0, O_TYPE):
            row_put(kind, grp).start()

    each(lambda step: back_copy(1, step).wait_recv())

    @pl.loop(0, n_group)
    def _(grp):
        at = span(grp * group, group)
        st = diagonal(1, grp)
        d_k = dot(st, rows_ref[2, at, :], INNER)
        d_v = dot(st, rows_ref[1, at, :], OUTER)
        finish(1, at, tail, d_k)
        finish(2, at, tail, d_v)
        for kind in (1, 2):
            row_put(kind, grp).start()

    for kind in range(TYPES):
        pl.loop(0, n_group)(lambda grp, kind=kind: row_put(kind, grp).wait())
    for which in range(2):
        each(lambda step, which=which: out_copy(which, step).wait_send())
        each(lambda step, which=which: back_copy(which, step).wait_send())
    for k in range(1, TYPES):
        pl.loop(0, n_piece)(lambda n, k=k: token_copy(k, n)(x_ref).wait())


def front(flags, x_loc, dy_loc, weights, scale, n_dev, n_heads):
    tok, d_model = x_loc.shape
    width = weights[0].shape[0]
    dim = width // n_heads
    per_dev = n_heads // n_dev
    n_piece = SLOTS
    pack = (2, n_dev, per_dev, dim // 2 + 8, 2 * dim)
    back = (2, n_dev, per_dev, dim // 2, 2 * dim)
    return pl.pallas_call(
        functools.partial(front_kernel, scale, dim),
        name='front',
        out_shape=(jax.ShapeDtypeStruct((TYPES, width, tok), BF16), jax.ShapeDtypeStruct((TYPES - 1, tok, d_model), BF16)),
        in_specs=[VMEM] + [ANY] * 6,
        out_specs=(ANY, ANY),
        scratch_shapes=[
            pltpu.VMEM((tok, 1), F32), pltpu.VMEM((1, tok), F32), pltpu.VMEM((1, tok), F32), pltpu.VMEM((1, tok), F32), pltpu.VMEM((8, 2 * dim), F32),
            pltpu.VMEM((2, tok, d_model), BF16), pltpu.VMEM((4, width // RING, d_model), BF16),
            pltpu.VMEM((TYPES, width, tok), BF16), pltpu.VMEM((TYPES, width, tok), F32),
            pltpu.VMEM(pack, F32), pltpu.VMEM(pack, F32), pltpu.VMEM(back, BF16), pltpu.VMEM(back, BF16),
            DMA((2,)), DMA((4,)), DMA((TYPES, SLOTS)), DMA((TYPES - 1, n_piece)), DMA((TYPES - 1, n_piece)),
            DMA((2, n_dev)), DMA((2, n_dev)), DMA((2, n_dev)), DMA((2, n_dev))],
        compiler_params=pltpu.CompilerParams(collective_id=0, has_side_effects=True, vmem_limit_bytes=56 * MIB),
    )(flags[None, :], x_loc, dy_loc, *weights)


def row_products(g_ref, w_refs, y_ref, dx_ref, rows_in, rows_t, w_tile, total, done, g_sem, w_sem, put_sem):
    width = rows_in.shape[0]
    cols = w_tile.shape[2]
    n_tile = total.shape[1] // cols
    step = width // SLOTS
    order = (O_TYPE, 0, 1, 2)

    def g_copy(i):
        return pltpu.make_async_copy(g_ref.at[order[i]], rows_in, g_sem)

    def w_copy(i, n, slot):
        return pltpu.make_async_copy(w_refs[order[i]].at[:, span(n * cols, cols)], w_tile.at[slot], w_sem.at[slot])

    puts = [pltpu.make_async_copy(done, ref, put_sem) for ref in (y_ref, dx_ref)]

    def turned(i):
        if i == 1:
            puts[0].start()
        if i == O_TYPE:
            puts[0].wait()
        g_copy(i).wait()

        @pl.loop(0, width // step)
        def _(b):
            at = span(b * step, step)
            rows_t[:, at] = jnp.transpose(rows_in[at, :])

        if i < O_TYPE:
            g_copy(i + 1).start()

    def use(i, n, slot):
        at = span(n * cols, cols)
        prod = dot(rows_t[...], w_tile[slot], INNER)
        if i == 0:
            done[:, at] = prod.astype(BF16)
        elif i == 1:
            total[:, at] = prod
        elif i < O_TYPE:
            total[:, at] = total[:, at] + prod
        else:
            done[:, at] = (total[:, at] + prod).astype(BF16)

    g_copy(0).start()
    stream(TYPES, n_tile, w_tile.shape[0], w_copy, use, turned)
    puts[1].start()
    return puts[1]


FLIPS = ((1, 1), (1, 0), (0, 1), (0, 0))


def reduce_kernel(g_ref, z_ref, x_ref, dy_ref, wq_ref, wk_ref, wv_ref, wo_ref, out_ref, y_ref, dx_ref,
                  zbuf, rows_in, side_out, side_in, first_out, first_in, second_out, second_in, kind_rows, rows_t, w_tile, sums, done,
                  z_sem, row_send, row_recv, side_send, side_recv, first_send, first_recv, second_send, second_recv, g_sem, w_sem, put_sem):
    me = lax.axis_index('sp')
    x, y, core = place(me)
    square = Square(me)
    block = rows_in.shape[3]
    part = block // 2
    n_col, cols = second_out.shape[1], second_out.shape[3]
    sibling = index_of(x, y, 1 - core)
    across = (index_of(x + 2, y, core), index_of(x, y + 2, core))

    meet([sibling, *across] + [square.peer(k) for k in range(1, TYPES)])

    def own_copy(ref):
        return pltpu.make_async_copy(ref, zbuf.at[0], z_sem.at[0])

    z_copies = [pltpu.make_async_copy(z_ref.at[k - 1], zbuf.at[k], z_sem.at[k]) for k in range(1, TYPES)]

    def row_source(k, mine, t):
        px, py = lattice(*square.chips[k])
        half = core if mine else 1 - core
        index = half * RING + lax.rem(px + FLIPS[t][0], 2) + 2 * lax.rem(py + FLIPS[t][1], 2)
        return g_ref.at[square.kind(k), span(index * block, block)]

    def row_copy(k, mine, t):
        dst, recv = rows_in.at[k, mine, t], row_recv.at[k, mine, t]
        if k == 0:
            return pltpu.make_async_copy(row_source(k, mine, t), dst, recv)
        return remote(row_source(k, mine, t), dst, row_send.at[k - 1, mine, t], recv, square.peer(k))

    every_row = [(k, mine, t) for t in range(TYPES) for mine in range(2) for k in range(TYPES)]
    for where in every_row:
        row_copy(*where).start()
    start_tokens(square.kind(0), x_ref, dy_ref, own_copy)
    for copy in z_copies:
        copy.start()

    last_put = row_products(g_ref, (wq_ref, wk_ref, wv_ref, wo_ref), y_ref, dx_ref, kind_rows, rows_t, w_tile, sums, done, g_sem, w_sem, put_sem)

    own_copy(x_ref).wait()
    for copy in z_copies:
        copy.wait()

    def product(mine, t, ch):
        at = span(ch * cols, cols)
        total = dot(rows_in[0, mine, t], zbuf[0, :, at], INNER)
        for k in range(1, TYPES):
            total = total + dot(rows_in[k, mine, t], zbuf[k, :, at], INNER)
        return total

    def side_copy(t, ch):
        return remote(side_out.at[t % 2, ch], side_in.at[t, ch], side_send.at[t, ch], side_recv.at[t, ch], sibling)

    def first_copy(leg, q, ch):
        return remote(first_out.at[leg, q, ch], first_in.at[leg, q, ch], first_send.at[leg, q, ch], first_recv.at[leg, q, ch], across[leg])

    def second_copy(leg, ch):
        return remote(second_out.at[leg, ch], second_in.at[leg, ch], second_send.at[leg, ch], second_recv.at[leg, ch], across[1 - leg])

    for t in range(TYPES):
        for mine in range(2):
            for k in range(TYPES):
                copy = row_copy(k, mine, t)
                if k:
                    copy.wait_recv()
                else:
                    copy.wait()

        @pl.loop(0, n_col)
        def _(ch, t=t):
            if t >= 2:
                side_copy(t - 2, ch).wait_send()
            side_out[t % 2, ch] = product(0, t, ch)
            side_copy(t, ch).start()

        @pl.loop(0, n_col)
        def _(ch, t=t):
            total = product(1, t, ch)
            side_copy(t, ch).wait_recv()
            total = total + side_in[t, ch]
            for leg in range(2):
                half = total[leg * part:(leg + 1) * part]
                step, other = FLIPS[t][leg], FLIPS[t][1 - leg]
                if step:
                    first_out[leg, other, ch] = half
                    first_copy(leg, other, ch).start()
                    continue
                first_copy(leg, other, ch).wait_recv()
                half = half + first_in[leg, other, ch]
                if other:
                    second_out[leg, ch] = half
                    second_copy(leg, ch).start()
                else:
                    second_copy(leg, ch).wait_recv()
                    out_ref[leg * part:(leg + 1) * part, span(ch * cols, cols)] = half + second_in[leg, ch]

    last_put.wait()
    for where in every_row:
        if where[0]:
            row_copy(*where).wait_send()

    @pl.loop(0, n_col)
    def _(ch):
        for t in range(2, TYPES):
            side_copy(t, ch).wait_send()
        for leg in range(2):
            for q in range(2):
                first_copy(leg, q, ch).wait_send()
            second_copy(leg, ch).wait_send()


def reduce_rows(g, z, x_loc, dy_loc, weights):
    width, tok = g.shape[1], g.shape[2]
    d_model = x_loc.shape[1]
    block = width // SLOTS
    n_col = RING
    cols = d_model // n_col
    tokens = jax.ShapeDtypeStruct((tok, d_model), BF16)
    halves = lambda *lead: pltpu.VMEM((*lead, n_col, block // 2, cols), F32)
    blocks = lambda lead: pltpu.VMEM((lead, n_col, block, cols), F32)
    return pl.pallas_call(
        reduce_kernel,
        name='reduce_rows',
        out_shape=(pltpu.VMEM((block, d_model), F32), tokens, tokens),
        in_specs=[ANY] * 8,
        out_specs=(VMEM, ANY, ANY),
        scratch_shapes=[
            pltpu.VMEM((TYPES, tok, d_model), BF16), pltpu.VMEM((TYPES, 2, TYPES, block, tok), BF16),
            blocks(2), blocks(TYPES), halves(2, 2), halves(2, 2), halves(2), halves(2),
            pltpu.VMEM((width, tok), BF16), pltpu.VMEM((tok, width), BF16), pltpu.VMEM((3, width, min(256, d_model // 4)), BF16),
            pltpu.VMEM((tok, d_model), F32), pltpu.VMEM((tok, d_model), BF16),
            DMA((TYPES,)), DMA((TYPES - 1, 2, TYPES)), DMA((TYPES, 2, TYPES)), DMA((TYPES, n_col)), DMA((TYPES, n_col)),
            DMA((2, 2, n_col)), DMA((2, 2, n_col)), DMA((2, n_col)), DMA((2, n_col)), DMA, DMA((3,)), DMA],
        compiler_params=pltpu.CompilerParams(collective_id=1, has_side_effects=True, vmem_limit_bytes=58 * MIB),
    )(g, z, x_loc, dy_loc, *weights)


def gather_kernel(piece_ref, near_ref, far_a_ref, far_b_ref, send_sem, recv_sem, side_send, side_recv):
    me = lax.axis_index('sp')
    x, y, core = place(me)
    rows = piece_ref.shape[0]
    part = rows // 2
    quarter = part // 2

    def number(leg, i, j):
        sx, sy = (i, j) if leg == 0 else (j, i)
        px, py = lax.rem(x + sx, RING), lax.rem(y + sy, RING)
        lx, ly = lattice(px, py)
        return owned_type(px, py) * RING + lx + 2 * ly

    def spot(leg, i, j, half=None):
        lo, size = (0, part) if half is None else (half * quarter, quarter)
        return near_ref.at[pl.ds(pl.multiple_of(number(leg, i, j) * rows + leg * part + lo, quarter), size)]

    def far_spot(leg, i, j):
        return (far_a_ref, far_b_ref)[leg].at[span(number(leg, i, j) * part, part)]

    def own(leg, half=None):
        lo, size = (0, part) if half is None else (half * quarter, quarter)
        return piece_ref.at[pl.ds(leg * part + lo, size)]

    def step_peer(leg, second, step):
        along_x = (leg == 0) != second
        return index_of(x + step, y, core) if along_x else index_of(x, y + step, core)

    started = []

    def push(leg, second, i, j, step, half):
        there = (i, (j - step) % RING) if second else ((i - step) % RING, j)
        src = own(leg, half) if i == 0 and j == 0 else spot(leg, i, j, half)
        copy = remote(src, spot(leg, i, j, half), send_sem.at[len(started)],
                      recv_sem.at[leg, there[0], there[1], half or 0], step_peer(leg, second, step))
        copy.start()
        started.append(copy)

    def landed(leg, i, j):
        in_halves = j == 2 or (j == 0 and i == 2)
        for half in ((0, 1) if in_halves else (None,)):
            here = spot(leg, i, j, half)
            remote(here, here, send_sem.at[0], recv_sem.at[leg, i, j, half or 0], me).wait_recv()

    side = []

    def to_sibling(leg, i, j):
        src = own(leg) if i == 0 and j == 0 else spot(leg, i, j)
        copy = remote(src, far_spot(leg, i, j), side_send.at[leg, i, j], side_recv.at[leg, i, j],
                      index_of(x, y, 1 - core))
        copy.start()
        side.append(copy)

    meet([index_of(x, y, 1 - core)] + [index_of(*chip, core) for chip in chips_around(x, y)])

    def spread(leg, i):
        push(leg, True, i, 0, 1, None)
        push(leg, True, i, 0, 3, None)
        to_sibling(leg, i, 0)

    for leg in range(2):
        push(leg, False, 0, 0, 1, None)
        push(leg, False, 0, 0, 3, None)
    for leg in range(2):
        spread(leg, 0)
    near_ref[span(number(0, 0, 0) * rows, rows), :] = piece_ref[...]

    for leg in range(2):
        landed(leg, 3, 0)
        push(leg, False, 3, 0, 1, 0)
        spread(leg, 3)
        landed(leg, 1, 0)
        push(leg, False, 1, 0, 3, 1)
        spread(leg, 1)

    def second_near(leg, i):
        landed(leg, i, 3)
        push(leg, True, i, 3, 1, 0)
        to_sibling(leg, i, 3)
        landed(leg, i, 1)
        push(leg, True, i, 1, 3, 1)
        to_sibling(leg, i, 1)

    for leg in range(2):
        second_near(leg, 0)
    for leg in range(2):
        landed(leg, 2, 0)
        spread(leg, 2)
    for i in (3, 1, 2):
        for leg in range(2):
            second_near(leg, i)
    for i in (0, 3, 1, 2):
        for leg in range(2):
            landed(leg, i, 2)
            to_sibling(leg, i, 2)

    for copy in started + side:
        copy.wait_send()

    for leg in range(2):
        for i in range(RING):
            for j in range(RING):
                here = far_spot(leg, i, j)
                remote(here, here, side_send.at[leg, i, j], side_recv.at[leg, i, j], me).wait_recv()


def gather_rows(piece, n_dev):
    rows, d_model = piece.shape
    half = n_dev * rows // CORES
    return pl.pallas_call(
        gather_kernel,
        name='gather_rows',
        out_shape=(pltpu.VMEM((half, d_model), F32), pltpu.VMEM((half // 2, d_model), F32), jax.ShapeDtypeStruct((half // 2, d_model), F32)),
        in_specs=[VMEM],
        out_specs=(VMEM, VMEM, ANY),
        scratch_shapes=[DMA((40,)), DMA((2, RING, RING, 2)), DMA((2, RING, RING)), DMA((2, RING, RING))],
        compiler_params=pltpu.CompilerParams(collective_id=2, has_side_effects=True, vmem_limit_bytes=STORE_LIMIT),
    )(piece)


def store_kernel(near_ref, far_a_ref, far_b_ref, dq_out, dk_out, dv_out, do_out, tile, put_sem, side_sem, in_sem, out_sem):
    core = lax.rem(lax.axis_index('sp'), CORES)
    outs = (dq_out, dk_out, dv_out, do_out)
    rows = near_ref.shape[0] // TYPES
    n_slot, chunk = tile.shape[0], tile.shape[1]
    n = far_b_ref.shape[0] // chunk

    def far_out(i, leg):
        first = (1 - core) * rows + (i % RING * 2 + leg) * chunk
        return outs[i // RING].at[pl.ds(pl.multiple_of(first, chunk), chunk)]

    puts = [pltpu.make_async_copy(near_ref.at[pl.ds(kind * rows, rows)], outs[kind].at[span(core * rows, rows)], put_sem.at[kind])
            for kind in range(TYPES)]
    puts += [pltpu.make_async_copy(far_a_ref.at[pl.ds(i * chunk, chunk)], far_out(i, 0), side_sem.at[i]) for i in range(n)]

    def load(i):
        return pltpu.make_async_copy(far_b_ref.at[pl.ds(i * chunk, chunk)], tile.at[i % n_slot], in_sem.at[i % n_slot])

    def save(i):
        return pltpu.make_async_copy(tile.at[i % n_slot], far_out(i, 1), out_sem.at[i % n_slot])

    ahead = n_slot // 2
    for i in range(ahead):
        load(i).start()
    for put in puts:
        put.start()
    for i in range(n):
        load(i).wait()
        save(i).start()
        if i + ahead < n:
            if i + ahead >= n_slot:
                save(i + ahead - n_slot).wait()
            load(i + ahead).start()
    for i in range(n - n_slot, n):
        save(i).wait()
    for put in puts:
        put.wait()


def store(near, far_a, far_b):
    half, d_model = near.shape
    n = RING * RING
    chunk = far_b.shape[0] // n
    grad = jax.ShapeDtypeStruct((half * CORES // TYPES, d_model), F32)
    return pl.pallas_call(
        store_kernel,
        name='store',
        out_shape=(grad,) * TYPES,
        in_specs=[VMEM, VMEM, ANY],
        out_specs=(ANY,) * TYPES,
        scratch_shapes=[pltpu.VMEM((8, chunk, d_model), F32), DMA((TYPES,)), DMA((n,)), DMA((8,)), DMA((8,))],
        compiler_params=pltpu.CompilerParams(vmem_limit_bytes=STORE_LIMIT),
    )(in_vmem(near), in_vmem(far_a), pltpu.with_memory_space_constraint(far_b, pltpu.HBM))


def solution(mesh):
    n_dev = mesh.shape['sp']
    assert n_dev == CORES * RING * RING

    def device_body(x_loc, flag_loc, w_q, w_k, w_v, w_o, dy_loc):
        tok_count, d_model = x_loc.shape
        n_heads, head_dim = w_q.shape[1], w_q.shape[2]
        width = n_heads * head_dim
        score_scale = 1.0 / (math.sqrt(head_dim) * tok_count)
        weights = [w.transpose(1, 2, 0).reshape(width, d_model) for w in (w_q, w_k, w_v)] + [w_o.reshape(width, d_model)]
        g, z = front(flag_loc, x_loc, dy_loc, weights, score_scale, n_dev, n_heads)
        piece, y_loc, dx_loc = reduce_rows(g, z, x_loc, dy_loc, weights)
        grads = store(*gather_rows(piece, n_dev))
        dw_q, dw_k, dw_v, dw_o = (grad.reshape(n_heads, head_dim, d_model) for grad in grads)
        return y_loc, dx_loc, dw_q.transpose(2, 0, 1), dw_k.transpose(2, 0, 1), dw_v.transpose(2, 0, 1), dw_o

    row_spec = P(('dp', 'sp'), None)
    flag_spec = P(('dp', 'sp'))
    w_spec = P(None, None, None)
    dw_spec = P('dp', None, None)
    return jax.shard_map(device_body, mesh=mesh,
                         in_specs=(row_spec, flag_spec, w_spec, w_spec, w_spec, w_spec, row_spec),
                         out_specs=(row_spec, row_spec, dw_spec, dw_spec, dw_spec, dw_spec),
                         check_vma=False)
```

```python
import functools
import math
import jax
import jax.numpy as jnp
from jax import lax
from jax.experimental import pallas as pl
from jax.experimental.pallas import tpu as pltpu
from jax.sharding import PartitionSpec as P

MESH = pl.DeviceIdType.MESH
CORES = 2
RING = 4
SLOTS = CORES * RING
TYPES = 4
O_TYPE = TYPES - 1
MIB = 1024 * 1024
STORE_LIMIT = 4 * MIB
BF16 = jnp.bfloat16
F32 = jnp.float32
ROWS = ((1,), (1,))
INNER = ((1,), (0,))
OUTER = ((0,), (0,))
VMEM = pl.BlockSpec(memory_space=pltpu.VMEM)
ANY = pl.BlockSpec(memory_space=pltpu.HBM)
DMA = pltpu.SemaphoreType.DMA


def place(me):
    core = lax.rem(me, CORES)
    chip = me // CORES
    return lax.rem(chip, RING), chip // RING, core


def index_of(x, y, core):
    return (lax.rem(y, RING) * RING + lax.rem(x, RING)) * CORES + core


def remote(src, dst, send_sem, recv_sem, peer):
    return pltpu.make_async_remote_copy(src_ref=src, dst_ref=dst, send_sem=send_sem, recv_sem=recv_sem,
                                        device_id={'sp': peer}, device_id_type=MESH)


def signal(peer):
    pl.semaphore_signal(pltpu.get_barrier_semaphore(), inc=1, device_id={'sp': peer}, device_id_type=MESH)


def meet(peers):
    for peer in peers:
        signal(peer)
    pl.semaphore_wait(pltpu.get_barrier_semaphore(), len(peers))


def chips_around(x, y):
    return ((x + 1, y), (x + RING - 1, y), (x, y + 1), (x, y + RING - 1))


def dot(a, b, dims):
    return lax.dot_general(a, b, (dims, ((), ())), preferred_element_type=F32)


def in_vmem(value):
    return pltpu.with_memory_space_constraint(value, pltpu.VMEM)


def span(start, size):
    return pl.ds(pl.multiple_of(start, size), size)


def stream(n_outer, n_inner, depth, copy, use, before):
    ahead = depth - 1
    for n in range(ahead):
        copy(0, n, n).start()
    for i in range(n_outer):
        before(i)

        @pl.loop(0, n_inner)
        def _(n):
            at = i * n_inner + n
            slot, free = lax.rem(at, depth), lax.rem(at + ahead, depth)

            @pl.when(n + ahead < n_inner)
            def _():
                copy(i, n + ahead, free).start()

            if i + 1 < n_outer:
                @pl.when(n + ahead >= n_inner)
                def _():
                    copy(i + 1, n + ahead - n_inner, free).start()

            copy(i, n, slot).wait()
            use(i, n, slot)


def form_masks(flag_ref, seg_col_ref, seg_row_ref, head_ref, tail_ref, gate_ref):
    tok = flag_ref.shape[1]
    flags = flag_ref[...] > 0
    t_pos = lax.broadcasted_iota(jnp.int32, (tok, tok), 0)
    s_pos = lax.broadcasted_iota(jnp.int32, (tok, tok), 1)
    seg_col = jnp.sum(jnp.where(flags & (s_pos <= t_pos), 1.0, 0), axis=1, keepdims=True)
    seg_col_ref[...] = seg_col
    seg_row_ref[...] = jnp.sum(jnp.where(s_pos == t_pos, seg_col, 0), axis=0, keepdims=True)
    positions = lax.broadcasted_iota(jnp.int32, (1, tok), 1).astype(F32)
    first_pos = jnp.min(jnp.where(flags, positions, tok), axis=1, keepdims=True)
    last_pos = jnp.max(jnp.where(flags, positions, -1), axis=1, keepdims=True)
    head_ref[...] = jnp.where(positions < first_pos, 1.0, 0)
    tail_ref[...] = jnp.where(positions >= last_pos, 1.0, 0)
    gate_ref[...] = jnp.broadcast_to(jnp.where(last_pos < 0, 1.0, 0), gate_ref.shape)


class Square:
    def __init__(self, me):
        x, y, core = place(me)
        across_x, across_y = (lax.rem(a + 1 + RING - 2 * lax.rem(a + core, 2), RING) for a in (x, y))
        self.core = core
        self.chips = [(x, y), (across_x, y), (x, across_y), (across_x, across_y)]

    def peer(self, k):
        return index_of(*self.chips[k], self.core)

    def kind(self, k):
        return owned_type(*self.chips[k])


def owned_type(x, y):
    return lax.rem(x, 2) + 2 * lax.rem(y, 2)


def lattice(x, y):
    return lax.rem(x // 2, 2), lax.rem(y // 2, 2)


def start_tokens(kind, x_ref, dy_ref, copy):
    @pl.when(kind == O_TYPE)
    def _():
        copy(dy_ref).start()

    @pl.when(kind != O_TYPE)
    def _():
        copy(x_ref).start()


def front_kernel(scale, dim, flag_ref, x_ref, dy_ref, wq_ref, wk_ref, wv_ref, wo_ref,
                 g_ref, z_ref, seg_col_ref, seg_row_ref, head_ref, tail_ref, gate_ref, tok_in, w_tile, rows_ref, total,
                 packed, held, formed, states,
                 tok_sem, w_sem, g_sem, z_send, z_recv, send_sem, recv_sem, back_send, back_recv):
    me = lax.axis_index('sp')
    n_dev, per_dev, low = formed.shape[1:4]
    width, tok = rows_ref.shape[1], rows_ref.shape[2]
    half = tok // 2
    n_piece = z_recv.shape[1]
    piece = tok // n_piece
    n_group = SLOTS
    group = width // n_group
    tile_rows = w_tile.shape[1]

    @pl.loop(1, n_dev)
    def _(step):
        signal(lax.rem(me + step, n_dev))

    loads = [pltpu.make_async_copy(ref, tok_in.at[i], tok_sem.at[i]) for i, ref in enumerate((x_ref, dy_ref))]
    for load in loads:
        load.start()

    square = Square(me)

    def token_copy(k, n):
        at = span(n * piece, piece)
        return lambda ref: remote(ref.at[at], z_ref.at[k - 1, at], z_send.at[k - 1, n], z_recv.at[k - 1, n], square.peer(k))

    def push_tokens(n):
        for k in range(1, TYPES):
            start_tokens(square.kind(k), x_ref, dy_ref, token_copy(k, n))

    form_masks(flag_ref, seg_col_ref, seg_row_ref, head_ref, tail_ref, gate_ref)
    pl.semaphore_wait(pltpu.get_barrier_semaphore(), n_dev - 1)
    pl.loop(0, 2)(push_tokens)

    weights = (wk_ref, wv_ref, wq_ref, wo_ref)
    kinds = (1, 2, 0, O_TYPE)

    def w_copy(i, n, slot):
        return pltpu.make_async_copy(weights[i].at[span(n * tile_rows, tile_rows)], w_tile.at[slot], w_sem.at[slot])

    def project(i, n, slot):
        rows_ref[kinds[i], span(n * tile_rows, tile_rows), :] = dot(w_tile[slot], tok_in[i // O_TYPE], ROWS).astype(BF16)

    def loaded(i):
        if i in (0, O_TYPE):
            loads[i // O_TYPE].wait()
        if i == 2:
            send_products(0)
        if i in (1, O_TYPE):
            push_tokens(2 + i // O_TYPE)

    head = head_ref[...] > 0.5
    tail = tail_ref[...] > 0.5

    def each(do):
        pl.loop(1, n_dev)(do)

    def out_copy(which, step):
        peer = lax.rem(me + step, n_dev)
        at = pl.ds(0, packed.shape[3] if which == 0 else low)
        return remote(packed.at[which, peer, :, at], held.at[which, me, :, at], send_sem.at[which, step], recv_sem.at[which, step], peer)

    def back_copy(which, step):
        peer = lax.rem(me + step, n_dev)
        return remote(formed.at[which, peer], states.at[which, me], back_send.at[which, step], back_recv.at[which, step], peer)

    pair_lane = lax.broadcasted_iota(jnp.int32, (low, 2 * dim), 1) // dim

    def turn(pair):
        return pltpu.roll(pair, dim, 1)

    def send_products(which):
        left, right, mask = ((1, 2, tail), (0, O_TYPE, head))[which]

        @pl.loop(0, n_group)
        def _(grp):
            at = span(grp * group, group)
            full = dot(rows_ref[left, at, :], jnp.where(mask, rows_ref[right, at, :], jnp.zeros((group, tok), BF16)), ROWS)
            for sub in range(group // dim):
                spot = sub % 2
                block = full[sub * dim:(sub + 1) * dim, (sub // 2) * 2 * dim:(sub // 2 + 1) * 2 * dim]
                first, second = block[0:low], block[low:]
                if spot == 0:
                    second = turn(second)
                else:
                    first = turn(first)
                index = grp * (group // dim) + sub
                dev, own = index // per_dev, lax.rem(index, per_dev)
                packed[which, dev, own, 0:low, :] = jnp.where(pair_lane == 0, first, second)
                packed[which, dev, own, low:, :] = gate_ref[...]

        each(lambda step: out_copy(which, step).start())
        held[which, me] = packed[which, me]

    def form_states(which):
        each(lambda step: out_copy(which, step).wait_recv())

        def advance(step, state):
            block = step if which == 0 else n_dev - 1 - step
            formed[which, block] = state.astype(BF16)
            return held[0, block, :, low:low + 1, :] * state + held[which, block, :, 0:low, :]

        lax.fori_loop(0, n_dev, advance, jnp.zeros((per_dev, low, 2 * dim), F32))
        each(lambda step: back_copy(which, step).start())
        states[which, me] = formed[which, me]

    stream(TYPES, width // tile_rows, w_tile.shape[0], w_copy, project, loaded)
    send_products(1)

    seg_row = seg_row_ref[...]
    t_pos = lax.broadcasted_iota(jnp.int32, (half, tok), 0)
    s_pos = lax.broadcasted_iota(jnp.int32, (half, tok), 1)

    def pair(a, b):
        see_top = ((seg_col_ref[0:half, :] == seg_row) & (s_pos <= t_pos))[:, 0:half]
        see_low = (seg_col_ref[half:, :] == seg_row) & (s_pos <= t_pos + half)
        top = dot(a[:, 0:half], b[:, 0:half], OUTER)
        low = dot(a[:, half:], b, OUTER)
        return (jnp.where(see_top, top * scale, 0).astype(BF16), jnp.where(see_low, low * scale, 0).astype(BF16))

    def over_keys(at, rows_t, probs):
        total[at[0], at[1], 0:half] = dot(rows_t[:, 0:half], probs[0], ROWS)
        total[at[0], at[1], half:] = dot(rows_t, probs[1], ROWS)

    def over_queries(at, rows_t, probs):
        from_low = dot(rows_t[:, half:], probs[1], INNER)
        total[at[0], at[1], 0:half] = dot(rows_t[:, 0:half], probs[0], INNER) + from_low[:, 0:half]
        total[at[0], at[1], half:] = from_low[:, half:]

    def heads_of(grp):
        return [grp * (group // dim) + sub for sub in range(group // dim)]

    @pl.loop(0, n_group)
    def _(grp):
        @pl.when(grp == 1)
        def _():
            form_states(0)

        @pl.when(grp == n_group // 2 + 1)
        def _():
            form_states(1)
            push_tokens(n_group // 2)

        @pl.when(grp > n_group // 2)
        def _():
            push_tokens(grp)

        for index in heads_of(grp):
            rows = span(index * dim, dim)
            q, k, v, do = (rows_ref[kind, rows, :] for kind in range(TYPES))
            d_probs = pair(do, v)
            over_keys((0, rows), k, d_probs)
            over_queries((1, rows), q, d_probs)
            probs = pair(q, k)
            over_queries((2, rows), do, probs)
            over_keys((O_TYPE, rows), v, probs)

    def diagonal(which, grp):
        rows = []
        for sub in range(group // dim):
            index = grp * (group // dim) + sub
            pair = states[which, index // per_dev, lax.rem(index, per_dev)].astype(F32)
            spot = sub % 2
            block = jnp.concatenate([turn(pair), pair] if spot else [pair, turn(pair)], axis=0)
            block = jnp.where(jnp.concatenate([pair_lane, pair_lane], axis=0) == spot, block, 0)
            empty = jnp.zeros_like(block)
            rows.append(jnp.concatenate([empty, block] if sub // 2 else [block, empty], axis=1))
        return jnp.concatenate(rows, axis=0).astype(BF16)

    def finish(kind, at, mask, inter):
        rows_ref[kind, at, :] = (total[kind, at, :] + jnp.where(mask, inter * scale, 0)).astype(BF16)

    def row_put(kind, grp):
        at = span(grp * group, group)
        return pltpu.make_async_copy(rows_ref.at[kind, at], g_ref.at[kind, at], g_sem.at[kind, grp])

    each(lambda step: back_copy(0, step).wait_recv())

    @pl.loop(0, n_group)
    def _(grp):
        at = span(grp * group, group)
        st = diagonal(0, grp)
        d_q = dot(st, rows_ref[O_TYPE, at, :], INNER)
        out = dot(st, rows_ref[0, at, :], OUTER)
        finish(0, at, head, d_q)
        finish(O_TYPE, at, head, out)
        for kind in (0, O_TYPE):
            row_put(kind, grp).start()

    each(lambda step: back_copy(1, step).wait_recv())

    @pl.loop(0, n_group)
    def _(grp):
        at = span(grp * group, group)
        st = diagonal(1, grp)
        d_k = dot(st, rows_ref[2, at, :], INNER)
        d_v = dot(st, rows_ref[1, at, :], OUTER)
        finish(1, at, tail, d_k)
        finish(2, at, tail, d_v)
        for kind in (1, 2):
            row_put(kind, grp).start()

    for kind in range(TYPES):
        pl.loop(0, n_group)(lambda grp, kind=kind: row_put(kind, grp).wait())
    for which in range(2):
        each(lambda step, which=which: out_copy(which, step).wait_send())
        each(lambda step, which=which: back_copy(which, step).wait_send())
    for k in range(1, TYPES):
        pl.loop(0, n_piece)(lambda n, k=k: token_copy(k, n)(x_ref).wait())


def front(flags, x_loc, dy_loc, weights, scale, n_dev, n_heads):
    tok, d_model = x_loc.shape
    width = weights[0].shape[0]
    dim = width // n_heads
    per_dev = n_heads // n_dev
    n_piece = SLOTS
    pack = (2, n_dev, per_dev, dim // 2 + 8, 2 * dim)
    back = (2, n_dev, per_dev, dim // 2, 2 * dim)
    return pl.pallas_call(
        functools.partial(front_kernel, scale, dim),
        name='front',
        out_shape=(jax.ShapeDtypeStruct((TYPES, width, tok), BF16), jax.ShapeDtypeStruct((TYPES - 1, tok, d_model), BF16)),
        in_specs=[VMEM] + [ANY] * 6,
        out_specs=(ANY, ANY),
        scratch_shapes=[
            pltpu.VMEM((tok, 1), F32), pltpu.VMEM((1, tok), F32), pltpu.VMEM((1, tok), F32), pltpu.VMEM((1, tok), F32), pltpu.VMEM((8, 2 * dim), F32),
            pltpu.VMEM((2, tok, d_model), BF16), pltpu.VMEM((4, width // RING, d_model), BF16),
            pltpu.VMEM((TYPES, width, tok), BF16), pltpu.VMEM((TYPES, width, tok), F32),
            pltpu.VMEM(pack, F32), pltpu.VMEM(pack, F32), pltpu.VMEM(back, BF16), pltpu.VMEM(back, BF16),
            DMA((2,)), DMA((4,)), DMA((TYPES, SLOTS)), DMA((TYPES - 1, n_piece)), DMA((TYPES - 1, n_piece)),
            DMA((2, n_dev)), DMA((2, n_dev)), DMA((2, n_dev)), DMA((2, n_dev))],
        compiler_params=pltpu.CompilerParams(collective_id=0, has_side_effects=True, vmem_limit_bytes=56 * MIB),
    )(flags[None, :], x_loc, dy_loc, *weights)


def row_products(g_ref, w_refs, y_ref, dx_ref, rows_in, rows_t, w_tile, total, done, g_sem, w_sem, put_sem):
    width = rows_in.shape[0]
    cols = w_tile.shape[2]
    n_tile = total.shape[1] // cols
    step = width // SLOTS
    order = (O_TYPE, 0, 1, 2)

    def g_copy(i):
        return pltpu.make_async_copy(g_ref.at[order[i]], rows_in, g_sem)

    def w_copy(i, n, slot):
        return pltpu.make_async_copy(w_refs[order[i]].at[:, span(n * cols, cols)], w_tile.at[slot], w_sem.at[slot])

    puts = [pltpu.make_async_copy(done, ref, put_sem) for ref in (y_ref, dx_ref)]

    def turned(i):
        if i == 1:
            puts[0].start()
        if i == O_TYPE:
            puts[0].wait()
        g_copy(i).wait()

        @pl.loop(0, width // step)
        def _(b):
            at = span(b * step, step)
            rows_t[:, at] = jnp.transpose(rows_in[at, :])

        if i < O_TYPE:
            g_copy(i + 1).start()

    def use(i, n, slot):
        at = span(n * cols, cols)
        prod = dot(rows_t[...], w_tile[slot], INNER)
        if i == 0:
            done[:, at] = prod.astype(BF16)
        elif i == 1:
            total[:, at] = prod
        elif i < O_TYPE:
            total[:, at] = total[:, at] + prod
        else:
            done[:, at] = (total[:, at] + prod).astype(BF16)

    g_copy(0).start()
    stream(TYPES, n_tile, w_tile.shape[0], w_copy, use, turned)
    puts[1].start()
    return puts[1]


FLIPS = ((1, 1), (1, 0), (0, 1), (0, 0))


def reduce_kernel(g_ref, z_ref, x_ref, dy_ref, wq_ref, wk_ref, wv_ref, wo_ref, out_ref, y_ref, dx_ref,
                  zbuf, rows_in, side_out, side_in, first_out, first_in, second_out, second_in, kind_rows, rows_t, w_tile, sums, done,
                  z_sem, row_send, row_recv, side_send, side_recv, first_send, first_recv, second_send, second_recv, g_sem, w_sem, put_sem):
    me = lax.axis_index('sp')
    x, y, core = place(me)
    square = Square(me)
    block = rows_in.shape[3]
    part = block // 2
    n_col, cols = second_out.shape[1], second_out.shape[3]
    sibling = index_of(x, y, 1 - core)
    across = (index_of(x + 2, y, core), index_of(x, y + 2, core))

    meet([sibling, *across] + [square.peer(k) for k in range(1, TYPES)])

    def own_copy(ref):
        return pltpu.make_async_copy(ref, zbuf.at[0], z_sem.at[0])

    z_copies = [pltpu.make_async_copy(z_ref.at[k - 1], zbuf.at[k], z_sem.at[k]) for k in range(1, TYPES)]

    def row_source(k, mine, t):
        px, py = lattice(*square.chips[k])
        half = core if mine else 1 - core
        index = half * RING + lax.rem(px + FLIPS[t][0], 2) + 2 * lax.rem(py + FLIPS[t][1], 2)
        return g_ref.at[square.kind(k), span(index * block, block)]

    def row_copy(k, mine, t):
        dst, recv = rows_in.at[k, mine, t], row_recv.at[k, mine, t]
        if k == 0:
            return pltpu.make_async_copy(row_source(k, mine, t), dst, recv)
        return remote(row_source(k, mine, t), dst, row_send.at[k - 1, mine, t], recv, square.peer(k))

    every_row = [(k, mine, t) for t in range(TYPES) for mine in range(2) for k in range(TYPES)]
    for where in every_row:
        row_copy(*where).start()
    start_tokens(square.kind(0), x_ref, dy_ref, own_copy)
    for copy in z_copies:
        copy.start()

    last_put = row_products(g_ref, (wq_ref, wk_ref, wv_ref, wo_ref), y_ref, dx_ref, kind_rows, rows_t, w_tile, sums, done, g_sem, w_sem, put_sem)

    own_copy(x_ref).wait()
    for copy in z_copies:
        copy.wait()

    def product(mine, t, ch):
        at = span(ch * cols, cols)
        total = dot(rows_in[0, mine, t], zbuf[0, :, at], INNER)
        for k in range(1, TYPES):
            total = total + dot(rows_in[k, mine, t], zbuf[k, :, at], INNER)
        return total

    def side_copy(t, ch):
        return remote(side_out.at[t % 2, ch], side_in.at[t, ch], side_send.at[t, ch], side_recv.at[t, ch], sibling)

    def first_copy(leg, q, ch):
        return remote(first_out.at[leg, q, ch], first_in.at[leg, q, ch], first_send.at[leg, q, ch], first_recv.at[leg, q, ch], across[leg])

    def second_copy(leg, ch):
        return remote(second_out.at[leg, ch], second_in.at[leg, ch], second_send.at[leg, ch], second_recv.at[leg, ch], across[1 - leg])

    for t in range(TYPES):
        for mine in range(2):
            for k in range(TYPES):
                copy = row_copy(k, mine, t)
                if k:
                    copy.wait_recv()
                else:
                    copy.wait()

        @pl.loop(0, n_col)
        def _(ch, t=t):
            if t >= 2:
                side_copy(t - 2, ch).wait_send()
            side_out[t % 2, ch] = product(0, t, ch)
            side_copy(t, ch).start()

        @pl.loop(0, n_col)
        def _(ch, t=t):
            total = product(1, t, ch)
            side_copy(t, ch).wait_recv()
            total = total + side_in[t, ch]
            for leg in range(2):
                half = total[leg * part:(leg + 1) * part]
                step, other = FLIPS[t][leg], FLIPS[t][1 - leg]
                if step:
                    first_out[leg, other, ch] = half
                    first_copy(leg, other, ch).start()
                    continue
                first_copy(leg, other, ch).wait_recv()
                half = half + first_in[leg, other, ch]
                if other:
                    second_out[leg, ch] = half
                    second_copy(leg, ch).start()
                else:
                    second_copy(leg, ch).wait_recv()
                    out_ref[leg * part:(leg + 1) * part, span(ch * cols, cols)] = half + second_in[leg, ch]

    last_put.wait()
    for where in every_row:
        if where[0]:
            row_copy(*where).wait_send()

    @pl.loop(0, n_col)
    def _(ch):
        for t in range(2, TYPES):
            side_copy(t, ch).wait_send()
        for leg in range(2):
            for q in range(2):
                first_copy(leg, q, ch).wait_send()
            second_copy(leg, ch).wait_send()


def reduce_rows(g, z, x_loc, dy_loc, weights):
    width, tok = g.shape[1], g.shape[2]
    d_model = x_loc.shape[1]
    block = width // SLOTS
    n_col = RING
    cols = d_model // n_col
    tokens = jax.ShapeDtypeStruct((tok, d_model), BF16)
    halves = lambda *lead: pltpu.VMEM((*lead, n_col, block // 2, cols), F32)
    blocks = lambda lead: pltpu.VMEM((lead, n_col, block, cols), F32)
    return pl.pallas_call(
        reduce_kernel,
        name='reduce_rows',
        out_shape=(pltpu.VMEM((block, d_model), F32), tokens, tokens),
        in_specs=[ANY] * 8,
        out_specs=(VMEM, ANY, ANY),
        scratch_shapes=[
            pltpu.VMEM((TYPES, tok, d_model), BF16), pltpu.VMEM((TYPES, 2, TYPES, block, tok), BF16),
            blocks(2), blocks(TYPES), halves(2, 2), halves(2, 2), halves(2), halves(2),
            pltpu.VMEM((width, tok), BF16), pltpu.VMEM((tok, width), BF16), pltpu.VMEM((3, width, min(256, d_model // 4)), BF16),
            pltpu.VMEM((tok, d_model), F32), pltpu.VMEM((tok, d_model), BF16),
            DMA((TYPES,)), DMA((TYPES - 1, 2, TYPES)), DMA((TYPES, 2, TYPES)), DMA((TYPES, n_col)), DMA((TYPES, n_col)),
            DMA((2, 2, n_col)), DMA((2, 2, n_col)), DMA((2, n_col)), DMA((2, n_col)), DMA, DMA((3,)), DMA],
        compiler_params=pltpu.CompilerParams(collective_id=1, has_side_effects=True, vmem_limit_bytes=58 * MIB),
    )(g, z, x_loc, dy_loc, *weights)


def gather_kernel(piece_ref, near_ref, far_a_ref, far_b_ref, far_c_ref, send_sem, recv_sem, side_send, side_recv):
    me = lax.axis_index('sp')
    x, y, core = place(me)
    rows = piece_ref.shape[0]
    part = rows // 2
    quarter = part // 2

    def number(leg, i, j):
        sx, sy = (i, j) if leg == 0 else (j, i)
        px, py = lax.rem(x + sx, RING), lax.rem(y + sy, RING)
        lx, ly = lattice(px, py)
        return owned_type(px, py) * RING + lx + 2 * ly

    def spot(leg, i, j, half=None):
        lo, size = (0, part) if half is None else (half * quarter, quarter)
        return near_ref.at[pl.ds(pl.multiple_of(number(leg, i, j) * rows + leg * part + lo, quarter), size)]

    def far_spots(leg, i, j):
        refs = [(far_a_ref, part)] if leg == 0 else [(far_b_ref, quarter), (far_c_ref, quarter)]
        return [ref.at[span(number(leg, i, j) * size, size)] for ref, size in refs]

    def own(leg, half=None):
        lo, size = (0, part) if half is None else (half * quarter, quarter)
        return piece_ref.at[pl.ds(leg * part + lo, size)]

    def step_peer(leg, second, step):
        along_x = (leg == 0) != second
        return index_of(x + step, y, core) if along_x else index_of(x, y + step, core)

    started = []

    def push(leg, second, i, j, step, half):
        there = (i, (j - step) % RING) if second else ((i - step) % RING, j)
        src = own(leg, half) if i == 0 and j == 0 else spot(leg, i, j, half)
        copy = remote(src, spot(leg, i, j, half), send_sem.at[len(started)],
                      recv_sem.at[leg, there[0], there[1], half or 0], step_peer(leg, second, step))
        copy.start()
        started.append(copy)

    def landed(leg, i, j):
        in_halves = j == 2 or (j == 0 and i == 2)
        for half in ((0, 1) if in_halves else (None,)):
            here = spot(leg, i, j, half)
            remote(here, here, send_sem.at[0], recv_sem.at[leg, i, j, half or 0], me).wait_recv()

    side = []

    def to_sibling(leg, i, j):
        for half, dst in enumerate(far_spots(leg, i, j)):
            half = half if leg else None
            src = own(leg, half) if i == 0 and j == 0 else spot(leg, i, j, half)
            copy = remote(src, dst, side_send.at[leg, i, j, half or 0], side_recv.at[leg, i, j, half or 0], index_of(x, y, 1 - core))
            copy.start()
            side.append(copy)

    meet([index_of(x, y, 1 - core)] + [index_of(*chip, core) for chip in chips_around(x, y)])

    def spread(leg, i):
        push(leg, True, i, 0, 1, None)
        push(leg, True, i, 0, 3, None)
        to_sibling(leg, i, 0)

    for leg in range(2):
        push(leg, False, 0, 0, 1, None)
        push(leg, False, 0, 0, 3, None)
    for leg in range(2):
        spread(leg, 0)
    near_ref[span(number(0, 0, 0) * rows, rows), :] = piece_ref[...]

    for leg in range(2):
        landed(leg, 3, 0)
        push(leg, False, 3, 0, 1, 0)
        spread(leg, 3)
        landed(leg, 1, 0)
        push(leg, False, 1, 0, 3, 1)
        spread(leg, 1)

    def second_near(leg, i):
        landed(leg, i, 3)
        push(leg, True, i, 3, 1, 0)
        to_sibling(leg, i, 3)
        landed(leg, i, 1)
        push(leg, True, i, 1, 3, 1)
        to_sibling(leg, i, 1)

    for leg in range(2):
        second_near(leg, 0)
    for leg in range(2):
        landed(leg, 2, 0)
        spread(leg, 2)
    for i in (3, 1, 2):
        for leg in range(2):
            second_near(leg, i)
    for i in (0, 3, 1, 2):
        for leg in range(2):
            landed(leg, i, 2)
            to_sibling(leg, i, 2)

    for copy in started + side:
        copy.wait_send()

    for leg in range(2):
        for i in range(RING):
            for j in range(RING):
                for half, here in enumerate(far_spots(leg, i, j)):
                    remote(here, here, side_send.at[leg, i, j, half], side_recv.at[leg, i, j, half], me).wait_recv()


def gather_rows(piece, n_dev):
    rows, d_model = piece.shape
    half = n_dev * rows // CORES
    return pl.pallas_call(
        gather_kernel,
        name='gather_rows',
        out_shape=(pltpu.VMEM((half, d_model), F32), pltpu.VMEM((half // 2, d_model), F32), pltpu.VMEM((half // 4, d_model), F32),
                   jax.ShapeDtypeStruct((half // 4, d_model), F32)),
        in_specs=[VMEM],
        out_specs=(VMEM, VMEM, VMEM, ANY),
        scratch_shapes=[DMA((40,)), DMA((2, RING, RING, 2)), DMA((2, RING, RING, 2)), DMA((2, RING, RING, 2))],
        compiler_params=pltpu.CompilerParams(collective_id=2, has_side_effects=True, vmem_limit_bytes=STORE_LIMIT),
    )(piece)


def store_kernel(near_ref, far_a_ref, far_b_ref, far_c_ref, dq_out, dk_out, dv_out, do_out, tile, put_sem, a_sem, b_sem, in_sem, out_sem):
    core = lax.rem(lax.axis_index('sp'), CORES)
    outs = (dq_out, dk_out, dv_out, do_out)
    rows = near_ref.shape[0] // TYPES
    n_slot, chunk = tile.shape[0], tile.shape[1]
    n = far_c_ref.shape[0] // chunk
    piece = 4 * chunk

    def far_out(i, lo, size):
        first = (1 - core) * rows + i % RING * piece + lo
        return outs[i // RING].at[pl.ds(pl.multiple_of(first, chunk), size)]

    puts = [pltpu.make_async_copy(near_ref.at[pl.ds(kind * rows, rows)], outs[kind].at[span(core * rows, rows)], put_sem.at[kind])
            for kind in range(TYPES)]
    for i in range(n):
        puts.append(pltpu.make_async_copy(far_a_ref.at[pl.ds(i * 2 * chunk, 2 * chunk)], far_out(i, 0, 2 * chunk), a_sem.at[i]))
        puts.append(pltpu.make_async_copy(far_b_ref.at[pl.ds(i * chunk, chunk)], far_out(i, 2 * chunk, chunk), b_sem.at[i]))

    def load(i):
        return pltpu.make_async_copy(far_c_ref.at[pl.ds(i * chunk, chunk)], tile.at[i % n_slot], in_sem.at[i % n_slot])

    def save(i):
        return pltpu.make_async_copy(tile.at[i % n_slot], far_out(i, piece - chunk, chunk), out_sem.at[i % n_slot])

    ahead = n_slot // 2
    for i in range(ahead):
        load(i).start()
    for put in puts:
        put.start()
    for i in range(n):
        load(i).wait()
        save(i).start()
        if i + ahead < n:
            if i + ahead >= n_slot:
                save(i + ahead - n_slot).wait()
            load(i + ahead).start()
    for i in range(n - n_slot, n):
        save(i).wait()
    for put in puts:
        put.wait()


def store(near, far_a, far_b, far_c):
    half, d_model = near.shape
    n = RING * RING
    chunk = far_c.shape[0] // n
    grad = jax.ShapeDtypeStruct((half * CORES // TYPES, d_model), F32)
    return pl.pallas_call(
        store_kernel,
        name='store',
        out_shape=(grad,) * TYPES,
        in_specs=[VMEM, VMEM, VMEM, ANY],
        out_specs=(ANY,) * TYPES,
        scratch_shapes=[pltpu.VMEM((6, chunk, d_model), F32), DMA((TYPES,)), DMA((n,)), DMA((n,)), DMA((6,)), DMA((6,))],
        compiler_params=pltpu.CompilerParams(vmem_limit_bytes=STORE_LIMIT),
    )(in_vmem(near), in_vmem(far_a), in_vmem(far_b), pltpu.with_memory_space_constraint(far_c, pltpu.HBM))


def solution(mesh):
    n_dev = mesh.shape['sp']
    assert n_dev == CORES * RING * RING

    def device_body(x_loc, flag_loc, w_q, w_k, w_v, w_o, dy_loc):
        tok_count, d_model = x_loc.shape
        n_heads, head_dim = w_q.shape[1], w_q.shape[2]
        width = n_heads * head_dim
        score_scale = 1.0 / (math.sqrt(head_dim) * tok_count)
        weights = [w.transpose(1, 2, 0).reshape(width, d_model) for w in (w_q, w_k, w_v)] + [w_o.reshape(width, d_model)]
        g, z = front(flag_loc, x_loc, dy_loc, weights, score_scale, n_dev, n_heads)
        piece, y_loc, dx_loc = reduce_rows(g, z, x_loc, dy_loc, weights)
        grads = store(*gather_rows(piece, n_dev))
        dw_q, dw_k, dw_v, dw_o = (grad.reshape(n_heads, head_dim, d_model) for grad in grads)
        return y_loc, dx_loc, dw_q.transpose(2, 0, 1), dw_k.transpose(2, 0, 1), dw_v.transpose(2, 0, 1), dw_o

    row_spec = P(('dp', 'sp'), None)
    flag_spec = P(('dp', 'sp'))
    w_spec = P(None, None, None)
    dw_spec = P('dp', None, None)
    return jax.shard_map(device_body, mesh=mesh,
                         in_specs=(row_spec, flag_spec, w_spec, w_spec, w_spec, w_spec, row_spec),
                         out_specs=(row_spec, row_spec, dw_spec, dw_spec, dw_spec, dw_spec),
                         check_vma=False)
```

```python
import functools
import math
import jax
import jax.numpy as jnp
from jax import lax
from jax.experimental import pallas as pl
from jax.experimental.pallas import tpu as pltpu
from jax.sharding import PartitionSpec as P

MESH = pl.DeviceIdType.MESH
CORES = 2
RING = 4
SLOTS = CORES * RING
TYPES = 4
O_TYPE = TYPES - 1
MIB = 1024 * 1024
STORE_LIMIT = 5 * MIB
BF16 = jnp.bfloat16
F32 = jnp.float32
ROWS = ((1,), (1,))
INNER = ((1,), (0,))
OUTER = ((0,), (0,))
VMEM = pl.BlockSpec(memory_space=pltpu.VMEM)
ANY = pl.BlockSpec(memory_space=pltpu.HBM)
DMA = pltpu.SemaphoreType.DMA


def place(me):
    core = lax.rem(me, CORES)
    chip = me // CORES
    return lax.rem(chip, RING), chip // RING, core


def index_of(x, y, core):
    return (lax.rem(y, RING) * RING + lax.rem(x, RING)) * CORES + core


def remote(src, dst, send_sem, recv_sem, peer):
    return pltpu.make_async_remote_copy(src_ref=src, dst_ref=dst, send_sem=send_sem, recv_sem=recv_sem,
                                        device_id={'sp': peer}, device_id_type=MESH)


def signal(peer):
    pl.semaphore_signal(pltpu.get_barrier_semaphore(), inc=1, device_id={'sp': peer}, device_id_type=MESH)


def meet(peers):
    for peer in peers:
        signal(peer)
    pl.semaphore_wait(pltpu.get_barrier_semaphore(), len(peers))


def chips_around(x, y):
    return ((x + 1, y), (x + RING - 1, y), (x, y + 1), (x, y + RING - 1))


def dot(a, b, dims):
    return lax.dot_general(a, b, (dims, ((), ())), preferred_element_type=F32)


def in_vmem(value):
    return pltpu.with_memory_space_constraint(value, pltpu.VMEM)


def in_hbm(value):
    return pltpu.with_memory_space_constraint(value, pltpu.HBM)


def span(start, size):
    return pl.ds(pl.multiple_of(start, size), size)


def stream(n_outer, n_inner, depth, copy, use, before):
    ahead = depth - 1
    for n in range(ahead):
        copy(0, n, n).start()
    for i in range(n_outer):
        before(i)

        @pl.loop(0, n_inner)
        def _(n):
            at = i * n_inner + n
            slot, free = lax.rem(at, depth), lax.rem(at + ahead, depth)

            @pl.when(n + ahead < n_inner)
            def _():
                copy(i, n + ahead, free).start()

            if i + 1 < n_outer:
                @pl.when(n + ahead >= n_inner)
                def _():
                    copy(i + 1, n + ahead - n_inner, free).start()

            copy(i, n, slot).wait()
            use(i, n, slot)


def form_masks(flag_ref, seg_col_ref, seg_row_ref, head_ref, tail_ref, gate_ref):
    tok = flag_ref.shape[1]
    flags = flag_ref[...] > 0
    t_pos = lax.broadcasted_iota(jnp.int32, (tok, tok), 0)
    s_pos = lax.broadcasted_iota(jnp.int32, (tok, tok), 1)
    seg_col = jnp.sum(jnp.where(flags & (s_pos <= t_pos), 1.0, 0), axis=1, keepdims=True)
    seg_col_ref[...] = seg_col
    seg_row_ref[...] = jnp.sum(jnp.where(s_pos == t_pos, seg_col, 0), axis=0, keepdims=True)
    positions = lax.broadcasted_iota(jnp.int32, (1, tok), 1).astype(F32)
    first_pos = jnp.min(jnp.where(flags, positions, tok), axis=1, keepdims=True)
    last_pos = jnp.max(jnp.where(flags, positions, -1), axis=1, keepdims=True)
    head_ref[...] = jnp.where(positions < first_pos, 1.0, 0)
    tail_ref[...] = jnp.where(positions >= last_pos, 1.0, 0)
    gate_ref[...] = jnp.broadcast_to(jnp.where(last_pos < 0, 1.0, 0), gate_ref.shape)


class Square:
    def __init__(self, me):
        x, y, core = place(me)
        across_x, across_y = (lax.rem(a + 1 + RING - 2 * lax.rem(a + core, 2), RING) for a in (x, y))
        self.core = core
        self.chips = [(x, y), (across_x, y), (x, across_y), (across_x, across_y)]

    def peer(self, k):
        return index_of(*self.chips[k], self.core)

    def kind(self, k):
        return owned_type(*self.chips[k])


def owned_type(x, y):
    return lax.rem(x, 2) + 2 * lax.rem(y, 2)


def lattice(x, y):
    return lax.rem(x // 2, 2), lax.rem(y // 2, 2)


def start_tokens(kind, x_ref, dy_ref, copy):
    @pl.when(kind == O_TYPE)
    def _():
        copy(dy_ref).start()

    @pl.when(kind != O_TYPE)
    def _():
        copy(x_ref).start()


def front_kernel(scale, dim, flag_ref, x_ref, dy_ref, wq_ref, wk_ref, wv_ref, wo_ref,
                 g_ref, z_ref, seg_col_ref, seg_row_ref, head_ref, tail_ref, gate_ref, tok_in, w_tile, rows_ref, total,
                 packed, held, formed, states,
                 tok_sem, w_sem, g_sem, z_send, z_recv, send_sem, recv_sem, back_send, back_recv):
    me = lax.axis_index('sp')
    n_dev, per_dev, low = formed.shape[1:4]
    width, tok = rows_ref.shape[1], rows_ref.shape[2]
    half = tok // 2
    n_piece = z_recv.shape[1]
    piece = tok // SLOTS
    n_group = SLOTS
    group = width // n_group
    tile_rows = w_tile.shape[1]

    @pl.loop(1, n_dev)
    def _(step):
        signal(lax.rem(me + step, n_dev))

    loads = [pltpu.make_async_copy(ref, tok_in.at[i], tok_sem.at[i]) for i, ref in enumerate((x_ref, dy_ref))]
    for load in loads:
        load.start()

    square = Square(me)

    cuts = (0, 2, 3, TYPES, SLOTS)

    def token_copy(k, n):
        at = pl.ds(cuts[n] * piece, (cuts[n + 1] - cuts[n]) * piece)
        return lambda ref: remote(ref.at[at], z_ref.at[k - 1, at], z_send.at[k - 1, n], z_recv.at[k - 1, n], square.peer(k))

    def push_tokens(n):
        for k in range(1, TYPES):
            start_tokens(square.kind(k), x_ref, dy_ref, token_copy(k, n))

    form_masks(flag_ref, seg_col_ref, seg_row_ref, head_ref, tail_ref, gate_ref)
    pl.semaphore_wait(pltpu.get_barrier_semaphore(), n_dev - 1)
    push_tokens(0)

    weights = (wk_ref, wv_ref, wq_ref, wo_ref)
    kinds = (1, 2, 0, O_TYPE)

    def w_copy(i, n, slot):
        return pltpu.make_async_copy(weights[i].at[span(n * tile_rows, tile_rows)], w_tile.at[slot], w_sem.at[slot])

    def project(i, n, slot):
        rows_ref[kinds[i], span(n * tile_rows, tile_rows), :] = dot(w_tile[slot], tok_in[i // O_TYPE], ROWS).astype(BF16)

    def loaded(i):
        if i in (0, O_TYPE):
            loads[i // O_TYPE].wait()
        if i == 2:
            send_products(0)
        if i in (1, O_TYPE):
            push_tokens(1 + i // O_TYPE)

    head = head_ref[...] > 0.5
    tail = tail_ref[...] > 0.5

    def each(do):
        pl.loop(1, n_dev)(do)

    def out_copy(which, step):
        peer = lax.rem(me + step, n_dev)
        at = pl.ds(0, low + 1 - which)
        return remote(packed.at[which, peer, :, at], held.at[which, me, :, at], send_sem.at[which, step], recv_sem.at[which, step], peer)

    def back_copy(which, step):
        peer = lax.rem(me + step, n_dev)
        return remote(formed.at[which, peer], states.at[which, me], back_send.at[which, step], back_recv.at[which, step], peer)

    pair_lane = lax.broadcasted_iota(jnp.int32, (low, 2 * dim), 1) // dim

    def turn(pair):
        return pltpu.roll(pair, dim, 1)

    def send_products(which):
        left, right, mask = ((1, 2, tail), (0, O_TYPE, head))[which]

        @pl.loop(0, n_group)
        def _(grp):
            at = span(grp * group, group)
            full = dot(rows_ref[left, at, :], jnp.where(mask, rows_ref[right, at, :], jnp.zeros((group, tok), BF16)), ROWS)
            for sub in range(group // dim):
                spot = sub % 2
                block = full[sub * dim:(sub + 1) * dim, (sub // 2) * 2 * dim:(sub // 2 + 1) * 2 * dim]
                first, second = block[0:low], block[low:]
                if spot == 0:
                    second = turn(second)
                else:
                    first = turn(first)
                index = grp * (group // dim) + sub
                dev, own = index // per_dev, lax.rem(index, per_dev)
                packed[which, dev, own, 0:low, :] = jnp.where(pair_lane == 0, first, second)
                packed[which, dev, own, low:, :] = gate_ref[...]

        each(lambda step: out_copy(which, step).start())
        held[which, me] = packed[which, me]

    def form_states(which):
        each(lambda step: out_copy(which, step).wait_recv())

        def advance(step, state):
            block = step if which == 0 else n_dev - 1 - step
            formed[which, block] = state.astype(BF16)
            return held[0, block, :, low:low + 1, :] * state + held[which, block, :, 0:low, :]

        lax.fori_loop(0, n_dev, advance, jnp.zeros((per_dev, low, 2 * dim), F32))
        each(lambda step: back_copy(which, step).start())
        states[which, me] = formed[which, me]

    stream(TYPES, width // tile_rows, w_tile.shape[0], w_copy, project, loaded)
    send_products(1)

    seg_row = seg_row_ref[...]
    t_pos = lax.broadcasted_iota(jnp.int32, (half, tok), 0)
    s_pos = lax.broadcasted_iota(jnp.int32, (half, tok), 1)

    def pair(a, b):
        see_top = ((seg_col_ref[0:half, :] == seg_row) & (s_pos <= t_pos))[:, 0:half]
        see_low = (seg_col_ref[half:, :] == seg_row) & (s_pos <= t_pos + half)
        top = dot(a[:, 0:half], b[:, 0:half], OUTER)
        low = dot(a[:, half:], b, OUTER)
        return (jnp.where(see_top, top * scale, 0).astype(BF16), jnp.where(see_low, low * scale, 0).astype(BF16))

    def over_keys(at, rows_t, probs):
        total[at[0], at[1], 0:half] = dot(rows_t[:, 0:half], probs[0], ROWS)
        total[at[0], at[1], half:] = dot(rows_t, probs[1], ROWS)

    def over_queries(at, rows_t, probs):
        from_low = dot(rows_t[:, half:], probs[1], INNER)
        total[at[0], at[1], 0:half] = dot(rows_t[:, 0:half], probs[0], INNER) + from_low[:, 0:half]
        total[at[0], at[1], half:] = from_low[:, half:]

    def heads_of(grp):
        return [grp * (group // dim) + sub for sub in range(group // dim)]

    @pl.loop(0, n_group)
    def _(grp):
        @pl.when(grp == 1)
        def _():
            form_states(0)

        @pl.when(grp == n_group // 2 + 1)
        def _():
            form_states(1)
            push_tokens(O_TYPE)

        for index in heads_of(grp):
            rows = span(index * dim, dim)
            q, k, v, do = (rows_ref[kind, rows, :] for kind in range(TYPES))
            d_probs = pair(do, v)
            over_keys((0, rows), k, d_probs)
            over_queries((1, rows), q, d_probs)
            probs = pair(q, k)
            over_queries((2, rows), do, probs)
            over_keys((O_TYPE, rows), v, probs)

    def diagonal(which, grp):
        rows = []
        for sub in range(group // dim):
            index = grp * (group // dim) + sub
            pair = states[which, index // per_dev, lax.rem(index, per_dev)].astype(F32)
            spot = sub % 2
            block = jnp.concatenate([turn(pair), pair] if spot else [pair, turn(pair)], axis=0)
            block = jnp.where(jnp.concatenate([pair_lane, pair_lane], axis=0) == spot, block, 0)
            empty = jnp.zeros_like(block)
            rows.append(jnp.concatenate([empty, block] if sub // 2 else [block, empty], axis=1))
        return jnp.concatenate(rows, axis=0).astype(BF16)

    def finish(kind, at, mask, inter):
        rows_ref[kind, at, :] = (total[kind, at, :] + jnp.where(mask, inter * scale, 0)).astype(BF16)

    def row_put(kind, grp):
        at = span(grp * group, group)
        return pltpu.make_async_copy(rows_ref.at[kind, at], g_ref.at[kind, at], g_sem.at[kind, grp])

    each(lambda step: back_copy(0, step).wait_recv())

    @pl.loop(0, n_group)
    def _(grp):
        at = span(grp * group, group)
        st = diagonal(0, grp)
        d_q = dot(st, rows_ref[O_TYPE, at, :], INNER)
        out = dot(st, rows_ref[0, at, :], OUTER)
        finish(0, at, head, d_q)
        finish(O_TYPE, at, head, out)
        for kind in (0, O_TYPE):
            row_put(kind, grp).start()

    each(lambda step: back_copy(1, step).wait_recv())

    @pl.loop(0, n_group)
    def _(grp):
        at = span(grp * group, group)
        st = diagonal(1, grp)
        d_k = dot(st, rows_ref[2, at, :], INNER)
        d_v = dot(st, rows_ref[1, at, :], OUTER)
        finish(1, at, tail, d_k)
        finish(2, at, tail, d_v)
        for kind in (1, 2):
            row_put(kind, grp).start()

    for kind in range(TYPES):
        pl.loop(0, n_group)(lambda grp, kind=kind: row_put(kind, grp).wait())
    for which in range(2):
        each(lambda step, which=which: out_copy(which, step).wait_send())
        each(lambda step, which=which: back_copy(which, step).wait_send())
    for k in range(1, TYPES):
        for n in range(n_piece):
            token_copy(k, n)(x_ref).wait()


def front(flags, x_loc, dy_loc, weights, scale, n_dev, n_heads):
    tok, d_model = x_loc.shape
    width = weights[0].shape[0]
    dim = width // n_heads
    per_dev = n_heads // n_dev
    n_piece = TYPES
    pack = (2, n_dev, per_dev, dim // 2 + 8, 2 * dim)
    back = (2, n_dev, per_dev, dim // 2, 2 * dim)
    return pl.pallas_call(
        functools.partial(front_kernel, scale, dim),
        name='front',
        out_shape=(jax.ShapeDtypeStruct((TYPES, width, tok), BF16), jax.ShapeDtypeStruct((TYPES - 1, tok, d_model), BF16)),
        in_specs=[VMEM] + [ANY] * 6,
        out_specs=(ANY, ANY),
        scratch_shapes=[
            pltpu.VMEM((tok, 1), F32), pltpu.VMEM((1, tok), F32), pltpu.VMEM((1, tok), F32), pltpu.VMEM((1, tok), F32), pltpu.VMEM((8, 2 * dim), F32),
            pltpu.VMEM((2, tok, d_model), BF16), pltpu.VMEM((4, width // RING, d_model), BF16),
            pltpu.VMEM((TYPES, width, tok), BF16), pltpu.VMEM((TYPES, width, tok), F32),
            pltpu.VMEM(pack, F32), pltpu.VMEM(pack, F32), pltpu.VMEM(back, BF16), pltpu.VMEM(back, BF16),
            DMA((2,)), DMA((4,)), DMA((TYPES, SLOTS)), DMA((TYPES - 1, n_piece)), DMA((TYPES - 1, n_piece)),
            DMA((2, n_dev)), DMA((2, n_dev)), DMA((2, n_dev)), DMA((2, n_dev))],
        compiler_params=pltpu.CompilerParams(collective_id=0, has_side_effects=True, vmem_limit_bytes=56 * MIB),
    )(flags[None, :], x_loc, dy_loc, *weights)


def row_products(g_ref, w_refs, y_ref, dx_ref, rows_in, rows_t, w_tile, total, done, g_sem, w_sem, put_sem):
    width = rows_in.shape[0]
    cols = w_tile.shape[2]
    n_tile = total.shape[1] // cols
    step = width // SLOTS
    order = (O_TYPE, 0, 1, 2)

    def g_copy(i):
        return pltpu.make_async_copy(g_ref.at[order[i]], rows_in, g_sem)

    def w_copy(i, n, slot):
        return pltpu.make_async_copy(w_refs[order[i]].at[:, span(n * cols, cols)], w_tile.at[slot], w_sem.at[slot])

    puts = [pltpu.make_async_copy(done, ref, put_sem) for ref in (y_ref, dx_ref)]

    def turned(i):
        if i == 1:
            puts[0].start()
        if i == O_TYPE:
            puts[0].wait()
        g_copy(i).wait()

        @pl.loop(0, width // step)
        def _(b):
            at = span(b * step, step)
            rows_t[:, at] = jnp.transpose(rows_in[at, :])

        if i < O_TYPE:
            g_copy(i + 1).start()

    def use(i, n, slot):
        at = span(n * cols, cols)
        prod = dot(rows_t[...], w_tile[slot], INNER)
        if i == 0:
            done[:, at] = prod.astype(BF16)
        elif i == 1:
            total[:, at] = prod
        elif i < O_TYPE:
            total[:, at] = total[:, at] + prod
        else:
            done[:, at] = (total[:, at] + prod).astype(BF16)

    g_copy(0).start()
    stream(TYPES, n_tile, w_tile.shape[0], w_copy, use, turned)
    puts[1].start()
    return puts[1]


FLIPS = ((1, 1), (1, 0), (0, 1), (0, 0))


def reduce_kernel(g_ref, z_ref, x_ref, dy_ref, wq_ref, wk_ref, wv_ref, wo_ref, out_ref, y_ref, dx_ref,
                  zbuf, rows_in, side_out, side_in, first_out, first_in, second_out, second_in, kind_rows, rows_t, w_tile, sums, done,
                  z_sem, row_send, row_recv, side_send, side_recv, first_send, first_recv, second_send, second_recv, g_sem, w_sem, put_sem):
    me = lax.axis_index('sp')
    x, y, core = place(me)
    square = Square(me)
    block = rows_in.shape[3]
    part = block // 2
    n_col, cols = second_out.shape[1], second_out.shape[3]
    sibling = index_of(x, y, 1 - core)
    across = (index_of(x + 2, y, core), index_of(x, y + 2, core))

    meet([sibling, *across] + [square.peer(k) for k in range(1, TYPES)])

    def own_copy(ref):
        return pltpu.make_async_copy(ref, zbuf.at[0], z_sem.at[0])

    z_copies = [pltpu.make_async_copy(z_ref.at[k - 1], zbuf.at[k], z_sem.at[k]) for k in range(1, TYPES)]

    def row_source(k, mine, t):
        px, py = lattice(*square.chips[k])
        half = core if mine else 1 - core
        index = half * RING + lax.rem(px + FLIPS[t][0], 2) + 2 * lax.rem(py + FLIPS[t][1], 2)
        return g_ref.at[square.kind(k), span(index * block, block)]

    def row_copy(k, mine, t):
        dst, recv = rows_in.at[k, mine, t], row_recv.at[k, mine, t]
        if k == 0:
            return pltpu.make_async_copy(row_source(k, mine, t), dst, recv)
        return remote(row_source(k, mine, t), dst, row_send.at[k - 1, mine, t], recv, square.peer(k))

    every_row = [(k, mine, t) for t in range(TYPES) for mine in range(2) for k in range(TYPES)]
    for where in every_row:
        row_copy(*where).start()
    start_tokens(square.kind(0), x_ref, dy_ref, own_copy)
    for copy in z_copies:
        copy.start()

    last_put = row_products(g_ref, (wq_ref, wk_ref, wv_ref, wo_ref), y_ref, dx_ref, kind_rows, rows_t, w_tile, sums, done, g_sem, w_sem, put_sem)

    own_copy(x_ref).wait()
    for copy in z_copies:
        copy.wait()

    def product(mine, t, ch):
        at = span(ch * cols, cols)
        total = dot(rows_in[0, mine, t], zbuf[0, :, at], INNER)
        for k in range(1, TYPES):
            total = total + dot(rows_in[k, mine, t], zbuf[k, :, at], INNER)
        return total

    def side_copy(t, ch):
        return remote(side_out.at[t % 2, ch], side_in.at[t, ch], side_send.at[t, ch], side_recv.at[t, ch], sibling)

    def first_copy(leg, q, ch):
        return remote(first_out.at[leg, q, ch], first_in.at[leg, q, ch], first_send.at[leg, q, ch], first_recv.at[leg, q, ch], across[leg])

    def second_copy(leg, ch):
        return remote(second_out.at[leg, ch], second_in.at[leg, ch], second_send.at[leg, ch], second_recv.at[leg, ch], across[1 - leg])

    for t in range(TYPES):
        for mine in range(2):
            for k in range(TYPES):
                copy = row_copy(k, mine, t)
                if k:
                    copy.wait_recv()
                else:
                    copy.wait()

        @pl.loop(0, n_col)
        def _(ch, t=t):
            if t >= 2:
                side_copy(t - 2, ch).wait_send()
            side_out[t % 2, ch] = product(0, t, ch)
            side_copy(t, ch).start()

        @pl.loop(0, n_col)
        def _(ch, t=t):
            total = product(1, t, ch)
            side_copy(t, ch).wait_recv()
            total = total + side_in[t, ch]
            for leg in range(2):
                half = total[leg * part:(leg + 1) * part]
                step, other = FLIPS[t][leg], FLIPS[t][1 - leg]
                if step:
                    first_out[leg, other, ch] = half
                    first_copy(leg, other, ch).start()
                    continue
                first_copy(leg, other, ch).wait_recv()
                half = half + first_in[leg, other, ch]
                if other:
                    second_out[leg, ch] = half
                    second_copy(leg, ch).start()
                else:
                    second_copy(leg, ch).wait_recv()
                    out_ref[leg * part:(leg + 1) * part, span(ch * cols, cols)] = half + second_in[leg, ch]

    last_put.wait()
    for where in every_row:
        if where[0]:
            row_copy(*where).wait_send()

    @pl.loop(0, n_col)
    def _(ch):
        for t in range(2, TYPES):
            side_copy(t, ch).wait_send()
        for leg in range(2):
            for q in range(2):
                first_copy(leg, q, ch).wait_send()
            second_copy(leg, ch).wait_send()


def reduce_rows(g, z, x_loc, dy_loc, weights):
    width, tok = g.shape[1], g.shape[2]
    d_model = x_loc.shape[1]
    block = width // SLOTS
    n_col = RING
    cols = d_model // n_col
    tokens = jax.ShapeDtypeStruct((tok, d_model), BF16)
    halves = lambda *lead: pltpu.VMEM((*lead, n_col, block // 2, cols), F32)
    blocks = lambda lead: pltpu.VMEM((lead, n_col, block, cols), F32)
    return pl.pallas_call(
        reduce_kernel,
        name='reduce_rows',
        out_shape=(pltpu.VMEM((block, d_model), F32), tokens, tokens),
        in_specs=[ANY] * 8,
        out_specs=(VMEM, ANY, ANY),
        scratch_shapes=[
            pltpu.VMEM((TYPES, tok, d_model), BF16), pltpu.VMEM((TYPES, 2, TYPES, block, tok), BF16),
            blocks(2), blocks(TYPES), halves(2, 2), halves(2, 2), halves(2), halves(2),
            pltpu.VMEM((width, tok), BF16), pltpu.VMEM((tok, width), BF16), pltpu.VMEM((3, width, min(256, d_model // 4)), BF16),
            pltpu.VMEM((tok, d_model), F32), pltpu.VMEM((tok, d_model), BF16),
            DMA((TYPES,)), DMA((TYPES - 1, 2, TYPES)), DMA((TYPES, 2, TYPES)), DMA((TYPES, n_col)), DMA((TYPES, n_col)),
            DMA((2, 2, n_col)), DMA((2, 2, n_col)), DMA((2, n_col)), DMA((2, n_col)), DMA, DMA((3,)), DMA],
        compiler_params=pltpu.CompilerParams(collective_id=1, has_side_effects=True, vmem_limit_bytes=58 * MIB),
    )(g, z, x_loc, dy_loc, *weights)


def gather_kernel(piece_ref, near_ref, far_a_ref, far_b_ref, far_c_ref, send_sem, recv_sem, side_send, side_recv):
    me = lax.axis_index('sp')
    x, y, core = place(me)
    rows = piece_ref.shape[0]
    part = rows // 2
    quarter = part // 2

    def number(leg, i, j):
        sx, sy = (i, j) if leg == 0 else (j, i)
        px, py = lax.rem(x + sx, RING), lax.rem(y + sy, RING)
        lx, ly = lattice(px, py)
        return owned_type(px, py) * RING + lx + 2 * ly

    def spot(leg, i, j, half=None):
        lo, size = (0, part) if half is None else (half * quarter, quarter)
        return near_ref.at[pl.ds(pl.multiple_of(number(leg, i, j) * rows + leg * part + lo, quarter), size)]

    def far_spots(leg, i, j):
        refs = [(far_a_ref, part)] if leg == 0 else [(far_b_ref, quarter), (far_c_ref, quarter)]
        return [ref.at[span(number(leg, i, j) * size, size)] for ref, size in refs]

    def own(leg, half=None):
        lo, size = (0, part) if half is None else (half * quarter, quarter)
        return piece_ref.at[pl.ds(leg * part + lo, size)]

    def step_peer(leg, second, step):
        along_x = (leg == 0) != second
        return index_of(x + step, y, core) if along_x else index_of(x, y + step, core)

    started = []

    def push(leg, second, i, j, step, half):
        there = (i, (j - step) % RING) if second else ((i - step) % RING, j)
        src = own(leg, half) if i == 0 and j == 0 else spot(leg, i, j, half)
        copy = remote(src, spot(leg, i, j, half), send_sem.at[len(started)],
                      recv_sem.at[leg, there[0], there[1], half or 0], step_peer(leg, second, step))
        copy.start()
        started.append(copy)

    def landed(leg, i, j):
        in_halves = j == 2 or (j == 0 and i == 2)
        for half in ((0, 1) if in_halves else (None,)):
            here = spot(leg, i, j, half)
            remote(here, here, send_sem.at[0], recv_sem.at[leg, i, j, half or 0], me).wait_recv()

    side = []

    def to_sibling(leg, i, j):
        for half, dst in enumerate(far_spots(leg, i, j)):
            half = half if leg else None
            src = own(leg, half) if i == 0 and j == 0 else spot(leg, i, j, half)
            copy = remote(src, dst, side_send.at[leg, i, j, half or 0], side_recv.at[leg, i, j, half or 0], index_of(x, y, 1 - core))
            copy.start()
            side.append(copy)

    meet([index_of(x, y, 1 - core)] + [index_of(*chip, core) for chip in chips_around(x, y)])

    def spread(leg, i):
        push(leg, True, i, 0, 1, None)
        push(leg, True, i, 0, 3, None)
        to_sibling(leg, i, 0)

    for leg in range(2):
        push(leg, False, 0, 0, 1, None)
        push(leg, False, 0, 0, 3, None)
    for leg in range(2):
        spread(leg, 0)
    near_ref[span(number(0, 0, 0) * rows, rows), :] = piece_ref[...]

    for leg in range(2):
        landed(leg, 3, 0)
        push(leg, False, 3, 0, 1, 0)
        spread(leg, 3)
        landed(leg, 1, 0)
        push(leg, False, 1, 0, 3, 1)
        spread(leg, 1)

    def second_near(leg, i):
        landed(leg, i, 3)
        push(leg, True, i, 3, 1, 0)
        to_sibling(leg, i, 3)
        landed(leg, i, 1)
        push(leg, True, i, 1, 3, 1)
        to_sibling(leg, i, 1)

    for leg in range(2):
        second_near(leg, 0)
    for leg in range(2):
        landed(leg, 2, 0)
        spread(leg, 2)
    for i in (3, 1, 2):
        for leg in range(2):
            second_near(leg, i)
    for i in (0, 3, 1, 2):
        for leg in range(2):
            landed(leg, i, 2)
            to_sibling(leg, i, 2)

    for copy in started + side:
        copy.wait_send()

    for leg in range(2):
        for i in range(RING):
            for j in range(RING):
                for half, here in enumerate(far_spots(leg, i, j)):
                    remote(here, here, side_send.at[leg, i, j, half], side_recv.at[leg, i, j, half], me).wait_recv()


def gather_rows(piece, n_dev):
    rows, d_model = piece.shape
    half = n_dev * rows // CORES
    return pl.pallas_call(
        gather_kernel,
        name='gather_rows',
        out_shape=(pltpu.VMEM((half, d_model), F32), pltpu.VMEM((half // 2, d_model), F32), pltpu.VMEM((half // 4, d_model), F32),
                   jax.ShapeDtypeStruct((half // 4, d_model), F32)),
        in_specs=[VMEM],
        out_specs=(VMEM, VMEM, VMEM, ANY),
        scratch_shapes=[DMA((40,)), DMA((2, RING, RING, 2)), DMA((2, RING, RING, 2)), DMA((2, RING, RING, 2))],
        compiler_params=pltpu.CompilerParams(collective_id=2, has_side_effects=True, vmem_limit_bytes=STORE_LIMIT),
    )(piece)


def store_kernel(near_ref, far_a_ref, far_b_ref, far_c_ref, y_ref, dx_ref, dq_out, dk_out, dv_out, do_out, y_out, dx_out,
                 tile, rows_buf, put_sem, a_sem, b_sem, in_sem, out_sem, row_in, row_out):
    core = lax.rem(lax.axis_index('sp'), CORES)
    outs = (dq_out, dk_out, dv_out, do_out)
    rows = near_ref.shape[0] // TYPES
    n_slot, chunk = tile.shape[0], tile.shape[1]
    n = far_c_ref.shape[0] // chunk
    piece = 4 * chunk

    def far_out(i, lo, size):
        first = (1 - core) * rows + i % RING * piece + lo
        return outs[i // RING].at[pl.ds(pl.multiple_of(first, chunk), size)]

    puts = [pltpu.make_async_copy(near_ref.at[pl.ds(kind * rows, rows)], outs[kind].at[span(core * rows, rows)], put_sem.at[kind])
            for kind in range(TYPES)]
    for i in range(n):
        puts.append(pltpu.make_async_copy(far_a_ref.at[pl.ds(i * 2 * chunk, 2 * chunk)], far_out(i, 0, 2 * chunk), a_sem.at[i]))
        puts.append(pltpu.make_async_copy(far_b_ref.at[pl.ds(i * chunk, chunk)], far_out(i, 2 * chunk, chunk), b_sem.at[i]))

    def load(i):
        return pltpu.make_async_copy(far_c_ref.at[pl.ds(i * chunk, chunk)], tile.at[i % n_slot], in_sem.at[i % n_slot])

    def save(i):
        return pltpu.make_async_copy(tile.at[i % n_slot], far_out(i, piece - chunk, chunk), out_sem.at[i % n_slot])

    steps = []
    for src, dst in ((y_ref, y_out), (dx_ref, dx_out)):
        take, give = pltpu.make_async_copy(src, rows_buf, row_in), pltpu.make_async_copy(rows_buf, dst, row_out)
        steps += [(take.start,), (take.wait, give.start), (give.wait,)]

    ahead = n_slot // 2
    for i in range(ahead):
        load(i).start()
    for put in puts:
        put.start()
    for i in range(n):
        load(i).wait()
        save(i).start()
        if i % 2 == 0 and i // 2 < len(steps):
            for action in steps[i // 2]:
                action()
        if i + ahead < n:
            if i + ahead >= n_slot:
                save(i + ahead - n_slot).wait()
            load(i + ahead).start()
    for i in range(n - n_slot, n):
        save(i).wait()
    for put in puts:
        put.wait()


def store(near, far_a, far_b, far_c, y_rows, dx_rows):
    half, d_model = near.shape
    n = RING * RING
    chunk = far_c.shape[0] // n
    grad = jax.ShapeDtypeStruct((half * CORES // TYPES, d_model), F32)
    tokens = jax.ShapeDtypeStruct(y_rows.shape, BF16)
    return pl.pallas_call(
        store_kernel,
        name='store',
        out_shape=(grad,) * TYPES + (tokens,) * 2,
        in_specs=[VMEM, VMEM, VMEM] + [ANY] * 3,
        out_specs=(ANY,) * (TYPES + 2),
        scratch_shapes=[pltpu.VMEM((4, chunk, d_model), F32), pltpu.VMEM(y_rows.shape, BF16),
                        DMA((TYPES,)), DMA((n,)), DMA((n,)), DMA((4,)), DMA((4,)), DMA, DMA],
        compiler_params=pltpu.CompilerParams(vmem_limit_bytes=STORE_LIMIT),
    )(in_vmem(near), in_vmem(far_a), in_vmem(far_b), in_hbm(far_c), in_hbm(y_rows), in_hbm(dx_rows))


def solution(mesh):
    n_dev = mesh.shape['sp']
    assert n_dev == CORES * RING * RING

    def device_body(x_loc, flag_loc, w_q, w_k, w_v, w_o, dy_loc):
        tok_count, d_model = x_loc.shape
        n_heads, head_dim = w_q.shape[1], w_q.shape[2]
        width = n_heads * head_dim
        score_scale = 1.0 / (math.sqrt(head_dim) * tok_count)
        weights = [w.transpose(1, 2, 0).reshape(width, d_model) for w in (w_q, w_k, w_v)] + [w_o.reshape(width, d_model)]
        g, z = front(flag_loc, x_loc, dy_loc, weights, score_scale, n_dev, n_heads)
        piece, y_rows, dx_rows = reduce_rows(g, z, x_loc, dy_loc, weights)
        *grads, y_loc, dx_loc = store(*gather_rows(piece, n_dev), y_rows, dx_rows)
        dw_q, dw_k, dw_v, dw_o = (grad.reshape(n_heads, head_dim, d_model) for grad in grads)
        return y_loc, dx_loc, dw_q.transpose(2, 0, 1), dw_k.transpose(2, 0, 1), dw_v.transpose(2, 0, 1), dw_o

    row_spec = P(('dp', 'sp'), None)
    flag_spec = P(('dp', 'sp'))
    w_spec = P(None, None, None)
    dw_spec = P('dp', None, None)
    return jax.shard_map(device_body, mesh=mesh,
                         in_specs=(row_spec, flag_spec, w_spec, w_spec, w_spec, w_spec, row_spec),
                         out_specs=(row_spec, row_spec, dw_spec, dw_spec, dw_spec, dw_spec),
                         check_vma=False)
```

```python
import functools
import math
import jax
import jax.numpy as jnp
from jax import lax
from jax.experimental import pallas as pl
from jax.experimental.pallas import tpu as pltpu
from jax.sharding import PartitionSpec as P

MESH = pl.DeviceIdType.MESH
CORES = 2
RING = 4
SLOTS = CORES * RING
TYPES = 4
O_TYPE = TYPES - 1
MIB = 1024 * 1024
STORE_LIMIT = 5 * MIB
BF16 = jnp.bfloat16
F32 = jnp.float32
ROWS = ((1,), (1,))
INNER = ((1,), (0,))
OUTER = ((0,), (0,))
VMEM = pl.BlockSpec(memory_space=pltpu.VMEM)
ANY = pl.BlockSpec(memory_space=pltpu.HBM)
DMA = pltpu.SemaphoreType.DMA


def place(me):
    core = lax.rem(me, CORES)
    chip = me // CORES
    return lax.rem(chip, RING), chip // RING, core


def index_of(x, y, core):
    return (lax.rem(y, RING) * RING + lax.rem(x, RING)) * CORES + core


def remote(src, dst, send_sem, recv_sem, peer):
    return pltpu.make_async_remote_copy(src_ref=src, dst_ref=dst, send_sem=send_sem, recv_sem=recv_sem,
                                        device_id={'sp': peer}, device_id_type=MESH)


def signal(peer):
    pl.semaphore_signal(pltpu.get_barrier_semaphore(), inc=1, device_id={'sp': peer}, device_id_type=MESH)


def meet(peers):
    for peer in peers:
        signal(peer)
    pl.semaphore_wait(pltpu.get_barrier_semaphore(), len(peers))


def chips_around(x, y):
    return ((x + 1, y), (x + RING - 1, y), (x, y + 1), (x, y + RING - 1))


def dot(a, b, dims):
    return lax.dot_general(a, b, (dims, ((), ())), preferred_element_type=F32)


def in_vmem(value):
    return pltpu.with_memory_space_constraint(value, pltpu.VMEM)


def in_hbm(value):
    return pltpu.with_memory_space_constraint(value, pltpu.HBM)


def span(start, size):
    return pl.ds(pl.multiple_of(start, size), size)


def stream(n_outer, n_inner, depth, copy, use, before):
    ahead = depth - 1
    for n in range(ahead):
        copy(0, n, n).start()
    for i in range(n_outer):
        before(i)

        @pl.loop(0, n_inner)
        def _(n):
            at = i * n_inner + n
            slot, free = lax.rem(at, depth), lax.rem(at + ahead, depth)

            @pl.when(n + ahead < n_inner)
            def _():
                copy(i, n + ahead, free).start()

            if i + 1 < n_outer:
                @pl.when(n + ahead >= n_inner)
                def _():
                    copy(i + 1, n + ahead - n_inner, free).start()

            copy(i, n, slot).wait()
            use(i, n, slot)


def form_masks(flag_ref, seg_col_ref, seg_row_ref, head_ref, tail_ref, gate_ref):
    tok = flag_ref.shape[1]
    flags = flag_ref[...] > 0
    t_pos = lax.broadcasted_iota(jnp.int32, (tok, tok), 0)
    s_pos = lax.broadcasted_iota(jnp.int32, (tok, tok), 1)
    seg_col = jnp.sum(jnp.where(flags & (s_pos <= t_pos), 1.0, 0), axis=1, keepdims=True)
    seg_col_ref[...] = seg_col
    seg_row_ref[...] = jnp.sum(jnp.where(s_pos == t_pos, seg_col, 0), axis=0, keepdims=True)
    positions = lax.broadcasted_iota(jnp.int32, (1, tok), 1).astype(F32)
    first_pos = jnp.min(jnp.where(flags, positions, tok), axis=1, keepdims=True)
    last_pos = jnp.max(jnp.where(flags, positions, -1), axis=1, keepdims=True)
    head_ref[...] = jnp.where(positions < first_pos, 1.0, 0)
    tail_ref[...] = jnp.where(positions >= last_pos, 1.0, 0)
    gate_ref[...] = jnp.broadcast_to(jnp.where(last_pos < 0, 1.0, 0), gate_ref.shape)


class Square:
    def __init__(self, me):
        x, y, core = place(me)
        across_x, across_y = (lax.rem(a + 1 + RING - 2 * lax.rem(a + core, 2), RING) for a in (x, y))
        self.core = core
        self.chips = [(x, y), (across_x, y), (x, across_y), (across_x, across_y)]

    def peer(self, k):
        return index_of(*self.chips[k], self.core)

    def kind(self, k):
        return owned_type(*self.chips[k])


def owned_type(x, y):
    return lax.rem(x, 2) + 2 * lax.rem(y, 2)


def lattice(x, y):
    return lax.rem(x // 2, 2), lax.rem(y // 2, 2)


def start_tokens(kind, x_ref, dy_ref, copy):
    @pl.when(kind == O_TYPE)
    def _():
        copy(dy_ref).start()

    @pl.when(kind != O_TYPE)
    def _():
        copy(x_ref).start()


def front_kernel(scale, dim, flag_ref, x_ref, dy_ref, wq_ref, wk_ref, wv_ref, wo_ref,
                 g_ref, z_ref, seg_col_ref, seg_row_ref, head_ref, tail_ref, gate_ref, tok_in, w_tile, rows_ref, total,
                 packed, held, formed, states,
                 tok_sem, w_sem, g_sem, z_send, z_recv, send_sem, recv_sem, back_send, back_recv):
    me = lax.axis_index('sp')
    n_dev, per_dev, low = formed.shape[1:4]
    width, tok = rows_ref.shape[1], rows_ref.shape[2]
    half = tok // 2
    n_piece = z_recv.shape[1]
    piece = tok // SLOTS
    n_group = SLOTS
    group = width // n_group
    tile_rows = w_tile.shape[1]

    @pl.loop(1, n_dev)
    def _(step):
        signal(lax.rem(me + step, n_dev))

    loads = [pltpu.make_async_copy(ref, tok_in.at[i], tok_sem.at[i]) for i, ref in enumerate((x_ref, dy_ref))]
    for load in loads:
        load.start()

    square = Square(me)

    cuts = (0, 2, 3, TYPES, SLOTS)

    def token_copy(k, n):
        at = pl.ds(cuts[n] * piece, (cuts[n + 1] - cuts[n]) * piece)
        return lambda ref: remote(ref.at[at], z_ref.at[k - 1, at], z_send.at[k - 1, n], z_recv.at[k - 1, n], square.peer(k))

    def push_tokens(n):
        for k in range(1, TYPES):
            start_tokens(square.kind(k), x_ref, dy_ref, token_copy(k, n))

    form_masks(flag_ref, seg_col_ref, seg_row_ref, head_ref, tail_ref, gate_ref)
    pl.semaphore_wait(pltpu.get_barrier_semaphore(), n_dev - 1)
    push_tokens(0)

    weights = (wk_ref, wv_ref, wq_ref, wo_ref)
    kinds = (1, 2, 0, O_TYPE)

    def w_copy(i, n, slot):
        return pltpu.make_async_copy(weights[i].at[span(n * tile_rows, tile_rows)], w_tile.at[slot], w_sem.at[slot])

    def project(i, n, slot):
        rows_ref[kinds[i], span(n * tile_rows, tile_rows), :] = dot(w_tile[slot], tok_in[i // O_TYPE], ROWS).astype(BF16)

    def loaded(i):
        if i in (0, O_TYPE):
            loads[i // O_TYPE].wait()
        if i == 2:
            send_products(0)
        if i in (1, O_TYPE):
            push_tokens(1 + i // O_TYPE)

    head = head_ref[...] > 0.5
    tail = tail_ref[...] > 0.5

    def each(do):
        pl.loop(1, n_dev)(do)

    def out_copy(which, step):
        peer = lax.rem(me + step, n_dev)
        at = pl.ds(0, low + 1 - which)
        return remote(packed.at[which, peer, :, at], held.at[which, me, :, at], send_sem.at[which, step], recv_sem.at[which, step], peer)

    def back_copy(which, step):
        peer = lax.rem(me + step, n_dev)
        return remote(formed.at[which, peer], states.at[which, me], back_send.at[which, step], back_recv.at[which, step], peer)

    pair_lane = lax.broadcasted_iota(jnp.int32, (low, 2 * dim), 1) // dim

    def turn(pair):
        return pltpu.roll(pair, dim, 1)

    def send_products(which):
        left, right, mask = ((1, 2, tail), (0, O_TYPE, head))[which]

        @pl.loop(0, n_group)
        def _(grp):
            at = span(grp * group, group)
            full = dot(rows_ref[left, at, :], jnp.where(mask, rows_ref[right, at, :], jnp.zeros((group, tok), BF16)), ROWS)
            for sub in range(group // dim):
                spot = sub % 2
                block = full[sub * dim:(sub + 1) * dim, (sub // 2) * 2 * dim:(sub // 2 + 1) * 2 * dim]
                first, second = block[0:low], block[low:]
                if spot == 0:
                    second = turn(second)
                else:
                    first = turn(first)
                index = grp * (group // dim) + sub
                dev, own = index // per_dev, lax.rem(index, per_dev)
                packed[which, dev, own, 0:low, :] = jnp.where(pair_lane == 0, first, second)
                packed[which, dev, own, low:, :] = gate_ref[...]

        each(lambda step: out_copy(which, step).start())
        held[which, me] = packed[which, me]

    def form_states(which):
        each(lambda step: out_copy(which, step).wait_recv())

        def advance(step, state):
            block = step if which == 0 else n_dev - 1 - step
            formed[which, block] = state.astype(BF16)
            return held[0, block, :, low:low + 1, :] * state + held[which, block, :, 0:low, :]

        lax.fori_loop(0, n_dev, advance, jnp.zeros((per_dev, low, 2 * dim), F32), unroll=4)
        each(lambda step: back_copy(which, step).start())
        states[which, me] = formed[which, me]

    stream(TYPES, width // tile_rows, w_tile.shape[0], w_copy, project, loaded)
    send_products(1)

    seg_row = seg_row_ref[...]
    t_pos = lax.broadcasted_iota(jnp.int32, (half, tok), 0)
    s_pos = lax.broadcasted_iota(jnp.int32, (half, tok), 1)

    def pair(a, b):
        see_top = ((seg_col_ref[0:half, :] == seg_row) & (s_pos <= t_pos))[:, 0:half]
        see_low = (seg_col_ref[half:, :] == seg_row) & (s_pos <= t_pos + half)
        top = dot(a[:, 0:half], b[:, 0:half], OUTER)
        low = dot(a[:, half:], b, OUTER)
        return (jnp.where(see_top, top * scale, 0).astype(BF16), jnp.where(see_low, low * scale, 0).astype(BF16))

    def over_keys(at, rows_t, probs):
        total[at[0], at[1], 0:half] = dot(rows_t[:, 0:half], probs[0], ROWS)
        total[at[0], at[1], half:] = dot(rows_t, probs[1], ROWS)

    def over_queries(at, rows_t, probs):
        from_low = dot(rows_t[:, half:], probs[1], INNER)
        total[at[0], at[1], 0:half] = dot(rows_t[:, 0:half], probs[0], INNER) + from_low[:, 0:half]
        total[at[0], at[1], half:] = from_low[:, half:]

    def heads_of(grp):
        return [grp * (group // dim) + sub for sub in range(group // dim)]

    @pl.loop(0, n_group)
    def _(grp):
        @pl.when(grp == 1)
        def _():
            form_states(0)

        @pl.when(grp == n_group // 2 + 1)
        def _():
            form_states(1)
            push_tokens(O_TYPE)

        for index in heads_of(grp):
            rows = span(index * dim, dim)
            q, k, v, do = (rows_ref[kind, rows, :] for kind in range(TYPES))
            d_probs = pair(do, v)
            over_keys((0, rows), k, d_probs)
            over_queries((1, rows), q, d_probs)
            probs = pair(q, k)
            over_queries((2, rows), do, probs)
            over_keys((O_TYPE, rows), v, probs)

    def diagonal(which, grp):
        rows = []
        for sub in range(group // dim):
            index = grp * (group // dim) + sub
            pair = states[which, index // per_dev, lax.rem(index, per_dev)].astype(F32)
            spot = sub % 2
            block = jnp.concatenate([turn(pair), pair] if spot else [pair, turn(pair)], axis=0)
            block = jnp.where(jnp.concatenate([pair_lane, pair_lane], axis=0) == spot, block, 0)
            empty = jnp.zeros_like(block)
            rows.append(jnp.concatenate([empty, block] if sub // 2 else [block, empty], axis=1))
        return jnp.concatenate(rows, axis=0).astype(BF16)

    def finish(kind, at, mask, inter):
        rows_ref[kind, at, :] = (total[kind, at, :] + jnp.where(mask, inter * scale, 0)).astype(BF16)

    def row_put(kind, grp):
        at = span(grp * group, group)
        return pltpu.make_async_copy(rows_ref.at[kind, at], g_ref.at[kind, at], g_sem.at[kind, grp])

    each(lambda step: back_copy(0, step).wait_recv())

    @pl.loop(0, n_group)
    def _(grp):
        at = span(grp * group, group)
        st = diagonal(0, grp)
        d_q = dot(st, rows_ref[O_TYPE, at, :], INNER)
        out = dot(st, rows_ref[0, at, :], OUTER)
        finish(0, at, head, d_q)
        finish(O_TYPE, at, head, out)
        for kind in (0, O_TYPE):
            row_put(kind, grp).start()

    each(lambda step: back_copy(1, step).wait_recv())

    @pl.loop(0, n_group)
    def _(grp):
        at = span(grp * group, group)
        st = diagonal(1, grp)
        d_k = dot(st, rows_ref[2, at, :], INNER)
        d_v = dot(st, rows_ref[1, at, :], OUTER)
        finish(1, at, tail, d_k)
        finish(2, at, tail, d_v)
        for kind in (1, 2):
            row_put(kind, grp).start()

    for kind in range(TYPES):
        pl.loop(0, n_group)(lambda grp, kind=kind: row_put(kind, grp).wait())
    for which in range(2):
        each(lambda step, which=which: out_copy(which, step).wait_send())
        each(lambda step, which=which: back_copy(which, step).wait_send())
    for k in range(1, TYPES):
        for n in range(n_piece):
            token_copy(k, n)(x_ref).wait()


def front(flags, x_loc, dy_loc, weights, scale, n_dev, n_heads):
    tok, d_model = x_loc.shape
    width = weights[0].shape[0]
    dim = width // n_heads
    per_dev = n_heads // n_dev
    n_piece = TYPES
    pack = (2, n_dev, per_dev, dim // 2 + 8, 2 * dim)
    back = (2, n_dev, per_dev, dim // 2, 2 * dim)
    return pl.pallas_call(
        functools.partial(front_kernel, scale, dim),
        name='front',
        out_shape=(jax.ShapeDtypeStruct((TYPES, width, tok), BF16), jax.ShapeDtypeStruct((TYPES - 1, tok, d_model), BF16)),
        in_specs=[VMEM] + [ANY] * 6,
        out_specs=(ANY, ANY),
        scratch_shapes=[
            pltpu.VMEM((tok, 1), F32), pltpu.VMEM((1, tok), F32), pltpu.VMEM((1, tok), F32), pltpu.VMEM((1, tok), F32), pltpu.VMEM((8, 2 * dim), F32),
            pltpu.VMEM((2, tok, d_model), BF16), pltpu.VMEM((4, width // RING, d_model), BF16),
            pltpu.VMEM((TYPES, width, tok), BF16), pltpu.VMEM((TYPES, width, tok), F32),
            pltpu.VMEM(pack, F32), pltpu.VMEM(pack, F32), pltpu.VMEM(back, BF16), pltpu.VMEM(back, BF16),
            DMA((2,)), DMA((4,)), DMA((TYPES, SLOTS)), DMA((TYPES - 1, n_piece)), DMA((TYPES - 1, n_piece)),
            DMA((2, n_dev)), DMA((2, n_dev)), DMA((2, n_dev)), DMA((2, n_dev))],
        compiler_params=pltpu.CompilerParams(collective_id=0, has_side_effects=True, vmem_limit_bytes=56 * MIB),
    )(flags[None, :], x_loc, dy_loc, *weights)


def row_products(g_ref, w_refs, y_ref, dx_ref, rows_in, rows_t, w_tile, total, done, g_sem, w_sem, put_sem):
    width = rows_in.shape[0]
    cols = w_tile.shape[2]
    n_tile = total.shape[1] // cols
    step = width // SLOTS
    order = (O_TYPE, 0, 1, 2)

    def g_copy(i):
        return pltpu.make_async_copy(g_ref.at[order[i]], rows_in, g_sem)

    def w_copy(i, n, slot):
        return pltpu.make_async_copy(w_refs[order[i]].at[:, span(n * cols, cols)], w_tile.at[slot], w_sem.at[slot])

    puts = [pltpu.make_async_copy(done, ref, put_sem) for ref in (y_ref, dx_ref)]

    def turned(i):
        if i == 1:
            puts[0].start()
        if i == O_TYPE:
            puts[0].wait()
        g_copy(i).wait()

        @pl.loop(0, width // step)
        def _(b):
            at = span(b * step, step)
            rows_t[:, at] = jnp.transpose(rows_in[at, :])

        if i < O_TYPE:
            g_copy(i + 1).start()

    def use(i, n, slot):
        at = span(n * cols, cols)
        prod = dot(rows_t[...], w_tile[slot], INNER)
        if i == 0:
            done[:, at] = prod.astype(BF16)
        elif i == 1:
            total[:, at] = prod
        elif i < O_TYPE:
            total[:, at] = total[:, at] + prod
        else:
            done[:, at] = (total[:, at] + prod).astype(BF16)

    g_copy(0).start()
    stream(TYPES, n_tile, w_tile.shape[0], w_copy, use, turned)
    puts[1].start()
    return puts[1]


FLIPS = ((1, 1), (1, 0), (0, 1), (0, 0))


def reduce_kernel(g_ref, z_ref, x_ref, dy_ref, wq_ref, wk_ref, wv_ref, wo_ref, out_ref, y_ref, dx_ref,
                  zbuf, rows_in, side_out, side_in, first_out, first_in, second_out, second_in, kind_rows, rows_t, w_tile, sums, done,
                  z_sem, row_send, row_recv, side_send, side_recv, first_send, first_recv, second_send, second_recv, g_sem, w_sem, put_sem):
    me = lax.axis_index('sp')
    x, y, core = place(me)
    square = Square(me)
    block = rows_in.shape[3]
    part = block // 2
    n_col, cols = second_out.shape[1], second_out.shape[3]
    sibling = index_of(x, y, 1 - core)
    across = (index_of(x + 2, y, core), index_of(x, y + 2, core))

    meet([sibling, *across] + [square.peer(k) for k in range(1, TYPES)])

    def own_copy(ref):
        return pltpu.make_async_copy(ref, zbuf.at[0], z_sem.at[0])

    z_copies = [pltpu.make_async_copy(z_ref.at[k - 1], zbuf.at[k], z_sem.at[k]) for k in range(1, TYPES)]

    def row_source(k, mine, t):
        px, py = lattice(*square.chips[k])
        half = core if mine else 1 - core
        index = half * RING + lax.rem(px + FLIPS[t][0], 2) + 2 * lax.rem(py + FLIPS[t][1], 2)
        return g_ref.at[square.kind(k), span(index * block, block)]

    def row_copy(k, mine, t):
        dst, recv = rows_in.at[k, mine, t], row_recv.at[k, mine, t]
        if k == 0:
            return pltpu.make_async_copy(row_source(k, mine, t), dst, recv)
        return remote(row_source(k, mine, t), dst, row_send.at[k - 1, mine, t], recv, square.peer(k))

    every_row = [(k, mine, t) for t in range(TYPES) for mine in range(2) for k in range(TYPES)]
    for where in every_row:
        row_copy(*where).start()
    start_tokens(square.kind(0), x_ref, dy_ref, own_copy)
    for copy in z_copies:
        copy.start()

    last_put = row_products(g_ref, (wq_ref, wk_ref, wv_ref, wo_ref), y_ref, dx_ref, kind_rows, rows_t, w_tile, sums, done, g_sem, w_sem, put_sem)

    own_copy(x_ref).wait()
    for copy in z_copies:
        copy.wait()

    def product(mine, t, ch):
        at = span(ch * cols, cols)
        total = dot(rows_in[0, mine, t], zbuf[0, :, at], INNER)
        for k in range(1, TYPES):
            total = total + dot(rows_in[k, mine, t], zbuf[k, :, at], INNER)
        return total

    def side_copy(t, ch):
        return remote(side_out.at[t % 2, ch], side_in.at[t, ch], side_send.at[t, ch], side_recv.at[t, ch], sibling)

    def first_copy(leg, q, ch):
        return remote(first_out.at[leg, q, ch], first_in.at[leg, q, ch], first_send.at[leg, q, ch], first_recv.at[leg, q, ch], across[leg])

    def second_copy(leg, ch):
        return remote(second_out.at[leg, ch], second_in.at[leg, ch], second_send.at[leg, ch], second_recv.at[leg, ch], across[1 - leg])

    for t in range(TYPES):
        for mine in range(2):
            for k in range(TYPES):
                copy = row_copy(k, mine, t)
                if k:
                    copy.wait_recv()
                else:
                    copy.wait()

        @pl.loop(0, n_col)
        def _(ch, t=t):
            if t >= 2:
                side_copy(t - 2, ch).wait_send()
            side_out[t % 2, ch] = product(0, t, ch)
            side_copy(t, ch).start()

        @pl.loop(0, n_col)
        def _(ch, t=t):
            total = product(1, t, ch)
            side_copy(t, ch).wait_recv()
            total = total + side_in[t, ch]
            for leg in range(2):
                half = total[leg * part:(leg + 1) * part]
                step, other = FLIPS[t][leg], FLIPS[t][1 - leg]
                if step:
                    first_out[leg, other, ch] = half
                    first_copy(leg, other, ch).start()
                    continue
                first_copy(leg, other, ch).wait_recv()
                half = half + first_in[leg, other, ch]
                if other:
                    second_out[leg, ch] = half
                    second_copy(leg, ch).start()
                else:
                    second_copy(leg, ch).wait_recv()
                    out_ref[leg * part:(leg + 1) * part, span(ch * cols, cols)] = half + second_in[leg, ch]

    last_put.wait()
    for where in every_row:
        if where[0]:
            row_copy(*where).wait_send()

    @pl.loop(0, n_col)
    def _(ch):
        for t in range(2, TYPES):
            side_copy(t, ch).wait_send()
        for leg in range(2):
            for q in range(2):
                first_copy(leg, q, ch).wait_send()
            second_copy(leg, ch).wait_send()


def reduce_rows(g, z, x_loc, dy_loc, weights):
    width, tok = g.shape[1], g.shape[2]
    d_model = x_loc.shape[1]
    block = width // SLOTS
    n_col = RING
    cols = d_model // n_col
    tokens = jax.ShapeDtypeStruct((tok, d_model), BF16)
    halves = lambda *lead: pltpu.VMEM((*lead, n_col, block // 2, cols), F32)
    blocks = lambda lead: pltpu.VMEM((lead, n_col, block, cols), F32)
    return pl.pallas_call(
        reduce_kernel,
        name='reduce_rows',
        out_shape=(pltpu.VMEM((block, d_model), F32), tokens, tokens),
        in_specs=[ANY] * 8,
        out_specs=(VMEM, ANY, ANY),
        scratch_shapes=[
            pltpu.VMEM((TYPES, tok, d_model), BF16), pltpu.VMEM((TYPES, 2, TYPES, block, tok), BF16),
            blocks(2), blocks(TYPES), halves(2, 2), halves(2, 2), halves(2), halves(2),
            pltpu.VMEM((width, tok), BF16), pltpu.VMEM((tok, width), BF16), pltpu.VMEM((3, width, min(256, d_model // 4)), BF16),
            pltpu.VMEM((tok, d_model), F32), pltpu.VMEM((tok, d_model), BF16),
            DMA((TYPES,)), DMA((TYPES - 1, 2, TYPES)), DMA((TYPES, 2, TYPES)), DMA((TYPES, n_col)), DMA((TYPES, n_col)),
            DMA((2, 2, n_col)), DMA((2, 2, n_col)), DMA((2, n_col)), DMA((2, n_col)), DMA, DMA((3,)), DMA],
        compiler_params=pltpu.CompilerParams(collective_id=1, has_side_effects=True, vmem_limit_bytes=58 * MIB),
    )(g, z, x_loc, dy_loc, *weights)


def gather_kernel(piece_ref, near_ref, far_a_ref, far_b_ref, far_c_ref, send_sem, recv_sem, side_send, side_recv):
    me = lax.axis_index('sp')
    x, y, core = place(me)
    rows = piece_ref.shape[0]
    part = rows // 2
    quarter = part // 2

    def number(leg, i, j):
        sx, sy = (i, j) if leg == 0 else (j, i)
        px, py = lax.rem(x + sx, RING), lax.rem(y + sy, RING)
        lx, ly = lattice(px, py)
        return owned_type(px, py) * RING + lx + 2 * ly

    def spot(leg, i, j, half=None):
        lo, size = (0, part) if half is None else (half * quarter, quarter)
        return near_ref.at[pl.ds(pl.multiple_of(number(leg, i, j) * rows + leg * part + lo, quarter), size)]

    def far_spot(leg, i, j, half):
        if leg == 0:
            return far_a_ref.at[span(number(leg, i, j) * part + half * quarter, quarter)]
        return (far_b_ref, far_c_ref)[half].at[span(number(leg, i, j) * quarter, quarter)]

    def own(leg, half=None):
        lo, size = (0, part) if half is None else (half * quarter, quarter)
        return piece_ref.at[pl.ds(leg * part + lo, size)]

    def step_peer(leg, second, step):
        along_x = (leg == 0) != second
        return index_of(x + step, y, core) if along_x else index_of(x, y + step, core)

    started = []

    def push(leg, second, i, j, step, half):
        there = (i, (j - step) % RING) if second else ((i - step) % RING, j)
        src = own(leg, half) if i == 0 and j == 0 else spot(leg, i, j, half)
        copy = remote(src, spot(leg, i, j, half), send_sem.at[len(started)],
                      recv_sem.at[leg, there[0], there[1], half or 0], step_peer(leg, second, step))
        copy.start()
        started.append(copy)

    def landed(leg, i, j, half=None):
        here = spot(leg, i, j, half)
        remote(here, here, send_sem.at[0], recv_sem.at[leg, i, j, half or 0], me).wait_recv()

    side = []

    def to_sibling(leg, i, j, halves=(0, 1)):
        for half in halves:
            src = own(leg, half) if i == 0 and j == 0 else spot(leg, i, j, half)
            copy = remote(src, far_spot(leg, i, j, half), side_send.at[leg, i, j, half], side_recv.at[leg, i, j, half], index_of(x, y, 1 - core))
            copy.start()
            side.append(copy)

    meet([index_of(x, y, 1 - core)] + [index_of(*chip, core) for chip in chips_around(x, y)])

    def spread(leg, i):
        push(leg, True, i, 0, 1, None)
        push(leg, True, i, 0, 3, None)
        to_sibling(leg, i, 0)

    for leg in range(2):
        push(leg, False, 0, 0, 1, None)
        push(leg, False, 0, 0, 3, None)
    for leg in range(2):
        spread(leg, 0)
    near_ref[span(number(0, 0, 0) * rows, rows), :] = piece_ref[...]

    for leg in range(2):
        landed(leg, 3, 0)
        push(leg, False, 3, 0, 1, 0)
        spread(leg, 3)
        landed(leg, 1, 0)
        push(leg, False, 1, 0, 3, 1)
        spread(leg, 1)

    def second_near(leg, i):
        landed(leg, i, 3)
        push(leg, True, i, 3, 1, 0)
        to_sibling(leg, i, 3)
        landed(leg, i, 1)
        push(leg, True, i, 1, 3, 1)
        to_sibling(leg, i, 1)

    for leg in range(2):
        second_near(leg, 0)
    for leg in range(2):
        for half in range(2):
            landed(leg, 2, 0, half)
        spread(leg, 2)
    for i in (3, 1, 2):
        for leg in range(2):
            second_near(leg, i)
    for i in (0, 3, 1, 2):
        for half in range(2):
            for leg in range(2):
                landed(leg, i, 2, half)
                to_sibling(leg, i, 2, (half,))

    for copy in started + side:
        copy.wait_send()

    for leg in range(2):
        for i in range(RING):
            for j in range(RING):
                for half in range(2):
                    here = far_spot(leg, i, j, half)
                    remote(here, here, side_send.at[leg, i, j, half], side_recv.at[leg, i, j, half], me).wait_recv()


def gather_rows(piece, n_dev):
    rows, d_model = piece.shape
    half = n_dev * rows // CORES
    return pl.pallas_call(
        gather_kernel,
        name='gather_rows',
        out_shape=(pltpu.VMEM((half, d_model), F32), pltpu.VMEM((half // 2, d_model), F32), pltpu.VMEM((half // 4, d_model), F32),
                   jax.ShapeDtypeStruct((half // 4, d_model), F32)),
        in_specs=[VMEM],
        out_specs=(VMEM, VMEM, VMEM, ANY),
        scratch_shapes=[DMA((40,)), DMA((2, RING, RING, 2)), DMA((2, RING, RING, 2)), DMA((2, RING, RING, 2))],
        compiler_params=pltpu.CompilerParams(collective_id=2, has_side_effects=True, vmem_limit_bytes=STORE_LIMIT),
    )(piece)


def store_kernel(near_ref, far_a_ref, far_b_ref, far_c_ref, y_ref, dx_ref, dq_out, dk_out, dv_out, do_out, y_out, dx_out,
                 tile, rows_buf, put_sem, a_sem, b_sem, in_sem, out_sem, row_in, row_out):
    core = lax.rem(lax.axis_index('sp'), CORES)
    outs = (dq_out, dk_out, dv_out, do_out)
    rows = near_ref.shape[0] // TYPES
    n_slot, chunk = tile.shape[0], tile.shape[1]
    n = far_c_ref.shape[0] // chunk
    piece = 4 * chunk

    def far_out(i, lo, size):
        first = (1 - core) * rows + i % RING * piece + lo
        return outs[i // RING].at[pl.ds(pl.multiple_of(first, chunk), size)]

    puts = []
    for i in range(n * 2):
        kind, size = i // SLOTS, 2 * chunk
        lo = i % SLOTS * size
        puts.append(pltpu.make_async_copy(near_ref.at[pl.ds(i * size, size)], outs[kind].at[span(core * rows + lo, size)], put_sem.at[i]))
    for i in range(n):
        puts.append(pltpu.make_async_copy(far_a_ref.at[pl.ds(i * 2 * chunk, 2 * chunk)], far_out(i, 0, 2 * chunk), a_sem.at[i]))
        puts.append(pltpu.make_async_copy(far_b_ref.at[pl.ds(i * chunk, chunk)], far_out(i, 2 * chunk, chunk), b_sem.at[i]))

    def load(i):
        return pltpu.make_async_copy(far_c_ref.at[pl.ds(i * chunk, chunk)], tile.at[i % n_slot], in_sem.at[i % n_slot])

    def save(i):
        return pltpu.make_async_copy(tile.at[i % n_slot], far_out(i, piece - chunk, chunk), out_sem.at[i % n_slot])

    steps = []
    for src, dst in ((y_ref, y_out), (dx_ref, dx_out)):
        take, give = pltpu.make_async_copy(src, rows_buf, row_in), pltpu.make_async_copy(rows_buf, dst, row_out)
        steps += [(take.start,), (take.wait, give.start), (give.wait,)]

    ahead = n_slot // 2
    for i in range(ahead):
        load(i).start()
    for put in puts:
        put.start()
    for i in range(n):
        load(i).wait()
        save(i).start()
        if i % 2 == 0 and i // 2 < len(steps):
            for action in steps[i // 2]:
                action()
        if i + ahead < n:
            if i + ahead >= n_slot:
                save(i + ahead - n_slot).wait()
            load(i + ahead).start()
    for i in range(n - n_slot, n):
        save(i).wait()
    for put in puts:
        put.wait()


def store(near, far_a, far_b, far_c, y_rows, dx_rows):
    half, d_model = near.shape
    n = RING * RING
    chunk = far_c.shape[0] // n
    grad = jax.ShapeDtypeStruct((half * CORES // TYPES, d_model), F32)
    tokens = jax.ShapeDtypeStruct(y_rows.shape, BF16)
    return pl.pallas_call(
        store_kernel,
        name='store',
        out_shape=(grad,) * TYPES + (tokens,) * 2,
        in_specs=[VMEM, VMEM, VMEM] + [ANY] * 3,
        out_specs=(ANY,) * (TYPES + 2),
        scratch_shapes=[pltpu.VMEM((4, chunk, d_model), F32), pltpu.VMEM(y_rows.shape, BF16),
                        DMA((2 * n,)), DMA((n,)), DMA((n,)), DMA((4,)), DMA((4,)), DMA, DMA],
        compiler_params=pltpu.CompilerParams(vmem_limit_bytes=STORE_LIMIT),
    )(in_vmem(near), in_vmem(far_a), in_vmem(far_b), in_hbm(far_c), in_hbm(y_rows), in_hbm(dx_rows))


def solution(mesh):
    n_dev = mesh.shape['sp']
    assert n_dev == CORES * RING * RING

    def device_body(x_loc, flag_loc, w_q, w_k, w_v, w_o, dy_loc):
        tok_count, d_model = x_loc.shape
        n_heads, head_dim = w_q.shape[1], w_q.shape[2]
        width = n_heads * head_dim
        score_scale = 1.0 / (math.sqrt(head_dim) * tok_count)
        weights = [w.transpose(1, 2, 0).reshape(width, d_model) for w in (w_q, w_k, w_v)] + [w_o.reshape(width, d_model)]
        g, z = front(flag_loc, x_loc, dy_loc, weights, score_scale, n_dev, n_heads)
        piece, y_rows, dx_rows = reduce_rows(g, z, x_loc, dy_loc, weights)
        *grads, y_loc, dx_loc = store(*gather_rows(piece, n_dev), y_rows, dx_rows)
        dw_q, dw_k, dw_v, dw_o = (grad.reshape(n_heads, head_dim, d_model) for grad in grads)
        return y_loc, dx_loc, dw_q.transpose(2, 0, 1), dw_k.transpose(2, 0, 1), dw_v.transpose(2, 0, 1), dw_o

    row_spec = P(('dp', 'sp'), None)
    flag_spec = P(('dp', 'sp'))
    w_spec = P(None, None, None)
    dw_spec = P('dp', None, None)
    return jax.shard_map(device_body, mesh=mesh,
                         in_specs=(row_spec, flag_spec, w_spec, w_spec, w_spec, w_spec, row_spec),
                         out_specs=(row_spec, row_spec, dw_spec, dw_spec, dw_spec, dw_spec),
                         check_vma=False)
```

```python
import functools
import math
import jax
import jax.numpy as jnp
from jax import lax
from jax.experimental import pallas as pl
from jax.experimental.pallas import tpu as pltpu
from jax.sharding import PartitionSpec as P

MESH = pl.DeviceIdType.MESH
CORES = 2
RING = 4
SLOTS = CORES * RING
TYPES = 4
O_TYPE = TYPES - 1
MIB = 1024 * 1024
STORE_LIMIT = 5 * MIB
BF16 = jnp.bfloat16
F32 = jnp.float32
ROWS = ((1,), (1,))
INNER = ((1,), (0,))
OUTER = ((0,), (0,))
VMEM = pl.BlockSpec(memory_space=pltpu.VMEM)
ANY = pl.BlockSpec(memory_space=pltpu.HBM)
DMA = pltpu.SemaphoreType.DMA


def place(me):
    core = lax.rem(me, CORES)
    chip = me // CORES
    return lax.rem(chip, RING), chip // RING, core


def index_of(x, y, core):
    return (lax.rem(y, RING) * RING + lax.rem(x, RING)) * CORES + core


def remote(src, dst, send_sem, recv_sem, peer):
    return pltpu.make_async_remote_copy(src_ref=src, dst_ref=dst, send_sem=send_sem, recv_sem=recv_sem,
                                        device_id={'sp': peer}, device_id_type=MESH)


def signal(peer):
    pl.semaphore_signal(pltpu.get_barrier_semaphore(), inc=1, device_id={'sp': peer}, device_id_type=MESH)


def meet(peers):
    for peer in peers:
        signal(peer)
    pl.semaphore_wait(pltpu.get_barrier_semaphore(), len(peers))


def chips_around(x, y):
    return ((x + 1, y), (x + RING - 1, y), (x, y + 1), (x, y + RING - 1))


def dot(a, b, dims):
    return lax.dot_general(a, b, (dims, ((), ())), preferred_element_type=F32)


def in_vmem(value):
    return pltpu.with_memory_space_constraint(value, pltpu.VMEM)


def in_hbm(value):
    return pltpu.with_memory_space_constraint(value, pltpu.HBM)


def span(start, size):
    return pl.ds(pl.multiple_of(start, size), size)


def stream(n_outer, n_inner, depth, copy, use, before):
    ahead = depth - 1
    for n in range(ahead):
        copy(0, n, n).start()
    for i in range(n_outer):
        before(i)

        @pl.loop(0, n_inner)
        def _(n):
            at = i * n_inner + n
            slot, free = lax.rem(at, depth), lax.rem(at + ahead, depth)

            @pl.when(n + ahead < n_inner)
            def _():
                copy(i, n + ahead, free).start()

            if i + 1 < n_outer:
                @pl.when(n + ahead >= n_inner)
                def _():
                    copy(i + 1, n + ahead - n_inner, free).start()

            copy(i, n, slot).wait()
            use(i, n, slot)


def form_masks(flag_ref, seg_col_ref, seg_row_ref, head_ref, tail_ref, gate_ref):
    tok = flag_ref.shape[1]
    flags = flag_ref[...] > 0
    t_pos = lax.broadcasted_iota(jnp.int32, (tok, tok), 0)
    s_pos = lax.broadcasted_iota(jnp.int32, (tok, tok), 1)
    seg_col = jnp.sum(jnp.where(flags & (s_pos <= t_pos), 1.0, 0), axis=1, keepdims=True)
    seg_col_ref[...] = seg_col
    seg_row_ref[...] = jnp.sum(jnp.where(s_pos == t_pos, seg_col, 0), axis=0, keepdims=True)
    positions = lax.broadcasted_iota(jnp.int32, (1, tok), 1).astype(F32)
    first_pos = jnp.min(jnp.where(flags, positions, tok), axis=1, keepdims=True)
    last_pos = jnp.max(jnp.where(flags, positions, -1), axis=1, keepdims=True)
    head_ref[...] = jnp.where(positions < first_pos, 1.0, 0)
    tail_ref[...] = jnp.where(positions >= last_pos, 1.0, 0)
    gate_ref[...] = jnp.broadcast_to(jnp.where(last_pos < 0, 1.0, 0), gate_ref.shape)


class Square:
    def __init__(self, me):
        x, y, core = place(me)
        across_x, across_y = (lax.rem(a + 1 + RING - 2 * lax.rem(a + core, 2), RING) for a in (x, y))
        self.core = core
        self.chips = [(x, y), (across_x, y), (x, across_y), (across_x, across_y)]

    def peer(self, k):
        return index_of(*self.chips[k], self.core)

    def kind(self, k):
        return owned_type(*self.chips[k])


def owned_type(x, y):
    return lax.rem(x, 2) + 2 * lax.rem(y, 2)


def lattice(x, y):
    return lax.rem(x // 2, 2), lax.rem(y // 2, 2)


def start_tokens(kind, x_ref, dy_ref, copy):
    @pl.when(kind == O_TYPE)
    def _():
        copy(dy_ref).start()

    @pl.when(kind != O_TYPE)
    def _():
        copy(x_ref).start()


def front_kernel(scale, dim, flag_ref, x_ref, dy_ref, wq_ref, wk_ref, wv_ref, wo_ref,
                 g_ref, z_ref, seg_col_ref, seg_row_ref, head_ref, tail_ref, gate_ref, tok_in, w_tile, rows_ref, total,
                 packed, held, formed, states,
                 tok_sem, w_sem, g_sem, z_send, z_recv, send_sem, recv_sem, back_send, back_recv):
    me = lax.axis_index('sp')
    n_dev, per_dev, low = formed.shape[1:4]
    width, tok = rows_ref.shape[1], rows_ref.shape[2]
    half = tok // 2
    n_piece = z_recv.shape[1]
    piece = tok // SLOTS
    n_group = SLOTS
    group = width // n_group
    tile_rows = w_tile.shape[1]

    @pl.loop(1, n_dev)
    def _(step):
        signal(lax.rem(me + step, n_dev))

    loads = [pltpu.make_async_copy(ref, tok_in.at[i], tok_sem.at[i]) for i, ref in enumerate((x_ref, dy_ref))]
    for load in loads:
        load.start()

    square = Square(me)

    cuts = (0, 2, 3, TYPES, SLOTS)

    def token_copy(k, n):
        at = pl.ds(cuts[n] * piece, (cuts[n + 1] - cuts[n]) * piece)
        return lambda ref: remote(ref.at[at], z_ref.at[k - 1, at], z_send.at[k - 1, n], z_recv.at[k - 1, n], square.peer(k))

    def push_tokens(n):
        for k in range(1, TYPES):
            start_tokens(square.kind(k), x_ref, dy_ref, token_copy(k, n))

    form_masks(flag_ref, seg_col_ref, seg_row_ref, head_ref, tail_ref, gate_ref)
    pl.semaphore_wait(pltpu.get_barrier_semaphore(), n_dev - 1)
    push_tokens(0)

    weights = (wk_ref, wv_ref, wq_ref, wo_ref)
    kinds = (1, 2, 0, O_TYPE)

    def w_copy(i, n, slot):
        return pltpu.make_async_copy(weights[i].at[span(n * tile_rows, tile_rows)], w_tile.at[slot], w_sem.at[slot])

    def project(i, n, slot):
        rows_ref[kinds[i], span(n * tile_rows, tile_rows), :] = dot(w_tile[slot], tok_in[i // O_TYPE], ROWS).astype(BF16)

    def loaded(i):
        if i in (0, O_TYPE):
            loads[i // O_TYPE].wait()
        if i == 2:
            send_products(0)
        if i in (1, O_TYPE):
            push_tokens(1 + i // O_TYPE)

    head = head_ref[...] > 0.5
    tail = tail_ref[...] > 0.5

    def each(do):
        pl.loop(1, n_dev)(do)

    def out_copy(which, step):
        peer = lax.rem(me + step, n_dev)
        at = pl.ds(0, low + 1 - which)
        return remote(packed.at[which, peer, :, at], held.at[which, me, :, at], send_sem.at[which, step], recv_sem.at[which, step], peer)

    def back_copy(which, step):
        peer = lax.rem(me + step, n_dev)
        return remote(formed.at[which, peer], states.at[which, me], back_send.at[which, step], back_recv.at[which, step], peer)

    pair_lane = lax.broadcasted_iota(jnp.int32, (low, 2 * dim), 1) // dim

    def turn(pair):
        return pltpu.roll(pair, dim, 1)

    def send_products(which):
        left, right, mask = ((1, 2, tail), (0, O_TYPE, head))[which]

        @pl.loop(0, n_group)
        def _(grp):
            at = span(grp * group, group)
            full = dot(rows_ref[left, at, :], jnp.where(mask, rows_ref[right, at, :], jnp.zeros((group, tok), BF16)), ROWS)
            for sub in range(group // dim):
                spot = sub % 2
                block = full[sub * dim:(sub + 1) * dim, (sub // 2) * 2 * dim:(sub // 2 + 1) * 2 * dim]
                first, second = block[0:low], block[low:]
                if spot == 0:
                    second = turn(second)
                else:
                    first = turn(first)
                index = grp * (group // dim) + sub
                dev, own = index // per_dev, lax.rem(index, per_dev)
                packed[which, dev, own, 0:low, :] = jnp.where(pair_lane == 0, first, second)
                packed[which, dev, own, low:, :] = gate_ref[...]

        each(lambda step: out_copy(which, step).start())
        held[which, me] = packed[which, me]

    def form_states(which):
        each(lambda step: out_copy(which, step).wait_recv())

        def advance(step, state):
            block = step if which == 0 else n_dev - 1 - step
            formed[which, block] = state.astype(BF16)
            return held[0, block, :, low:low + 1, :] * state + held[which, block, :, 0:low, :]

        lax.fori_loop(0, n_dev, advance, jnp.zeros((per_dev, low, 2 * dim), F32), unroll=4)
        each(lambda step: back_copy(which, step).start())
        states[which, me] = formed[which, me]

    stream(TYPES, width // tile_rows, w_tile.shape[0], w_copy, project, loaded)
    send_products(1)

    seg_row = seg_row_ref[...]
    t_pos = lax.broadcasted_iota(jnp.int32, (half, tok), 0)
    s_pos = lax.broadcasted_iota(jnp.int32, (half, tok), 1)

    def pair(a, b):
        see_top = ((seg_col_ref[0:half, :] == seg_row) & (s_pos <= t_pos))[:, 0:half]
        see_low = (seg_col_ref[half:, :] == seg_row) & (s_pos <= t_pos + half)
        top = dot(a[:, 0:half], b[:, 0:half], OUTER)
        low = dot(a[:, half:], b, OUTER)
        return (jnp.where(see_top, top * scale, 0).astype(BF16), jnp.where(see_low, low * scale, 0).astype(BF16))

    def over_keys(at, rows_t, probs):
        total[at[0], at[1], 0:half] = dot(rows_t[:, 0:half], probs[0], ROWS)
        total[at[0], at[1], half:] = dot(rows_t, probs[1], ROWS)

    def over_queries(at, rows_t, probs):
        from_low = dot(rows_t[:, half:], probs[1], INNER)
        total[at[0], at[1], 0:half] = dot(rows_t[:, 0:half], probs[0], INNER) + from_low[:, 0:half]
        total[at[0], at[1], half:] = from_low[:, half:]

    def heads_of(grp):
        return [grp * (group // dim) + sub for sub in range(group // dim)]

    @pl.loop(0, n_group)
    def _(grp):
        @pl.when(grp == 1)
        def _():
            form_states(0)

        @pl.when(grp == n_group // 2 + 1)
        def _():
            form_states(1)
            push_tokens(O_TYPE)

        for index in heads_of(grp):
            rows = span(index * dim, dim)
            q, k, v, do = (rows_ref[kind, rows, :] for kind in range(TYPES))
            d_probs = pair(do, v)
            over_keys((0, rows), k, d_probs)
            over_queries((1, rows), q, d_probs)
            probs = pair(q, k)
            over_queries((2, rows), do, probs)
            over_keys((O_TYPE, rows), v, probs)

    def diagonal(which, grp):
        rows = []
        for sub in range(group // dim):
            index = grp * (group // dim) + sub
            pair = states[which, index // per_dev, lax.rem(index, per_dev)].astype(F32)
            spot = sub % 2
            block = jnp.concatenate([turn(pair), pair] if spot else [pair, turn(pair)], axis=0)
            block = jnp.where(jnp.concatenate([pair_lane, pair_lane], axis=0) == spot, block, 0)
            empty = jnp.zeros_like(block)
            rows.append(jnp.concatenate([empty, block] if sub // 2 else [block, empty], axis=1))
        return jnp.concatenate(rows, axis=0).astype(BF16)

    def finish(kind, at, mask, inter):
        rows_ref[kind, at, :] = (total[kind, at, :] + jnp.where(mask, inter * scale, 0)).astype(BF16)

    def row_put(kind, grp):
        at = span(grp * group, group)
        return pltpu.make_async_copy(rows_ref.at[kind, at], g_ref.at[kind, at], g_sem.at[kind, grp])

    each(lambda step: back_copy(0, step).wait_recv())

    @pl.loop(0, n_group)
    def _(grp):
        at = span(grp * group, group)
        st = diagonal(0, grp)
        d_q = dot(st, rows_ref[O_TYPE, at, :], INNER)
        out = dot(st, rows_ref[0, at, :], OUTER)
        finish(0, at, head, d_q)
        finish(O_TYPE, at, head, out)
        for kind in (0, O_TYPE):
            row_put(kind, grp).start()

    each(lambda step: back_copy(1, step).wait_recv())

    @pl.loop(0, n_group)
    def _(grp):
        at = span(grp * group, group)
        st = diagonal(1, grp)
        d_k = dot(st, rows_ref[2, at, :], INNER)
        d_v = dot(st, rows_ref[1, at, :], OUTER)
        finish(1, at, tail, d_k)
        finish(2, at, tail, d_v)
        for kind in (1, 2):
            row_put(kind, grp).start()

    for kind in range(TYPES):
        pl.loop(0, n_group)(lambda grp, kind=kind: row_put(kind, grp).wait())
    for which in range(2):
        each(lambda step, which=which: out_copy(which, step).wait_send())
        each(lambda step, which=which: back_copy(which, step).wait_send())
    for k in range(1, TYPES):
        for n in range(n_piece):
            token_copy(k, n)(x_ref).wait()


def front(flags, x_loc, dy_loc, weights, scale, n_dev, n_heads):
    tok, d_model = x_loc.shape
    width = weights[0].shape[0]
    dim = width // n_heads
    per_dev = n_heads // n_dev
    n_piece = TYPES
    pack = (2, n_dev, per_dev, dim // 2 + 8, 2 * dim)
    back = (2, n_dev, per_dev, dim // 2, 2 * dim)
    return pl.pallas_call(
        functools.partial(front_kernel, scale, dim),
        name='front',
        out_shape=(jax.ShapeDtypeStruct((TYPES, width, tok), BF16), jax.ShapeDtypeStruct((TYPES - 1, tok, d_model), BF16)),
        in_specs=[VMEM] + [ANY] * 6,
        out_specs=(ANY, ANY),
        scratch_shapes=[
            pltpu.VMEM((tok, 1), F32), pltpu.VMEM((1, tok), F32), pltpu.VMEM((1, tok), F32), pltpu.VMEM((1, tok), F32), pltpu.VMEM((8, 2 * dim), F32),
            pltpu.VMEM((2, tok, d_model), BF16), pltpu.VMEM((4, width // RING, d_model), BF16),
            pltpu.VMEM((TYPES, width, tok), BF16), pltpu.VMEM((TYPES, width, tok), F32),
            pltpu.VMEM(pack, F32), pltpu.VMEM(pack, F32), pltpu.VMEM(back, BF16), pltpu.VMEM(back, BF16),
            DMA((2,)), DMA((4,)), DMA((TYPES, SLOTS)), DMA((TYPES - 1, n_piece)), DMA((TYPES - 1, n_piece)),
            DMA((2, n_dev)), DMA((2, n_dev)), DMA((2, n_dev)), DMA((2, n_dev))],
        compiler_params=pltpu.CompilerParams(collective_id=0, has_side_effects=True, vmem_limit_bytes=56 * MIB),
    )(flags[None, :], x_loc, dy_loc, *weights)


def row_products(g_ref, w_refs, y_ref, dx_ref, rows_in, rows_t, w_tile, total, done, g_sem, w_sem, put_sem):
    width = rows_in.shape[0]
    cols = w_tile.shape[2]
    n_tile = total.shape[1] // cols
    step = width // SLOTS
    order = (O_TYPE, 0, 1, 2)

    def g_copy(i):
        return pltpu.make_async_copy(g_ref.at[order[i]], rows_in, g_sem)

    def w_copy(i, n, slot):
        return pltpu.make_async_copy(w_refs[order[i]].at[:, span(n * cols, cols)], w_tile.at[slot], w_sem.at[slot])

    puts = [pltpu.make_async_copy(done, ref, put_sem) for ref in (y_ref, dx_ref)]

    def turned(i):
        if i == 1:
            puts[0].start()
        if i == O_TYPE:
            puts[0].wait()
        g_copy(i).wait()

        @pl.loop(0, width // step)
        def _(b):
            at = span(b * step, step)
            rows_t[:, at] = jnp.transpose(rows_in[at, :])

        if i < O_TYPE:
            g_copy(i + 1).start()

    def use(i, n, slot):
        at = span(n * cols, cols)
        prod = dot(rows_t[...], w_tile[slot], INNER)
        if i == 0:
            done[:, at] = prod.astype(BF16)
        elif i == 1:
            total[:, at] = prod
        elif i < O_TYPE:
            total[:, at] = total[:, at] + prod
        else:
            done[:, at] = (total[:, at] + prod).astype(BF16)

    g_copy(0).start()
    stream(TYPES, n_tile, w_tile.shape[0], w_copy, use, turned)
    puts[1].start()
    return puts[1]


FLIPS = ((1, 1), (1, 0), (0, 1), (0, 0))


def reduce_kernel(g_ref, z_ref, x_ref, dy_ref, wq_ref, wk_ref, wv_ref, wo_ref, out_ref, y_ref, dx_ref,
                  zbuf, rows_in, side_out, side_in, first_out, first_in, second_out, second_in, kind_rows, rows_t, w_tile, sums, done,
                  z_sem, row_send, row_recv, side_send, side_recv, first_send, first_recv, second_send, second_recv, g_sem, w_sem, put_sem):
    me = lax.axis_index('sp')
    x, y, core = place(me)
    square = Square(me)
    block = rows_in.shape[3]
    part = block // 2
    n_col, cols = second_out.shape[1], second_out.shape[3]
    sibling = index_of(x, y, 1 - core)
    across = (index_of(x + 2, y, core), index_of(x, y + 2, core))

    meet([sibling, *across] + [square.peer(k) for k in range(1, TYPES)])

    def own_copy(ref):
        return pltpu.make_async_copy(ref, zbuf.at[0], z_sem.at[0])

    z_copies = [pltpu.make_async_copy(z_ref.at[k - 1], zbuf.at[k], z_sem.at[k]) for k in range(1, TYPES)]

    def row_source(k, mine, t):
        px, py = lattice(*square.chips[k])
        half = core if mine else 1 - core
        index = half * RING + lax.rem(px + FLIPS[t][0], 2) + 2 * lax.rem(py + FLIPS[t][1], 2)
        return g_ref.at[square.kind(k), span(index * block, block)]

    def row_copy(k, mine, t):
        dst, recv = rows_in.at[k, mine, t], row_recv.at[k, mine, t]
        if k == 0:
            return pltpu.make_async_copy(row_source(k, mine, t), dst, recv)
        return remote(row_source(k, mine, t), dst, row_send.at[k - 1, mine, t], recv, square.peer(k))

    every_row = [(k, mine, t) for t in range(TYPES) for mine in range(2) for k in range(TYPES)]
    for where in every_row:
        row_copy(*where).start()
    start_tokens(square.kind(0), x_ref, dy_ref, own_copy)
    for copy in z_copies:
        copy.start()

    last_put = row_products(g_ref, (wq_ref, wk_ref, wv_ref, wo_ref), y_ref, dx_ref, kind_rows, rows_t, w_tile, sums, done, g_sem, w_sem, put_sem)

    own_copy(x_ref).wait()
    for copy in z_copies:
        copy.wait()

    def product(mine, t, ch):
        at = span(ch * cols, cols)
        total = dot(rows_in[0, mine, t], zbuf[0, :, at], INNER)
        for k in range(1, TYPES):
            total = total + dot(rows_in[k, mine, t], zbuf[k, :, at], INNER)
        return total

    def side_copy(t, ch):
        return remote(side_out.at[t % 2, ch], side_in.at[t, ch], side_send.at[t, ch], side_recv.at[t, ch], sibling)

    def first_copy(leg, q, ch):
        return remote(first_out.at[leg, q, ch], first_in.at[leg, q, ch], first_send.at[leg, q, ch], first_recv.at[leg, q, ch], across[leg])

    def second_copy(leg, ch):
        return remote(second_out.at[leg, ch], second_in.at[leg, ch], second_send.at[leg, ch], second_recv.at[leg, ch], across[1 - leg])

    for t in range(TYPES):
        for mine in range(2):
            for k in range(TYPES):
                copy = row_copy(k, mine, t)
                if k:
                    copy.wait_recv()
                else:
                    copy.wait()

        @pl.loop(0, n_col)
        def _(ch, t=t):
            if t >= 2:
                side_copy(t - 2, ch).wait_send()
            side_out[t % 2, ch] = product(0, t, ch)
            side_copy(t, ch).start()

        @pl.loop(0, n_col)
        def _(ch, t=t):
            total = product(1, t, ch)
            side_copy(t, ch).wait_recv()
            total = total + side_in[t, ch]
            for leg in range(2):
                half = total[leg * part:(leg + 1) * part]
                step, other = FLIPS[t][leg], FLIPS[t][1 - leg]
                if step:
                    first_out[leg, other, ch] = half
                    first_copy(leg, other, ch).start()
                elif other:
                    second_out[leg, ch] = half
                else:
                    out_ref[leg * part:(leg + 1) * part, span(ch * cols, cols)] = half

    for leg in (1, 0):
        @pl.loop(0, n_col)
        def _(ch, leg=leg):
            first_copy(leg, 1, ch).wait_recv()
            second_out[leg, ch] += first_in[leg, 1, ch]
            second_copy(leg, ch).start()

    for leg in (1, 0):
        @pl.loop(0, n_col)
        def _(ch, leg=leg):
            first_copy(leg, 0, ch).wait_recv()
            second_copy(leg, ch).wait_recv()
            out_ref[leg * part:(leg + 1) * part, span(ch * cols, cols)] += first_in[leg, 0, ch] + second_in[leg, ch]

    last_put.wait()
    for where in every_row:
        if where[0]:
            row_copy(*where).wait_send()

    @pl.loop(0, n_col)
    def _(ch):
        for t in range(2, TYPES):
            side_copy(t, ch).wait_send()
        for leg in range(2):
            for q in range(2):
                first_copy(leg, q, ch).wait_send()
            second_copy(leg, ch).wait_send()


def reduce_rows(g, z, x_loc, dy_loc, weights):
    width, tok = g.shape[1], g.shape[2]
    d_model = x_loc.shape[1]
    block = width // SLOTS
    n_col = RING
    cols = d_model // n_col
    tokens = jax.ShapeDtypeStruct((tok, d_model), BF16)
    halves = lambda *lead: pltpu.VMEM((*lead, n_col, block // 2, cols), F32)
    blocks = lambda lead: pltpu.VMEM((lead, n_col, block, cols), F32)
    return pl.pallas_call(
        reduce_kernel,
        name='reduce_rows',
        out_shape=(pltpu.VMEM((block, d_model), F32), tokens, tokens),
        in_specs=[ANY] * 8,
        out_specs=(VMEM, ANY, ANY),
        scratch_shapes=[
            pltpu.VMEM((TYPES, tok, d_model), BF16), pltpu.VMEM((TYPES, 2, TYPES, block, tok), BF16),
            blocks(2), blocks(TYPES), halves(2, 2), halves(2, 2), halves(2), halves(2),
            pltpu.VMEM((width, tok), BF16), pltpu.VMEM((tok, width), BF16), pltpu.VMEM((3, width, min(256, d_model // 4)), BF16),
            pltpu.VMEM((tok, d_model), F32), pltpu.VMEM((tok, d_model), BF16),
            DMA((TYPES,)), DMA((TYPES - 1, 2, TYPES)), DMA((TYPES, 2, TYPES)), DMA((TYPES, n_col)), DMA((TYPES, n_col)),
            DMA((2, 2, n_col)), DMA((2, 2, n_col)), DMA((2, n_col)), DMA((2, n_col)), DMA, DMA((3,)), DMA],
        compiler_params=pltpu.CompilerParams(collective_id=1, has_side_effects=True, vmem_limit_bytes=58 * MIB),
    )(g, z, x_loc, dy_loc, *weights)


def gather_kernel(piece_ref, near_ref, far_a_ref, far_b_ref, far_c_ref, send_sem, recv_sem, side_send, side_recv):
    me = lax.axis_index('sp')
    x, y, core = place(me)
    rows = piece_ref.shape[0]
    part = rows // 2
    quarter = part // 2

    def number(leg, i, j):
        sx, sy = (i, j) if leg == 0 else (j, i)
        px, py = lax.rem(x + sx, RING), lax.rem(y + sy, RING)
        lx, ly = lattice(px, py)
        return owned_type(px, py) * RING + lx + 2 * ly

    def spot(leg, i, j, half=None):
        lo, size = (0, part) if half is None else (half * quarter, quarter)
        return near_ref.at[pl.ds(pl.multiple_of(number(leg, i, j) * rows + leg * part + lo, quarter), size)]

    def far_spot(leg, i, j, half):
        if leg == 0:
            return far_a_ref.at[span(number(leg, i, j) * part + half * quarter, quarter)]
        return (far_b_ref, far_c_ref)[half].at[span(number(leg, i, j) * quarter, quarter)]

    def own(leg, half=None):
        lo, size = (0, part) if half is None else (half * quarter, quarter)
        return piece_ref.at[pl.ds(leg * part + lo, size)]

    def step_peer(leg, second, step):
        along_x = (leg == 0) != second
        return index_of(x + step, y, core) if along_x else index_of(x, y + step, core)

    started = []

    def push(leg, second, i, j, step, half):
        there = (i, (j - step) % RING) if second else ((i - step) % RING, j)
        src = own(leg, half) if i == 0 and j == 0 else spot(leg, i, j, half)
        copy = remote(src, spot(leg, i, j, half), send_sem.at[len(started)],
                      recv_sem.at[leg, there[0], there[1], half or 0], step_peer(leg, second, step))
        copy.start()
        started.append(copy)

    def landed(leg, i, j, half=None):
        here = spot(leg, i, j, half)
        remote(here, here, send_sem.at[0], recv_sem.at[leg, i, j, half or 0], me).wait_recv()

    side = []

    def to_sibling(leg, i, j, halves=(0, 1)):
        for half in halves:
            src = own(leg, half) if i == 0 and j == 0 else spot(leg, i, j, half)
            copy = remote(src, far_spot(leg, i, j, half), side_send.at[leg, i, j, half], side_recv.at[leg, i, j, half], index_of(x, y, 1 - core))
            copy.start()
            side.append(copy)

    meet([index_of(x, y, 1 - core)] + [index_of(*chip, core) for chip in chips_around(x, y)])

    def spread(leg, i):
        push(leg, True, i, 0, 1, None)
        push(leg, True, i, 0, 3, None)
        to_sibling(leg, i, 0)

    for leg in range(2):
        push(leg, False, 0, 0, 1, None)
        push(leg, False, 0, 0, 3, None)
    for leg in range(2):
        spread(leg, 0)
    near_ref[span(number(0, 0, 0) * rows, rows), :] = piece_ref[...]

    for leg in range(2):
        landed(leg, 3, 0)
        push(leg, False, 3, 0, 1, 0)
        spread(leg, 3)
        landed(leg, 1, 0)
        push(leg, False, 1, 0, 3, 1)
        spread(leg, 1)

    def second_near(leg, i):
        landed(leg, i, 3)
        push(leg, True, i, 3, 1, 0)
        to_sibling(leg, i, 3)
        landed(leg, i, 1)
        push(leg, True, i, 1, 3, 1)
        to_sibling(leg, i, 1)

    for leg in range(2):
        second_near(leg, 0)
    for leg in range(2):
        for half in range(2):
            landed(leg, 2, 0, half)
        spread(leg, 2)
    for i in (3, 1, 2):
        for leg in range(2):
            second_near(leg, i)
    for i in (0, 3, 1, 2):
        for half in range(2):
            for leg in range(2):
                landed(leg, i, 2, half)
                to_sibling(leg, i, 2, (half,))

    for copy in started + side:
        copy.wait_send()

    for leg in range(2):
        for i in range(RING):
            for j in range(RING):
                for half in range(2):
                    here = far_spot(leg, i, j, half)
                    remote(here, here, side_send.at[leg, i, j, half], side_recv.at[leg, i, j, half], me).wait_recv()


def gather_rows(piece, n_dev):
    rows, d_model = piece.shape
    half = n_dev * rows // CORES
    return pl.pallas_call(
        gather_kernel,
        name='gather_rows',
        out_shape=(pltpu.VMEM((half, d_model), F32), pltpu.VMEM((half // 2, d_model), F32), pltpu.VMEM((half // 4, d_model), F32),
                   jax.ShapeDtypeStruct((half // 4, d_model), F32)),
        in_specs=[VMEM],
        out_specs=(VMEM, VMEM, VMEM, ANY),
        scratch_shapes=[DMA((40,)), DMA((2, RING, RING, 2)), DMA((2, RING, RING, 2)), DMA((2, RING, RING, 2))],
        compiler_params=pltpu.CompilerParams(collective_id=2, has_side_effects=True, vmem_limit_bytes=STORE_LIMIT),
    )(piece)


def store_kernel(near_ref, far_a_ref, far_b_ref, far_c_ref, y_ref, dx_ref, dq_out, dk_out, dv_out, do_out, y_out, dx_out,
                 tile, rows_buf, put_sem, a_sem, b_sem, in_sem, out_sem, row_in, row_out):
    core = lax.rem(lax.axis_index('sp'), CORES)
    outs = (dq_out, dk_out, dv_out, do_out)
    rows = near_ref.shape[0] // TYPES
    n_slot, chunk = tile.shape[0], tile.shape[1]
    n = far_c_ref.shape[0] // chunk
    piece = 4 * chunk

    def far_out(i, lo, size):
        first = (1 - core) * rows + i % RING * piece + lo
        return outs[i // RING].at[pl.ds(pl.multiple_of(first, chunk), size)]

    puts = []
    for i in range(n * 2):
        kind, size = i // SLOTS, 2 * chunk
        lo = i % SLOTS * size
        puts.append(pltpu.make_async_copy(near_ref.at[pl.ds(i * size, size)], outs[kind].at[span(core * rows + lo, size)], put_sem.at[i]))
    for i in range(n):
        puts.append(pltpu.make_async_copy(far_a_ref.at[pl.ds(i * 2 * chunk, 2 * chunk)], far_out(i, 0, 2 * chunk), a_sem.at[i]))
        puts.append(pltpu.make_async_copy(far_b_ref.at[pl.ds(i * chunk, chunk)], far_out(i, 2 * chunk, chunk), b_sem.at[i]))

    def load(i):
        return pltpu.make_async_copy(far_c_ref.at[pl.ds(i * chunk, chunk)], tile.at[i % n_slot], in_sem.at[i % n_slot])

    def save(i):
        return pltpu.make_async_copy(tile.at[i % n_slot], far_out(i, piece - chunk, chunk), out_sem.at[i % n_slot])

    steps = []
    for src, dst in ((y_ref, y_out), (dx_ref, dx_out)):
        take, give = pltpu.make_async_copy(src, rows_buf, row_in), pltpu.make_async_copy(rows_buf, dst, row_out)
        steps += [(take.start,), (take.wait, give.start), (give.wait,)]

    ahead = n_slot // 2
    for i in range(ahead):
        load(i).start()
    for put in puts:
        put.start()
    for i in range(n):
        load(i).wait()
        save(i).start()
        if i % 2 == 0 and i // 2 < len(steps):
            for action in steps[i // 2]:
                action()
        if i + ahead < n:
            if i + ahead >= n_slot:
                save(i + ahead - n_slot).wait()
            load(i + ahead).start()
    for i in range(n - n_slot, n):
        save(i).wait()
    for put in puts:
        put.wait()


def store(near, far_a, far_b, far_c, y_rows, dx_rows):
    half, d_model = near.shape
    n = RING * RING
    chunk = far_c.shape[0] // n
    grad = jax.ShapeDtypeStruct((half * CORES // TYPES, d_model), F32)
    tokens = jax.ShapeDtypeStruct(y_rows.shape, BF16)
    return pl.pallas_call(
        store_kernel,
        name='store',
        out_shape=(grad,) * TYPES + (tokens,) * 2,
        in_specs=[VMEM, VMEM, VMEM] + [ANY] * 3,
        out_specs=(ANY,) * (TYPES + 2),
        scratch_shapes=[pltpu.VMEM((4, chunk, d_model), F32), pltpu.VMEM(y_rows.shape, BF16),
                        DMA((2 * n,)), DMA((n,)), DMA((n,)), DMA((4,)), DMA((4,)), DMA, DMA],
        compiler_params=pltpu.CompilerParams(vmem_limit_bytes=STORE_LIMIT),
    )(in_vmem(near), in_vmem(far_a), in_vmem(far_b), in_hbm(far_c), in_hbm(y_rows), in_hbm(dx_rows))


def solution(mesh):
    n_dev = mesh.shape['sp']
    assert n_dev == CORES * RING * RING

    def device_body(x_loc, flag_loc, w_q, w_k, w_v, w_o, dy_loc):
        tok_count, d_model = x_loc.shape
        n_heads, head_dim = w_q.shape[1], w_q.shape[2]
        width = n_heads * head_dim
        score_scale = 1.0 / (math.sqrt(head_dim) * tok_count)
        weights = [w.transpose(1, 2, 0).reshape(width, d_model) for w in (w_q, w_k, w_v)] + [w_o.reshape(width, d_model)]
        g, z = front(flag_loc, x_loc, dy_loc, weights, score_scale, n_dev, n_heads)
        piece, y_rows, dx_rows = reduce_rows(g, z, x_loc, dy_loc, weights)
        *grads, y_loc, dx_loc = store(*gather_rows(piece, n_dev), y_rows, dx_rows)
        dw_q, dw_k, dw_v, dw_o = (grad.reshape(n_heads, head_dim, d_model) for grad in grads)
        return y_loc, dx_loc, dw_q.transpose(2, 0, 1), dw_k.transpose(2, 0, 1), dw_v.transpose(2, 0, 1), dw_o

    row_spec = P(('dp', 'sp'), None)
    flag_spec = P(('dp', 'sp'))
    w_spec = P(None, None, None)
    dw_spec = P('dp', None, None)
    return jax.shard_map(device_body, mesh=mesh,
                         in_specs=(row_spec, flag_spec, w_spec, w_spec, w_spec, w_spec, row_spec),
                         out_specs=(row_spec, row_spec, dw_spec, dw_spec, dw_spec, dw_spec),
                         check_vma=False)
```

```python
import functools
import math
import jax
import jax.numpy as jnp
from jax import lax
from jax.experimental import pallas as pl
from jax.experimental.pallas import tpu as pltpu
from jax.sharding import PartitionSpec as P

MESH = pl.DeviceIdType.MESH
CORES = 2
RING = 4
SLOTS = CORES * RING
TYPES = 4
O_TYPE = TYPES - 1
MIB = 1024 * 1024
STORE_LIMIT = 5 * MIB
BF16 = jnp.bfloat16
F32 = jnp.float32
ROWS = ((1,), (1,))
INNER = ((1,), (0,))
OUTER = ((0,), (0,))
VMEM = pl.BlockSpec(memory_space=pltpu.VMEM)
ANY = pl.BlockSpec(memory_space=pltpu.HBM)
DMA = pltpu.SemaphoreType.DMA


def place(me):
    core = lax.rem(me, CORES)
    chip = me // CORES
    return lax.rem(chip, RING), chip // RING, core


def index_of(x, y, core):
    return (lax.rem(y, RING) * RING + lax.rem(x, RING)) * CORES + core


def remote(src, dst, send_sem, recv_sem, peer):
    return pltpu.make_async_remote_copy(src_ref=src, dst_ref=dst, send_sem=send_sem, recv_sem=recv_sem,
                                        device_id={'sp': peer}, device_id_type=MESH)


def signal(peer):
    pl.semaphore_signal(pltpu.get_barrier_semaphore(), inc=1, device_id={'sp': peer}, device_id_type=MESH)


def meet(peers):
    for peer in peers:
        signal(peer)
    pl.semaphore_wait(pltpu.get_barrier_semaphore(), len(peers))


def chips_around(x, y):
    return ((x + 1, y), (x + RING - 1, y), (x, y + 1), (x, y + RING - 1))


def dot(a, b, dims):
    return lax.dot_general(a, b, (dims, ((), ())), preferred_element_type=F32)


def in_vmem(value):
    return pltpu.with_memory_space_constraint(value, pltpu.VMEM)


def in_hbm(value):
    return pltpu.with_memory_space_constraint(value, pltpu.HBM)


def span(start, size):
    return pl.ds(pl.multiple_of(start, size), size)


def stream(n_outer, n_inner, depth, copy, use, before):
    ahead = depth - 1
    for n in range(ahead):
        copy(0, n, n).start()
    for i in range(n_outer):
        before(i)

        @pl.loop(0, n_inner)
        def _(n):
            at = i * n_inner + n
            slot, free = lax.rem(at, depth), lax.rem(at + ahead, depth)

            @pl.when(n + ahead < n_inner)
            def _():
                copy(i, n + ahead, free).start()

            if i + 1 < n_outer:
                @pl.when(n + ahead >= n_inner)
                def _():
                    copy(i + 1, n + ahead - n_inner, free).start()

            copy(i, n, slot).wait()
            use(i, n, slot)


def form_masks(flag_ref, seg_col_ref, seg_row_ref, head_ref, tail_ref, gate_ref):
    tok = flag_ref.shape[1]
    flags = flag_ref[...] > 0
    t_pos = lax.broadcasted_iota(jnp.int32, (tok, tok), 0)
    s_pos = lax.broadcasted_iota(jnp.int32, (tok, tok), 1)
    seg_col = jnp.sum(jnp.where(flags & (s_pos <= t_pos), 1.0, 0), axis=1, keepdims=True)
    seg_col_ref[...] = seg_col
    seg_row_ref[...] = jnp.sum(jnp.where(s_pos == t_pos, seg_col, 0), axis=0, keepdims=True)
    positions = lax.broadcasted_iota(jnp.int32, (1, tok), 1).astype(F32)
    first_pos = jnp.min(jnp.where(flags, positions, tok), axis=1, keepdims=True)
    last_pos = jnp.max(jnp.where(flags, positions, -1), axis=1, keepdims=True)
    head_ref[...] = jnp.where(positions < first_pos, 1.0, 0)
    tail_ref[...] = jnp.where(positions >= last_pos, 1.0, 0)
    gate_ref[...] = jnp.broadcast_to(jnp.where(last_pos < 0, 1.0, 0), gate_ref.shape)


class Square:
    def __init__(self, me):
        x, y, core = place(me)
        across_x, across_y = (lax.rem(a + 1 + RING - 2 * lax.rem(a + core, 2), RING) for a in (x, y))
        self.core = core
        self.chips = [(x, y), (across_x, y), (x, across_y), (across_x, across_y)]

    def peer(self, k):
        return index_of(*self.chips[k], self.core)

    def kind(self, k):
        return owned_type(*self.chips[k])


def owned_type(x, y):
    return lax.rem(x, 2) + 2 * lax.rem(y, 2)


def lattice(x, y):
    return lax.rem(x // 2, 2), lax.rem(y // 2, 2)


def start_tokens(kind, x_ref, dy_ref, copy):
    @pl.when(kind == O_TYPE)
    def _():
        copy(dy_ref).start()

    @pl.when(kind != O_TYPE)
    def _():
        copy(x_ref).start()


def front_kernel(scale, dim, flag_ref, x_ref, dy_ref, wq_ref, wk_ref, wv_ref, wo_ref,
                 g_ref, z_ref, seg_col_ref, seg_row_ref, head_ref, tail_ref, gate_ref, tok_in, w_tile, rows_ref, total,
                 packed, held, formed, states,
                 tok_sem, w_sem, g_sem, z_send, z_recv, send_sem, recv_sem, back_send, back_recv):
    me = lax.axis_index('sp')
    n_dev, per_dev, low = formed.shape[1:4]
    width, tok = rows_ref.shape[1], rows_ref.shape[2]
    half = tok // 2
    n_piece = z_recv.shape[1]
    piece = tok // SLOTS
    n_group = SLOTS
    group = width // n_group
    tile_rows = w_tile.shape[1]

    @pl.loop(1, n_dev)
    def _(step):
        signal(lax.rem(me + step, n_dev))

    loads = [pltpu.make_async_copy(ref, tok_in.at[i], tok_sem.at[i]) for i, ref in enumerate((x_ref, dy_ref))]
    for load in loads:
        load.start()

    square = Square(me)

    cuts = (0, 2, 3, TYPES, SLOTS)

    def token_copy(k, n):
        at = pl.ds(cuts[n] * piece, (cuts[n + 1] - cuts[n]) * piece)
        return lambda ref: remote(ref.at[at], z_ref.at[k - 1, at], z_send.at[k - 1, n], z_recv.at[k - 1, n], square.peer(k))

    def push_tokens(n):
        for k in range(1, TYPES):
            start_tokens(square.kind(k), x_ref, dy_ref, token_copy(k, n))

    form_masks(flag_ref, seg_col_ref, seg_row_ref, head_ref, tail_ref, gate_ref)
    pl.semaphore_wait(pltpu.get_barrier_semaphore(), n_dev - 1)
    push_tokens(0)

    weights = (wk_ref, wv_ref, wq_ref, wo_ref)
    kinds = (1, 2, 0, O_TYPE)

    def w_copy(i, n, slot):
        return pltpu.make_async_copy(weights[i].at[span(n * tile_rows, tile_rows)], w_tile.at[slot], w_sem.at[slot])

    def project(i, n, slot):
        rows_ref[kinds[i], span(n * tile_rows, tile_rows), :] = dot(w_tile[slot], tok_in[i // O_TYPE], ROWS).astype(BF16)

    def loaded(i):
        if i in (0, O_TYPE):
            loads[i // O_TYPE].wait()
        if i == 2:
            send_products(0)
        if i in (1, O_TYPE):
            push_tokens(1 + i // O_TYPE)

    head = head_ref[...] > 0.5
    tail = tail_ref[...] > 0.5

    def each(do):
        pl.loop(1, n_dev)(do)

    def out_copy(which, step):
        peer = lax.rem(me + step, n_dev)
        at = pl.ds(0, low + 1 - which)
        return remote(packed.at[which, peer, :, at], held.at[which, me, :, at], send_sem.at[which, step], recv_sem.at[which, step], peer)

    def back_copy(which, step):
        peer = lax.rem(me + step, n_dev)
        return remote(formed.at[which, peer], states.at[which, me], back_send.at[which, step], back_recv.at[which, step], peer)

    pair_lane = lax.broadcasted_iota(jnp.int32, (low, 2 * dim), 1) // dim

    def turn(pair):
        return pltpu.roll(pair, dim, 1)

    def send_products(which):
        left, right, mask = ((1, 2, tail), (0, O_TYPE, head))[which]

        @pl.loop(0, n_group)
        def _(grp):
            at = span(grp * group, group)
            full = dot(rows_ref[left, at, :], jnp.where(mask, rows_ref[right, at, :], jnp.zeros((group, tok), BF16)), ROWS)
            for sub in range(group // dim):
                spot = sub % 2
                block = full[sub * dim:(sub + 1) * dim, (sub // 2) * 2 * dim:(sub // 2 + 1) * 2 * dim]
                first, second = block[0:low], block[low:]
                if spot == 0:
                    second = turn(second)
                else:
                    first = turn(first)
                index = grp * (group // dim) + sub
                dev, own = index // per_dev, lax.rem(index, per_dev)
                packed[which, dev, own, 0:low, :] = jnp.where(pair_lane == 0, first, second)
                packed[which, dev, own, low:, :] = gate_ref[...]

        each(lambda step: out_copy(which, step).start())
        held[which, me] = packed[which, me]

    def form_states(which):
        each(lambda step: out_copy(which, step).wait_recv())

        def advance(step, state):
            block = step if which == 0 else n_dev - 1 - step
            formed[which, block] = state.astype(BF16)
            return held[0, block, :, low:low + 1, :] * state + held[which, block, :, 0:low, :]

        lax.fori_loop(0, n_dev, advance, jnp.zeros((per_dev, low, 2 * dim), F32), unroll=4)
        each(lambda step: back_copy(which, step).start())
        states[which, me] = formed[which, me]

    stream(TYPES, width // tile_rows, w_tile.shape[0], w_copy, project, loaded)
    send_products(1)

    seg_row = seg_row_ref[...]
    t_pos = lax.broadcasted_iota(jnp.int32, (half, tok), 0)
    s_pos = lax.broadcasted_iota(jnp.int32, (half, tok), 1)

    def pair(a, b):
        see_top = ((seg_col_ref[0:half, :] == seg_row) & (s_pos <= t_pos))[:, 0:half]
        see_low = (seg_col_ref[half:, :] == seg_row) & (s_pos <= t_pos + half)
        top = dot(a[:, 0:half], b[:, 0:half], OUTER)
        low = dot(a[:, half:], b, OUTER)
        return (jnp.where(see_top, top * scale, 0).astype(BF16), jnp.where(see_low, low * scale, 0).astype(BF16))

    def over_keys(at, rows_t, probs):
        total[at[0], at[1], 0:half] = dot(rows_t[:, 0:half], probs[0], ROWS)
        total[at[0], at[1], half:] = dot(rows_t, probs[1], ROWS)

    def over_queries(at, rows_t, probs):
        from_low = dot(rows_t[:, half:], probs[1], INNER)
        total[at[0], at[1], 0:half] = dot(rows_t[:, 0:half], probs[0], INNER) + from_low[:, 0:half]
        total[at[0], at[1], half:] = from_low[:, half:]

    def heads_of(grp):
        return [grp * (group // dim) + sub for sub in range(group // dim)]

    @pl.loop(0, n_group)
    def _(grp):
        @pl.when(grp == 1)
        def _():
            form_states(0)

        @pl.when(grp == n_group // 2 + 1)
        def _():
            form_states(1)
            push_tokens(O_TYPE)

        for index in heads_of(grp):
            rows = span(index * dim, dim)
            q, k, v, do = (rows_ref[kind, rows, :] for kind in range(TYPES))
            d_probs = pair(do, v)
            over_keys((0, rows), k, d_probs)
            over_queries((1, rows), q, d_probs)
            probs = pair(q, k)
            over_queries((2, rows), do, probs)
            over_keys((O_TYPE, rows), v, probs)

    def diagonal(which, grp):
        rows = []
        for sub in range(group // dim):
            index = grp * (group // dim) + sub
            pair = states[which, index // per_dev, lax.rem(index, per_dev)].astype(F32)
            spot = sub % 2
            block = jnp.concatenate([turn(pair), pair] if spot else [pair, turn(pair)], axis=0)
            block = jnp.where(jnp.concatenate([pair_lane, pair_lane], axis=0) == spot, block, 0)
            empty = jnp.zeros_like(block)
            rows.append(jnp.concatenate([empty, block] if sub // 2 else [block, empty], axis=1))
        return jnp.concatenate(rows, axis=0).astype(BF16)

    def finish(kind, at, mask, inter):
        rows_ref[kind, at, :] = (total[kind, at, :] + jnp.where(mask, inter * scale, 0)).astype(BF16)

    def row_put(kind, grp):
        at = span(grp * group, group)
        return pltpu.make_async_copy(rows_ref.at[kind, at], g_ref.at[kind, at], g_sem.at[kind, grp])

    each(lambda step: back_copy(0, step).wait_recv())

    @pl.loop(0, n_group)
    def _(grp):
        at = span(grp * group, group)
        st = diagonal(0, grp)
        d_q = dot(st, rows_ref[O_TYPE, at, :], INNER)
        out = dot(st, rows_ref[0, at, :], OUTER)
        finish(0, at, head, d_q)
        finish(O_TYPE, at, head, out)
        for kind in (0, O_TYPE):
            row_put(kind, grp).start()

    each(lambda step: back_copy(1, step).wait_recv())

    @pl.loop(0, n_group)
    def _(grp):
        at = span(grp * group, group)
        st = diagonal(1, grp)
        d_k = dot(st, rows_ref[2, at, :], INNER)
        d_v = dot(st, rows_ref[1, at, :], OUTER)
        finish(1, at, tail, d_k)
        finish(2, at, tail, d_v)
        for kind in (1, 2):
            row_put(kind, grp).start()

    for kind in range(TYPES):
        pl.loop(0, n_group)(lambda grp, kind=kind: row_put(kind, grp).wait())
    for which in range(2):
        each(lambda step, which=which: out_copy(which, step).wait_send())
        each(lambda step, which=which: back_copy(which, step).wait_send())
    for k in range(1, TYPES):
        for n in range(n_piece):
            token_copy(k, n)(x_ref).wait()


def front(flags, x_loc, dy_loc, weights, scale, n_dev, n_heads):
    tok, d_model = x_loc.shape
    width = weights[0].shape[0]
    dim = width // n_heads
    per_dev = n_heads // n_dev
    n_piece = TYPES
    pack = (2, n_dev, per_dev, dim // 2 + 8, 2 * dim)
    back = (2, n_dev, per_dev, dim // 2, 2 * dim)
    return pl.pallas_call(
        functools.partial(front_kernel, scale, dim),
        name='front',
        out_shape=(jax.ShapeDtypeStruct((TYPES, width, tok), BF16), jax.ShapeDtypeStruct((TYPES - 1, tok, d_model), BF16)),
        in_specs=[VMEM] + [ANY] * 6,
        out_specs=(ANY, ANY),
        scratch_shapes=[
            pltpu.VMEM((tok, 1), F32), pltpu.VMEM((1, tok), F32), pltpu.VMEM((1, tok), F32), pltpu.VMEM((1, tok), F32), pltpu.VMEM((8, 2 * dim), F32),
            pltpu.VMEM((2, tok, d_model), BF16), pltpu.VMEM((4, width // RING, d_model), BF16),
            pltpu.VMEM((TYPES, width, tok), BF16), pltpu.VMEM((TYPES, width, tok), F32),
            pltpu.VMEM(pack, F32), pltpu.VMEM(pack, F32), pltpu.VMEM(back, BF16), pltpu.VMEM(back, BF16),
            DMA((2,)), DMA((4,)), DMA((TYPES, SLOTS)), DMA((TYPES - 1, n_piece)), DMA((TYPES - 1, n_piece)),
            DMA((2, n_dev)), DMA((2, n_dev)), DMA((2, n_dev)), DMA((2, n_dev))],
        compiler_params=pltpu.CompilerParams(collective_id=0, has_side_effects=True, vmem_limit_bytes=56 * MIB),
    )(flags[None, :], x_loc, dy_loc, *weights)


def row_products(g_ref, w_refs, y_ref, dx_ref, rows_in, rows_t, w_tile, total, done, g_sem, w_sem, put_sem):
    width = rows_in.shape[0]
    cols = w_tile.shape[2]
    n_tile = total.shape[1] // cols
    step = width // SLOTS
    order = (O_TYPE, 0, 1, 2)

    def g_copy(i):
        return pltpu.make_async_copy(g_ref.at[order[i]], rows_in, g_sem)

    def w_copy(i, n, slot):
        return pltpu.make_async_copy(w_refs[order[i]].at[:, span(n * cols, cols)], w_tile.at[slot], w_sem.at[slot])

    puts = [pltpu.make_async_copy(done, ref, put_sem) for ref in (y_ref, dx_ref)]

    def turned(i):
        if i == 1:
            puts[0].start()
        if i == O_TYPE:
            puts[0].wait()
        g_copy(i).wait()

        @pl.loop(0, width // step)
        def _(b):
            at = span(b * step, step)
            rows_t[:, at] = jnp.transpose(rows_in[at, :])

        if i < O_TYPE:
            g_copy(i + 1).start()

    def use(i, n, slot):
        at = span(n * cols, cols)
        prod = dot(rows_t[...], w_tile[slot], INNER)
        if i == 0:
            done[:, at] = prod.astype(BF16)
        elif i == 1:
            total[:, at] = prod
        elif i < O_TYPE:
            total[:, at] = total[:, at] + prod
        else:
            done[:, at] = (total[:, at] + prod).astype(BF16)

    g_copy(0).start()
    stream(TYPES, n_tile, w_tile.shape[0], w_copy, use, turned)
    puts[1].start()
    return puts[1]


FLIPS = ((1, 1), (1, 0), (0, 1), (0, 0))


def reduce_kernel(g_ref, z_ref, x_ref, dy_ref, wq_ref, wk_ref, wv_ref, wo_ref, out_ref, y_ref, dx_ref,
                  zbuf, rows_in, side_out, side_in, first_out, first_in, second_out, second_in, kind_rows, rows_t, w_tile, sums, done,
                  z_sem, row_send, row_recv, side_send, side_recv, first_send, first_recv, second_send, second_recv, g_sem, w_sem, put_sem):
    me = lax.axis_index('sp')
    x, y, core = place(me)
    square = Square(me)
    block = rows_in.shape[3]
    part = block // 2
    n_col, cols = second_out.shape[1], second_out.shape[3]
    sibling = index_of(x, y, 1 - core)
    across = (index_of(x + 2, y, core), index_of(x, y + 2, core))

    meet([sibling, *across] + [square.peer(k) for k in range(1, TYPES)])

    def own_copy(ref):
        return pltpu.make_async_copy(ref, zbuf.at[0], z_sem.at[0])

    z_copies = [pltpu.make_async_copy(z_ref.at[k - 1], zbuf.at[k], z_sem.at[k]) for k in range(1, TYPES)]

    def row_source(k, mine, t):
        px, py = lattice(*square.chips[k])
        half = core if mine else 1 - core
        index = half * RING + lax.rem(px + FLIPS[t][0], 2) + 2 * lax.rem(py + FLIPS[t][1], 2)
        return g_ref.at[square.kind(k), span(index * block, block)]

    def row_copy(k, mine, t):
        dst, recv = rows_in.at[k, mine, t], row_recv.at[k, mine, t]
        if k == 0:
            return pltpu.make_async_copy(row_source(k, mine, t), dst, recv)
        return remote(row_source(k, mine, t), dst, row_send.at[k - 1, mine, t], recv, square.peer(k))

    every_row = [(k, mine, t) for t in range(TYPES) for mine in range(2) for k in range(TYPES)]
    for where in every_row:
        row_copy(*where).start()
    start_tokens(square.kind(0), x_ref, dy_ref, own_copy)
    for copy in z_copies:
        copy.start()

    last_put = row_products(g_ref, (wq_ref, wk_ref, wv_ref, wo_ref), y_ref, dx_ref, kind_rows, rows_t, w_tile, sums, done, g_sem, w_sem, put_sem)

    own_copy(x_ref).wait()
    for copy in z_copies:
        copy.wait()

    def product(mine, t, ch):
        at = span(ch * cols, cols)
        total = dot(rows_in[0, mine, t], zbuf[0, :, at], INNER)
        for k in range(1, TYPES):
            total = total + dot(rows_in[k, mine, t], zbuf[k, :, at], INNER)
        return total

    def side_copy(t, ch):
        return remote(side_out.at[t % 2, ch], side_in.at[t, ch], side_send.at[t, ch], side_recv.at[t, ch], sibling)

    def first_copy(leg, q, ch):
        return remote(first_out.at[leg, q, ch], first_in.at[leg, q, ch], first_send.at[leg, q, ch], first_recv.at[leg, q, ch], across[leg])

    def second_copy(leg, ch):
        return remote(second_out.at[leg, ch], second_in.at[leg, ch], second_send.at[leg, ch], second_recv.at[leg, ch], across[1 - leg])

    def sibling_part(t, ch):
        if t >= 2:
            side_copy(t - 2, ch).wait_send()
        side_out[t % 2, ch] = product(0, t, ch)
        side_copy(t, ch).start()

    def own_part(t, ch):
        total = product(1, t, ch)
        side_copy(t, ch).wait_recv()
        total = total + side_in[t, ch]
        for leg in range(2):
            half = total[leg * part:(leg + 1) * part]
            step, other = FLIPS[t][leg], FLIPS[t][1 - leg]
            if step:
                first_out[leg, other, ch] = half
                first_copy(leg, other, ch).start()
                continue
            first_copy(leg, other, ch).wait_recv()
            half = half + first_in[leg, other, ch]
            if other:
                second_out[leg, ch] = half
                second_copy(leg, ch).start()
            else:
                second_copy(leg, ch).wait_recv()
                out_ref[leg * part:(leg + 1) * part, span(ch * cols, cols)] = half + second_in[leg, ch]

    for stage in ((0,), (1, 2), (O_TYPE,)):
        for t in stage:
            for mine in range(2):
                for k in range(TYPES):
                    copy = row_copy(k, mine, t)
                    if k:
                        copy.wait_recv()
                    else:
                        copy.wait()

        for work in (sibling_part, own_part):
            @pl.loop(0, n_col)
            def _(ch, stage=stage, work=work):
                for t in stage:
                    work(t, ch)

    last_put.wait()
    for where in every_row:
        if where[0]:
            row_copy(*where).wait_send()

    @pl.loop(0, n_col)
    def _(ch):
        for t in range(2, TYPES):
            side_copy(t, ch).wait_send()
        for leg in range(2):
            for q in range(2):
                first_copy(leg, q, ch).wait_send()
            second_copy(leg, ch).wait_send()


def reduce_rows(g, z, x_loc, dy_loc, weights):
    width, tok = g.shape[1], g.shape[2]
    d_model = x_loc.shape[1]
    block = width // SLOTS
    n_col = RING
    cols = d_model // n_col
    tokens = jax.ShapeDtypeStruct((tok, d_model), BF16)
    halves = lambda *lead: pltpu.VMEM((*lead, n_col, block // 2, cols), F32)
    blocks = lambda lead: pltpu.VMEM((lead, n_col, block, cols), F32)
    return pl.pallas_call(
        reduce_kernel,
        name='reduce_rows',
        out_shape=(pltpu.VMEM((block, d_model), F32), tokens, tokens),
        in_specs=[ANY] * 8,
        out_specs=(VMEM, ANY, ANY),
        scratch_shapes=[
            pltpu.VMEM((TYPES, tok, d_model), BF16), pltpu.VMEM((TYPES, 2, TYPES, block, tok), BF16),
            blocks(2), blocks(TYPES), halves(2, 2), halves(2, 2), halves(2), halves(2),
            pltpu.VMEM((width, tok), BF16), pltpu.VMEM((tok, width), BF16), pltpu.VMEM((3, width, min(256, d_model // 4)), BF16),
            pltpu.VMEM((tok, d_model), F32), pltpu.VMEM((tok, d_model), BF16),
            DMA((TYPES,)), DMA((TYPES - 1, 2, TYPES)), DMA((TYPES, 2, TYPES)), DMA((TYPES, n_col)), DMA((TYPES, n_col)),
            DMA((2, 2, n_col)), DMA((2, 2, n_col)), DMA((2, n_col)), DMA((2, n_col)), DMA, DMA((3,)), DMA],
        compiler_params=pltpu.CompilerParams(collective_id=1, has_side_effects=True, vmem_limit_bytes=58 * MIB),
    )(g, z, x_loc, dy_loc, *weights)


def gather_kernel(piece_ref, near_ref, far_a_ref, far_b_ref, far_c_ref, send_sem, recv_sem, side_send, side_recv):
    me = lax.axis_index('sp')
    x, y, core = place(me)
    rows = piece_ref.shape[0]
    part = rows // 2
    quarter = part // 2

    def number(leg, i, j):
        sx, sy = (i, j) if leg == 0 else (j, i)
        px, py = lax.rem(x + sx, RING), lax.rem(y + sy, RING)
        lx, ly = lattice(px, py)
        return owned_type(px, py) * RING + lx + 2 * ly

    def spot(leg, i, j, half=None):
        lo, size = (0, part) if half is None else (half * quarter, quarter)
        return near_ref.at[pl.ds(pl.multiple_of(number(leg, i, j) * rows + leg * part + lo, quarter), size)]

    def far_spot(leg, i, j, half):
        if leg == 0:
            return far_a_ref.at[span(number(leg, i, j) * part + half * quarter, quarter)]
        return (far_b_ref, far_c_ref)[half].at[span(number(leg, i, j) * quarter, quarter)]

    def own(leg, half=None):
        lo, size = (0, part) if half is None else (half * quarter, quarter)
        return piece_ref.at[pl.ds(leg * part + lo, size)]

    def step_peer(leg, second, step):
        along_x = (leg == 0) != second
        return index_of(x + step, y, core) if along_x else index_of(x, y + step, core)

    started = []

    def push(leg, second, i, j, step, half):
        there = (i, (j - step) % RING) if second else ((i - step) % RING, j)
        src = own(leg, half) if i == 0 and j == 0 else spot(leg, i, j, half)
        copy = remote(src, spot(leg, i, j, half), send_sem.at[len(started)],
                      recv_sem.at[leg, there[0], there[1], half or 0], step_peer(leg, second, step))
        copy.start()
        started.append(copy)

    def landed(leg, i, j, half=None):
        here = spot(leg, i, j, half)
        remote(here, here, send_sem.at[0], recv_sem.at[leg, i, j, half or 0], me).wait_recv()

    side = []

    def to_sibling(leg, i, j, halves=(0, 1)):
        for half in halves:
            src = own(leg, half) if i == 0 and j == 0 else spot(leg, i, j, half)
            copy = remote(src, far_spot(leg, i, j, half), side_send.at[leg, i, j, half], side_recv.at[leg, i, j, half], index_of(x, y, 1 - core))
            copy.start()
            side.append(copy)

    meet([index_of(x, y, 1 - core)] + [index_of(*chip, core) for chip in chips_around(x, y)])

    def spread(leg, i):
        push(leg, True, i, 0, 1, None)
        push(leg, True, i, 0, 3, None)
        to_sibling(leg, i, 0)

    for leg in range(2):
        push(leg, False, 0, 0, 1, None)
        push(leg, False, 0, 0, 3, None)
    for leg in range(2):
        spread(leg, 0)
    near_ref[span(number(0, 0, 0) * rows, rows), :] = piece_ref[...]

    for leg in range(2):
        landed(leg, 3, 0)
        push(leg, False, 3, 0, 1, 0)
        spread(leg, 3)
        landed(leg, 1, 0)
        push(leg, False, 1, 0, 3, 1)
        spread(leg, 1)

    def second_near(leg, i):
        landed(leg, i, 3)
        push(leg, True, i, 3, 1, 0)
        to_sibling(leg, i, 3)
        landed(leg, i, 1)
        push(leg, True, i, 1, 3, 1)
        to_sibling(leg, i, 1)

    for leg in range(2):
        second_near(leg, 0)
    for leg in range(2):
        for half in range(2):
            landed(leg, 2, 0, half)
        spread(leg, 2)
    for i in (3, 1, 2):
        for leg in range(2):
            second_near(leg, i)
    for i in (0, 3, 1, 2):
        for half in range(2):
            for leg in range(2):
                landed(leg, i, 2, half)
                to_sibling(leg, i, 2, (half,))

    for copy in started + side:
        copy.wait_send()

    for leg in range(2):
        for i in range(RING):
            for j in range(RING):
                for half in range(2):
                    here = far_spot(leg, i, j, half)
                    remote(here, here, side_send.at[leg, i, j, half], side_recv.at[leg, i, j, half], me).wait_recv()


def gather_rows(piece, n_dev):
    rows, d_model = piece.shape
    half = n_dev * rows // CORES
    return pl.pallas_call(
        gather_kernel,
        name='gather_rows',
        out_shape=(pltpu.VMEM((half, d_model), F32), pltpu.VMEM((half // 2, d_model), F32), pltpu.VMEM((half // 4, d_model), F32),
                   jax.ShapeDtypeStruct((half // 4, d_model), F32)),
        in_specs=[VMEM],
        out_specs=(VMEM, VMEM, VMEM, ANY),
        scratch_shapes=[DMA((40,)), DMA((2, RING, RING, 2)), DMA((2, RING, RING, 2)), DMA((2, RING, RING, 2))],
        compiler_params=pltpu.CompilerParams(collective_id=2, has_side_effects=True, vmem_limit_bytes=STORE_LIMIT),
    )(piece)


def store_kernel(near_ref, far_a_ref, far_b_ref, far_c_ref, y_ref, dx_ref, dq_out, dk_out, dv_out, do_out, y_out, dx_out,
                 tile, rows_buf, put_sem, a_sem, b_sem, in_sem, out_sem, row_in, row_out):
    core = lax.rem(lax.axis_index('sp'), CORES)
    outs = (dq_out, dk_out, dv_out, do_out)
    rows = near_ref.shape[0] // TYPES
    n_slot, chunk = tile.shape[0], tile.shape[1]
    n = far_c_ref.shape[0] // chunk
    piece = 4 * chunk

    def far_out(i, lo, size):
        first = (1 - core) * rows + i % RING * piece + lo
        return outs[i // RING].at[pl.ds(pl.multiple_of(first, chunk), size)]

    puts = []
    for i in range(n * 2):
        kind, size = i // SLOTS, 2 * chunk
        lo = i % SLOTS * size
        puts.append(pltpu.make_async_copy(near_ref.at[pl.ds(i * size, size)], outs[kind].at[span(core * rows + lo, size)], put_sem.at[i]))
    for i in range(n):
        puts.append(pltpu.make_async_copy(far_a_ref.at[pl.ds(i * 2 * chunk, 2 * chunk)], far_out(i, 0, 2 * chunk), a_sem.at[i]))
        puts.append(pltpu.make_async_copy(far_b_ref.at[pl.ds(i * chunk, chunk)], far_out(i, 2 * chunk, chunk), b_sem.at[i]))

    def load(i):
        return pltpu.make_async_copy(far_c_ref.at[pl.ds(i * chunk, chunk)], tile.at[i % n_slot], in_sem.at[i % n_slot])

    def save(i):
        return pltpu.make_async_copy(tile.at[i % n_slot], far_out(i, piece - chunk, chunk), out_sem.at[i % n_slot])

    steps = []
    for src, dst in ((y_ref, y_out), (dx_ref, dx_out)):
        take, give = pltpu.make_async_copy(src, rows_buf, row_in), pltpu.make_async_copy(rows_buf, dst, row_out)
        steps += [(take.start,), (take.wait, give.start), (give.wait,)]

    ahead = n_slot // 2
    for i in range(ahead):
        load(i).start()
    for put in puts:
        put.start()
    for i in range(n):
        load(i).wait()
        save(i).start()
        if i % 2 == 0 and i // 2 < len(steps):
            for action in steps[i // 2]:
                action()
        if i + ahead < n:
            if i + ahead >= n_slot:
                save(i + ahead - n_slot).wait()
            load(i + ahead).start()
    for i in range(n - n_slot, n):
        save(i).wait()
    for put in puts:
        put.wait()


def store(near, far_a, far_b, far_c, y_rows, dx_rows):
    half, d_model = near.shape
    n = RING * RING
    chunk = far_c.shape[0] // n
    grad = jax.ShapeDtypeStruct((half * CORES // TYPES, d_model), F32)
    tokens = jax.ShapeDtypeStruct(y_rows.shape, BF16)
    return pl.pallas_call(
        store_kernel,
        name='store',
        out_shape=(grad,) * TYPES + (tokens,) * 2,
        in_specs=[VMEM, VMEM, VMEM] + [ANY] * 3,
        out_specs=(ANY,) * (TYPES + 2),
        scratch_shapes=[pltpu.VMEM((4, chunk, d_model), F32), pltpu.VMEM(y_rows.shape, BF16),
                        DMA((2 * n,)), DMA((n,)), DMA((n,)), DMA((4,)), DMA((4,)), DMA, DMA],
        compiler_params=pltpu.CompilerParams(vmem_limit_bytes=STORE_LIMIT),
    )(in_vmem(near), in_vmem(far_a), in_vmem(far_b), in_hbm(far_c), in_hbm(y_rows), in_hbm(dx_rows))


def solution(mesh):
    n_dev = mesh.shape['sp']
    assert n_dev == CORES * RING * RING

    def device_body(x_loc, flag_loc, w_q, w_k, w_v, w_o, dy_loc):
        tok_count, d_model = x_loc.shape
        n_heads, head_dim = w_q.shape[1], w_q.shape[2]
        width = n_heads * head_dim
        score_scale = 1.0 / (math.sqrt(head_dim) * tok_count)
        weights = [w.transpose(1, 2, 0).reshape(width, d_model) for w in (w_q, w_k, w_v)] + [w_o.reshape(width, d_model)]
        g, z = front(flag_loc, x_loc, dy_loc, weights, score_scale, n_dev, n_heads)
        piece, y_rows, dx_rows = reduce_rows(g, z, x_loc, dy_loc, weights)
        *grads, y_loc, dx_loc = store(*gather_rows(piece, n_dev), y_rows, dx_rows)
        dw_q, dw_k, dw_v, dw_o = (grad.reshape(n_heads, head_dim, d_model) for grad in grads)
        return y_loc, dx_loc, dw_q.transpose(2, 0, 1), dw_k.transpose(2, 0, 1), dw_v.transpose(2, 0, 1), dw_o

    row_spec = P(('dp', 'sp'), None)
    flag_spec = P(('dp', 'sp'))
    w_spec = P(None, None, None)
    dw_spec = P('dp', None, None)
    return jax.shard_map(device_body, mesh=mesh,
                         in_specs=(row_spec, flag_spec, w_spec, w_spec, w_spec, w_spec, row_spec),
                         out_specs=(row_spec, row_spec, dw_spec, dw_spec, dw_spec, dw_spec),
                         check_vma=False)
```

```python
import functools
import math
import jax
import jax.numpy as jnp
from jax import lax
from jax.experimental import pallas as pl
from jax.experimental.pallas import tpu as pltpu
from jax.sharding import PartitionSpec as P

MESH = pl.DeviceIdType.MESH
CORES = 2
RING = 4
SLOTS = CORES * RING
TYPES = 4
O_TYPE = TYPES - 1
MIB = 1024 * 1024
STORE_LIMIT = 5 * MIB
BF16 = jnp.bfloat16
F32 = jnp.float32
ROWS = ((1,), (1,))
INNER = ((1,), (0,))
OUTER = ((0,), (0,))
VMEM = pl.BlockSpec(memory_space=pltpu.VMEM)
ANY = pl.BlockSpec(memory_space=pltpu.HBM)
DMA = pltpu.SemaphoreType.DMA


def place(me):
    core = lax.rem(me, CORES)
    chip = me // CORES
    return lax.rem(chip, RING), chip // RING, core


def index_of(x, y, core):
    return (lax.rem(y, RING) * RING + lax.rem(x, RING)) * CORES + core


def remote(src, dst, send_sem, recv_sem, peer):
    return pltpu.make_async_remote_copy(src_ref=src, dst_ref=dst, send_sem=send_sem, recv_sem=recv_sem,
                                        device_id={'sp': peer}, device_id_type=MESH)


def signal(peer):
    pl.semaphore_signal(pltpu.get_barrier_semaphore(), inc=1, device_id={'sp': peer}, device_id_type=MESH)


def meet(peers):
    for peer in peers:
        signal(peer)
    pl.semaphore_wait(pltpu.get_barrier_semaphore(), len(peers))


def chips_around(x, y):
    return ((x + 1, y), (x + RING - 1, y), (x, y + 1), (x, y + RING - 1))


def dot(a, b, dims):
    return lax.dot_general(a, b, (dims, ((), ())), preferred_element_type=F32)


def in_vmem(value):
    return pltpu.with_memory_space_constraint(value, pltpu.VMEM)


def in_hbm(value):
    return pltpu.with_memory_space_constraint(value, pltpu.HBM)


def span(start, size):
    return pl.ds(pl.multiple_of(start, size), size)


def stream(n_outer, n_inner, depth, copy, use, before):
    ahead = depth - 1
    for n in range(ahead):
        copy(0, n, n).start()
    for i in range(n_outer):
        before(i)

        @pl.loop(0, n_inner)
        def _(n):
            at = i * n_inner + n
            slot, free = lax.rem(at, depth), lax.rem(at + ahead, depth)

            @pl.when(n + ahead < n_inner)
            def _():
                copy(i, n + ahead, free).start()

            if i + 1 < n_outer:
                @pl.when(n + ahead >= n_inner)
                def _():
                    copy(i + 1, n + ahead - n_inner, free).start()

            copy(i, n, slot).wait()
            use(i, n, slot)


def form_masks(flag_ref, seg_col_ref, seg_row_ref, head_ref, tail_ref, gate_ref):
    tok = flag_ref.shape[1]
    flags = flag_ref[...] > 0
    t_pos = lax.broadcasted_iota(jnp.int32, (tok, tok), 0)
    s_pos = lax.broadcasted_iota(jnp.int32, (tok, tok), 1)
    seg_col = jnp.sum(jnp.where(flags & (s_pos <= t_pos), 1.0, 0), axis=1, keepdims=True)
    seg_col_ref[...] = seg_col
    seg_row_ref[...] = jnp.sum(jnp.where(s_pos == t_pos, seg_col, 0), axis=0, keepdims=True)
    positions = lax.broadcasted_iota(jnp.int32, (1, tok), 1).astype(F32)
    first_pos = jnp.min(jnp.where(flags, positions, tok), axis=1, keepdims=True)
    last_pos = jnp.max(jnp.where(flags, positions, -1), axis=1, keepdims=True)
    head_ref[...] = jnp.where(positions < first_pos, 1.0, 0)
    tail_ref[...] = jnp.where(positions >= last_pos, 1.0, 0)
    gate_ref[...] = jnp.broadcast_to(jnp.where(last_pos < 0, 1.0, 0), gate_ref.shape)


class Square:
    def __init__(self, me):
        x, y, core = place(me)
        across_x, across_y = (lax.rem(a + 1 + RING - 2 * lax.rem(a + core, 2), RING) for a in (x, y))
        self.core = core
        self.chips = [(x, y), (across_x, y), (x, across_y), (across_x, across_y)]

    def peer(self, k):
        return index_of(*self.chips[k], self.core)

    def kind(self, k):
        return owned_type(*self.chips[k])


def owned_type(x, y):
    return lax.rem(x, 2) + 2 * lax.rem(y, 2)


def lattice(x, y):
    return lax.rem(x // 2, 2), lax.rem(y // 2, 2)


def start_tokens(kind, x_ref, dy_ref, copy):
    @pl.when(kind == O_TYPE)
    def _():
        copy(dy_ref).start()

    @pl.when(kind != O_TYPE)
    def _():
        copy(x_ref).start()


def front_kernel(scale, dim, flag_ref, x_ref, dy_ref, wq_ref, wk_ref, wv_ref, wo_ref,
                 g_ref, z_ref, seg_col_ref, seg_row_ref, head_ref, tail_ref, gate_ref, tok_in, w_tile, rows_ref, total,
                 packed, held, formed, states,
                 tok_sem, w_sem, g_sem, z_send, z_recv, send_sem, recv_sem, back_send, back_recv):
    me = lax.axis_index('sp')
    n_dev, per_dev, low = formed.shape[1:4]
    width, tok = rows_ref.shape[1], rows_ref.shape[2]
    half = tok // 2
    n_piece = z_recv.shape[1]
    piece = tok // SLOTS
    n_group = SLOTS
    group = width // n_group
    tile_rows = w_tile.shape[1]

    @pl.loop(1, n_dev)
    def _(step):
        signal(lax.rem(me + step, n_dev))

    loads = [pltpu.make_async_copy(ref, tok_in.at[i], tok_sem.at[i]) for i, ref in enumerate((x_ref, dy_ref))]
    for load in loads:
        load.start()

    square = Square(me)

    cuts = (0, 2, 3, TYPES, SLOTS - 2, SLOTS)

    def token_copy(k, n):
        at = pl.ds(cuts[n] * piece, (cuts[n + 1] - cuts[n]) * piece)
        return lambda ref: remote(ref.at[at], z_ref.at[k - 1, at], z_send.at[k - 1, n], z_recv.at[k - 1, n], square.peer(k))

    def push_tokens(n):
        for k in range(1, TYPES):
            start_tokens(square.kind(k), x_ref, dy_ref, token_copy(k, n))

    form_masks(flag_ref, seg_col_ref, seg_row_ref, head_ref, tail_ref, gate_ref)
    pl.semaphore_wait(pltpu.get_barrier_semaphore(), n_dev - 1)
    push_tokens(0)

    weights = (wk_ref, wv_ref, wq_ref, wo_ref)
    kinds = (1, 2, 0, O_TYPE)

    def w_copy(i, n, slot):
        return pltpu.make_async_copy(weights[i].at[span(n * tile_rows, tile_rows)], w_tile.at[slot], w_sem.at[slot])

    def project(i, n, slot):
        rows_ref[kinds[i], span(n * tile_rows, tile_rows), :] = dot(w_tile[slot], tok_in[i // O_TYPE], ROWS).astype(BF16)

    def loaded(i):
        if i in (0, O_TYPE):
            loads[i // O_TYPE].wait()
        if i == 2:
            send_products(0)
        if i in (1, O_TYPE):
            push_tokens(1 + i // O_TYPE)

    head = head_ref[...] > 0.5
    tail = tail_ref[...] > 0.5

    def each(do):
        pl.loop(1, n_dev)(do)

    def out_copy(which, step):
        peer = lax.rem(me + step, n_dev)
        at = pl.ds(0, low + 1 - which)
        return remote(packed.at[which, peer, :, at], held.at[which, me, :, at], send_sem.at[which, step], recv_sem.at[which, step], peer)

    def back_copy(which, step):
        peer = lax.rem(me + step, n_dev)
        return remote(formed.at[which, peer], states.at[which, me], back_send.at[which, step], back_recv.at[which, step], peer)

    pair_lane = lax.broadcasted_iota(jnp.int32, (low, 2 * dim), 1) // dim

    def turn(pair):
        return pltpu.roll(pair, dim, 1)

    def send_products(which):
        left, right, mask = ((1, 2, tail), (0, O_TYPE, head))[which]

        @pl.loop(0, n_group)
        def _(grp):
            at = span(grp * group, group)
            full = dot(rows_ref[left, at, :], jnp.where(mask, rows_ref[right, at, :], jnp.zeros((group, tok), BF16)), ROWS)
            for sub in range(group // dim):
                spot = sub % 2
                block = full[sub * dim:(sub + 1) * dim, (sub // 2) * 2 * dim:(sub // 2 + 1) * 2 * dim]
                first, second = block[0:low], block[low:]
                if spot == 0:
                    second = turn(second)
                else:
                    first = turn(first)
                index = grp * (group // dim) + sub
                dev, own = index // per_dev, lax.rem(index, per_dev)
                packed[which, dev, own, 0:low, :] = jnp.where(pair_lane == 0, first, second)
                packed[which, dev, own, low:, :] = gate_ref[...]

        each(lambda step: out_copy(which, step).start())
        held[which, me] = packed[which, me]

    def form_states(which):
        each(lambda step: out_copy(which, step).wait_recv())

        def advance(step, state):
            block = step if which == 0 else n_dev - 1 - step
            formed[which, block] = state.astype(BF16)
            return held[0, block, :, low:low + 1, :] * state + held[which, block, :, 0:low, :]

        lax.fori_loop(0, n_dev, advance, jnp.zeros((per_dev, low, 2 * dim), F32), unroll=4)
        each(lambda step: back_copy(which, step).start())
        states[which, me] = formed[which, me]

    stream(TYPES, width // tile_rows, w_tile.shape[0], w_copy, project, loaded)
    send_products(1)

    seg_row = seg_row_ref[...]
    t_pos = lax.broadcasted_iota(jnp.int32, (half, tok), 0)
    s_pos = lax.broadcasted_iota(jnp.int32, (half, tok), 1)

    def pair(a, b):
        see_top = ((seg_col_ref[0:half, :] == seg_row) & (s_pos <= t_pos))[:, 0:half]
        see_low = (seg_col_ref[half:, :] == seg_row) & (s_pos <= t_pos + half)
        top = dot(a[:, 0:half], b[:, 0:half], OUTER)
        low = dot(a[:, half:], b, OUTER)
        return (jnp.where(see_top, top * scale, 0).astype(BF16), jnp.where(see_low, low * scale, 0).astype(BF16))

    def over_keys(at, rows_t, probs):
        total[at[0], at[1], 0:half] = dot(rows_t[:, 0:half], probs[0], ROWS)
        total[at[0], at[1], half:] = dot(rows_t, probs[1], ROWS)

    def over_queries(at, rows_t, probs):
        from_low = dot(rows_t[:, half:], probs[1], INNER)
        total[at[0], at[1], 0:half] = dot(rows_t[:, 0:half], probs[0], INNER) + from_low[:, 0:half]
        total[at[0], at[1], half:] = from_low[:, half:]

    def heads_of(grp):
        return [grp * (group // dim) + sub for sub in range(group // dim)]

    @pl.loop(0, n_group)
    def _(grp):
        @pl.when(grp == 1)
        def _():
            form_states(0)

        @pl.when(grp == n_group // 2 + 1)
        def _():
            form_states(1)
            push_tokens(TYPES)

        @pl.when(grp == O_TYPE)
        def _():
            push_tokens(O_TYPE)

        for index in heads_of(grp):
            rows = span(index * dim, dim)
            q, k, v, do = (rows_ref[kind, rows, :] for kind in range(TYPES))
            d_probs = pair(do, v)
            over_keys((0, rows), k, d_probs)
            over_queries((1, rows), q, d_probs)
            probs = pair(q, k)
            over_queries((2, rows), do, probs)
            over_keys((O_TYPE, rows), v, probs)

    def diagonal(which, grp):
        rows = []
        for sub in range(group // dim):
            index = grp * (group // dim) + sub
            pair = states[which, index // per_dev, lax.rem(index, per_dev)].astype(F32)
            spot = sub % 2
            block = jnp.concatenate([turn(pair), pair] if spot else [pair, turn(pair)], axis=0)
            block = jnp.where(jnp.concatenate([pair_lane, pair_lane], axis=0) == spot, block, 0)
            empty = jnp.zeros_like(block)
            rows.append(jnp.concatenate([empty, block] if sub // 2 else [block, empty], axis=1))
        return jnp.concatenate(rows, axis=0).astype(BF16)

    def finish(kind, at, mask, inter):
        rows_ref[kind, at, :] = (total[kind, at, :] + jnp.where(mask, inter * scale, 0)).astype(BF16)

    def row_put(kind, grp):
        at = span(grp * group, group)
        return pltpu.make_async_copy(rows_ref.at[kind, at], g_ref.at[kind, at], g_sem.at[kind, grp])

    each(lambda step: back_copy(0, step).wait_recv())

    @pl.loop(0, n_group)
    def _(grp):
        at = span(grp * group, group)
        st = diagonal(0, grp)
        d_q = dot(st, rows_ref[O_TYPE, at, :], INNER)
        out = dot(st, rows_ref[0, at, :], OUTER)
        finish(0, at, head, d_q)
        finish(O_TYPE, at, head, out)
        for kind in (0, O_TYPE):
            row_put(kind, grp).start()

    each(lambda step: back_copy(1, step).wait_recv())

    @pl.loop(0, n_group)
    def _(grp):
        at = span(grp * group, group)
        st = diagonal(1, grp)
        d_k = dot(st, rows_ref[2, at, :], INNER)
        d_v = dot(st, rows_ref[1, at, :], OUTER)
        finish(1, at, tail, d_k)
        finish(2, at, tail, d_v)
        for kind in (1, 2):
            row_put(kind, grp).start()

    for kind in range(TYPES):
        pl.loop(0, n_group)(lambda grp, kind=kind: row_put(kind, grp).wait())
    for which in range(2):
        each(lambda step, which=which: out_copy(which, step).wait_send())
        each(lambda step, which=which: back_copy(which, step).wait_send())
    for k in range(1, TYPES):
        for n in range(n_piece):
            token_copy(k, n)(x_ref).wait()


def front(flags, x_loc, dy_loc, weights, scale, n_dev, n_heads):
    tok, d_model = x_loc.shape
    width = weights[0].shape[0]
    dim = width // n_heads
    per_dev = n_heads // n_dev
    n_piece = TYPES + 1
    pack = (2, n_dev, per_dev, dim // 2 + 8, 2 * dim)
    back = (2, n_dev, per_dev, dim // 2, 2 * dim)
    return pl.pallas_call(
        functools.partial(front_kernel, scale, dim),
        name='front',
        out_shape=(jax.ShapeDtypeStruct((TYPES, width, tok), BF16), jax.ShapeDtypeStruct((TYPES - 1, tok, d_model), BF16)),
        in_specs=[VMEM] + [ANY] * 6,
        out_specs=(ANY, ANY),
        scratch_shapes=[
            pltpu.VMEM((tok, 1), F32), pltpu.VMEM((1, tok), F32), pltpu.VMEM((1, tok), F32), pltpu.VMEM((1, tok), F32), pltpu.VMEM((8, 2 * dim), F32),
            pltpu.VMEM((2, tok, d_model), BF16), pltpu.VMEM((4, width // RING, d_model), BF16),
            pltpu.VMEM((TYPES, width, tok), BF16), pltpu.VMEM((TYPES, width, tok), F32),
            pltpu.VMEM(pack, F32), pltpu.VMEM(pack, F32), pltpu.VMEM(back, BF16), pltpu.VMEM(back, BF16),
            DMA((2,)), DMA((4,)), DMA((TYPES, SLOTS)), DMA((TYPES - 1, n_piece)), DMA((TYPES - 1, n_piece)),
            DMA((2, n_dev)), DMA((2, n_dev)), DMA((2, n_dev)), DMA((2, n_dev))],
        compiler_params=pltpu.CompilerParams(collective_id=0, has_side_effects=True, vmem_limit_bytes=56 * MIB),
    )(flags[None, :], x_loc, dy_loc, *weights)


def row_products(g_ref, w_refs, y_ref, dx_ref, rows_in, rows_t, w_tile, total, done, g_sem, w_sem, put_sem):
    width = rows_in.shape[0]
    cols = w_tile.shape[2]
    n_tile = total.shape[1] // cols
    step = width // SLOTS
    order = (O_TYPE, 0, 1, 2)

    def g_copy(i):
        return pltpu.make_async_copy(g_ref.at[order[i]], rows_in, g_sem)

    def w_copy(i, n, slot):
        return pltpu.make_async_copy(w_refs[order[i]].at[:, span(n * cols, cols)], w_tile.at[slot], w_sem.at[slot])

    puts = [pltpu.make_async_copy(done, ref, put_sem) for ref in (y_ref, dx_ref)]

    def turned(i):
        if i == 1:
            puts[0].start()
        if i == O_TYPE:
            puts[0].wait()
        g_copy(i).wait()

        @pl.loop(0, width // step)
        def _(b):
            at = span(b * step, step)
            rows_t[:, at] = jnp.transpose(rows_in[at, :])

        if i < O_TYPE:
            g_copy(i + 1).start()

    def use(i, n, slot):
        at = span(n * cols, cols)
        prod = dot(rows_t[...], w_tile[slot], INNER)
        if i == 0:
            done[:, at] = prod.astype(BF16)
        elif i == 1:
            total[:, at] = prod
        elif i < O_TYPE:
            total[:, at] = total[:, at] + prod
        else:
            done[:, at] = (total[:, at] + prod).astype(BF16)

    g_copy(0).start()
    stream(TYPES, n_tile, w_tile.shape[0], w_copy, use, turned)
    puts[1].start()
    return puts[1]


FLIPS = ((1, 1), (1, 0), (0, 1), (0, 0))


def reduce_kernel(g_ref, z_ref, x_ref, dy_ref, wq_ref, wk_ref, wv_ref, wo_ref, piece_ref, y_ref, dx_ref,
                  out_ref, zbuf, rows_in, side_out, side_in, first_out, first_in, second_out, second_in, kind_rows, rows_t, w_tile, sums, done,
                  z_sem, row_send, row_recv, side_send, side_recv, first_send, first_recv, second_send, second_recv, g_sem, w_sem, put_sem, out_sem):
    me = lax.axis_index('sp')
    x, y, core = place(me)
    square = Square(me)
    block = rows_in.shape[3]
    part = block // 2
    n_col, cols = second_out.shape[1], second_out.shape[3]
    sibling = index_of(x, y, 1 - core)
    across = (index_of(x + 2, y, core), index_of(x, y + 2, core))

    meet([sibling, *across] + [square.peer(k) for k in range(1, TYPES)])

    def own_copy(ref):
        return pltpu.make_async_copy(ref, zbuf.at[0], z_sem.at[0])

    z_copies = [pltpu.make_async_copy(z_ref.at[k - 1], zbuf.at[k], z_sem.at[k]) for k in range(1, TYPES)]

    def row_source(k, mine, t):
        px, py = lattice(*square.chips[k])
        half = core if mine else 1 - core
        index = half * RING + lax.rem(px + FLIPS[t][0], 2) + 2 * lax.rem(py + FLIPS[t][1], 2)
        return g_ref.at[square.kind(k), span(index * block, block)]

    def row_copy(k, mine, t):
        dst, recv = rows_in.at[k, mine, t], row_recv.at[k, mine, t]
        if k == 0:
            return pltpu.make_async_copy(row_source(k, mine, t), dst, recv)
        return remote(row_source(k, mine, t), dst, row_send.at[k - 1, mine, t], recv, square.peer(k))

    every_row = [(k, mine, t) for t in range(TYPES) for mine in range(2) for k in range(TYPES)]
    for where in every_row:
        row_copy(*where).start()
    start_tokens(square.kind(0), x_ref, dy_ref, own_copy)
    for copy in z_copies:
        copy.start()

    last_put = row_products(g_ref, (wq_ref, wk_ref, wv_ref, wo_ref), y_ref, dx_ref, kind_rows, rows_t, w_tile, sums, done, g_sem, w_sem, put_sem)

    own_copy(x_ref).wait()
    for copy in z_copies:
        copy.wait()

    def product(mine, t, ch):
        at = span(ch * cols, cols)
        total = dot(rows_in[0, mine, t], zbuf[0, :, at], INNER)
        for k in range(1, TYPES):
            total = total + dot(rows_in[k, mine, t], zbuf[k, :, at], INNER)
        return total

    def side_copy(t, ch):
        return remote(side_out.at[t % 2, ch], side_in.at[t, ch], side_send.at[t, ch], side_recv.at[t, ch], sibling)

    def first_copy(leg, q, ch):
        return remote(first_out.at[leg, q, ch], first_in.at[leg, q, ch], first_send.at[leg, q, ch], first_recv.at[leg, q, ch], across[leg])

    def second_copy(leg, ch):
        return remote(second_out.at[leg, ch], second_in.at[leg, ch], second_send.at[leg, ch], second_recv.at[leg, ch], across[1 - leg])

    def sibling_part(t, ch):
        if t >= 2:
            side_copy(t - 2, ch).wait_send()
        side_out[t % 2, ch] = product(0, t, ch)
        side_copy(t, ch).start()

    def own_part(t, ch):
        total = product(1, t, ch)
        side_copy(t, ch).wait_recv()
        total = total + side_in[t, ch]
        for leg in range(2):
            half = total[leg * part:(leg + 1) * part]
            step, other = FLIPS[t][leg], FLIPS[t][1 - leg]
            if step:
                first_out[leg, other, ch] = half
                first_copy(leg, other, ch).start()
                continue
            first_copy(leg, other, ch).wait_recv()
            half = half + first_in[leg, other, ch]
            if other:
                second_out[leg, ch] = half
                second_copy(leg, ch).start()
            else:
                second_copy(leg, ch).wait_recv()
                out_ref[leg * part:(leg + 1) * part, span(ch * cols, cols)] = half + second_in[leg, ch]
        if t == O_TYPE:
            out_copy(ch).start()

    def out_copy(ch):
        at = span(ch * cols, cols)
        return pltpu.make_async_copy(out_ref.at[:, at], piece_ref.at[:, at], out_sem.at[ch])

    for stage in ((0,), (1, 2), (O_TYPE,)):
        for t in stage:
            for mine in range(2):
                for k in range(TYPES):
                    copy = row_copy(k, mine, t)
                    if k:
                        copy.wait_recv()
                    else:
                        copy.wait()

        for work in (sibling_part, own_part):
            @pl.loop(0, n_col)
            def _(ch, stage=stage, work=work):
                for t in stage:
                    work(t, ch)

    last_put.wait()
    for where in every_row:
        if where[0]:
            row_copy(*where).wait_send()

    @pl.loop(0, n_col)
    def _(ch):
        out_copy(ch).wait()
        for t in range(2, TYPES):
            side_copy(t, ch).wait_send()
        for leg in range(2):
            for q in range(2):
                first_copy(leg, q, ch).wait_send()
            second_copy(leg, ch).wait_send()


def reduce_rows(g, z, x_loc, dy_loc, weights):
    width, tok = g.shape[1], g.shape[2]
    d_model = x_loc.shape[1]
    block = width // SLOTS
    n_col = RING
    cols = d_model // n_col
    tokens = jax.ShapeDtypeStruct((tok, d_model), BF16)
    halves = lambda *lead: pltpu.VMEM((*lead, n_col, block // 2, cols), F32)
    blocks = lambda lead: pltpu.VMEM((lead, n_col, block, cols), F32)
    return pl.pallas_call(
        reduce_kernel,
        name='reduce_rows',
        out_shape=(jax.ShapeDtypeStruct((block, d_model), F32), tokens, tokens),
        in_specs=[ANY] * 8,
        out_specs=(ANY,) * O_TYPE,
        scratch_shapes=[
            pltpu.VMEM((block, d_model), F32),
            pltpu.VMEM((TYPES, tok, d_model), BF16), pltpu.VMEM((TYPES, 2, TYPES, block, tok), BF16),
            blocks(2), blocks(TYPES), halves(2, 2), halves(2, 2), halves(2), halves(2),
            pltpu.VMEM((width, tok), BF16), pltpu.VMEM((tok, width), BF16), pltpu.VMEM((3, width, min(256, d_model // 4)), BF16),
            pltpu.VMEM((tok, d_model), F32), pltpu.VMEM((tok, d_model), BF16),
            DMA((TYPES,)), DMA((TYPES - 1, 2, TYPES)), DMA((TYPES, 2, TYPES)), DMA((TYPES, n_col)), DMA((TYPES, n_col)),
            DMA((2, 2, n_col)), DMA((2, 2, n_col)), DMA((2, n_col)), DMA((2, n_col)), DMA, DMA((3,)), DMA, DMA((n_col,))],
        compiler_params=pltpu.CompilerParams(collective_id=1, has_side_effects=True, vmem_limit_bytes=58 * MIB),
    )(g, z, x_loc, dy_loc, *weights)


def gather_kernel(piece_ref, near_ref, far_a_ref, far_b_ref, far_c_ref, send_sem, recv_sem, side_send, side_recv):
    me = lax.axis_index('sp')
    x, y, core = place(me)
    rows = piece_ref.shape[0]
    part = rows // 2
    quarter = part // 2

    def number(leg, i, j):
        sx, sy = (i, j) if leg == 0 else (j, i)
        px, py = lax.rem(x + sx, RING), lax.rem(y + sy, RING)
        lx, ly = lattice(px, py)
        return owned_type(px, py) * RING + lx + 2 * ly

    def spot(leg, i, j, half=None):
        lo, size = (0, part) if half is None else (half * quarter, quarter)
        return near_ref.at[pl.ds(pl.multiple_of(number(leg, i, j) * rows + leg * part + lo, quarter), size)]

    def far_spot(leg, i, j, half):
        if leg == 0:
            return far_a_ref.at[span(number(leg, i, j) * part + half * quarter, quarter)]
        return (far_b_ref, far_c_ref)[half].at[span(number(leg, i, j) * quarter, quarter)]

    def own(leg, half=None):
        lo, size = (0, part) if half is None else (half * quarter, quarter)
        return piece_ref.at[pl.ds(leg * part + lo, size)]

    def step_peer(leg, second, step):
        along_x = (leg == 0) != second
        return index_of(x + step, y, core) if along_x else index_of(x, y + step, core)

    started = []

    def push(leg, second, i, j, step, half):
        there = (i, (j - step) % RING) if second else ((i - step) % RING, j)
        src = own(leg, half) if i == 0 and j == 0 else spot(leg, i, j, half)
        copy = remote(src, spot(leg, i, j, half), send_sem.at[len(started)],
                      recv_sem.at[leg, there[0], there[1], half or 0], step_peer(leg, second, step))
        copy.start()
        started.append(copy)

    def landed(leg, i, j, half=None):
        here = spot(leg, i, j, half)
        remote(here, here, send_sem.at[0], recv_sem.at[leg, i, j, half or 0], me).wait_recv()

    side = []

    def to_sibling(leg, i, j, halves=(0, 1)):
        for half in halves:
            src = own(leg, half) if i == 0 and j == 0 else spot(leg, i, j, half)
            copy = remote(src, far_spot(leg, i, j, half), side_send.at[leg, i, j, half], side_recv.at[leg, i, j, half], index_of(x, y, 1 - core))
            copy.start()
            side.append(copy)

    meet([index_of(x, y, 1 - core)] + [index_of(*chip, core) for chip in chips_around(x, y)])

    def spread(leg, i):
        push(leg, True, i, 0, 1, None)
        push(leg, True, i, 0, 3, None)
        to_sibling(leg, i, 0)

    for leg in range(2):
        push(leg, False, 0, 0, 1, None)
        push(leg, False, 0, 0, 3, None)
    for leg in range(2):
        spread(leg, 0)
    near_ref[span(number(0, 0, 0) * rows, rows), :] = piece_ref[...]

    for leg in range(2):
        landed(leg, 3, 0)
        push(leg, False, 3, 0, 1, 0)
        spread(leg, 3)
        landed(leg, 1, 0)
        push(leg, False, 1, 0, 3, 1)
        spread(leg, 1)

    def second_near(leg, i):
        landed(leg, i, 3)
        push(leg, True, i, 3, 1, 0)
        to_sibling(leg, i, 3)
        landed(leg, i, 1)
        push(leg, True, i, 1, 3, 1)
        to_sibling(leg, i, 1)

    for leg in range(2):
        second_near(leg, 0)
    for leg in range(2):
        for half in range(2):
            landed(leg, 2, 0, half)
        spread(leg, 2)
    for i in (3, 1, 2):
        for leg in range(2):
            second_near(leg, i)
    for i in (0, 3, 1, 2):
        for half in range(2):
            for leg in range(2):
                landed(leg, i, 2, half)
                to_sibling(leg, i, 2, (half,))

    for copy in started + side:
        copy.wait_send()

    for leg in range(2):
        for i in range(RING):
            for j in range(RING):
                for half in range(2):
                    here = far_spot(leg, i, j, half)
                    remote(here, here, side_send.at[leg, i, j, half], side_recv.at[leg, i, j, half], me).wait_recv()


def gather_rows(piece, n_dev):
    rows, d_model = piece.shape
    half = n_dev * rows // CORES
    return pl.pallas_call(
        gather_kernel,
        name='gather_rows',
        out_shape=(pltpu.VMEM((half, d_model), F32), pltpu.VMEM((half // 2, d_model), F32), pltpu.VMEM((half // 4, d_model), F32),
                   jax.ShapeDtypeStruct((half // 4, d_model), F32)),
        in_specs=[VMEM],
        out_specs=(VMEM, VMEM, VMEM, ANY),
        scratch_shapes=[DMA((40,)), DMA((2, RING, RING, 2)), DMA((2, RING, RING, 2)), DMA((2, RING, RING, 2))],
        compiler_params=pltpu.CompilerParams(collective_id=2, has_side_effects=True, vmem_limit_bytes=STORE_LIMIT),
    )(piece)


def store_kernel(near_ref, far_a_ref, far_b_ref, far_c_ref, y_ref, dx_ref, dq_out, dk_out, dv_out, do_out, y_out, dx_out,
                 tile, rows_buf, put_sem, a_sem, b_sem, in_sem, out_sem, row_in, row_out):
    core = lax.rem(lax.axis_index('sp'), CORES)
    outs = (dq_out, dk_out, dv_out, do_out)
    rows = near_ref.shape[0] // TYPES
    n_slot, chunk = tile.shape[0], tile.shape[1]
    n = far_c_ref.shape[0] // chunk
    piece = 4 * chunk

    def far_out(i, lo, size):
        first = (1 - core) * rows + i % RING * piece + lo
        return outs[i // RING].at[pl.ds(pl.multiple_of(first, chunk), size)]

    puts = []
    for i in range(n * 2):
        kind, size = i // SLOTS, 2 * chunk
        lo = i % SLOTS * size
        puts.append(pltpu.make_async_copy(near_ref.at[pl.ds(i * size, size)], outs[kind].at[span(core * rows + lo, size)], put_sem.at[i]))
    for i in range(n):
        puts.append(pltpu.make_async_copy(far_a_ref.at[pl.ds(i * 2 * chunk, 2 * chunk)], far_out(i, 0, 2 * chunk), a_sem.at[i]))
        puts.append(pltpu.make_async_copy(far_b_ref.at[pl.ds(i * chunk, chunk)], far_out(i, 2 * chunk, chunk), b_sem.at[i]))

    def load(i):
        return pltpu.make_async_copy(far_c_ref.at[pl.ds(i * chunk, chunk)], tile.at[i % n_slot], in_sem.at[i % n_slot])

    def save(i):
        return pltpu.make_async_copy(tile.at[i % n_slot], far_out(i, piece - chunk, chunk), out_sem.at[i % n_slot])

    steps = []
    for src, dst in ((y_ref, y_out), (dx_ref, dx_out)):
        take, give = pltpu.make_async_copy(src, rows_buf, row_in), pltpu.make_async_copy(rows_buf, dst, row_out)
        steps += [(take.start,), (take.wait, give.start), (give.wait,)]

    ahead = n_slot // 2
    for i in range(ahead):
        load(i).start()
    for put in puts:
        put.start()
    for i in range(n):
        load(i).wait()
        save(i).start()
        if i % 2 == 0 and i // 2 < len(steps):
            for action in steps[i // 2]:
                action()
        if i + ahead < n:
            if i + ahead >= n_slot:
                save(i + ahead - n_slot).wait()
            load(i + ahead).start()
    for i in range(n - n_slot, n):
        save(i).wait()
    for put in puts:
        put.wait()


def store(near, far_a, far_b, far_c, y_rows, dx_rows):
    half, d_model = near.shape
    n = RING * RING
    chunk = far_c.shape[0] // n
    grad = jax.ShapeDtypeStruct((half * CORES // TYPES, d_model), F32)
    tokens = jax.ShapeDtypeStruct(y_rows.shape, BF16)
    return pl.pallas_call(
        store_kernel,
        name='store',
        out_shape=(grad,) * TYPES + (tokens,) * 2,
        in_specs=[VMEM, VMEM, VMEM] + [ANY] * 3,
        out_specs=(ANY,) * (TYPES + 2),
        scratch_shapes=[pltpu.VMEM((4, chunk, d_model), F32), pltpu.VMEM(y_rows.shape, BF16),
                        DMA((2 * n,)), DMA((n,)), DMA((n,)), DMA((4,)), DMA((4,)), DMA, DMA],
        compiler_params=pltpu.CompilerParams(vmem_limit_bytes=STORE_LIMIT),
    )(in_vmem(near), in_vmem(far_a), in_vmem(far_b), in_hbm(far_c), in_hbm(y_rows), in_hbm(dx_rows))


def solution(mesh):
    n_dev = mesh.shape['sp']
    assert n_dev == CORES * RING * RING

    def device_body(x_loc, flag_loc, w_q, w_k, w_v, w_o, dy_loc):
        tok_count, d_model = x_loc.shape
        n_heads, head_dim = w_q.shape[1], w_q.shape[2]
        width = n_heads * head_dim
        score_scale = 1.0 / (math.sqrt(head_dim) * tok_count)
        weights = [w.transpose(1, 2, 0).reshape(width, d_model) for w in (w_q, w_k, w_v)] + [w_o.reshape(width, d_model)]
        g, z = front(flag_loc, x_loc, dy_loc, weights, score_scale, n_dev, n_heads)
        piece, y_rows, dx_rows = reduce_rows(g, z, x_loc, dy_loc, weights)
        *grads, y_loc, dx_loc = store(*gather_rows(piece, n_dev), y_rows, dx_rows)
        dw_q, dw_k, dw_v, dw_o = (grad.reshape(n_heads, head_dim, d_model) for grad in grads)
        return y_loc, dx_loc, dw_q.transpose(2, 0, 1), dw_k.transpose(2, 0, 1), dw_v.transpose(2, 0, 1), dw_o

    row_spec = P(('dp', 'sp'), None)
    flag_spec = P(('dp', 'sp'))
    w_spec = P(None, None, None)
    dw_spec = P('dp', None, None)
    return jax.shard_map(device_body, mesh=mesh,
                         in_specs=(row_spec, flag_spec, w_spec, w_spec, w_spec, w_spec, row_spec),
                         out_specs=(row_spec, row_spec, dw_spec, dw_spec, dw_spec, dw_spec),
                         check_vma=False)
```

```python
import functools
import math
import jax
import jax.numpy as jnp
from jax import lax
from jax.experimental import pallas as pl
from jax.experimental.pallas import tpu as pltpu
from jax.sharding import PartitionSpec as P

MESH = pl.DeviceIdType.MESH
CORES = 2
RING = 4
SLOTS = CORES * RING
TYPES = 4
O_TYPE = TYPES - 1
MIB = 1024 * 1024
STORE_LIMIT = 5 * MIB
BF16 = jnp.bfloat16
F32 = jnp.float32
ROWS = ((1,), (1,))
INNER = ((1,), (0,))
OUTER = ((0,), (0,))
VMEM = pl.BlockSpec(memory_space=pltpu.VMEM)
ANY = pl.BlockSpec(memory_space=pltpu.HBM)
DMA = pltpu.SemaphoreType.DMA


def place(me):
    core = lax.rem(me, CORES)
    chip = me // CORES
    return lax.rem(chip, RING), chip // RING, core


def index_of(x, y, core):
    return (lax.rem(y, RING) * RING + lax.rem(x, RING)) * CORES + core


def remote(src, dst, send_sem, recv_sem, peer):
    return pltpu.make_async_remote_copy(src_ref=src, dst_ref=dst, send_sem=send_sem, recv_sem=recv_sem,
                                        device_id={'sp': peer}, device_id_type=MESH)


def signal(peer):
    pl.semaphore_signal(pltpu.get_barrier_semaphore(), inc=1, device_id={'sp': peer}, device_id_type=MESH)


def meet(peers):
    for peer in peers:
        signal(peer)
    pl.semaphore_wait(pltpu.get_barrier_semaphore(), len(peers))


def chips_around(x, y):
    return ((x + 1, y), (x + RING - 1, y), (x, y + 1), (x, y + RING - 1))


def dot(a, b, dims):
    return lax.dot_general(a, b, (dims, ((), ())), preferred_element_type=F32)


def in_vmem(value):
    return pltpu.with_memory_space_constraint(value, pltpu.VMEM)


def in_hbm(value):
    return pltpu.with_memory_space_constraint(value, pltpu.HBM)


def span(start, size):
    return pl.ds(pl.multiple_of(start, size), size)


def stream(n_outer, n_inner, depth, copy, use, before):
    ahead = depth - 1
    for n in range(ahead):
        copy(0, n, n).start()
    for i in range(n_outer):
        before(i)

        @pl.loop(0, n_inner)
        def _(n):
            at = i * n_inner + n
            slot, free = lax.rem(at, depth), lax.rem(at + ahead, depth)

            @pl.when(n + ahead < n_inner)
            def _():
                copy(i, n + ahead, free).start()

            if i + 1 < n_outer:
                @pl.when(n + ahead >= n_inner)
                def _():
                    copy(i + 1, n + ahead - n_inner, free).start()

            copy(i, n, slot).wait()
            use(i, n, slot)


def form_masks(flag_ref, seg_col_ref, seg_row_ref, head_ref, tail_ref, gate_ref):
    tok = flag_ref.shape[1]
    flags = flag_ref[...] > 0
    t_pos = lax.broadcasted_iota(jnp.int32, (tok, tok), 0)
    s_pos = lax.broadcasted_iota(jnp.int32, (tok, tok), 1)
    seg_col = jnp.sum(jnp.where(flags & (s_pos <= t_pos), 1.0, 0), axis=1, keepdims=True)
    seg_col_ref[...] = seg_col
    seg_row_ref[...] = jnp.sum(jnp.where(s_pos == t_pos, seg_col, 0), axis=0, keepdims=True)
    positions = lax.broadcasted_iota(jnp.int32, (1, tok), 1).astype(F32)
    first_pos = jnp.min(jnp.where(flags, positions, tok), axis=1, keepdims=True)
    last_pos = jnp.max(jnp.where(flags, positions, -1), axis=1, keepdims=True)
    head_ref[...] = jnp.where(positions < first_pos, 1.0, 0)
    tail_ref[...] = jnp.where(positions >= last_pos, 1.0, 0)
    gate_ref[...] = jnp.broadcast_to(jnp.where(last_pos < 0, 1.0, 0), gate_ref.shape)


class Square:
    def __init__(self, me):
        x, y, core = place(me)
        across_x, across_y = (lax.rem(a + 1 + RING - 2 * lax.rem(a + core, 2), RING) for a in (x, y))
        self.core = core
        self.chips = [(x, y), (across_x, y), (x, across_y), (across_x, across_y)]

    def peer(self, k):
        return index_of(*self.chips[k], self.core)

    def kind(self, k):
        return owned_type(*self.chips[k])


def owned_type(x, y):
    return lax.rem(x, 2) + 2 * lax.rem(y, 2)


def lattice(x, y):
    return lax.rem(x // 2, 2), lax.rem(y // 2, 2)


def start_tokens(kind, x_ref, dy_ref, copy):
    @pl.when(kind == O_TYPE)
    def _():
        copy(dy_ref).start()

    @pl.when(kind != O_TYPE)
    def _():
        copy(x_ref).start()


def front_kernel(scale, dim, flag_ref, x_ref, dy_ref, wq_ref, wk_ref, wv_ref, wo_ref,
                 g_ref, z_ref, seg_col_ref, seg_row_ref, head_ref, tail_ref, gate_ref, tok_in, w_tile, rows_ref, total,
                 packed, held, formed, states,
                 tok_sem, w_sem, g_sem, z_send, z_recv, send_sem, recv_sem, back_send, back_recv):
    me = lax.axis_index('sp')
    n_dev, per_dev, low = formed.shape[1:4]
    width, tok = rows_ref.shape[1], rows_ref.shape[2]
    half = tok // 2
    n_piece = z_recv.shape[1]
    piece = tok // SLOTS
    n_group = SLOTS
    group = width // n_group
    tile_rows = w_tile.shape[1]

    @pl.loop(1, n_dev)
    def _(step):
        signal(lax.rem(me + step, n_dev))

    loads = [pltpu.make_async_copy(ref, tok_in.at[i], tok_sem.at[i]) for i, ref in enumerate((x_ref, dy_ref))]
    for load in loads:
        load.start()

    square = Square(me)

    cuts = (0, 2, 3, TYPES, SLOTS - 2, SLOTS)

    def token_copy(k, n):
        at = pl.ds(cuts[n] * piece, (cuts[n + 1] - cuts[n]) * piece)
        return lambda ref: remote(ref.at[at], z_ref.at[k - 1, at], z_send.at[k - 1, n], z_recv.at[k - 1, n], square.peer(k))

    def push_tokens(n):
        for k in range(1, TYPES):
            start_tokens(square.kind(k), tok_in.at[0], tok_in.at[1], token_copy(k, n))

    form_masks(flag_ref, seg_col_ref, seg_row_ref, head_ref, tail_ref, gate_ref)
    for load in loads:
        load.wait()
    pl.semaphore_wait(pltpu.get_barrier_semaphore(), n_dev - 1)
    push_tokens(0)

    weights = (wk_ref, wv_ref, wq_ref, wo_ref)
    kinds = (1, 2, 0, O_TYPE)

    def w_copy(i, n, slot):
        return pltpu.make_async_copy(weights[i].at[span(n * tile_rows, tile_rows)], w_tile.at[slot], w_sem.at[slot])

    def project(i, n, slot):
        rows_ref[kinds[i], span(n * tile_rows, tile_rows), :] = dot(w_tile[slot], tok_in[i // O_TYPE], ROWS).astype(BF16)

    def loaded(i):
        if i == 2:
            send_products(0)
        if i in (1, O_TYPE):
            push_tokens(1 + i // O_TYPE)

    head = head_ref[...] > 0.5
    tail = tail_ref[...] > 0.5

    def each(do):
        pl.loop(1, n_dev)(do)

    def out_copy(which, step):
        peer = lax.rem(me + step, n_dev)
        at = pl.ds(0, low + 1 - which)
        return remote(packed.at[which, peer, :, at], held.at[which, me, :, at], send_sem.at[which, step], recv_sem.at[which, step], peer)

    def back_copy(which, step):
        peer = lax.rem(me + step, n_dev)
        return remote(formed.at[which, peer], states.at[which, me], back_send.at[which, step], back_recv.at[which, step], peer)

    pair_lane = lax.broadcasted_iota(jnp.int32, (low, 2 * dim), 1) // dim

    def turn(pair):
        return pltpu.roll(pair, dim, 1)

    def send_products(which):
        left, right, mask = ((1, 2, tail), (0, O_TYPE, head))[which]

        @pl.loop(0, n_group)
        def _(grp):
            at = span(grp * group, group)
            full = dot(rows_ref[left, at, :], jnp.where(mask, rows_ref[right, at, :], jnp.zeros((group, tok), BF16)), ROWS)
            for sub in range(group // dim):
                spot = sub % 2
                block = full[sub * dim:(sub + 1) * dim, (sub // 2) * 2 * dim:(sub // 2 + 1) * 2 * dim]
                first, second = block[0:low], block[low:]
                if spot == 0:
                    second = turn(second)
                else:
                    first = turn(first)
                index = grp * (group // dim) + sub
                dev, own = index // per_dev, lax.rem(index, per_dev)
                packed[which, dev, own, 0:low, :] = jnp.where(pair_lane == 0, first, second)
                packed[which, dev, own, low:, :] = gate_ref[...]

        each(lambda step: out_copy(which, step).start())
        held[which, me] = packed[which, me]

    def form_states(which):
        each(lambda step: out_copy(which, step).wait_recv())

        def advance(step, state):
            block = step if which == 0 else n_dev - 1 - step
            formed[which, block] = state.astype(BF16)
            return held[0, block, :, low:low + 1, :] * state + held[which, block, :, 0:low, :]

        lax.fori_loop(0, n_dev, advance, jnp.zeros((per_dev, low, 2 * dim), F32), unroll=4)
        each(lambda step: back_copy(which, step).start())
        states[which, me] = formed[which, me]

    stream(TYPES, width // tile_rows, w_tile.shape[0], w_copy, project, loaded)
    send_products(1)

    seg_row = seg_row_ref[...]
    t_pos = lax.broadcasted_iota(jnp.int32, (half, tok), 0)
    s_pos = lax.broadcasted_iota(jnp.int32, (half, tok), 1)

    def pair(a, b):
        see_top = ((seg_col_ref[0:half, :] == seg_row) & (s_pos <= t_pos))[:, 0:half]
        see_low = (seg_col_ref[half:, :] == seg_row) & (s_pos <= t_pos + half)
        top = dot(a[:, 0:half], b[:, 0:half], OUTER)
        low = dot(a[:, half:], b, OUTER)
        return (jnp.where(see_top, top * scale, 0).astype(BF16), jnp.where(see_low, low * scale, 0).astype(BF16))

    def over_keys(at, rows_t, probs):
        total[at[0], at[1], 0:half] = dot(rows_t[:, 0:half], probs[0], ROWS)
        total[at[0], at[1], half:] = dot(rows_t, probs[1], ROWS)

    def over_queries(at, rows_t, probs):
        from_low = dot(rows_t[:, half:], probs[1], INNER)
        total[at[0], at[1], 0:half] = dot(rows_t[:, 0:half], probs[0], INNER) + from_low[:, 0:half]
        total[at[0], at[1], half:] = from_low[:, half:]

    def heads_of(grp):
        return [grp * (group // dim) + sub for sub in range(group // dim)]

    @pl.loop(0, n_group)
    def _(grp):
        @pl.when(grp == 1)
        def _():
            form_states(0)

        @pl.when(grp == n_group // 2 + 1)
        def _():
            form_states(1)
            push_tokens(TYPES)

        @pl.when(grp == O_TYPE)
        def _():
            push_tokens(O_TYPE)

        for index in heads_of(grp):
            rows = span(index * dim, dim)
            q, k, v, do = (rows_ref[kind, rows, :] for kind in range(TYPES))
            d_probs = pair(do, v)
            over_keys((0, rows), k, d_probs)
            over_queries((1, rows), q, d_probs)
            probs = pair(q, k)
            over_queries((2, rows), do, probs)
            over_keys((O_TYPE, rows), v, probs)

    def diagonal(which, grp):
        rows = []
        for sub in range(group // dim):
            index = grp * (group // dim) + sub
            pair = states[which, index // per_dev, lax.rem(index, per_dev)].astype(F32)
            spot = sub % 2
            block = jnp.concatenate([turn(pair), pair] if spot else [pair, turn(pair)], axis=0)
            block = jnp.where(jnp.concatenate([pair_lane, pair_lane], axis=0) == spot, block, 0)
            empty = jnp.zeros_like(block)
            rows.append(jnp.concatenate([empty, block] if sub // 2 else [block, empty], axis=1))
        return jnp.concatenate(rows, axis=0).astype(BF16)

    def finish(kind, at, mask, inter):
        rows_ref[kind, at, :] = (total[kind, at, :] + jnp.where(mask, inter * scale, 0)).astype(BF16)

    def row_put(kind, grp):
        at = span(grp * group, group)
        return pltpu.make_async_copy(rows_ref.at[kind, at], g_ref.at[kind, at], g_sem.at[kind, grp])

    each(lambda step: back_copy(0, step).wait_recv())

    @pl.loop(0, n_group)
    def _(grp):
        at = span(grp * group, group)
        st = diagonal(0, grp)
        d_q = dot(st, rows_ref[O_TYPE, at, :], INNER)
        out = dot(st, rows_ref[0, at, :], OUTER)
        finish(0, at, head, d_q)
        finish(O_TYPE, at, head, out)
        for kind in (0, O_TYPE):
            row_put(kind, grp).start()

    each(lambda step: back_copy(1, step).wait_recv())

    @pl.loop(0, n_group)
    def _(grp):
        at = span(grp * group, group)
        st = diagonal(1, grp)
        d_k = dot(st, rows_ref[2, at, :], INNER)
        d_v = dot(st, rows_ref[1, at, :], OUTER)
        finish(1, at, tail, d_k)
        finish(2, at, tail, d_v)
        for kind in (1, 2):
            row_put(kind, grp).start()

    for kind in range(TYPES):
        pl.loop(0, n_group)(lambda grp, kind=kind: row_put(kind, grp).wait())
    for which in range(2):
        each(lambda step, which=which: out_copy(which, step).wait_send())
        each(lambda step, which=which: back_copy(which, step).wait_send())
    for k in range(1, TYPES):
        for n in range(n_piece):
            token_copy(k, n)(tok_in.at[0]).wait()


def front(flags, x_loc, dy_loc, weights, scale, n_dev, n_heads):
    tok, d_model = x_loc.shape
    width = weights[0].shape[0]
    dim = width // n_heads
    per_dev = n_heads // n_dev
    n_piece = TYPES + 1
    pack = (2, n_dev, per_dev, dim // 2 + 8, 2 * dim)
    back = (2, n_dev, per_dev, dim // 2, 2 * dim)
    return pl.pallas_call(
        functools.partial(front_kernel, scale, dim),
        name='front',
        out_shape=(jax.ShapeDtypeStruct((TYPES, width, tok), BF16), jax.ShapeDtypeStruct((TYPES - 1, tok, d_model), BF16)),
        in_specs=[VMEM] + [ANY] * 6,
        out_specs=(ANY, ANY),
        scratch_shapes=[
            pltpu.VMEM((tok, 1), F32), pltpu.VMEM((1, tok), F32), pltpu.VMEM((1, tok), F32), pltpu.VMEM((1, tok), F32), pltpu.VMEM((8, 2 * dim), F32),
            pltpu.VMEM((2, tok, d_model), BF16), pltpu.VMEM((4, width // RING, d_model), BF16),
            pltpu.VMEM((TYPES, width, tok), BF16), pltpu.VMEM((TYPES, width, tok), F32),
            pltpu.VMEM(pack, F32), pltpu.VMEM(pack, F32), pltpu.VMEM(back, BF16), pltpu.VMEM(back, BF16),
            DMA((2,)), DMA((4,)), DMA((TYPES, SLOTS)), DMA((TYPES - 1, n_piece)), DMA((TYPES - 1, n_piece)),
            DMA((2, n_dev)), DMA((2, n_dev)), DMA((2, n_dev)), DMA((2, n_dev))],
        compiler_params=pltpu.CompilerParams(collective_id=0, has_side_effects=True, vmem_limit_bytes=56 * MIB),
    )(flags[None, :], x_loc, dy_loc, *weights)


def row_products(g_ref, w_refs, y_ref, dx_ref, rows_in, rows_t, w_tile, total, done, g_sem, w_sem, put_sem):
    width = rows_in.shape[0]
    cols = w_tile.shape[2]
    n_tile = total.shape[1] // cols
    step = width // SLOTS
    order = (O_TYPE, 0, 1, 2)

    def g_copy(i):
        return pltpu.make_async_copy(g_ref.at[order[i]], rows_in, g_sem)

    def w_copy(i, n, slot):
        return pltpu.make_async_copy(w_refs[order[i]].at[:, span(n * cols, cols)], w_tile.at[slot], w_sem.at[slot])

    puts = [pltpu.make_async_copy(done, ref, put_sem) for ref in (y_ref, dx_ref)]

    def turned(i):
        if i == 1:
            puts[0].start()
        if i == O_TYPE:
            puts[0].wait()
        g_copy(i).wait()

        @pl.loop(0, width // step)
        def _(b):
            at = span(b * step, step)
            rows_t[:, at] = jnp.transpose(rows_in[at, :])

        if i < O_TYPE:
            g_copy(i + 1).start()

    def use(i, n, slot):
        at = span(n * cols, cols)
        prod = dot(rows_t[...], w_tile[slot], INNER)
        if i == 0:
            done[:, at] = prod.astype(BF16)
        elif i == 1:
            total[:, at] = prod
        elif i < O_TYPE:
            total[:, at] = total[:, at] + prod
        else:
            done[:, at] = (total[:, at] + prod).astype(BF16)

    g_copy(0).start()
    stream(TYPES, n_tile, w_tile.shape[0], w_copy, use, turned)
    puts[1].start()
    return puts[1]


FLIPS = ((1, 1), (1, 0), (0, 1), (0, 0))


def reduce_kernel(g_ref, z_ref, x_ref, dy_ref, wq_ref, wk_ref, wv_ref, wo_ref, piece_ref, y_ref, dx_ref,
                  out_ref, zbuf, rows_in, side_out, side_in, first_out, first_in, second_out, second_in, kind_rows, rows_t, w_tile, sums, done,
                  z_sem, row_send, row_recv, side_send, side_recv, first_send, first_recv, second_send, second_recv, g_sem, w_sem, put_sem, out_sem):
    me = lax.axis_index('sp')
    x, y, core = place(me)
    square = Square(me)
    block = rows_in.shape[3]
    part = block // 2
    n_col, cols = second_out.shape[1], second_out.shape[3]
    sibling = index_of(x, y, 1 - core)
    across = (index_of(x + 2, y, core), index_of(x, y + 2, core))

    meet([sibling, *across] + [square.peer(k) for k in range(1, TYPES)])

    def own_copy(ref):
        return pltpu.make_async_copy(ref, zbuf.at[0], z_sem.at[0])

    z_copies = [pltpu.make_async_copy(z_ref.at[k - 1], zbuf.at[k], z_sem.at[k]) for k in range(1, TYPES)]

    def row_source(k, mine, t):
        px, py = lattice(*square.chips[k])
        half = core if mine else 1 - core
        index = half * RING + lax.rem(px + FLIPS[t][0], 2) + 2 * lax.rem(py + FLIPS[t][1], 2)
        return g_ref.at[square.kind(k), span(index * block, block)]

    def row_copy(k, mine, t):
        dst, recv = rows_in.at[k, mine, t], row_recv.at[k, mine, t]
        if k == 0:
            return pltpu.make_async_copy(row_source(k, mine, t), dst, recv)
        return remote(row_source(k, mine, t), dst, row_send.at[k - 1, mine, t], recv, square.peer(k))

    every_row = [(k, mine, t) for t in range(TYPES) for mine in range(2) for k in range(TYPES)]
    for where in every_row:
        row_copy(*where).start()
    start_tokens(square.kind(0), x_ref, dy_ref, own_copy)
    for copy in z_copies:
        copy.start()

    last_put = row_products(g_ref, (wq_ref, wk_ref, wv_ref, wo_ref), y_ref, dx_ref, kind_rows, rows_t, w_tile, sums, done, g_sem, w_sem, put_sem)

    own_copy(x_ref).wait()
    for copy in z_copies:
        copy.wait()

    def product(mine, t, ch):
        at = span(ch * cols, cols)
        total = dot(rows_in[0, mine, t], zbuf[0, :, at], INNER)
        for k in range(1, TYPES):
            total = total + dot(rows_in[k, mine, t], zbuf[k, :, at], INNER)
        return total

    def side_copy(t, ch):
        return remote(side_out.at[t % 2, ch], side_in.at[t, ch], side_send.at[t, ch], side_recv.at[t, ch], sibling)

    def first_copy(leg, q, ch):
        return remote(first_out.at[leg, q, ch], first_in.at[leg, q, ch], first_send.at[leg, q, ch], first_recv.at[leg, q, ch], across[leg])

    def second_copy(leg, ch):
        return remote(second_out.at[leg, ch], second_in.at[leg, ch], second_send.at[leg, ch], second_recv.at[leg, ch], across[1 - leg])

    def sibling_part(t, ch):
        if t >= 2:
            side_copy(t - 2, ch).wait_send()
        side_out[t % 2, ch] = product(0, t, ch)
        side_copy(t, ch).start()

    def own_part(t, ch):
        total = product(1, t, ch)
        side_copy(t, ch).wait_recv()
        total = total + side_in[t, ch]
        for leg in range(2):
            half = total[leg * part:(leg + 1) * part]
            step, other = FLIPS[t][leg], FLIPS[t][1 - leg]
            if step:
                first_out[leg, other, ch] = half
                first_copy(leg, other, ch).start()
                continue
            first_copy(leg, other, ch).wait_recv()
            half = half + first_in[leg, other, ch]
            if other:
                second_out[leg, ch] = half
                second_copy(leg, ch).start()
            else:
                second_copy(leg, ch).wait_recv()
                out_ref[leg * part:(leg + 1) * part, span(ch * cols, cols)] = half + second_in[leg, ch]
        if t == O_TYPE:
            out_copy(ch).start()

    def out_copy(ch):
        at = span(ch * cols, cols)
        return pltpu.make_async_copy(out_ref.at[:, at], piece_ref.at[:, at], out_sem.at[ch])

    for stage in ((0,), (1, 2), (O_TYPE,)):
        for t in stage:
            for mine in range(2):
                for k in range(TYPES):
                    copy = row_copy(k, mine, t)
                    if k:
                        copy.wait_recv()
                    else:
                        copy.wait()

        for work in (sibling_part, own_part):
            @pl.loop(0, n_col)
            def _(ch, stage=stage, work=work):
                for t in stage:
                    work(t, ch)

    last_put.wait()
    for where in every_row:
        if where[0]:
            row_copy(*where).wait_send()

    @pl.loop(0, n_col)
    def _(ch):
        out_copy(ch).wait()
        for t in range(2, TYPES):
            side_copy(t, ch).wait_send()
        for leg in range(2):
            for q in range(2):
                first_copy(leg, q, ch).wait_send()
            second_copy(leg, ch).wait_send()


def reduce_rows(g, z, x_loc, dy_loc, weights):
    width, tok = g.shape[1], g.shape[2]
    d_model = x_loc.shape[1]
    block = width // SLOTS
    n_col = RING
    cols = d_model // n_col
    tokens = jax.ShapeDtypeStruct((tok, d_model), BF16)
    halves = lambda *lead: pltpu.VMEM((*lead, n_col, block // 2, cols), F32)
    blocks = lambda lead: pltpu.VMEM((lead, n_col, block, cols), F32)
    return pl.pallas_call(
        reduce_kernel,
        name='reduce_rows',
        out_shape=(jax.ShapeDtypeStruct((block, d_model), F32), tokens, tokens),
        in_specs=[ANY] * 8,
        out_specs=(ANY,) * O_TYPE,
        scratch_shapes=[
            pltpu.VMEM((block, d_model), F32),
            pltpu.VMEM((TYPES, tok, d_model), BF16), pltpu.VMEM((TYPES, 2, TYPES, block, tok), BF16),
            blocks(2), blocks(TYPES), halves(2, 2), halves(2, 2), halves(2), halves(2),
            pltpu.VMEM((width, tok), BF16), pltpu.VMEM((tok, width), BF16), pltpu.VMEM((3, width, min(256, d_model // 4)), BF16),
            pltpu.VMEM((tok, d_model), F32), pltpu.VMEM((tok, d_model), BF16),
            DMA((TYPES,)), DMA((TYPES - 1, 2, TYPES)), DMA((TYPES, 2, TYPES)), DMA((TYPES, n_col)), DMA((TYPES, n_col)),
            DMA((2, 2, n_col)), DMA((2, 2, n_col)), DMA((2, n_col)), DMA((2, n_col)), DMA, DMA((3,)), DMA, DMA((n_col,))],
        compiler_params=pltpu.CompilerParams(collective_id=1, has_side_effects=True, vmem_limit_bytes=58 * MIB),
    )(g, z, x_loc, dy_loc, *weights)


def gather_kernel(piece_ref, near_ref, far_a_ref, far_b_ref, far_c_ref, send_sem, recv_sem, side_send, side_recv):
    me = lax.axis_index('sp')
    x, y, core = place(me)
    rows = piece_ref.shape[0]
    part = rows // 2
    quarter = part // 2

    def number(leg, i, j):
        sx, sy = (i, j) if leg == 0 else (j, i)
        px, py = lax.rem(x + sx, RING), lax.rem(y + sy, RING)
        lx, ly = lattice(px, py)
        return owned_type(px, py) * RING + lx + 2 * ly

    def spot(leg, i, j, half=None):
        lo, size = (0, part) if half is None else (half * quarter, quarter)
        return near_ref.at[pl.ds(pl.multiple_of(number(leg, i, j) * rows + leg * part + lo, quarter), size)]

    def far_spot(leg, i, j, half):
        if leg == 0:
            return far_a_ref.at[span(number(leg, i, j) * part + half * quarter, quarter)]
        return (far_b_ref, far_c_ref)[half].at[span(number(leg, i, j) * quarter, quarter)]

    def own(leg, half=None):
        lo, size = (0, part) if half is None else (half * quarter, quarter)
        return piece_ref.at[pl.ds(leg * part + lo, size)]

    def step_peer(leg, second, step):
        along_x = (leg == 0) != second
        return index_of(x + step, y, core) if along_x else index_of(x, y + step, core)

    started = []

    def push(leg, second, i, j, step, half):
        there = (i, (j - step) % RING) if second else ((i - step) % RING, j)
        src = own(leg, half) if i == 0 and j == 0 else spot(leg, i, j, half)
        copy = remote(src, spot(leg, i, j, half), send_sem.at[len(started)],
                      recv_sem.at[leg, there[0], there[1], half or 0], step_peer(leg, second, step))
        copy.start()
        started.append(copy)

    def landed(leg, i, j, half=None):
        here = spot(leg, i, j, half)
        remote(here, here, send_sem.at[0], recv_sem.at[leg, i, j, half or 0], me).wait_recv()

    side = []

    def to_sibling(leg, i, j, halves=(0, 1)):
        for half in halves:
            src = own(leg, half) if i == 0 and j == 0 else spot(leg, i, j, half)
            copy = remote(src, far_spot(leg, i, j, half), side_send.at[leg, i, j, half], side_recv.at[leg, i, j, half], index_of(x, y, 1 - core))
            copy.start()
            side.append(copy)

    meet([index_of(x, y, 1 - core)] + [index_of(*chip, core) for chip in chips_around(x, y)])

    def spread(leg, i):
        push(leg, True, i, 0, 1, None)
        push(leg, True, i, 0, 3, None)
        to_sibling(leg, i, 0)

    for leg in range(2):
        push(leg, False, 0, 0, 1, None)
        push(leg, False, 0, 0, 3, None)
    for leg in range(2):
        spread(leg, 0)
    near_ref[span(number(0, 0, 0) * rows, rows), :] = piece_ref[...]

    for leg in range(2):
        landed(leg, 3, 0)
        push(leg, False, 3, 0, 1, 0)
        spread(leg, 3)
        landed(leg, 1, 0)
        push(leg, False, 1, 0, 3, 1)
        spread(leg, 1)

    def second_near(leg, i):
        landed(leg, i, 3)
        push(leg, True, i, 3, 1, 0)
        to_sibling(leg, i, 3)
        landed(leg, i, 1)
        push(leg, True, i, 1, 3, 1)
        to_sibling(leg, i, 1)

    for leg in range(2):
        second_near(leg, 0)
    for leg in range(2):
        for half in range(2):
            landed(leg, 2, 0, half)
        spread(leg, 2)
    for i in (3, 1, 2):
        for leg in range(2):
            second_near(leg, i)
    for i in (0, 3, 1, 2):
        for half in range(2):
            for leg in range(2):
                landed(leg, i, 2, half)
                to_sibling(leg, i, 2, (half,))

    for copy in started + side:
        copy.wait_send()

    for leg in range(2):
        for i in range(RING):
            for j in range(RING):
                for half in range(2):
                    here = far_spot(leg, i, j, half)
                    remote(here, here, side_send.at[leg, i, j, half], side_recv.at[leg, i, j, half], me).wait_recv()


def gather_rows(piece, n_dev):
    rows, d_model = piece.shape
    half = n_dev * rows // CORES
    return pl.pallas_call(
        gather_kernel,
        name='gather_rows',
        out_shape=(pltpu.VMEM((half, d_model), F32), pltpu.VMEM((half // 2, d_model), F32), pltpu.VMEM((half // 4, d_model), F32),
                   jax.ShapeDtypeStruct((half // 4, d_model), F32)),
        in_specs=[VMEM],
        out_specs=(VMEM, VMEM, VMEM, ANY),
        scratch_shapes=[DMA((40,)), DMA((2, RING, RING, 2)), DMA((2, RING, RING, 2)), DMA((2, RING, RING, 2))],
        compiler_params=pltpu.CompilerParams(collective_id=2, has_side_effects=True, vmem_limit_bytes=STORE_LIMIT),
    )(piece)


def store_kernel(near_ref, far_a_ref, far_b_ref, far_c_ref, y_ref, dx_ref, dq_out, dk_out, dv_out, do_out, y_out, dx_out,
                 tile, rows_buf, put_sem, a_sem, b_sem, in_sem, out_sem, row_in, row_out):
    core = lax.rem(lax.axis_index('sp'), CORES)
    outs = (dq_out, dk_out, dv_out, do_out)
    rows = near_ref.shape[0] // TYPES
    n_slot, chunk = tile.shape[0], tile.shape[1]
    n = far_c_ref.shape[0] // chunk
    piece = 4 * chunk

    def far_out(i, lo, size):
        first = (1 - core) * rows + i % RING * piece + lo
        return outs[i // RING].at[pl.ds(pl.multiple_of(first, chunk), size)]

    puts = []
    for i in range(n * 2):
        kind, size = i // SLOTS, 2 * chunk
        lo = i % SLOTS * size
        puts.append(pltpu.make_async_copy(near_ref.at[pl.ds(i * size, size)], outs[kind].at[span(core * rows + lo, size)], put_sem.at[i]))
    for i in range(n):
        puts.append(pltpu.make_async_copy(far_a_ref.at[pl.ds(i * 2 * chunk, 2 * chunk)], far_out(i, 0, 2 * chunk), a_sem.at[i]))
        puts.append(pltpu.make_async_copy(far_b_ref.at[pl.ds(i * chunk, chunk)], far_out(i, 2 * chunk, chunk), b_sem.at[i]))

    def load(i):
        return pltpu.make_async_copy(far_c_ref.at[pl.ds(i * chunk, chunk)], tile.at[i % n_slot], in_sem.at[i % n_slot])

    def save(i):
        return pltpu.make_async_copy(tile.at[i % n_slot], far_out(i, piece - chunk, chunk), out_sem.at[i % n_slot])

    steps = []
    for src, dst in ((y_ref, y_out), (dx_ref, dx_out)):
        take, give = pltpu.make_async_copy(src, rows_buf, row_in), pltpu.make_async_copy(rows_buf, dst, row_out)
        steps += [(take.start,), (take.wait, give.start), (give.wait,)]

    ahead = n_slot // 2
    for i in range(ahead):
        load(i).start()
    for put in puts:
        put.start()
    for i in range(n):
        load(i).wait()
        save(i).start()
        if i % 2 == 0 and i // 2 < len(steps):
            for action in steps[i // 2]:
                action()
        if i + ahead < n:
            if i + ahead >= n_slot:
                save(i + ahead - n_slot).wait()
            load(i + ahead).start()
    for i in range(n - n_slot, n):
        save(i).wait()
    for put in puts:
        put.wait()


def store(near, far_a, far_b, far_c, y_rows, dx_rows):
    half, d_model = near.shape
    n = RING * RING
    chunk = far_c.shape[0] // n
    grad = jax.ShapeDtypeStruct((half * CORES // TYPES, d_model), F32)
    tokens = jax.ShapeDtypeStruct(y_rows.shape, BF16)
    return pl.pallas_call(
        store_kernel,
        name='store',
        out_shape=(grad,) * TYPES + (tokens,) * 2,
        in_specs=[VMEM, VMEM, VMEM] + [ANY] * 3,
        out_specs=(ANY,) * (TYPES + 2),
        scratch_shapes=[pltpu.VMEM((4, chunk, d_model), F32), pltpu.VMEM(y_rows.shape, BF16),
                        DMA((2 * n,)), DMA((n,)), DMA((n,)), DMA((4,)), DMA((4,)), DMA, DMA],
        compiler_params=pltpu.CompilerParams(vmem_limit_bytes=STORE_LIMIT),
    )(in_vmem(near), in_vmem(far_a), in_vmem(far_b), in_hbm(far_c), in_hbm(y_rows), in_hbm(dx_rows))


def solution(mesh):
    n_dev = mesh.shape['sp']
    assert n_dev == CORES * RING * RING

    def device_body(x_loc, flag_loc, w_q, w_k, w_v, w_o, dy_loc):
        tok_count, d_model = x_loc.shape
        n_heads, head_dim = w_q.shape[1], w_q.shape[2]
        width = n_heads * head_dim
        score_scale = 1.0 / (math.sqrt(head_dim) * tok_count)
        weights = [w.transpose(1, 2, 0).reshape(width, d_model) for w in (w_q, w_k, w_v)] + [w_o.reshape(width, d_model)]
        g, z = front(flag_loc, x_loc, dy_loc, weights, score_scale, n_dev, n_heads)
        piece, y_rows, dx_rows = reduce_rows(g, z, x_loc, dy_loc, weights)
        *grads, y_loc, dx_loc = store(*gather_rows(piece, n_dev), y_rows, dx_rows)
        dw_q, dw_k, dw_v, dw_o = (grad.reshape(n_heads, head_dim, d_model) for grad in grads)
        return y_loc, dx_loc, dw_q.transpose(2, 0, 1), dw_k.transpose(2, 0, 1), dw_v.transpose(2, 0, 1), dw_o

    row_spec = P(('dp', 'sp'), None)
    flag_spec = P(('dp', 'sp'))
    w_spec = P(None, None, None)
    dw_spec = P('dp', None, None)
    return jax.shard_map(device_body, mesh=mesh,
                         in_specs=(row_spec, flag_spec, w_spec, w_spec, w_spec, w_spec, row_spec),
                         out_specs=(row_spec, row_spec, dw_spec, dw_spec, dw_spec, dw_spec),
                         check_vma=False)
```

```python
import functools
import math
import jax
import jax.numpy as jnp
from jax import lax
from jax.experimental import pallas as pl
from jax.experimental.pallas import tpu as pltpu
from jax.sharding import PartitionSpec as P

MESH = pl.DeviceIdType.MESH
CORES = 2
RING = 4
SLOTS = CORES * RING
TYPES = 4
O_TYPE = TYPES - 1
MIB = 1024 * 1024
STORE_LIMIT = 5 * MIB
BF16 = jnp.bfloat16
F32 = jnp.float32
ROWS = ((1,), (1,))
INNER = ((1,), (0,))
OUTER = ((0,), (0,))
VMEM = pl.BlockSpec(memory_space=pltpu.VMEM)
ANY = pl.BlockSpec(memory_space=pltpu.HBM)
DMA = pltpu.SemaphoreType.DMA


def place(me):
    core = lax.rem(me, CORES)
    chip = me // CORES
    return lax.rem(chip, RING), chip // RING, core


def index_of(x, y, core):
    return (lax.rem(y, RING) * RING + lax.rem(x, RING)) * CORES + core


def remote(src, dst, send_sem, recv_sem, peer):
    return pltpu.make_async_remote_copy(src_ref=src, dst_ref=dst, send_sem=send_sem, recv_sem=recv_sem,
                                        device_id={'sp': peer}, device_id_type=MESH)


def signal(peer):
    pl.semaphore_signal(pltpu.get_barrier_semaphore(), inc=1, device_id={'sp': peer}, device_id_type=MESH)


def meet(peers):
    for peer in peers:
        signal(peer)
    pl.semaphore_wait(pltpu.get_barrier_semaphore(), len(peers))


def chips_around(x, y):
    return ((x + 1, y), (x + RING - 1, y), (x, y + 1), (x, y + RING - 1))


def dot(a, b, dims):
    return lax.dot_general(a, b, (dims, ((), ())), preferred_element_type=F32)


def in_vmem(value):
    return pltpu.with_memory_space_constraint(value, pltpu.VMEM)


def in_hbm(value):
    return pltpu.with_memory_space_constraint(value, pltpu.HBM)


def span(start, size):
    return pl.ds(pl.multiple_of(start, size), size)


def stream(n_outer, n_inner, depth, copy, use, before):
    ahead = depth - 1
    for n in range(ahead):
        copy(0, n, n).start()
    for i in range(n_outer):
        before(i)

        @pl.loop(0, n_inner)
        def _(n):
            at = i * n_inner + n
            slot, free = lax.rem(at, depth), lax.rem(at + ahead, depth)

            @pl.when(n + ahead < n_inner)
            def _():
                copy(i, n + ahead, free).start()

            if i + 1 < n_outer:
                @pl.when(n + ahead >= n_inner)
                def _():
                    copy(i + 1, n + ahead - n_inner, free).start()

            copy(i, n, slot).wait()
            use(i, n, slot)


def form_masks(flag_ref, seg_col_ref, seg_row_ref, head_ref, tail_ref, gate_ref):
    tok = flag_ref.shape[1]
    flags = flag_ref[...] > 0
    t_pos = lax.broadcasted_iota(jnp.int32, (tok, tok), 0)
    s_pos = lax.broadcasted_iota(jnp.int32, (tok, tok), 1)
    seg_col = jnp.sum(jnp.where(flags & (s_pos <= t_pos), 1.0, 0), axis=1, keepdims=True)
    seg_col_ref[...] = seg_col
    seg_row_ref[...] = jnp.sum(jnp.where(s_pos == t_pos, seg_col, 0), axis=0, keepdims=True)
    positions = lax.broadcasted_iota(jnp.int32, (1, tok), 1).astype(F32)
    first_pos = jnp.min(jnp.where(flags, positions, tok), axis=1, keepdims=True)
    last_pos = jnp.max(jnp.where(flags, positions, -1), axis=1, keepdims=True)
    head_ref[...] = jnp.where(positions < first_pos, 1.0, 0)
    tail_ref[...] = jnp.where(positions >= last_pos, 1.0, 0)
    gate_ref[...] = jnp.broadcast_to(jnp.where(last_pos < 0, 1.0, 0), gate_ref.shape)


class Square:
    def __init__(self, me):
        x, y, core = place(me)
        across_x, across_y = (lax.rem(a + 1 + RING - 2 * lax.rem(a + core, 2), RING) for a in (x, y))
        self.core = core
        self.chips = [(x, y), (across_x, y), (x, across_y), (across_x, across_y)]

    def peer(self, k):
        return index_of(*self.chips[k], self.core)

    def kind(self, k):
        return owned_type(*self.chips[k])


def owned_type(x, y):
    return lax.rem(x, 2) + 2 * lax.rem(y, 2)


def lattice(x, y):
    return lax.rem(x // 2, 2), lax.rem(y // 2, 2)


def start_tokens(kind, x_ref, dy_ref, copy):
    @pl.when(kind == O_TYPE)
    def _():
        copy(dy_ref).start()

    @pl.when(kind != O_TYPE)
    def _():
        copy(x_ref).start()


def front_kernel(scale, dim, flag_ref, x_ref, dy_ref, wq_ref, wk_ref, wv_ref, wo_ref,
                 g_ref, z_ref, seg_col_ref, seg_row_ref, head_ref, tail_ref, gate_ref, tok_in, w_tile, rows_ref, total,
                 packed, held, formed, states,
                 tok_sem, w_sem, g_sem, z_send, z_recv, send_sem, recv_sem, back_send, back_recv):
    me = lax.axis_index('sp')
    n_dev, per_dev, low = formed.shape[1:4]
    width, tok = rows_ref.shape[1], rows_ref.shape[2]
    half = tok // 2
    n_piece = z_recv.shape[1]
    piece = tok // SLOTS
    n_group = SLOTS
    group = width // n_group
    tile_rows = w_tile.shape[1]

    @pl.loop(1, n_dev)
    def _(step):
        signal(lax.rem(me + step, n_dev))

    loads = [pltpu.make_async_copy(ref, tok_in.at[i], tok_sem.at[i]) for i, ref in enumerate((x_ref, dy_ref))]
    for load in loads:
        load.start()

    square = Square(me)

    cuts = (0, 2, 3, TYPES, SLOTS - 2, SLOTS)

    def token_copy(k, n):
        at = pl.ds(cuts[n] * piece, (cuts[n + 1] - cuts[n]) * piece)
        return lambda ref: remote(ref.at[at], z_ref.at[k - 1, at], z_send.at[k - 1, n], z_recv.at[k - 1, n], square.peer(k))

    def push_tokens(n):
        for k in range(1, TYPES):
            start_tokens(square.kind(k), x_ref, dy_ref, token_copy(k, n))

    form_masks(flag_ref, seg_col_ref, seg_row_ref, head_ref, tail_ref, gate_ref)
    pl.semaphore_wait(pltpu.get_barrier_semaphore(), n_dev - 1)
    push_tokens(0)

    weights = (wk_ref, wv_ref, wq_ref, wo_ref)
    kinds = (1, 2, 0, O_TYPE)

    def w_copy(i, n, slot):
        return pltpu.make_async_copy(weights[i].at[span(n * tile_rows, tile_rows)], w_tile.at[slot], w_sem.at[slot])

    def project(i, n, slot):
        rows_ref[kinds[i], span(n * tile_rows, tile_rows), :] = dot(w_tile[slot], tok_in[i // O_TYPE], ROWS).astype(BF16)

    def loaded(i):
        if i in (0, O_TYPE):
            loads[i // O_TYPE].wait()
        if i == 2:
            send_products(0)
        if i in (1, O_TYPE):
            push_tokens(1 + i // O_TYPE)

    head = head_ref[...] > 0.5
    tail = tail_ref[...] > 0.5

    def each(do):
        pl.loop(1, n_dev)(do)

    def out_copy(which, step):
        peer = lax.rem(me + step, n_dev)
        at = pl.ds(0, low + 1 - which)
        return remote(packed.at[which, peer, :, at], held.at[which, me, :, at], send_sem.at[which, step], recv_sem.at[which, step], peer)

    def back_copy(which, step):
        peer = lax.rem(me + step, n_dev)
        return remote(formed.at[which, peer], states.at[which, me], back_send.at[which, step], back_recv.at[which, step], peer)

    pair_lane = lax.broadcasted_iota(jnp.int32, (low, 2 * dim), 1) // dim

    def turn(pair):
        return pltpu.roll(pair, dim, 1)

    def send_products(which):
        left, right, mask = ((1, 2, tail), (0, O_TYPE, head))[which]

        @pl.loop(0, n_group)
        def _(grp):
            at = span(grp * group, group)
            full = dot(rows_ref[left, at, :], jnp.where(mask, rows_ref[right, at, :], jnp.zeros((group, tok), BF16)), ROWS)
            for sub in range(group // dim):
                spot = sub % 2
                block = full[sub * dim:(sub + 1) * dim, (sub // 2) * 2 * dim:(sub // 2 + 1) * 2 * dim]
                first, second = block[0:low], block[low:]
                if spot == 0:
                    second = turn(second)
                else:
                    first = turn(first)
                index = grp * (group // dim) + sub
                dev, own = index // per_dev, lax.rem(index, per_dev)
                packed[which, dev, own, 0:low, :] = jnp.where(pair_lane == 0, first, second)
                packed[which, dev, own, low:, :] = gate_ref[...]

        each(lambda step: out_copy(which, step).start())
        held[which, me] = packed[which, me]

    def form_states(which):
        each(lambda step: out_copy(which, step).wait_recv())

        def advance(step, state):
            block = step if which == 0 else n_dev - 1 - step
            formed[which, block] = state.astype(BF16)
            return held[0, block, :, low:low + 1, :] * state + held[which, block, :, 0:low, :]

        lax.fori_loop(0, n_dev, advance, jnp.zeros((per_dev, low, 2 * dim), F32), unroll=4)
        each(lambda step: back_copy(which, step).start())
        states[which, me] = formed[which, me]

    stream(TYPES, width // tile_rows, w_tile.shape[0], w_copy, project, loaded)
    send_products(1)

    seg_row = seg_row_ref[...]
    t_pos = lax.broadcasted_iota(jnp.int32, (half, tok), 0)
    s_pos = lax.broadcasted_iota(jnp.int32, (half, tok), 1)

    def pair(a, b):
        see_top = ((seg_col_ref[0:half, :] == seg_row) & (s_pos <= t_pos))[:, 0:half]
        see_low = (seg_col_ref[half:, :] == seg_row) & (s_pos <= t_pos + half)
        top = dot(a[:, 0:half], b[:, 0:half], OUTER)
        low = dot(a[:, half:], b, OUTER)
        return (jnp.where(see_top, top * scale, 0).astype(BF16), jnp.where(see_low, low * scale, 0).astype(BF16))

    def over_keys(at, rows_t, probs):
        total[at[0], at[1], 0:half] = dot(rows_t[:, 0:half], probs[0], ROWS)
        total[at[0], at[1], half:] = dot(rows_t, probs[1], ROWS)

    def over_queries(at, rows_t, probs):
        from_low = dot(rows_t[:, half:], probs[1], INNER)
        total[at[0], at[1], 0:half] = dot(rows_t[:, 0:half], probs[0], INNER) + from_low[:, 0:half]
        total[at[0], at[1], half:] = from_low[:, half:]

    def heads_of(grp):
        return [grp * (group // dim) + sub for sub in range(group // dim)]

    @pl.loop(0, n_group)
    def _(grp):
        @pl.when(grp == 1)
        def _():
            form_states(0)

        @pl.when(grp == n_group // 2 + 1)
        def _():
            form_states(1)
            push_tokens(TYPES)

        @pl.when(grp == O_TYPE)
        def _():
            push_tokens(O_TYPE)

        for index in heads_of(grp):
            rows = span(index * dim, dim)
            q, k, v, do = (rows_ref[kind, rows, :] for kind in range(TYPES))
            d_probs = pair(do, v)
            over_keys((0, rows), k, d_probs)
            over_queries((1, rows), q, d_probs)
            probs = pair(q, k)
            over_queries((2, rows), do, probs)
            over_keys((O_TYPE, rows), v, probs)

    def diagonal(which, grp):
        rows = []
        for sub in range(group // dim):
            index = grp * (group // dim) + sub
            pair = states[which, index // per_dev, lax.rem(index, per_dev)].astype(F32)
            spot = sub % 2
            block = jnp.concatenate([turn(pair), pair] if spot else [pair, turn(pair)], axis=0)
            block = jnp.where(jnp.concatenate([pair_lane, pair_lane], axis=0) == spot, block, 0)
            empty = jnp.zeros_like(block)
            rows.append(jnp.concatenate([empty, block] if sub // 2 else [block, empty], axis=1))
        return jnp.concatenate(rows, axis=0).astype(BF16)

    def finish(kind, at, mask, inter):
        rows_ref[kind, at, :] = (total[kind, at, :] + jnp.where(mask, inter * scale, 0)).astype(BF16)

    def row_put(kind, grp):
        at = span(grp * group, group)
        return pltpu.make_async_copy(rows_ref.at[kind, at], g_ref.at[kind, at], g_sem.at[kind, grp])

    each(lambda step: back_copy(0, step).wait_recv())

    @pl.loop(0, n_group)
    def _(grp):
        at = span(grp * group, group)
        st = diagonal(0, grp)
        d_q = dot(st, rows_ref[O_TYPE, at, :], INNER)
        out = dot(st, rows_ref[0, at, :], OUTER)
        finish(0, at, head, d_q)
        finish(O_TYPE, at, head, out)
        for kind in (0, O_TYPE):
            row_put(kind, grp).start()

    each(lambda step: back_copy(1, step).wait_recv())

    @pl.loop(0, n_group)
    def _(grp):
        at = span(grp * group, group)
        st = diagonal(1, grp)
        d_k = dot(st, rows_ref[2, at, :], INNER)
        d_v = dot(st, rows_ref[1, at, :], OUTER)
        finish(1, at, tail, d_k)
        finish(2, at, tail, d_v)
        for kind in (1, 2):
            row_put(kind, grp).start()

    for kind in range(TYPES):
        pl.loop(0, n_group)(lambda grp, kind=kind: row_put(kind, grp).wait())
    for which in range(2):
        each(lambda step, which=which: out_copy(which, step).wait_send())
        each(lambda step, which=which: back_copy(which, step).wait_send())
    for k in range(1, TYPES):
        for n in range(n_piece):
            token_copy(k, n)(x_ref).wait()


def front(flags, x_loc, dy_loc, weights, scale, n_dev, n_heads):
    tok, d_model = x_loc.shape
    width = weights[0].shape[0]
    dim = width // n_heads
    per_dev = n_heads // n_dev
    n_piece = TYPES + 1
    pack = (2, n_dev, per_dev, dim // 2 + 8, 2 * dim)
    back = (2, n_dev, per_dev, dim // 2, 2 * dim)
    return pl.pallas_call(
        functools.partial(front_kernel, scale, dim),
        name='front',
        out_shape=(jax.ShapeDtypeStruct((TYPES, width, tok), BF16), jax.ShapeDtypeStruct((TYPES - 1, tok, d_model), BF16)),
        in_specs=[VMEM] + [ANY] * 6,
        out_specs=(ANY, ANY),
        scratch_shapes=[
            pltpu.VMEM((tok, 1), F32), pltpu.VMEM((1, tok), F32), pltpu.VMEM((1, tok), F32), pltpu.VMEM((1, tok), F32), pltpu.VMEM((8, 2 * dim), F32),
            pltpu.VMEM((2, tok, d_model), BF16), pltpu.VMEM((4, width // RING, d_model), BF16),
            pltpu.VMEM((TYPES, width, tok), BF16), pltpu.VMEM((TYPES, width, tok), F32),
            pltpu.VMEM(pack, F32), pltpu.VMEM(pack, F32), pltpu.VMEM(back, BF16), pltpu.VMEM(back, BF16),
            DMA((2,)), DMA((4,)), DMA((TYPES, SLOTS)), DMA((TYPES - 1, n_piece)), DMA((TYPES - 1, n_piece)),
            DMA((2, n_dev)), DMA((2, n_dev)), DMA((2, n_dev)), DMA((2, n_dev))],
        compiler_params=pltpu.CompilerParams(collective_id=0, has_side_effects=True, vmem_limit_bytes=56 * MIB),
    )(flags[None, :], x_loc, dy_loc, *weights)


def row_products(g_ref, w_refs, y_ref, dx_ref, rows_in, rows_t, w_tile, total, done, g_sem, w_sem, put_sem):
    width = rows_in.shape[0]
    cols = w_tile.shape[2]
    n_tile = total.shape[1] // cols
    step = width // SLOTS
    order = (O_TYPE, 0, 1, 2)

    def g_copy(i):
        return pltpu.make_async_copy(g_ref.at[order[i]], rows_in, g_sem)

    def w_copy(i, n, slot):
        return pltpu.make_async_copy(w_refs[order[i]].at[:, span(n * cols, cols)], w_tile.at[slot], w_sem.at[slot])

    puts = [pltpu.make_async_copy(done, ref, put_sem) for ref in (y_ref, dx_ref)]

    def turned(i):
        if i == 1:
            puts[0].start()
        if i == O_TYPE:
            puts[0].wait()
        g_copy(i).wait()

        @pl.loop(0, width // step)
        def _(b):
            at = span(b * step, step)
            rows_t[:, at] = jnp.transpose(rows_in[at, :])

        if i < O_TYPE:
            g_copy(i + 1).start()

    def use(i, n, slot):
        at = span(n * cols, cols)
        prod = dot(rows_t[...], w_tile[slot], INNER)
        if i == 0:
            done[:, at] = prod.astype(BF16)
        elif i == 1:
            total[:, at] = prod
        elif i < O_TYPE:
            total[:, at] = total[:, at] + prod
        else:
            done[:, at] = (total[:, at] + prod).astype(BF16)

    g_copy(0).start()
    stream(TYPES, n_tile, w_tile.shape[0], w_copy, use, turned)
    puts[1].start()
    return puts[1]


FLIPS = ((1, 1), (1, 0), (0, 1), (0, 0))


def reduce_kernel(g_ref, z_ref, x_ref, dy_ref, wq_ref, wk_ref, wv_ref, wo_ref, piece_ref, y_ref, dx_ref,
                  out_ref, zbuf, rows_in, side_out, side_in, first_out, first_in, second_out, second_in, kind_rows, rows_t, w_tile, sums, done,
                  z_sem, row_send, row_recv, side_send, side_recv, first_send, first_recv, second_send, second_recv, g_sem, w_sem, put_sem, out_sem):
    me = lax.axis_index('sp')
    x, y, core = place(me)
    square = Square(me)
    block = rows_in.shape[3]
    part = block // 2
    n_col, cols = second_out.shape[1], second_out.shape[3]
    sibling = index_of(x, y, 1 - core)
    across = (index_of(x + 2, y, core), index_of(x, y + 2, core))

    meet([sibling, *across] + [square.peer(k) for k in range(1, TYPES)])

    def own_copy(ref):
        return pltpu.make_async_copy(ref, zbuf.at[0], z_sem.at[0])

    z_copies = [pltpu.make_async_copy(z_ref.at[k - 1], zbuf.at[k], z_sem.at[k]) for k in range(1, TYPES)]

    def row_source(k, mine, t):
        px, py = lattice(*square.chips[k])
        half = core if mine else 1 - core
        index = half * RING + lax.rem(px + FLIPS[t][0], 2) + 2 * lax.rem(py + FLIPS[t][1], 2)
        return g_ref.at[square.kind(k), span(index * block, block)]

    def row_copy(k, mine, t):
        dst, recv = rows_in.at[k, mine, t], row_recv.at[k, mine, t]
        if k == 0:
            return pltpu.make_async_copy(row_source(k, mine, t), dst, recv)
        return remote(row_source(k, mine, t), dst, row_send.at[k - 1, mine, t], recv, square.peer(k))

    every_row = [(k, mine, t) for t in range(TYPES) for mine in range(2) for k in range(TYPES)]
    for where in every_row:
        if where[-1] < O_TYPE:
            row_copy(*where).start()
    start_tokens(square.kind(0), x_ref, dy_ref, own_copy)
    for copy in z_copies:
        copy.start()

    last_put = row_products(g_ref, (wq_ref, wk_ref, wv_ref, wo_ref), y_ref, dx_ref, kind_rows, rows_t, w_tile, sums, done, g_sem, w_sem, put_sem)

    own_copy(x_ref).wait()
    for copy in z_copies:
        copy.wait()

    def product(mine, t, ch):
        at = span(ch * cols, cols)
        total = dot(rows_in[0, mine, t], zbuf[0, :, at], INNER)
        for k in range(1, TYPES):
            total = total + dot(rows_in[k, mine, t], zbuf[k, :, at], INNER)
        return total

    def side_copy(t, ch):
        return remote(side_out.at[t % 2, ch], side_in.at[t, ch], side_send.at[t, ch], side_recv.at[t, ch], sibling)

    def first_copy(leg, q, ch):
        return remote(first_out.at[leg, q, ch], first_in.at[leg, q, ch], first_send.at[leg, q, ch], first_recv.at[leg, q, ch], across[leg])

    def second_copy(leg, ch):
        return remote(second_out.at[leg, ch], second_in.at[leg, ch], second_send.at[leg, ch], second_recv.at[leg, ch], across[1 - leg])

    def sibling_part(t, ch):
        if t >= 2:
            side_copy(t - 2, ch).wait_send()
        side_out[t % 2, ch] = product(0, t, ch)
        side_copy(t, ch).start()

    def own_part(t, ch):
        total = product(1, t, ch)
        side_copy(t, ch).wait_recv()
        total = total + side_in[t, ch]
        for leg in range(2):
            half = total[leg * part:(leg + 1) * part]
            step, other = FLIPS[t][leg], FLIPS[t][1 - leg]
            if step:
                first_out[leg, other, ch] = half
                first_copy(leg, other, ch).start()
                continue
            first_copy(leg, other, ch).wait_recv()
            half = half + first_in[leg, other, ch]
            if other:
                second_out[leg, ch] = half
                second_copy(leg, ch).start()
            else:
                second_copy(leg, ch).wait_recv()
                out_ref[leg * part:(leg + 1) * part, span(ch * cols, cols)] = half + second_in[leg, ch]
        if t == O_TYPE:
            out_copy(ch).start()

    def out_copy(ch):
        at = span(ch * cols, cols)
        return pltpu.make_async_copy(out_ref.at[:, at], piece_ref.at[:, at], out_sem.at[ch])

    for stage in ((0,), (1, 2), (O_TYPE,)):
        if O_TYPE in stage:
            for where in every_row:
                if where[-1] == O_TYPE:
                    row_copy(*where).start()
        for t in stage:
            for mine in range(2):
                for k in range(TYPES):
                    copy = row_copy(k, mine, t)
                    if k:
                        copy.wait_recv()
                    else:
                        copy.wait()

        for work in (sibling_part, own_part):
            @pl.loop(0, n_col)
            def _(ch, stage=stage, work=work):
                for t in stage:
                    work(t, ch)

    last_put.wait()
    for where in every_row:
        if where[0]:
            row_copy(*where).wait_send()

    @pl.loop(0, n_col)
    def _(ch):
        out_copy(ch).wait()
        for t in range(2, TYPES):
            side_copy(t, ch).wait_send()
        for leg in range(2):
            for q in range(2):
                first_copy(leg, q, ch).wait_send()
            second_copy(leg, ch).wait_send()


def reduce_rows(g, z, x_loc, dy_loc, weights):
    width, tok = g.shape[1], g.shape[2]
    d_model = x_loc.shape[1]
    block = width // SLOTS
    n_col = RING
    cols = d_model // n_col
    tokens = jax.ShapeDtypeStruct((tok, d_model), BF16)
    halves = lambda *lead: pltpu.VMEM((*lead, n_col, block // 2, cols), F32)
    blocks = lambda lead: pltpu.VMEM((lead, n_col, block, cols), F32)
    return pl.pallas_call(
        reduce_kernel,
        name='reduce_rows',
        out_shape=(jax.ShapeDtypeStruct((block, d_model), F32), tokens, tokens),
        in_specs=[ANY] * 8,
        out_specs=(ANY,) * O_TYPE,
        scratch_shapes=[
            pltpu.VMEM((block, d_model), F32),
            pltpu.VMEM((TYPES, tok, d_model), BF16), pltpu.VMEM((TYPES, 2, TYPES, block, tok), BF16),
            blocks(2), blocks(TYPES), halves(2, 2), halves(2, 2), halves(2), halves(2),
            pltpu.VMEM((width, tok), BF16), pltpu.VMEM((tok, width), BF16), pltpu.VMEM((3, width, min(256, d_model // 4)), BF16),
            pltpu.VMEM((tok, d_model), F32), pltpu.VMEM((tok, d_model), BF16),
            DMA((TYPES,)), DMA((TYPES - 1, 2, TYPES)), DMA((TYPES, 2, TYPES)), DMA((TYPES, n_col)), DMA((TYPES, n_col)),
            DMA((2, 2, n_col)), DMA((2, 2, n_col)), DMA((2, n_col)), DMA((2, n_col)), DMA, DMA((3,)), DMA, DMA((n_col,))],
        compiler_params=pltpu.CompilerParams(collective_id=1, has_side_effects=True, vmem_limit_bytes=58 * MIB),
    )(g, z, x_loc, dy_loc, *weights)


def gather_kernel(piece_ref, near_ref, far_a_ref, far_b_ref, far_c_ref, send_sem, recv_sem, side_send, side_recv):
    me = lax.axis_index('sp')
    x, y, core = place(me)
    rows = piece_ref.shape[0]
    part = rows // 2
    quarter = part // 2

    def number(leg, i, j):
        sx, sy = (i, j) if leg == 0 else (j, i)
        px, py = lax.rem(x + sx, RING), lax.rem(y + sy, RING)
        lx, ly = lattice(px, py)
        return owned_type(px, py) * RING + lx + 2 * ly

    def spot(leg, i, j, half=None):
        lo, size = (0, part) if half is None else (half * quarter, quarter)
        return near_ref.at[pl.ds(pl.multiple_of(number(leg, i, j) * rows + leg * part + lo, quarter), size)]

    def far_spot(leg, i, j, half):
        if leg == 0:
            return far_a_ref.at[span(number(leg, i, j) * part + half * quarter, quarter)]
        return (far_b_ref, far_c_ref)[half].at[span(number(leg, i, j) * quarter, quarter)]

    def own(leg, half=None):
        lo, size = (0, part) if half is None else (half * quarter, quarter)
        return piece_ref.at[pl.ds(leg * part + lo, size)]

    def step_peer(leg, second, step):
        along_x = (leg == 0) != second
        return index_of(x + step, y, core) if along_x else index_of(x, y + step, core)

    started = []

    def push(leg, second, i, j, step, half):
        there = (i, (j - step) % RING) if second else ((i - step) % RING, j)
        src = own(leg, half) if i == 0 and j == 0 else spot(leg, i, j, half)
        copy = remote(src, spot(leg, i, j, half), send_sem.at[len(started)],
                      recv_sem.at[leg, there[0], there[1], half or 0], step_peer(leg, second, step))
        copy.start()
        started.append(copy)

    def landed(leg, i, j, half=None):
        here = spot(leg, i, j, half)
        remote(here, here, send_sem.at[0], recv_sem.at[leg, i, j, half or 0], me).wait_recv()

    side = []

    def to_sibling(leg, i, j, halves=(0, 1)):
        for half in halves:
            src = own(leg, half) if i == 0 and j == 0 else spot(leg, i, j, half)
            copy = remote(src, far_spot(leg, i, j, half), side_send.at[leg, i, j, half], side_recv.at[leg, i, j, half], index_of(x, y, 1 - core))
            copy.start()
            side.append(copy)

    meet([index_of(x, y, 1 - core)] + [index_of(*chip, core) for chip in chips_around(x, y)])

    def spread(leg, i):
        push(leg, True, i, 0, 1, None)
        push(leg, True, i, 0, 3, None)
        to_sibling(leg, i, 0)

    for leg in range(2):
        push(leg, False, 0, 0, 1, None)
        push(leg, False, 0, 0, 3, None)
    for leg in range(2):
        spread(leg, 0)
    near_ref[span(number(0, 0, 0) * rows, rows), :] = piece_ref[...]

    for leg in range(2):
        landed(leg, 3, 0)
        push(leg, False, 3, 0, 1, 0)
        spread(leg, 3)
        landed(leg, 1, 0)
        push(leg, False, 1, 0, 3, 1)
        spread(leg, 1)

    def second_near(leg, i):
        landed(leg, i, 3)
        push(leg, True, i, 3, 1, 0)
        to_sibling(leg, i, 3)
        landed(leg, i, 1)
        push(leg, True, i, 1, 3, 1)
        to_sibling(leg, i, 1)

    for leg in range(2):
        second_near(leg, 0)
    for leg in range(2):
        for half in range(2):
            landed(leg, 2, 0, half)
        spread(leg, 2)
    for i in (3, 1, 2):
        for leg in range(2):
            second_near(leg, i)
    for i in (0, 3, 1, 2):
        for half in range(2):
            for leg in range(2):
                landed(leg, i, 2, half)
                to_sibling(leg, i, 2, (half,))

    for copy in started + side:
        copy.wait_send()

    for leg in range(2):
        for i in range(RING):
            for j in range(RING):
                for half in range(2):
                    here = far_spot(leg, i, j, half)
                    remote(here, here, side_send.at[leg, i, j, half], side_recv.at[leg, i, j, half], me).wait_recv()


def gather_rows(piece, n_dev):
    rows, d_model = piece.shape
    half = n_dev * rows // CORES
    return pl.pallas_call(
        gather_kernel,
        name='gather_rows',
        out_shape=(pltpu.VMEM((half, d_model), F32), pltpu.VMEM((half // 2, d_model), F32), pltpu.VMEM((half // 4, d_model), F32),
                   jax.ShapeDtypeStruct((half // 4, d_model), F32)),
        in_specs=[VMEM],
        out_specs=(VMEM, VMEM, VMEM, ANY),
        scratch_shapes=[DMA((40,)), DMA((2, RING, RING, 2)), DMA((2, RING, RING, 2)), DMA((2, RING, RING, 2))],
        compiler_params=pltpu.CompilerParams(collective_id=2, has_side_effects=True, vmem_limit_bytes=STORE_LIMIT),
    )(piece)


def store_kernel(near_ref, far_a_ref, far_b_ref, far_c_ref, y_ref, dx_ref, dq_out, dk_out, dv_out, do_out, y_out, dx_out,
                 tile, rows_buf, put_sem, a_sem, b_sem, in_sem, out_sem, row_in, row_out):
    core = lax.rem(lax.axis_index('sp'), CORES)
    outs = (dq_out, dk_out, dv_out, do_out)
    rows = near_ref.shape[0] // TYPES
    n_slot, chunk = tile.shape[0], tile.shape[1]
    n = far_c_ref.shape[0] // chunk
    piece = 4 * chunk

    def far_out(i, lo, size):
        first = (1 - core) * rows + i % RING * piece + lo
        return outs[i // RING].at[pl.ds(pl.multiple_of(first, chunk), size)]

    puts = []
    for i in range(n * 2):
        kind, size = i // SLOTS, 2 * chunk
        lo = i % SLOTS * size
        puts.append(pltpu.make_async_copy(near_ref.at[pl.ds(i * size, size)], outs[kind].at[span(core * rows + lo, size)], put_sem.at[i]))
    for i in range(n):
        puts.append(pltpu.make_async_copy(far_a_ref.at[pl.ds(i * 2 * chunk, 2 * chunk)], far_out(i, 0, 2 * chunk), a_sem.at[i]))
        puts.append(pltpu.make_async_copy(far_b_ref.at[pl.ds(i * chunk, chunk)], far_out(i, 2 * chunk, chunk), b_sem.at[i]))

    def load(i):
        return pltpu.make_async_copy(far_c_ref.at[pl.ds(i * chunk, chunk)], tile.at[i % n_slot], in_sem.at[i % n_slot])

    def save(i):
        return pltpu.make_async_copy(tile.at[i % n_slot], far_out(i, piece - chunk, chunk), out_sem.at[i % n_slot])

    steps = []
    for src, dst in ((y_ref, y_out), (dx_ref, dx_out)):
        take, give = pltpu.make_async_copy(src, rows_buf, row_in), pltpu.make_async_copy(rows_buf, dst, row_out)
        steps += [(take.start,), (take.wait, give.start), (give.wait,)]

    ahead = n_slot // 2
    for i in range(ahead):
        load(i).start()
    for put in puts:
        put.start()
    for i in range(n):
        load(i).wait()
        save(i).start()
        if i % 2 == 0 and i // 2 < len(steps):
            for action in steps[i // 2]:
                action()
        if i + ahead < n:
            if i + ahead >= n_slot:
                save(i + ahead - n_slot).wait()
            load(i + ahead).start()
    for i in range(n - n_slot, n):
        save(i).wait()
    for put in puts:
        put.wait()


def store(near, far_a, far_b, far_c, y_rows, dx_rows):
    half, d_model = near.shape
    n = RING * RING
    chunk = far_c.shape[0] // n
    grad = jax.ShapeDtypeStruct((half * CORES // TYPES, d_model), F32)
    tokens = jax.ShapeDtypeStruct(y_rows.shape, BF16)
    return pl.pallas_call(
        store_kernel,
        name='store',
        out_shape=(grad,) * TYPES + (tokens,) * 2,
        in_specs=[VMEM, VMEM, VMEM] + [ANY] * 3,
        out_specs=(ANY,) * (TYPES + 2),
        scratch_shapes=[pltpu.VMEM((4, chunk, d_model), F32), pltpu.VMEM(y_rows.shape, BF16),
                        DMA((2 * n,)), DMA((n,)), DMA((n,)), DMA((4,)), DMA((4,)), DMA, DMA],
        compiler_params=pltpu.CompilerParams(vmem_limit_bytes=STORE_LIMIT),
    )(in_vmem(near), in_vmem(far_a), in_vmem(far_b), in_hbm(far_c), in_hbm(y_rows), in_hbm(dx_rows))


def solution(mesh):
    n_dev = mesh.shape['sp']
    assert n_dev == CORES * RING * RING

    def device_body(x_loc, flag_loc, w_q, w_k, w_v, w_o, dy_loc):
        tok_count, d_model = x_loc.shape
        n_heads, head_dim = w_q.shape[1], w_q.shape[2]
        width = n_heads * head_dim
        score_scale = 1.0 / (math.sqrt(head_dim) * tok_count)
        weights = [w.transpose(1, 2, 0).reshape(width, d_model) for w in (w_q, w_k, w_v)] + [w_o.reshape(width, d_model)]
        g, z = front(flag_loc, x_loc, dy_loc, weights, score_scale, n_dev, n_heads)
        piece, y_rows, dx_rows = reduce_rows(g, z, x_loc, dy_loc, weights)
        *grads, y_loc, dx_loc = store(*gather_rows(piece, n_dev), y_rows, dx_rows)
        dw_q, dw_k, dw_v, dw_o = (grad.reshape(n_heads, head_dim, d_model) for grad in grads)
        return y_loc, dx_loc, dw_q.transpose(2, 0, 1), dw_k.transpose(2, 0, 1), dw_v.transpose(2, 0, 1), dw_o

    row_spec = P(('dp', 'sp'), None)
    flag_spec = P(('dp', 'sp'))
    w_spec = P(None, None, None)
    dw_spec = P('dp', None, None)
    return jax.shard_map(device_body, mesh=mesh,
                         in_specs=(row_spec, flag_spec, w_spec, w_spec, w_spec, w_spec, row_spec),
                         out_specs=(row_spec, row_spec, dw_spec, dw_spec, dw_spec, dw_spec),
                         check_vma=False)
```
